32 devices in a mesh: dp: 4 (over z), seq: 4 (over x, core), tensor: 2 (over y).
Axes of the slice: x: 2, y: 2, z: 4, core: 2. Of those that a mesh axis runs over, the one named last changes fastest.
Arguments:
- latent_embed: bfloat16 [20480, 2, 1024], P(('dp', 'seq'), None, 'tensor'), may hold values from -6 to 6
- adapter: bfloat16 [2, 1024, 1024], P(None, 'tensor'), may hold values from -0.125 to 0.125
- first_gain: float32 [1024], replicated, may hold values from 0.5 to 1.5
- query_weight: bfloat16 [1024, 1024], P(None, 'tensor'), may hold values from -0.1875 to 0.1875
- key_weight: bfloat16 [1024, 1024], P(None, 'tensor'), may hold values from -0.1875 to 0.1875
- value_weight: bfloat16 [1024, 1024], P(None, 'tensor'), may hold values from -0.1875 to 0.1875
- output_weight: bfloat16 [1024, 1024], P('tensor'), may hold values from -0.1875 to 0.1875
- second_gain: float32 [1024], replicated, may hold values from 0.5 to 1.5
- third_gain: float32 [1024], replicated, may hold values from 0.5 to 1.5
- gate_weight: bfloat16 [1024, 2816], P(None, 'tensor'), may hold values from -0.1875 to 0.1875
- up_weight: bfloat16 [1024, 2816], P(None, 'tensor'), may hold values from -0.1875 to 0.1875
- down_weight: bfloat16 [2816, 1024], P('tensor'), may hold values from -0.109375 to 0.109375
- fourth_gain: float32 [1024], replicated, may hold values from 0.5 to 1.5
- parents: int32 [4, 20], P('dp'), may hold values from -1 to 19, as said below
- positions: int32 [20480], P(('dp', 'seq')), may hold values from 0 to 2559, as said below
- cotangent: bfloat16 [20480, 1024], P(('dp', 'seq')), may hold values from -6 to 6
Outputs:
- layer_out: float32 [20480, 1024], P(('dp', 'seq'))
- latent_gradient: float32 [20480, 2, 1024], P(('dp', 'seq'), None, 'tensor')
- adapter_gradient: float32 [2, 1024, 1024], P(None, 'tensor')
- first_gain_gradient: float32 [1024], replicated
- query_gradient: float32 [1024, 1024], P(None, 'tensor')
- key_gradient: float32 [1024, 1024], P(None, 'tensor')
- value_gradient: float32 [1024, 1024], P(None, 'tensor')
- output_gradient: float32 [1024, 1024], P('tensor')
- second_gain_gradient: float32 [1024], replicated
- third_gain_gradient: float32 [1024], replicated
- gate_gradient: float32 [1024, 2816], P(None, 'tensor')
- up_gradient: float32 [1024, 2816], P(None, 'tensor')
- down_gradient: float32 [2816, 1024], P('tensor')
- fourth_gain_gradient: float32 [1024], replicated
The draws below stay inside these ranges and needn't reach their ends.
Inputs may be any that keep to these rules, and one draw needn't show every extreme that they name: `parents`: each tree's segments form a trunk of 8 chained segments from the root, 4 branches whose parent is the trunk's last segment and 2 leaves under each branch; which segment number plays which role is drawn. `positions`: a token's position is 256 times the number of its segment's ancestors plus its place inside its segment.
All inputs are finite; a program needn't handle non-finite values.
Results may differ from the reference program's by a relative error of at most 0.025.
Values may be sent and summed in bfloat16 or wider, within the bound.
A program may use at most 896 MiB of HBM per device.

```python
import jax
import jax.numpy as jnp
from jax import lax

D = 1024
H = 16
DH = 64
FF = 2816
SEG = 256
TRUNK = 8
BRANCH = 4
LEAVES = 2
SEGS = 20
TREES = 4
TOKENS = 20480


def tree_layout(key):
    nodes = jnp.arange(SEGS, dtype=jnp.int32)
    labels = jax.random.permutation(jax.random.fold_in(key, 11), SEGS).astype(jnp.int32)
    above = jnp.where(nodes < TRUNK, nodes - 1, jnp.where(nodes < TRUNK + BRANCH, TRUNK - 1, TRUNK + (nodes - TRUNK - BRANCH) // LEAVES))
    depth = jnp.where(nodes < TRUNK, nodes, jnp.where(nodes < TRUNK + BRANCH, TRUNK, TRUNK + 1))
    parent_label = jnp.where(above >= 0, labels[jnp.maximum(above, 0)], -1)
    parent_table = jnp.zeros((SEGS,), jnp.int32).at[labels].set(parent_label)
    depth_table = jnp.zeros((SEGS,), jnp.int32).at[labels].set(depth)
    return (parent_table, depth_table)


def all_trees(key):
    tree_keys = jax.vmap(lambda index: jax.random.fold_in(key, index))(jnp.arange(TREES))
    return jax.vmap(tree_layout)(tree_keys)


def draw_parents(key, part):
    parent_table, depth_table = all_trees(key)
    return parent_table


def draw_positions(key, part):
    parent_table, depth_table = all_trees(key)
    inside = jnp.arange(SEG, dtype=jnp.int32)
    return (depth_table[:, :, None] * SEG + inside[None, None, :]).reshape(TOKENS)


def block_scale(own_key, shape, cuts, low, high):
    loudness = 1.0
    for axis_at, shards_of in cuts:
        heights = jax.random.uniform(jax.random.fold_in(jax.random.fold_in(own_key, 6), axis_at), (shards_of,), jnp.float32, low / len(cuts), high / len(cuts))
        loudness = loudness * jnp.repeat(jnp.exp(heights), shape[axis_at] // shards_of).reshape((-1,) + (1,) * (len(shape) - 1 - axis_at))
    return loudness


def noise(stream_key, dims, spread, limit, shards=(), held_as=jnp.bfloat16):
    entries = jax.random.normal(stream_key, dims, jnp.float32) * spread
    if len(shards) > 0:
        entries = block_scale(stream_key, dims, shards, -0.22, 0.18) * entries
    return jnp.clip(entries, min=-limit, max=limit).astype(held_as)


def setup_inputs(seed: int = 0) -> dict:
    seeds = jax.random.split(jax.random.key(seed), 17)
    latent_embed = noise(seeds[0], (TOKENS, 2, D), 1.0, 6.0, ((0, 16), (2, 2)))
    adapter = noise(seeds[1], (2, D, D), (2 * D) ** -0.5, 0.125, ((1, 2),))
    first_gain = jnp.clip(1.0 + 0.1 * jax.random.normal(seeds[2], (D,), jnp.float32), 0.5, 1.5)
    query_weight = noise(seeds[3], (D, H * DH), D ** -0.5, 0.1875, ((1, 2),))
    key_weight = noise(seeds[4], (D, H * DH), D ** -0.5, 0.1875, ((1, 2),))
    value_weight = noise(seeds[5], (D, H * DH), D ** -0.5, 0.1875, ((1, 2),))
    output_weight = noise(seeds[6], (H * DH, D), (H * DH) ** -0.5, 0.1875, ((0, 2),))
    second_gain = jnp.clip(1.0 + 0.1 * jax.random.normal(seeds[7], (D,), jnp.float32), 0.5, 1.5)
    third_gain = jnp.clip(1.0 + 0.1 * jax.random.normal(seeds[8], (D,), jnp.float32), 0.5, 1.5)
    gate_weight = noise(seeds[9], (D, FF), D ** -0.5, 0.1875, ((1, 2),))
    up_weight = noise(seeds[10], (D, FF), D ** -0.5, 0.1875, ((1, 2),))
    down_weight = noise(seeds[11], (FF, D), FF ** -0.5, 0.109375, ((0, 2),))
    fourth_gain = jnp.clip(1.0 + 0.1 * jax.random.normal(seeds[12], (D,), jnp.float32), 0.5, 1.5)
    parents = draw_parents(jax.random.fold_in(seeds[16], 71), 0)
    positions = draw_positions(jax.random.fold_in(seeds[16], 71), 0)
    cotangent = noise(seeds[15], (TOKENS, D), 1.0, 6.0, ((0, 16),))
    return dict(latent_embed=latent_embed, adapter=adapter, first_gain=first_gain, query_weight=query_weight, key_weight=key_weight, value_weight=value_weight, output_weight=output_weight, second_gain=second_gain, third_gain=third_gain, gate_weight=gate_weight, up_weight=up_weight, down_weight=down_weight, fourth_gain=fourth_gain, parents=parents, positions=positions, cotangent=cotangent)


EPSILON = 1e-06
THETA = 50000.0
HIGHEST = lax.Precision.HIGHEST

@jax.custom_vjp
def low(v):
    return lax.optimization_barrier(v.astype(jnp.bfloat16)).astype(jnp.float32)

@jax.custom_vjp
def low_back(v):
    return v

def low_keep(v):
    return (low(v), None)

def low_pass(kept, grad):
    return (grad,)

def back_keep(v):
    return (v, None)

def back_low(kept, grad):
    return (low(grad),)
low.defvjp(low_keep, low_pass)
low_back.defvjp(back_keep, back_low)

def normalize(values, gain):
    scale = lax.rsqrt(lax.optimization_barrier(jnp.mean(values * values, axis=-1, keepdims=True)) + EPSILON)
    return values * scale * gain

def angles(positions, width):
    half = width // 2
    freq = THETA ** (-jnp.arange(half, dtype=jnp.float32) * 2.0 / width)
    angle = positions.astype(jnp.float32)[:, None] * freq[None, :]
    return (jnp.cos(angle)[:, None, :], jnp.sin(angle)[:, None, :])

def rotate(values, cosine, sine, sign):
    half = values.shape[-1] // 2
    first = values[..., :half]
    second = values[..., half:]
    return jnp.concatenate([first * cosine - sign * second * sine, second * cosine + sign * first * sine], axis=-1)

def ancestry(parent_row):
    labels = jnp.arange(parent_row.shape[0], dtype=jnp.int32)

    def extend(index, state):
        current, total = state
        total = total | (current[:, None] == labels[None, :])
        current = jnp.where(current >= 0, jnp.take(parent_row, jnp.maximum(current, 0).astype(jnp.int32)), -1).astype(jnp.int32)
        return (current, total)
    start = (parent_row.astype(jnp.int32), jnp.zeros((parent_row.shape[0], parent_row.shape[0]), jnp.bool_))
    current, total = lax.fori_loop(0, parent_row.shape[0], extend, start)
    return total

def path_mask(parent_row, query_ids, key_ids):
    table = ancestry(parent_row)
    query_seg = (query_ids // SEG).astype(jnp.int32)
    key_seg = (key_ids // SEG).astype(jnp.int32)
    far = jnp.take(jnp.take(table, query_seg, axis=0), key_seg, axis=1)
    near = (query_seg[:, None] == key_seg[None, :]) & (key_ids[None, :] <= query_ids[:, None])
    return far | near

def reference(latent_embed, adapter, first_gain, query_weight, key_weight, value_weight, output_weight, second_gain, third_gain, gate_weight, up_weight, down_weight, fourth_gain, parents, positions, cotangent):
    tree_tokens = SEGS * SEG
    token_ids = jnp.arange(tree_tokens, dtype=jnp.int32)
    masks = lax.map(lambda row: path_mask(row, token_ids, token_ids), parents)
    cosine, sine = angles(positions, DH)
    scale = DH ** (-0.5)
    floats = tuple((item.astype(jnp.float32) for item in (latent_embed, adapter, first_gain, query_weight, key_weight, value_weight, output_weight, second_gain, third_gain, gate_weight, up_weight, down_weight, fourth_gain)))

    def one_tree(items):
        tree_queries, tree_keys, tree_values, tree_mask = items
        scores = low_back(jnp.einsum('qhd,khd->hqk', tree_queries, tree_keys, precision=HIGHEST) * scale)
        scores = jnp.where(tree_mask[None], scores, -1e+30)
        top = lax.optimization_barrier(jnp.max(scores, axis=-1, keepdims=True))
        weights = jnp.exp(scores - top)
        probs = weights / lax.optimization_barrier(jnp.sum(weights, axis=-1, keepdims=True))
        return jnp.einsum('hqk,khd->qhd', low(probs), tree_values, precision=HIGHEST)

    def forward(stacked, adapter_value, gain_one, query_value, key_value, value_value, output_value, gain_two, gain_three, gate_value, up_value, down_value, gain_four):
        adapted = low_back(jnp.dot(stacked.reshape(TOKENS, 2 * D), adapter_value.reshape(2 * D, D), precision=HIGHEST))
        first_low = low(normalize(adapted, gain_one))
        queries = low(rotate(low_back(jnp.dot(first_low, query_value, precision=HIGHEST)).reshape(TOKENS, H, DH), cosine, sine, 1.0))
        keys = low(rotate(low_back(jnp.dot(first_low, key_value, precision=HIGHEST)).reshape(TOKENS, H, DH), cosine, sine, 1.0))
        values = low_back(low(jnp.dot(first_low, value_value, precision=HIGHEST))).reshape(TOKENS, H, DH)
        tree_shape = (TREES, tree_tokens, H, DH)
        attended = lax.map(jax.checkpoint(one_tree), (queries.reshape(tree_shape), keys.reshape(tree_shape), values.reshape(tree_shape), masks))
        attended = low_back(low(attended.reshape(TOKENS, H * DH)))
        attention = low_back(jnp.dot(attended, output_value, precision=HIGHEST))
        middle = adapted + normalize(attention, gain_two)
        third_low = low(normalize(middle, gain_three))
        gate = low_back(jnp.dot(third_low, gate_value, precision=HIGHEST))
        upward = low_back(jnp.dot(third_low, up_value, precision=HIGHEST))
        hidden = low_back(low(jax.nn.silu(gate) * upward))
        mixed = low_back(jnp.dot(hidden, down_value, precision=HIGHEST))
        return middle + normalize(mixed, gain_four)
    layer_out, pullback = jax.vjp(forward, *floats)
    grads = pullback(cotangent.astype(jnp.float32))
    return (layer_out, grads[0], grads[1], grads[2], grads[3], grads[4], grads[5], grads[6], grads[7], grads[8], grads[9], grads[10], grads[11], grads[12])
```

```python
import functools

import jax
import jax.numpy as jnp
from jax import lax
from jax.experimental import pallas as pl
from jax.experimental.pallas import tpu as pltpu
from jax.sharding import Mesh
from jax.sharding import PartitionSpec as P

DH = 64
SEG = 256


EPSILON = 1e-06
THETA = 50000.0


def normalize(values, gain):
    scale = lax.rsqrt(jnp.mean(values * values, axis=-1, keepdims=True) + EPSILON)
    normed = values * scale
    return (normed * gain, normed, scale)


def normalize_back(upstream, gain, normed, scale):
    scaled = upstream * gain
    inward = scale * (scaled - normed * jnp.mean(scaled * normed, axis=-1, keepdims=True))
    return (inward, jnp.sum(upstream * normed, axis=0))


def angles(positions, width):
    half = width // 2
    freq = THETA ** (-jnp.arange(half, dtype=jnp.float32) * 2.0 / width)
    angle = positions.astype(jnp.float32)[:, None] * freq[None, :]
    return (jnp.cos(angle)[:, None, :], jnp.sin(angle)[:, None, :])


def rotate(values, cosine, sine, sign):
    half = values.shape[-1] // 2
    first = values[..., :half]
    second = values[..., half:]
    return jnp.concatenate(
        [first * cosine - sign * second * sine, second * cosine + sign * first * sine], axis=-1
    )


def ancestry(parent_row):
    labels = jnp.arange(parent_row.shape[0], dtype=jnp.int32)

    def extend(index, state):
        current, total = state
        total = total | (current[:, None] == labels[None, :])
        current = jnp.where(current >= 0, jnp.take(parent_row, jnp.maximum(current, 0)), -1)
        return (current, total)

    start = (parent_row, jnp.zeros((parent_row.shape[0], parent_row.shape[0]), jnp.bool_))
    current, total = lax.fori_loop(0, parent_row.shape[0], extend, start)
    return total


def path_mask(parent_row, query_ids, key_ids):
    table = ancestry(parent_row)
    query_seg = query_ids // SEG
    key_seg = key_ids // SEG
    far = jnp.take(jnp.take(table, query_seg, axis=0), key_seg, axis=1)
    near = (query_seg[:, None] == key_seg[None, :]) & (key_ids[None, :] <= query_ids[:, None])
    return far | near


def on_device(
    latent_embed,
    adapter,
    first_gain,
    query_weight,
    key_weight,
    value_weight,
    output_weight,
    second_gain,
    third_gain,
    gate_weight,
    up_weight,
    down_weight,
    fourth_gain,
    parents,
    positions,
    cotangent,
):
    rows = latent_embed.shape[0]
    local_heads = query_weight.shape[1] // DH
    scale = DH ** (-0.5)
    adapted = lax.psum(
        jnp.einsum("rcd,cde->re", latent_embed, adapter, preferred_element_type=jnp.float32),
        "tensor",
    )
    first_out, first_normed, first_scale = normalize(adapted, first_gain)
    first_low = first_out.astype(jnp.bfloat16)
    cosine, sine = angles(positions, DH)
    query_raw = jnp.dot(first_low, query_weight, preferred_element_type=jnp.float32).reshape(
        rows, local_heads, DH
    )
    queries = rotate(query_raw, cosine, sine, 1.0).astype(jnp.bfloat16)
    key_raw = jnp.dot(first_low, key_weight, preferred_element_type=jnp.float32).reshape(
        rows, local_heads, DH
    )
    keys_local = rotate(key_raw, cosine, sine, 1.0).astype(jnp.bfloat16)
    values_local = (
        jnp.dot(first_low, value_weight, preferred_element_type=jnp.float32)
        .astype(jnp.bfloat16)
        .reshape(rows, local_heads, DH)
    )
    keys_all, values_all = (
        lax.all_gather(keys_local, "seq", axis=0, tiled=True),
        lax.all_gather(values_local, "seq", axis=0, tiled=True),
    )
    tree_rows = keys_all.shape[0]
    query_ids = lax.axis_index("seq") * rows + jnp.arange(rows, dtype=jnp.int32)
    key_ids = jnp.arange(tree_rows, dtype=jnp.int32)
    allowed = path_mask(parents[0], query_ids, key_ids)[None]

    def score_block(keys):
        raw = jnp.einsum("qhd,khd->hqk", queries, keys, preferred_element_type=jnp.float32) * scale
        return jnp.where(allowed, raw, -1e30)

    scores = score_block(keys_all)
    top = jnp.max(scores, axis=-1, keepdims=True)
    weights = jnp.exp(scores - top)
    total = jnp.sum(weights, axis=-1, keepdims=True)
    probs = weights / total
    logsum = top + jnp.log(total)
    attended = jnp.einsum(
        "hqk,khd->qhd", probs.astype(jnp.bfloat16), values_all, preferred_element_type=jnp.float32
    )
    attended = attended.reshape(rows, local_heads * DH).astype(jnp.bfloat16)
    attention = lax.psum(
        jnp.dot(attended, output_weight, preferred_element_type=jnp.float32).astype(jnp.bfloat16),
        "tensor",
    ).astype(jnp.float32)
    second_out, second_normed, second_scale = normalize(attention, second_gain)
    middle = adapted + second_out
    third_out, third_normed, third_scale = normalize(middle, third_gain)
    third_low = third_out.astype(jnp.bfloat16)
    gate = jnp.dot(third_low, gate_weight, preferred_element_type=jnp.float32)
    upward = jnp.dot(third_low, up_weight, preferred_element_type=jnp.float32)
    hidden = (jax.nn.silu(gate) * upward).astype(jnp.bfloat16)
    mixed = lax.psum(
        jnp.dot(hidden, down_weight, preferred_element_type=jnp.float32).astype(jnp.bfloat16),
        "tensor",
    ).astype(jnp.float32)
    fourth_out, fourth_normed, fourth_scale = normalize(mixed, fourth_gain)
    layer_out = middle + fourth_out
    upstream = cotangent.astype(jnp.float32)
    mixed_back, fourth_gain_part = normalize_back(
        upstream, fourth_gain, fourth_normed, fourth_scale
    )
    mixed_low = mixed_back.astype(jnp.bfloat16)
    down_part = jnp.einsum("rf,rd->fd", hidden, mixed_low, preferred_element_type=jnp.float32)
    hidden_back = (
        jnp.einsum("rd,fd->rf", mixed_low, down_weight, preferred_element_type=jnp.float32)
        .astype(jnp.bfloat16)
        .astype(jnp.float32)
    )
    swiglu_value, product_back = jax.vjp(
        lambda left, right: jax.nn.silu(left) * right, gate, upward
    )
    gate_back, up_back = product_back(hidden_back)
    gate_low = gate_back.astype(jnp.bfloat16)
    up_low = up_back.astype(jnp.bfloat16)
    gate_part = jnp.einsum("rd,rf->df", third_low, gate_low, preferred_element_type=jnp.float32)
    up_part = jnp.einsum("rd,rf->df", third_low, up_low, preferred_element_type=jnp.float32)
    third_term = jnp.einsum(
        "rf,df->rd", gate_low, gate_weight, preferred_element_type=jnp.float32
    ) + jnp.einsum("rf,df->rd", up_low, up_weight, preferred_element_type=jnp.float32)
    third_back = lax.psum(third_term.astype(jnp.bfloat16), "tensor").astype(jnp.float32)
    middle_part, third_gain_part = normalize_back(third_back, third_gain, third_normed, third_scale)
    middle_back = upstream + middle_part
    attention_back, second_gain_part = normalize_back(
        middle_back, second_gain, second_normed, second_scale
    )
    attention_low = attention_back.astype(jnp.bfloat16)
    output_part = jnp.einsum(
        "re,rd->ed", attended, attention_low, preferred_element_type=jnp.float32
    )
    attended_back = (
        jnp.einsum("rd,ed->re", attention_low, output_weight, preferred_element_type=jnp.float32)
        .astype(jnp.bfloat16)
        .reshape(rows, local_heads, DH)
    )
    keys_back, values_back = (
        lax.all_gather(keys_local, "seq", axis=0, tiled=True),
        lax.all_gather(values_local, "seq", axis=0, tiled=True),
    )
    probs_back = jnp.exp(score_block(keys_back) - logsum)
    prob_grad = jnp.einsum(
        "qhd,khd->hqk", attended_back, values_back, preferred_element_type=jnp.float32
    )
    score_grad = (
        probs_back * (prob_grad - jnp.sum(prob_grad * probs_back, axis=-1, keepdims=True))
    ).astype(jnp.bfloat16)
    query_rot = (
        jnp.einsum("hqk,khd->qhd", score_grad, keys_back, preferred_element_type=jnp.float32)
        * scale
    )
    key_rot_all = (
        jnp.einsum("hqk,qhd->khd", score_grad, queries, preferred_element_type=jnp.float32) * scale
    )
    value_back_all = jnp.einsum(
        "hqk,qhd->khd",
        probs_back.astype(jnp.bfloat16),
        attended_back,
        preferred_element_type=jnp.float32,
    )
    key_rot, value_back = (
        lax.psum_scatter(
            key_rot_all.astype(jnp.bfloat16), "seq", scatter_dimension=0, tiled=True
        ).astype(jnp.float32),
        lax.psum_scatter(
            value_back_all.astype(jnp.bfloat16), "seq", scatter_dimension=0, tiled=True
        ).astype(jnp.float32),
    )
    query_low = (
        rotate(query_rot, cosine, sine, -1.0).astype(jnp.bfloat16).reshape(rows, local_heads * DH)
    )
    key_low = (
        rotate(key_rot, cosine, sine, -1.0).astype(jnp.bfloat16).reshape(rows, local_heads * DH)
    )
    value_low = value_back.astype(jnp.bfloat16).reshape(rows, local_heads * DH)
    query_part = jnp.einsum("rd,re->de", first_low, query_low, preferred_element_type=jnp.float32)
    key_part = jnp.einsum("rd,re->de", first_low, key_low, preferred_element_type=jnp.float32)
    value_part = jnp.einsum("rd,re->de", first_low, value_low, preferred_element_type=jnp.float32)
    first_term = jnp.einsum(
        "re,de->rd", query_low, query_weight, preferred_element_type=jnp.float32
    )
    first_term = first_term + jnp.einsum(
        "re,de->rd", key_low, key_weight, preferred_element_type=jnp.float32
    )
    first_term = first_term + jnp.einsum(
        "re,de->rd", value_low, value_weight, preferred_element_type=jnp.float32
    )
    first_back = lax.psum(first_term.astype(jnp.bfloat16), "tensor").astype(jnp.float32)
    adapted_part, first_gain_part = normalize_back(
        first_back, first_gain, first_normed, first_scale
    )
    adapted_low = (middle_back + adapted_part).astype(jnp.bfloat16)
    latent_gradient = jnp.einsum(
        "re,cde->rcd", adapted_low, adapter, preferred_element_type=jnp.float32
    )
    adapter_part = jnp.einsum(
        "rcd,re->cde", latent_embed, adapted_low, preferred_element_type=jnp.float32
    )
    summed = (
        lax.psum(gate_part.astype(jnp.bfloat16), ("dp", "seq")).astype(jnp.float32),
        lax.psum(up_part.astype(jnp.bfloat16), ("dp", "seq")).astype(jnp.float32),
        lax.psum(down_part.astype(jnp.bfloat16), ("dp", "seq")).astype(jnp.float32),
        lax.psum(third_gain_part.astype(jnp.bfloat16), ("dp", "seq")).astype(jnp.float32),
        lax.psum(fourth_gain_part.astype(jnp.bfloat16), ("dp", "seq")).astype(jnp.float32),
        lax.psum(query_part.astype(jnp.bfloat16), ("dp", "seq")).astype(jnp.float32),
        lax.psum(key_part.astype(jnp.bfloat16), ("dp", "seq")).astype(jnp.float32),
        lax.psum(value_part.astype(jnp.bfloat16), ("dp", "seq")).astype(jnp.float32),
        lax.psum(output_part.astype(jnp.bfloat16), ("dp", "seq")).astype(jnp.float32),
        lax.psum(first_gain_part.astype(jnp.bfloat16), ("dp", "seq")).astype(jnp.float32),
        lax.psum(second_gain_part.astype(jnp.bfloat16), ("dp", "seq")).astype(jnp.float32),
        lax.psum(adapter_part.astype(jnp.bfloat16), ("dp", "seq")).astype(jnp.float32),
    )
    gate_total, up_total, down_total, third_total, fourth_total = (
        summed[0],
        summed[1],
        summed[2],
        summed[3],
        summed[4],
    )
    query_total, key_total, value_total, output_total, first_total, second_total = (
        summed[5],
        summed[6],
        summed[7],
        summed[8],
        summed[9],
        summed[10],
    )
    adapter_total = summed[11]
    return (
        layer_out,
        latent_gradient,
        adapter_total,
        first_total,
        query_total,
        key_total,
        value_total,
        output_total,
        second_total,
        third_total,
        gate_total,
        up_total,
        down_total,
        fourth_total,
    )


TRUNK = 8
BRANCH = 4
LEAVES = 2
SEGS = TRUNK + BRANCH + BRANCH * LEAVES
WIDE = 2 * DH
NEG = -1e30
F32 = jnp.float32
BF16 = jnp.bfloat16
KEYS = 512
HIDDEN = 256
VMEM_BYTES = 60 << 20


def nt(left, right):
    return lax.dot_general(left, right, (((1,), (1,)), ((), ())), preferred_element_type=F32)


def nn(left, right):
    return lax.dot_general(left, right, (((1,), (0,)), ((), ())), preferred_element_type=F32)


def segment(index, size=SEG):
    return pl.ds(pl.multiple_of(index * SEG, SEG), size)


def find_roles(parents, child, count, role):
    for s in range(SEGS):
        count[s] = 0
    role[0] = 0
    for s in range(SEGS):
        parent = parents[0, s]

        @pl.when(parent < 0)
        def _():
            role[0] = s

        @pl.when(parent >= 0)
        def _():
            seen = count[parent]
            child[parent * BRANCH + seen] = s
            count[parent] = seen + 1

    for i in range(TRUNK - 1):
        role[i + 1] = child[role[i] * BRANCH]
    for b in range(BRANCH):
        role[TRUNK + b] = child[role[TRUNK - 1] * BRANCH + b]
    for b in range(BRANCH):
        for leaf in range(LEAVES):
            role[TRUNK + BRANCH + b * LEAVES + leaf] = child[role[TRUNK + b] * BRANCH + leaf]


def token_parts(refs):
    owners = refs[0].shape[0]
    rows = sum(ref.shape[1] for ref in refs)
    base = 0
    for ref in refs:
        for owner in range(owners):
            for at in range(0, ref.shape[1], SEG):
                yield ref, owner, at, (owner * rows + base + at) // SEG
        base += ref.shape[1]


def heads_apart(values, first):
    zero = jnp.zeros_like(values)
    return jnp.concatenate(
        [jnp.where(first, values, zero), jnp.where(first, zero, values)], axis=0
    )


def attention_kernel(n_parts, *refs):
    parents = refs[0]
    parts = refs[1 : 1 + n_parts]
    out, logsum, qr, kr, v0, v1, kept, acc, top, total, child, count, role, place = refs[
        1 + n_parts :
    ]
    find_roles(parents, child, count, role)
    for i in range(SEGS):
        place[role[i]] = i
    first = lax.broadcasted_iota(jnp.int32, (SEG, WIDE), 1) < DH
    for ref, owner, at, seg in token_parts(parts):
        here = segment(place[seg])
        block = slice(at, at + SEG)
        qr[here, :] = ref[owner, block, 0:WIDE] * jnp.asarray(DH**-0.5, BF16)
        kr[here, :] = ref[owner, block, WIDE : 2 * WIDE]
        value = ref[owner, block, 2 * WIDE : 3 * WIDE]
        zero = jnp.zeros_like(value)
        v0[here, :] = jnp.where(first, value, zero)
        v1[here, :] = jnp.where(first, zero, value)
    row = lax.broadcasted_iota(jnp.int32, (2 * SEG, SEG), 0)
    col = lax.broadcasted_iota(jnp.int32, (2 * SEG, SEG), 1)
    causal = col <= jnp.where(row >= SEG, row - SEG, row)

    def fold(values, op):
        result = values[:, 0:128]
        for at in range(128, values.shape[1], 128):
            result = op(result, values[:, at : at + 128])
        return result

    def query(index, count_big, big, extra):
        queries = heads_apart(qr[segment(index), :], first)
        own = jnp.where(causal, nt(queries, kr[segment(index), :]), NEG)
        top[...] = fold(own, jnp.maximum)
        others = []
        for other in extra:
            scores = nt(queries, kr[segment(other), :])
            top[...] = jnp.maximum(top[...], fold(scores, jnp.maximum))
            others.append(scores)

        def find(c, _):
            scores = nt(queries, kr[pl.ds(pl.multiple_of(c * big, big), big), :])
            kept[c, :, 0:big] = scores
            top[...] = jnp.maximum(top[...], fold(scores, jnp.maximum))
            return 0

        lax.fori_loop(0, count_big, find, 0)
        most = jnp.max(top[...], axis=1, keepdims=True)

        def add(scores, keys, fresh=False):
            weights = jnp.exp(scores - most)
            summed = fold(weights, jnp.add)
            low = weights.astype(BF16)
            product = nn(low[:SEG], v0[keys, :]) + nn(low[SEG:], v1[keys, :])
            total[...] = summed if fresh else total[...] + summed
            acc[...] = product if fresh else acc[...] + product

        add(own, segment(index), True)
        for other, scores in zip(extra, others):
            add(scores, segment(other))

        def use(c, _):
            add(kept[c, :, 0:big], pl.ds(pl.multiple_of(c * big, big), big))
            return 0

        lax.fori_loop(0, count_big, use, 0)
        whole = jnp.sum(total[...], axis=1, keepdims=True)
        inverse = 1.0 / whole
        log = most + jnp.log(whole)
        here = segment(role[index])
        out[here, :] = (acc[...] * jnp.where(first, inverse[:SEG], inverse[SEG:])).astype(BF16)
        logsum[here, :] = jnp.where(first, log[:SEG], log[SEG:])

    def trunk(i, _):
        query(i, i, SEG, [])
        return 0

    def branch(i, _):
        query(TRUNK + i, TRUNK * SEG // KEYS, KEYS, [])
        return 0

    def leaf(i, _):
        query(TRUNK + BRANCH + i, TRUNK * SEG // KEYS, KEYS, [TRUNK + i // LEAVES])
        return 0

    lax.fori_loop(0, TRUNK, trunk, 0)
    lax.fori_loop(0, BRANCH, branch, 0)
    lax.fori_loop(0, BRANCH * LEAVES, leaf, 0)


def attention_forward(parents, parts):
    tokens = SEGS * SEG
    vmem = pl.BlockSpec(memory_space=pltpu.VMEM)
    return pl.pallas_call(
        functools.partial(attention_kernel, len(parts)),
        out_shape=(
            jax.ShapeDtypeStruct((tokens, WIDE), BF16),
            jax.ShapeDtypeStruct((tokens, WIDE), F32),
        ),
        in_specs=[pl.BlockSpec(memory_space=pltpu.SMEM)] + [vmem] * len(parts),
        out_specs=(vmem, vmem),
        scratch_shapes=[pltpu.VMEM((tokens, WIDE), BF16)] * 4
        + [
            pltpu.VMEM((TRUNK, 2 * SEG, KEYS), F32),
            pltpu.VMEM((SEG, WIDE), F32),
            pltpu.VMEM((2 * SEG, 128), F32),
            pltpu.VMEM((2 * SEG, 128), F32),
            pltpu.SMEM((SEGS * BRANCH,), jnp.int32),
            pltpu.SMEM((SEGS,), jnp.int32),
            pltpu.SMEM((SEGS,), jnp.int32),
            pltpu.SMEM((SEGS,), jnp.int32),
        ],
        compiler_params=pltpu.CompilerParams(vmem_limit_bytes=VMEM_BYTES),
        cost_estimate=pl.CostEstimate(
            flops=152 * 2 * 4 * SEG * SEG * 128,
            bytes_accessed=tokens * WIDE * 12,
            transcendentals=152 * 2 * SEG * SEG,
        ),
        name="attention_forward",
    )(parents, *parts)


def swap_halves(values, low):
    return jnp.where(
        low, pltpu.roll(values, WIDE - DH // 2, 1), pltpu.roll(values, DH // 2, 1)
    )


def attention_back_kernel(n_parts, *refs):
    parents = refs[0]
    parts = refs[1 : 1 + n_parts]
    (
        upstream,
        attended,
        logsum,
        cosine,
        sine,
        out,
        qr,
        kr,
        vr,
        kt,
        dk,
        dv,
        dqt,
        child,
        count,
        role,
        place,
    ) = refs[1 + n_parts :]
    find_roles(parents, child, count, role)
    for i in range(SEGS):
        place[role[i]] = i
    lane = lax.broadcasted_iota(jnp.int32, (SEG, WIDE), 1)
    first = lane < DH
    low = (lane % DH) < (DH // 2)
    for ref, owner, at, seg in token_parts(parts):
        here = segment(place[seg])
        block = slice(at, at + SEG)
        qr[here, :] = ref[owner, block, 0:WIDE] * jnp.asarray(DH**-0.5, BF16)
        key = ref[owner, block, WIDE : 2 * WIDE]
        kr[here, :] = key
        kt[:, here] = key.T
        vr[here, :] = ref[owner, block, 2 * WIDE : 3 * WIDE]
    dk[...] = jnp.zeros_like(dk)
    dv[...] = jnp.zeros_like(dv)
    key_at = lax.broadcasted_iota(jnp.int32, (SEG, 2 * SEG), 0)
    query_at = lax.broadcasted_iota(jnp.int32, (SEG, 2 * SEG), 1)
    causal = key_at <= jnp.where(query_at >= SEG, query_at - SEG, query_at)

    def rope_back(values, depth):
        at = segment(depth)
        return values * cosine[at, :] - swap_halves(values, low) * sine[at, :]

    def query(index, depth, count_big, big, extra):
        here = segment(role[index])
        queries = heads_apart(qr[segment(index), :], first)
        up = upstream[here, :]
        ups = heads_apart(up, first)
        turned = logsum[here, :].T
        log = jnp.concatenate([turned[0:1, :], turned[DH : DH + 1, :]], axis=1)
        product = (up.astype(F32) * attended[here, :].astype(F32)).T
        inner = jnp.concatenate(
            [
                jnp.sum(product[:DH], axis=0, keepdims=True),
                jnp.sum(product[DH:], axis=0, keepdims=True),
            ],
            axis=1,
        )
        dqt[...] = jnp.zeros_like(dqt)

        def add(keys, mask=None):
            weights = jnp.exp(nt(kr[keys, :], queries) - log)
            if mask is not None:
                weights = jnp.where(mask, weights, 0.0)
            back = (weights * (nt(vr[keys, :], ups) - inner)).astype(BF16)
            dv[keys, :] += nn(weights.astype(BF16), ups)
            dk[keys, :] += nn(back, queries)
            dqt[...] += nn(kt[:, keys], back)

        add(segment(index), causal)
        for other in extra:
            add(segment(other))

        def use(c, _):
            add(pl.ds(pl.multiple_of(c * big, big), big))
            return 0

        lax.fori_loop(0, count_big, use, 0)
        both = jnp.concatenate([dqt[:DH, :SEG], dqt[DH:, SEG:]], axis=0) * (DH**-0.5)
        out[here, 0:WIDE] = rope_back(both.T, depth).astype(BF16)

    def leaf(i, _):
        query(TRUNK + BRANCH + i, TRUNK + 1, TRUNK * SEG // KEYS, KEYS, [TRUNK + i // LEAVES])
        return 0

    def branch(i, _):
        query(TRUNK + i, TRUNK, TRUNK * SEG // KEYS, KEYS, [])
        return 0

    def trunk(i, _):
        query(i, i, i, SEG, [])
        return 0

    lax.fori_loop(0, BRANCH * LEAVES, leaf, 0)
    lax.fori_loop(0, BRANCH, branch, 0)
    lax.fori_loop(0, TRUNK, trunk, 0)

    def finish(i, _):
        here = segment(role[i])
        depth = jnp.where(i < TRUNK + BRANCH, jnp.minimum(i, TRUNK), TRUNK + 1)
        out[here, WIDE : 2 * WIDE] = rope_back(dk[segment(i), :], depth).astype(BF16)
        out[here, 2 * WIDE : 3 * WIDE] = dv[segment(i), :].astype(BF16)
        return 0

    lax.fori_loop(0, SEGS, finish, 0)


def attention_backward(parents, parts, upstream, attended, logsum, cosine, sine):
    tokens = SEGS * SEG
    vmem = pl.BlockSpec(memory_space=pltpu.VMEM)
    return pl.pallas_call(
        functools.partial(attention_back_kernel, len(parts)),
        out_shape=jax.ShapeDtypeStruct((tokens, 3 * WIDE), BF16),
        in_specs=[pl.BlockSpec(memory_space=pltpu.SMEM)] + [vmem] * (len(parts) + 5),
        out_specs=vmem,
        scratch_shapes=[pltpu.VMEM((tokens, WIDE), BF16)] * 3
        + [pltpu.VMEM((WIDE, tokens), BF16)]
        + [pltpu.VMEM((tokens, WIDE), F32)] * 2
        + [
            pltpu.VMEM((WIDE, 2 * SEG), F32),
            pltpu.SMEM((SEGS * BRANCH,), jnp.int32),
            pltpu.SMEM((SEGS,), jnp.int32),
            pltpu.SMEM((SEGS,), jnp.int32),
            pltpu.SMEM((SEGS,), jnp.int32),
        ],
        compiler_params=pltpu.CompilerParams(vmem_limit_bytes=VMEM_BYTES),
        cost_estimate=pl.CostEstimate(
            flops=152 * 2 * 10 * SEG * SEG * 128,
            bytes_accessed=tokens * WIDE * 24,
            transcendentals=152 * 2 * SEG * SEG,
        ),
        name="attention_backward",
    )(parents, *parts, upstream, attended, logsum, cosine, sine)


def angle_tables(positions):
    lane = jnp.arange(WIDE)
    freq = THETA ** (-(lane % (DH // 2)).astype(F32) * 2.0 / DH)
    angle = positions.astype(F32)[:, None] * freq[None, :]
    sign = jnp.where((lane % DH) < DH // 2, -1.0, 1.0)
    return jnp.cos(angle), jnp.sin(angle) * sign[None, :]


def project_kernel(mine, theirs, gain, query_w, key_w, value_w, cosine, sine, out, low_out):
    total = mine[...].astype(F32) + theirs[...].astype(F32)
    scale = lax.rsqrt(jnp.mean(total * total, axis=-1, keepdims=True) + EPSILON)
    rounded = (total * scale * gain[...]).astype(BF16)
    low_out[...] = rounded
    low = (lax.broadcasted_iota(jnp.int32, (total.shape[0], WIDE), 1) % DH) < (DH // 2)
    for at, weight in enumerate((query_w, key_w, value_w)):
        raw = nn(rounded, weight[...])
        for peer in range(out.shape[0]):
            part = raw[:, peer * WIDE : (peer + 1) * WIDE]
            if at < 2:
                part = part * cosine[...] + swap_halves(part, low) * sine[...]
            out[peer, :, at * WIDE : (at + 1) * WIDE] = part.astype(BF16)


def project(mine, theirs, gain, query_w, key_w, value_w, cosine, sine):
    rows, width = mine.shape
    block = SEG
    inner = query_w.shape[1]
    peers = inner // WIDE
    by_row = pl.BlockSpec((block, width), lambda i: (i, 0))
    weight = pl.BlockSpec((width, inner), lambda i: (0, 0))
    table = pl.BlockSpec((block, WIDE), lambda i: (i, 0))
    return pl.pallas_call(
        project_kernel,
        grid=(rows // block,),
        out_shape=(
            jax.ShapeDtypeStruct((peers, rows, 3 * WIDE), BF16),
            jax.ShapeDtypeStruct((rows, width), BF16),
        ),
        in_specs=[
            by_row,
            by_row,
            pl.BlockSpec((1, width), lambda i: (0, 0)),
            weight,
            weight,
            weight,
            table,
            table,
        ],
        out_specs=(pl.BlockSpec((peers, block, 3 * WIDE), lambda i: (0, i, 0)), by_row),
        compiler_params=pltpu.CompilerParams(vmem_limit_bytes=VMEM_BYTES),
        cost_estimate=pl.CostEstimate(
            flops=2 * rows * width * 3 * inner,
            bytes_accessed=rows * width * 6 + 6 * width * inner + rows * inner * 6,
            transcendentals=rows,
        ),
        name="project",
    )(mine, theirs, gain, query_w, key_w, value_w, cosine, sine)


def middle_kernel(
    meta,
    adapted,
    heads,
    cotangent,
    second_gain,
    third_gain,
    fourth_gain,
    wo_own,
    wo_all,
    wg_own,
    wg_all,
    wu_own,
    wu_all,
    wd_own,
    wd_all,
    layer_out,
    middle_out,
    attended_out,
    attention_out,
    third_out,
    mixed_out,
    hidden_out,
    gate_out,
    up_out,
    heads_back,
    gains_out,
    wo,
    wg,
    wu,
    wd,
    gate_s,
    up_s,
    sums,
    sem,
):
    step = pl.program_id(0)
    tensor = meta[0]
    copies = []
    for weight, own, all_of, by_lane in (
        (wo, wo_own, wo_all, False),
        (wg, wg_own, wg_all, True),
        (wu, wu_own, wu_all, True),
        (wd, wd_own, wd_all, False),
    ):
        rows, lanes = own.shape
        other = all_of.at[pl.ds(pl.multiple_of((1 - tensor) * rows, 128), rows)]
        for src, row, lane in (
            (own, 0, 0),
            (other, 0 if by_lane else rows, lanes if by_lane else 0),
        ):
            dst = weight.at[pl.ds(row, rows), pl.ds(lane, lanes)]
            copies.append(pltpu.make_async_copy(src, dst, sem.at[len(copies)]))

    @pl.when(step == 0)
    def _():
        for copy in copies:
            copy.start()
        gains_out[...] = jnp.zeros_like(gains_out)
        for copy in copies[:2]:
            copy.wait()

    groups = heads.shape[0] // 2
    for side in range(2):
        for group in range(groups):
            at = (side * groups + group) * WIDE
            source = group * 2 + (tensor if side == 0 else 1 - tensor)
            attended_out[:, at : at + WIDE] = heads[source]
    attention = nn(attended_out[...], wo[...])

    def scaling(values):
        return lax.rsqrt(jnp.mean(values * values, axis=-1, keepdims=True) + EPSILON)

    def inward(upstream, gain, normed, scale):
        scaled = upstream * gain
        return scale * (scaled - normed * jnp.mean(scaled * normed, axis=-1, keepdims=True))

    second_scale = scaling(attention)
    second_normed = attention * second_scale
    middle = adapted[...] + second_normed * second_gain[...]
    third_scale = scaling(middle)
    third_normed = middle * third_scale
    third_out[...] = (third_normed * third_gain[...]).astype(BF16)

    @pl.when(step == 0)
    def _():
        for copy in copies[2:]:
            copy.wait()

    sums[...] = jnp.zeros_like(sums)

    def forward(c, _):
        cut = pl.ds(pl.multiple_of(c * HIDDEN, HIDDEN), HIDDEN)
        gate = nn(third_out[...], wg[:, cut])
        upward = nn(third_out[...], wu[:, cut])
        gate_s[c] = gate
        up_s[c] = upward
        hidden = (gate / (1.0 + jnp.exp(-gate)) * upward).astype(BF16)
        hidden_out[:, cut] = hidden
        sums[...] += nn(hidden, wd[cut, :])
        return 0

    lax.fori_loop(0, gate_s.shape[0], forward, 0)
    mixed = sums[...]
    fourth_scale = scaling(mixed)
    fourth_normed = mixed * fourth_scale
    layer_out[...] = (middle + fourth_normed * fourth_gain[...]).astype(BF16)
    upstream = cotangent[...].astype(F32)
    gains_out[2:3, :] += jnp.sum(upstream * fourth_normed, axis=0, keepdims=True)
    mixed_out[...] = inward(upstream, fourth_gain[...], fourth_normed, fourth_scale).astype(BF16)
    sums[...] = jnp.zeros_like(sums)

    def backward(c, _):
        cut = pl.ds(pl.multiple_of(c * HIDDEN, HIDDEN), HIDDEN)
        back = nt(mixed_out[...], wd[cut, :]).astype(BF16).astype(F32)
        gate = gate_s[c]
        sigmoid = 1.0 / (1.0 + jnp.exp(-gate))
        silu = gate * sigmoid
        gate_back = (back * up_s[c] * (sigmoid + silu * (1.0 - sigmoid))).astype(BF16)
        up_back = (back * silu).astype(BF16)
        gate_out[:, cut] = gate_back
        up_out[:, cut] = up_back
        sums[...] += nt(gate_back, wg[:, cut]) + nt(up_back, wu[:, cut])
        return 0

    lax.fori_loop(0, gate_s.shape[0], backward, 0)
    third_back = sums[...]
    gains_out[1:2, :] += jnp.sum(third_back * third_normed, axis=0, keepdims=True)
    middle_back = upstream + inward(third_back, third_gain[...], third_normed, third_scale)
    middle_out[...] = middle_back
    gains_out[0:1, :] += jnp.sum(middle_back * second_normed, axis=0, keepdims=True)
    attention_out[...] = inward(
        middle_back, second_gain[...], second_normed, second_scale
    ).astype(BF16)
    heads_low = nt(attention_out[...], wo[...]).astype(BF16)
    for side in range(2):
        for group in range(groups):
            at = (side * groups + group) * WIDE
            target = group * 2 + (tensor if side == 0 else 1 - tensor)
            heads_back[target] = heads_low[:, at : at + WIDE]


def middle_section(meta, adapted, heads, cotangent, gains, weights):
    rows, width = adapted.shape
    sources = heads.shape[0]
    inner = sources * WIDE
    hidden = 2 * weights[2].shape[1]
    block = rows // 2
    steps = rows // block
    row = pl.BlockSpec((block, width), lambda i, meta: (i, 0))
    wide = pl.BlockSpec((block, hidden), lambda i, meta: (i, 0))
    head = pl.BlockSpec((sources, block, WIDE), lambda i, meta: (0, i, 0))
    gain = pl.BlockSpec((1, width), lambda i, meta: (0, 0))
    hbm = pl.BlockSpec(memory_space=pl.ANY)
    return pl.pallas_call(
        middle_kernel,
        grid_spec=pltpu.PrefetchScalarGridSpec(
            num_scalar_prefetch=1,
            grid=(steps,),
            in_specs=[
                row,
                head,
                pl.BlockSpec((block, width), lambda i, meta: (meta[0] * steps + i, 0)),
                gain,
                gain,
                gain,
            ]
            + [hbm] * 8,
            out_specs=(
                row,
                row,
                pl.BlockSpec((block, inner), lambda i, meta: (i, 0)),
                row,
                row,
                row,
                wide,
                wide,
                wide,
                head,
                pl.BlockSpec((8, width), lambda i, meta: (0, 0)),
            ),
            scratch_shapes=[
                pltpu.VMEM((inner, width), BF16),
                pltpu.VMEM((width, hidden), BF16),
                pltpu.VMEM((width, hidden), BF16),
                pltpu.VMEM((hidden, width), BF16),
                pltpu.VMEM((hidden // HIDDEN, block, HIDDEN), F32),
                pltpu.VMEM((hidden // HIDDEN, block, HIDDEN), F32),
                pltpu.VMEM((block, width), F32),
                pltpu.SemaphoreType.DMA((8,)),
            ],
        ),
        out_shape=(
            jax.ShapeDtypeStruct((rows, width), BF16),
            jax.ShapeDtypeStruct((rows, width), F32),
            jax.ShapeDtypeStruct((rows, inner), BF16),
            jax.ShapeDtypeStruct((rows, width), BF16),
            jax.ShapeDtypeStruct((rows, width), BF16),
            jax.ShapeDtypeStruct((rows, width), BF16),
            jax.ShapeDtypeStruct((rows, hidden), BF16),
            jax.ShapeDtypeStruct((rows, hidden), BF16),
            jax.ShapeDtypeStruct((rows, hidden), BF16),
            jax.ShapeDtypeStruct((sources, rows, WIDE), BF16),
            jax.ShapeDtypeStruct((8, width), F32),
        ),
        compiler_params=pltpu.CompilerParams(vmem_limit_bytes=VMEM_BYTES),
        cost_estimate=pl.CostEstimate(
            flops=rows * width * (4 * inner + 12 * hidden),
            bytes_accessed=6 * width * hidden + 2 * width * inner + rows * (hidden * 6 + width * 20),
            transcendentals=rows * hidden * 2,
        ),
        name="middle_section",
    )(meta, adapted, heads, cotangent, *gains, *weights)


def input_back_kernel(meta, parts, query_w, key_w, value_w, out, joined):
    inner = query_w.shape[1]
    for at in range(3):
        for group in range(parts.shape[0]):
            to = at * inner + group * WIDE
            joined[:, to : to + WIDE] = parts[group, :, at * WIDE : (at + 1) * WIDE]
    total = nt(joined[:, 0:inner], query_w[...])
    total += nt(joined[:, inner : 2 * inner], key_w[...])
    total += nt(joined[:, 2 * inner : 3 * inner], value_w[...])
    out[...] = total.astype(out.dtype)


def input_back(meta, parts, query_w, key_w, value_w, dtype):
    groups, rows, lanes = parts.shape
    rows = rows // 2
    width, inner = query_w.shape
    block = rows // 2
    steps = 2
    weight = pl.BlockSpec((width, inner), lambda i, meta: (0, 0))
    return pl.pallas_call(
        input_back_kernel,
        grid_spec=pltpu.PrefetchScalarGridSpec(
            num_scalar_prefetch=1,
            grid=(steps,),
            in_specs=[
                pl.BlockSpec((groups, block, lanes), lambda i, meta: (0, meta[0] * steps + i, 0)),
                weight,
                weight,
                weight,
            ],
            out_specs=(
                pl.BlockSpec((block, width), lambda i, meta: (i, 0)),
                pl.BlockSpec((block, 3 * inner), lambda i, meta: (i, 0)),
            ),
        ),
        out_shape=(
            jax.ShapeDtypeStruct((rows, width), dtype),
            jax.ShapeDtypeStruct((rows, 3 * inner), BF16),
        ),
        compiler_params=pltpu.CompilerParams(vmem_limit_bytes=VMEM_BYTES),
        cost_estimate=pl.CostEstimate(
            flops=2 * rows * width * 3 * inner,
            bytes_accessed=rows * inner * 12 + 6 * width * inner + rows * width * 4,
            transcendentals=0,
        ),
        name="input_back",
    )(meta, parts, query_w, key_w, value_w)


def swap(value, axis):
    return lax.ppermute(value, axis, [(0, 1), (1, 0)])


def together(*values):
    return lax.optimization_barrier(values)


def cut(value, index, rows):
    return lax.dynamic_slice_in_dim(value, index * rows, rows, 0)


def add_low(left, right):
    return (left.astype(F32) + right.astype(F32)).astype(BF16)


def fold(value, index, axis):
    half = value.shape[0] // 2
    return add_low(cut(value, index, half), swap(cut(value, 1 - index, half), axis))


def unfold(value, index, axis):
    other = swap(value, axis)
    return jnp.concatenate(
        [jnp.where(index == 0, value, other), jnp.where(index == 0, other, value)], axis=0
    )


def sum_small(value):
    for axis in ("tensor", "core", "x"):
        value = value + swap(value, axis)
    for pairs in ([(0, 1), (1, 0), (2, 3), (3, 2)], [(0, 2), (2, 0), (1, 3), (3, 1)]):
        value = value + lax.ppermute(value, "dp", pairs)
    return value


def tn(left, right):
    return lax.dot_general(
        left, right, (((0,), (0,)), ((), ())), preferred_element_type=F32
    ).astype(BF16)


def on_device_paired(
    latent_embed,
    adapter,
    first_gain,
    query_weight,
    key_weight,
    value_weight,
    output_weight,
    second_gain,
    third_gain,
    gate_weight,
    up_weight,
    down_weight,
    fourth_gain,
    parents,
    positions,
    cotangent,
):
    rows = latent_embed.shape[0]
    width = adapter.shape[2]
    half_rows = rows // 2
    tensor = lax.axis_index("tensor")
    core = lax.axis_index("core")
    x = lax.axis_index("x")
    everyone = ("x", "core", "tensor")
    meta = jnp.stack([tensor, core]).astype(jnp.int32)
    meta_other = jnp.stack([1 - tensor, core]).astype(jnp.int32)
    one_row = lambda gain: gain.reshape(1, -1)

    cosine, sine = angle_tables(positions)
    cuts = [0, 2 * SEG, 4 * SEG, rows]
    adapted_parts, low_parts, head_parts = [], [], []
    mine = [
        jnp.einsum(
            "rcd,cde->re", latent_embed[start:stop], adapter, preferred_element_type=F32
        ).astype(BF16)
        for start, stop in zip(cuts[:-1], cuts[1:])
    ]
    theirs = []
    for i in range(len(mine)):
        if i > 0:
            mine[i], theirs[i - 1] = together(mine[i], theirs[i - 1])
        theirs.append(swap(mine[i], "tensor"))
    own_weights = (output_weight, gate_weight, up_weight, down_weight)
    pieces = [cut(weight, 2 * x + core, weight.shape[0] // 4) for weight in own_weights]
    *pieces, theirs[-1] = together(*pieces, theirs[-1])
    weights = []
    for weight, piece in zip(own_weights, pieces):
        weights.append(weight)
        weights.append(lax.all_gather(piece, ("tensor", "x", "core"), axis=0, tiled=True))
    for i in range(len(mine)):
        start, stop = cuts[i], cuts[i + 1]
        sent, low = project(
            mine[i],
            theirs[i],
            one_row(first_gain),
            query_weight,
            key_weight,
            value_weight,
            cosine[start:stop],
            sine[start:stop],
        )
        head_parts.append(lax.all_to_all(sent, ("x", "core"), 0, 0, tiled=False))
        low_parts.append(low)
        adapted_parts.append(mine[i].astype(F32) + theirs[i].astype(F32))
    adapted = cut(jnp.concatenate(adapted_parts, axis=0), tensor, half_rows)
    first_low = jnp.concatenate(low_parts, axis=0)

    attended, logsum = attention_forward(parents, head_parts)
    heads = lax.all_to_all(
        attended.reshape(8, half_rows, WIDE), everyone, 0, 0, tiled=False
    )
    (
        layer_half,
        middle_back,
        attended_all,
        attention_low,
        third_low,
        mixed_low,
        hidden,
        gate_low,
        up_low,
        heads_back,
        gain_parts,
    ) = middle_section(
        meta,
        adapted,
        heads,
        cotangent,
        (one_row(second_gain), one_row(third_gain), one_row(fourth_gain)),
        weights,
    )
    upstream = lax.all_to_all(heads_back, everyone, 0, 0, tiled=False).reshape(-1, WIDE)
    layer_other = swap(layer_half, "tensor")
    layer_out = jnp.concatenate(
        [
            jnp.where(tensor == 0, layer_half, layer_other),
            jnp.where(tensor == 0, layer_other, layer_half),
        ],
        axis=0,
    ).astype(F32)

    split = gate_weight.shape[1]
    inner = output_weight.shape[0]
    own, other = slice(None, split), slice(split, None)
    gate_sides = [fold(tn(third_low, gate_low[:, side]), core, "core") for side in (own, other)]
    up_sides = [fold(tn(third_low, up_low[:, side]), core, "core") for side in (own, other)]
    down_sides = [fold(tn(hidden[:, side], mixed_low), core, "core") for side in (own, other)]
    output_sides = [
        fold(tn(attended_all[:, side], attention_low), core, "core")
        for side in (slice(None, inner), slice(inner, None))
    ]
    upstream, *sides = together(
        upstream, *gate_sides, *up_sides, *down_sides, *output_sides
    )
    gate_sides, up_sides, down_sides, output_sides = (
        sides[0:2],
        sides[2:4],
        sides[4:6],
        sides[6:8],
    )
    gate_sides = [fold(side, x, "x") for side in gate_sides]
    up_sides = [fold(side, x, "x") for side in up_sides]
    down_kept = add_low(down_sides[0], swap(down_sides[1], "tensor"))
    output_kept = add_low(output_sides[0], swap(output_sides[1], "tensor"))

    table_cosine, table_sine = angle_tables(jnp.arange((TRUNK + 2) * SEG))
    sent = attention_backward(
        parents, head_parts, upstream, attended, logsum, table_cosine, table_sine
    )
    parts = lax.all_to_all(
        sent.reshape(4, rows, 3 * WIDE), ("x", "core"), 0, 0, tiled=False
    )

    def finish(value):
        return unfold(unfold(value, x, "x"), core, "core").astype(F32)

    gate_kept = add_low(gate_sides[0], swap(gate_sides[1], "tensor"))
    up_kept = add_low(up_sides[0], swap(up_sides[1], "tensor"))
    gate_sum, up_sum = lax.psum((gate_kept, up_kept), "dp")
    parts, down_kept, output_kept = together(parts, down_kept, output_kept)
    down_kept = fold(down_kept, x, "x")
    output_kept = fold(output_kept, x, "x")
    down_kept, output_kept, gate_sum, up_sum = together(down_kept, output_kept, gate_sum, up_sum)
    down_sum, output_sum = lax.psum((down_kept, output_kept), "dp")

    away, joined_away = input_back(
        meta_other, parts, query_weight, key_weight, value_weight, BF16
    )
    home, joined_home = input_back(meta, parts, query_weight, key_weight, value_weight, F32)
    away = swap(away, "tensor")
    first_low_home = cut(first_low, tensor, half_rows)
    first_low_away = cut(first_low, 1 - tensor, half_rows)
    input_part = (
        lax.dot_general(
            first_low_home, joined_home, (((0,), (0,)), ((), ())), preferred_element_type=F32
        )
        + lax.dot_general(
            first_low_away, joined_away, (((0,), (0,)), ((), ())), preferred_element_type=F32
        )
    ).astype(BF16)
    input_kept = fold(fold(input_part, core, "core"), x, "x")
    input_kept, down_sum, output_sum = together(input_kept, down_sum, output_sum)
    input_sum = lax.psum(input_kept, "dp")
    first_back = home + away.astype(F32)
    first_out, first_normed, first_scale = normalize(adapted, first_gain)
    adapted_part, first_gain_part = normalize_back(
        first_back, first_gain, first_normed, first_scale
    )
    adapted_home = (middle_back + adapted_part).astype(BF16)
    adapted_away = swap(adapted_home, "tensor")
    adapted_low = jnp.concatenate(
        [
            jnp.where(tensor == 0, adapted_home, adapted_away),
            jnp.where(tensor == 0, adapted_away, adapted_home),
        ],
        axis=0,
    )
    adapter_part = jnp.einsum(
        "rcd,re->cde", latent_embed, adapted_low, preferred_element_type=F32
    ).astype(BF16)
    adapter_kept = fold(fold(adapter_part.reshape(-1, width), core, "core"), x, "x")
    adapter_kept, input_sum = together(adapter_kept, input_sum)
    adapter_sum = lax.psum(adapter_kept, "dp")
    latent_gradient = jnp.einsum("re,cde->rcd", adapted_low, adapter, preferred_element_type=F32)
    gains = sum_small(jnp.concatenate([gain_parts[:3], first_gain_part[None]], axis=0))
    gate_total, up_total = finish(gate_sum), finish(up_sum)
    down_total, output_total = finish(down_sum), finish(output_sum)
    input_total = finish(input_sum)
    adapter_total = finish(adapter_sum).reshape(adapter.shape)
    return (
        layer_out,
        latent_gradient,
        adapter_total,
        gains[3],
        input_total[:, :inner],
        input_total[:, inner : 2 * inner],
        input_total[:, 2 * inner :],
        output_total,
        gains[0],
        gains[1],
        gate_total,
        up_total,
        down_total,
        gains[2],
    )


def specs(rows):
    split = P(None, "tensor")
    in_specs = (
        P(rows, None, "tensor"),
        P(None, "tensor", None),
        P(),
        split,
        split,
        split,
        P("tensor", None),
        P(),
        P(),
        split,
        split,
        P("tensor", None),
        P(),
        P("dp", None),
        P(rows),
        P(rows, None),
    )
    out_specs = (
        P(rows, None),
        P(rows, None, "tensor"),
        P(None, "tensor", None),
        P(),
        split,
        split,
        split,
        P("tensor", None),
        P(),
        P(),
        split,
        split,
        P("tensor", None),
        P(),
    )
    return in_specs, out_specs


def solution(mesh):
    sizes = dict(mesh.shape)
    if sizes["seq"] == 4 and sizes["tensor"] == 2:
        fine = Mesh(
            mesh.devices.reshape(sizes["dp"], 2, 2, 2), ("dp", "x", "core", "tensor")
        )
        in_specs, out_specs = specs(("dp", "x", "core"))
        return jax.shard_map(
            on_device_paired, mesh=fine, in_specs=in_specs, out_specs=out_specs, check_vma=False
        )
    in_specs, out_specs = specs(("dp", "seq"))
    return jax.shard_map(
        on_device, mesh=mesh, in_specs=in_specs, out_specs=out_specs, check_vma=False
    )
```

```python
import functools

import jax
import jax.numpy as jnp
from jax import lax
from jax.experimental import pallas as pl
from jax.experimental.pallas import tpu as pltpu
from jax.sharding import Mesh
from jax.sharding import PartitionSpec as P

DH = 64
SEG = 256


EPSILON = 1e-06
THETA = 50000.0


def normalize(values, gain):
    scale = lax.rsqrt(jnp.mean(values * values, axis=-1, keepdims=True) + EPSILON)
    normed = values * scale
    return (normed * gain, normed, scale)


def normalize_back(upstream, gain, normed, scale):
    scaled = upstream * gain
    inward = scale * (scaled - normed * jnp.mean(scaled * normed, axis=-1, keepdims=True))
    return (inward, jnp.sum(upstream * normed, axis=0))


def angles(positions, width):
    half = width // 2
    freq = THETA ** (-jnp.arange(half, dtype=jnp.float32) * 2.0 / width)
    angle = positions.astype(jnp.float32)[:, None] * freq[None, :]
    return (jnp.cos(angle)[:, None, :], jnp.sin(angle)[:, None, :])


def rotate(values, cosine, sine, sign):
    half = values.shape[-1] // 2
    first = values[..., :half]
    second = values[..., half:]
    return jnp.concatenate(
        [first * cosine - sign * second * sine, second * cosine + sign * first * sine], axis=-1
    )


def ancestry(parent_row):
    labels = jnp.arange(parent_row.shape[0], dtype=jnp.int32)

    def extend(index, state):
        current, total = state
        total = total | (current[:, None] == labels[None, :])
        current = jnp.where(current >= 0, jnp.take(parent_row, jnp.maximum(current, 0)), -1)
        return (current, total)

    start = (parent_row, jnp.zeros((parent_row.shape[0], parent_row.shape[0]), jnp.bool_))
    current, total = lax.fori_loop(0, parent_row.shape[0], extend, start)
    return total


def path_mask(parent_row, query_ids, key_ids):
    table = ancestry(parent_row)
    query_seg = query_ids // SEG
    key_seg = key_ids // SEG
    far = jnp.take(jnp.take(table, query_seg, axis=0), key_seg, axis=1)
    near = (query_seg[:, None] == key_seg[None, :]) & (key_ids[None, :] <= query_ids[:, None])
    return far | near


def on_device(
    latent_embed,
    adapter,
    first_gain,
    query_weight,
    key_weight,
    value_weight,
    output_weight,
    second_gain,
    third_gain,
    gate_weight,
    up_weight,
    down_weight,
    fourth_gain,
    parents,
    positions,
    cotangent,
):
    rows = latent_embed.shape[0]
    local_heads = query_weight.shape[1] // DH
    scale = DH ** (-0.5)
    adapted = lax.psum(
        jnp.einsum("rcd,cde->re", latent_embed, adapter, preferred_element_type=jnp.float32),
        "tensor",
    )
    first_out, first_normed, first_scale = normalize(adapted, first_gain)
    first_low = first_out.astype(jnp.bfloat16)
    cosine, sine = angles(positions, DH)
    query_raw = jnp.dot(first_low, query_weight, preferred_element_type=jnp.float32).reshape(
        rows, local_heads, DH
    )
    queries = rotate(query_raw, cosine, sine, 1.0).astype(jnp.bfloat16)
    key_raw = jnp.dot(first_low, key_weight, preferred_element_type=jnp.float32).reshape(
        rows, local_heads, DH
    )
    keys_local = rotate(key_raw, cosine, sine, 1.0).astype(jnp.bfloat16)
    values_local = (
        jnp.dot(first_low, value_weight, preferred_element_type=jnp.float32)
        .astype(jnp.bfloat16)
        .reshape(rows, local_heads, DH)
    )
    keys_all, values_all = (
        lax.all_gather(keys_local, "seq", axis=0, tiled=True),
        lax.all_gather(values_local, "seq", axis=0, tiled=True),
    )
    tree_rows = keys_all.shape[0]
    query_ids = lax.axis_index("seq") * rows + jnp.arange(rows, dtype=jnp.int32)
    key_ids = jnp.arange(tree_rows, dtype=jnp.int32)
    allowed = path_mask(parents[0], query_ids, key_ids)[None]

    def score_block(keys):
        raw = jnp.einsum("qhd,khd->hqk", queries, keys, preferred_element_type=jnp.float32) * scale
        return jnp.where(allowed, raw, -1e30)

    scores = score_block(keys_all)
    top = jnp.max(scores, axis=-1, keepdims=True)
    weights = jnp.exp(scores - top)
    total = jnp.sum(weights, axis=-1, keepdims=True)
    probs = weights / total
    logsum = top + jnp.log(total)
    attended = jnp.einsum(
        "hqk,khd->qhd", probs.astype(jnp.bfloat16), values_all, preferred_element_type=jnp.float32
    )
    attended = attended.reshape(rows, local_heads * DH).astype(jnp.bfloat16)
    attention = lax.psum(
        jnp.dot(attended, output_weight, preferred_element_type=jnp.float32).astype(jnp.bfloat16),
        "tensor",
    ).astype(jnp.float32)
    second_out, second_normed, second_scale = normalize(attention, second_gain)
    middle = adapted + second_out
    third_out, third_normed, third_scale = normalize(middle, third_gain)
    third_low = third_out.astype(jnp.bfloat16)
    gate = jnp.dot(third_low, gate_weight, preferred_element_type=jnp.float32)
    upward = jnp.dot(third_low, up_weight, preferred_element_type=jnp.float32)
    hidden = (jax.nn.silu(gate) * upward).astype(jnp.bfloat16)
    mixed = lax.psum(
        jnp.dot(hidden, down_weight, preferred_element_type=jnp.float32).astype(jnp.bfloat16),
        "tensor",
    ).astype(jnp.float32)
    fourth_out, fourth_normed, fourth_scale = normalize(mixed, fourth_gain)
    layer_out = middle + fourth_out
    upstream = cotangent.astype(jnp.float32)
    mixed_back, fourth_gain_part = normalize_back(
        upstream, fourth_gain, fourth_normed, fourth_scale
    )
    mixed_low = mixed_back.astype(jnp.bfloat16)
    down_part = jnp.einsum("rf,rd->fd", hidden, mixed_low, preferred_element_type=jnp.float32)
    hidden_back = (
        jnp.einsum("rd,fd->rf", mixed_low, down_weight, preferred_element_type=jnp.float32)
        .astype(jnp.bfloat16)
        .astype(jnp.float32)
    )
    swiglu_value, product_back = jax.vjp(
        lambda left, right: jax.nn.silu(left) * right, gate, upward
    )
    gate_back, up_back = product_back(hidden_back)
    gate_low = gate_back.astype(jnp.bfloat16)
    up_low = up_back.astype(jnp.bfloat16)
    gate_part = jnp.einsum("rd,rf->df", third_low, gate_low, preferred_element_type=jnp.float32)
    up_part = jnp.einsum("rd,rf->df", third_low, up_low, preferred_element_type=jnp.float32)
    third_term = jnp.einsum(
        "rf,df->rd", gate_low, gate_weight, preferred_element_type=jnp.float32
    ) + jnp.einsum("rf,df->rd", up_low, up_weight, preferred_element_type=jnp.float32)
    third_back = lax.psum(third_term.astype(jnp.bfloat16), "tensor").astype(jnp.float32)
    middle_part, third_gain_part = normalize_back(third_back, third_gain, third_normed, third_scale)
    middle_back = upstream + middle_part
    attention_back, second_gain_part = normalize_back(
        middle_back, second_gain, second_normed, second_scale
    )
    attention_low = attention_back.astype(jnp.bfloat16)
    output_part = jnp.einsum(
        "re,rd->ed", attended, attention_low, preferred_element_type=jnp.float32
    )
    attended_back = (
        jnp.einsum("rd,ed->re", attention_low, output_weight, preferred_element_type=jnp.float32)
        .astype(jnp.bfloat16)
        .reshape(rows, local_heads, DH)
    )
    keys_back, values_back = (
        lax.all_gather(keys_local, "seq", axis=0, tiled=True),
        lax.all_gather(values_local, "seq", axis=0, tiled=True),
    )
    probs_back = jnp.exp(score_block(keys_back) - logsum)
    prob_grad = jnp.einsum(
        "qhd,khd->hqk", attended_back, values_back, preferred_element_type=jnp.float32
    )
    score_grad = (
        probs_back * (prob_grad - jnp.sum(prob_grad * probs_back, axis=-1, keepdims=True))
    ).astype(jnp.bfloat16)
    query_rot = (
        jnp.einsum("hqk,khd->qhd", score_grad, keys_back, preferred_element_type=jnp.float32)
        * scale
    )
    key_rot_all = (
        jnp.einsum("hqk,qhd->khd", score_grad, queries, preferred_element_type=jnp.float32) * scale
    )
    value_back_all = jnp.einsum(
        "hqk,qhd->khd",
        probs_back.astype(jnp.bfloat16),
        attended_back,
        preferred_element_type=jnp.float32,
    )
    key_rot, value_back = (
        lax.psum_scatter(
            key_rot_all.astype(jnp.bfloat16), "seq", scatter_dimension=0, tiled=True
        ).astype(jnp.float32),
        lax.psum_scatter(
            value_back_all.astype(jnp.bfloat16), "seq", scatter_dimension=0, tiled=True
        ).astype(jnp.float32),
    )
    query_low = (
        rotate(query_rot, cosine, sine, -1.0).astype(jnp.bfloat16).reshape(rows, local_heads * DH)
    )
    key_low = (
        rotate(key_rot, cosine, sine, -1.0).astype(jnp.bfloat16).reshape(rows, local_heads * DH)
    )
    value_low = value_back.astype(jnp.bfloat16).reshape(rows, local_heads * DH)
    query_part = jnp.einsum("rd,re->de", first_low, query_low, preferred_element_type=jnp.float32)
    key_part = jnp.einsum("rd,re->de", first_low, key_low, preferred_element_type=jnp.float32)
    value_part = jnp.einsum("rd,re->de", first_low, value_low, preferred_element_type=jnp.float32)
    first_term = jnp.einsum(
        "re,de->rd", query_low, query_weight, preferred_element_type=jnp.float32
    )
    first_term = first_term + jnp.einsum(
        "re,de->rd", key_low, key_weight, preferred_element_type=jnp.float32
    )
    first_term = first_term + jnp.einsum(
        "re,de->rd", value_low, value_weight, preferred_element_type=jnp.float32
    )
    first_back = lax.psum(first_term.astype(jnp.bfloat16), "tensor").astype(jnp.float32)
    adapted_part, first_gain_part = normalize_back(
        first_back, first_gain, first_normed, first_scale
    )
    adapted_low = (middle_back + adapted_part).astype(jnp.bfloat16)
    latent_gradient = jnp.einsum(
        "re,cde->rcd", adapted_low, adapter, preferred_element_type=jnp.float32
    )
    adapter_part = jnp.einsum(
        "rcd,re->cde", latent_embed, adapted_low, preferred_element_type=jnp.float32
    )
    summed = (
        lax.psum(gate_part.astype(jnp.bfloat16), ("dp", "seq")).astype(jnp.float32),
        lax.psum(up_part.astype(jnp.bfloat16), ("dp", "seq")).astype(jnp.float32),
        lax.psum(down_part.astype(jnp.bfloat16), ("dp", "seq")).astype(jnp.float32),
        lax.psum(third_gain_part.astype(jnp.bfloat16), ("dp", "seq")).astype(jnp.float32),
        lax.psum(fourth_gain_part.astype(jnp.bfloat16), ("dp", "seq")).astype(jnp.float32),
        lax.psum(query_part.astype(jnp.bfloat16), ("dp", "seq")).astype(jnp.float32),
        lax.psum(key_part.astype(jnp.bfloat16), ("dp", "seq")).astype(jnp.float32),
        lax.psum(value_part.astype(jnp.bfloat16), ("dp", "seq")).astype(jnp.float32),
        lax.psum(output_part.astype(jnp.bfloat16), ("dp", "seq")).astype(jnp.float32),
        lax.psum(first_gain_part.astype(jnp.bfloat16), ("dp", "seq")).astype(jnp.float32),
        lax.psum(second_gain_part.astype(jnp.bfloat16), ("dp", "seq")).astype(jnp.float32),
        lax.psum(adapter_part.astype(jnp.bfloat16), ("dp", "seq")).astype(jnp.float32),
    )
    gate_total, up_total, down_total, third_total, fourth_total = (
        summed[0],
        summed[1],
        summed[2],
        summed[3],
        summed[4],
    )
    query_total, key_total, value_total, output_total, first_total, second_total = (
        summed[5],
        summed[6],
        summed[7],
        summed[8],
        summed[9],
        summed[10],
    )
    adapter_total = summed[11]
    return (
        layer_out,
        latent_gradient,
        adapter_total,
        first_total,
        query_total,
        key_total,
        value_total,
        output_total,
        second_total,
        third_total,
        gate_total,
        up_total,
        down_total,
        fourth_total,
    )


TRUNK = 8
BRANCH = 4
LEAVES = 2
SEGS = TRUNK + BRANCH + BRANCH * LEAVES
WIDE = 2 * DH
NEG = -1e30
F32 = jnp.float32
BF16 = jnp.bfloat16
KEYS = 512
HIDDEN = 256
VMEM_BYTES = 60 << 20


def nt(left, right):
    return lax.dot_general(left, right, (((1,), (1,)), ((), ())), preferred_element_type=F32)


def nn(left, right):
    return lax.dot_general(left, right, (((1,), (0,)), ((), ())), preferred_element_type=F32)


def segment(index, size=SEG):
    return pl.ds(pl.multiple_of(index * SEG, SEG), size)


def find_roles(parents, child, count, role):
    for s in range(SEGS):
        count[s] = 0
    role[0] = 0
    for s in range(SEGS):
        parent = parents[0, s]

        @pl.when(parent < 0)
        def _():
            role[0] = s

        @pl.when(parent >= 0)
        def _():
            seen = count[parent]
            child[parent * BRANCH + seen] = s
            count[parent] = seen + 1

    for i in range(TRUNK - 1):
        role[i + 1] = child[role[i] * BRANCH]
    for b in range(BRANCH):
        role[TRUNK + b] = child[role[TRUNK - 1] * BRANCH + b]
    for b in range(BRANCH):
        for leaf in range(LEAVES):
            role[TRUNK + BRANCH + b * LEAVES + leaf] = child[role[TRUNK + b] * BRANCH + leaf]


def heads_apart(values, first):
    zero = jnp.zeros_like(values)
    return jnp.concatenate(
        [jnp.where(first, values, zero), jnp.where(first, zero, values)], axis=0
    )


def attention_kernel(
    parents, parts, out, logsum, qr, kr, v0, v1, kept, acc, top, total, child, count, role
):
    find_roles(parents, child, count, role)
    first = lax.broadcasted_iota(jnp.int32, (SEG, WIDE), 1) < DH

    def sort(i, _):
        here, source = segment(i), segment(role[i])
        qr[here, :] = parts[source, 0:WIDE] * jnp.asarray(DH**-0.5, BF16)
        kr[here, :] = parts[source, WIDE : 2 * WIDE]
        value = parts[source, 2 * WIDE : 3 * WIDE]
        zero = jnp.zeros_like(value)
        v0[here, :] = jnp.where(first, value, zero)
        v1[here, :] = jnp.where(first, zero, value)
        return 0

    lax.fori_loop(0, SEGS, sort, 0)
    row = lax.broadcasted_iota(jnp.int32, (2 * SEG, SEG), 0)
    col = lax.broadcasted_iota(jnp.int32, (2 * SEG, SEG), 1)
    causal = col <= jnp.where(row >= SEG, row - SEG, row)

    def fold(values, op):
        result = values[:, 0:128]
        for at in range(128, values.shape[1], 128):
            result = op(result, values[:, at : at + 128])
        return result

    def query(index, count_big, big, extra):
        queries = heads_apart(qr[segment(index), :], first)
        own = jnp.where(causal, nt(queries, kr[segment(index), :]), NEG)
        top[...] = fold(own, jnp.maximum)
        others = []
        for other in extra:
            scores = nt(queries, kr[segment(other), :])
            top[...] = jnp.maximum(top[...], fold(scores, jnp.maximum))
            others.append(scores)

        def find(c, _):
            scores = nt(queries, kr[pl.ds(pl.multiple_of(c * big, big), big), :])
            kept[c, :, 0:big] = scores
            top[...] = jnp.maximum(top[...], fold(scores, jnp.maximum))
            return 0

        lax.fori_loop(0, count_big, find, 0)
        most = jnp.max(top[...], axis=1, keepdims=True)

        def add(scores, keys, fresh=False):
            weights = jnp.exp(scores - most)
            summed = fold(weights, jnp.add)
            low = weights.astype(BF16)
            product = nn(low[:SEG], v0[keys, :]) + nn(low[SEG:], v1[keys, :])
            total[...] = summed if fresh else total[...] + summed
            acc[...] = product if fresh else acc[...] + product

        add(own, segment(index), True)
        for other, scores in zip(extra, others):
            add(scores, segment(other))

        def use(c, _):
            add(kept[c, :, 0:big], pl.ds(pl.multiple_of(c * big, big), big))
            return 0

        lax.fori_loop(0, count_big, use, 0)
        whole = jnp.sum(total[...], axis=1, keepdims=True)
        inverse = 1.0 / whole
        log = most + jnp.log(whole)
        here = segment(role[index])
        out[here, :] = (acc[...] * jnp.where(first, inverse[:SEG], inverse[SEG:])).astype(BF16)
        logsum[here, :] = jnp.where(first, log[:SEG], log[SEG:])

    def trunk(i, _):
        query(i, i, SEG, [])
        return 0

    def branch(i, _):
        query(TRUNK + i, TRUNK * SEG // KEYS, KEYS, [])
        return 0

    def leaf(i, _):
        query(TRUNK + BRANCH + i, TRUNK * SEG // KEYS, KEYS, [TRUNK + i // LEAVES])
        return 0

    lax.fori_loop(0, TRUNK, trunk, 0)
    lax.fori_loop(0, BRANCH, branch, 0)
    lax.fori_loop(0, BRANCH * LEAVES, leaf, 0)


def attention_forward(parents, parts):
    tokens = SEGS * SEG
    vmem = pl.BlockSpec(memory_space=pltpu.VMEM)
    return pl.pallas_call(
        attention_kernel,
        out_shape=(
            jax.ShapeDtypeStruct((tokens, WIDE), BF16),
            jax.ShapeDtypeStruct((tokens, WIDE), F32),
        ),
        in_specs=[pl.BlockSpec(memory_space=pltpu.SMEM), vmem],
        out_specs=(vmem, vmem),
        scratch_shapes=[pltpu.VMEM((tokens, WIDE), BF16)] * 4
        + [
            pltpu.VMEM((TRUNK, 2 * SEG, KEYS), F32),
            pltpu.VMEM((SEG, WIDE), F32),
            pltpu.VMEM((2 * SEG, 128), F32),
            pltpu.VMEM((2 * SEG, 128), F32),
            pltpu.SMEM((SEGS * BRANCH,), jnp.int32),
            pltpu.SMEM((SEGS,), jnp.int32),
            pltpu.SMEM((SEGS,), jnp.int32),
        ],
        compiler_params=pltpu.CompilerParams(vmem_limit_bytes=VMEM_BYTES),
        cost_estimate=pl.CostEstimate(
            flops=152 * 2 * 4 * SEG * SEG * 128,
            bytes_accessed=tokens * WIDE * 12,
            transcendentals=152 * 2 * SEG * SEG,
        ),
        name="attention_forward",
    )(parents, parts.reshape(tokens, 3 * WIDE))


def swap_halves(values, low):
    return jnp.where(
        low, pltpu.roll(values, WIDE - DH // 2, 1), pltpu.roll(values, DH // 2, 1)
    )


def attention_back_kernel(
    parents,
    parts,
    upstream,
    attended,
    logsum,
    cosine,
    sine,
    out,
    qr,
    kr,
    vr,
    kt,
    dk,
    dv,
    dqt,
    child,
    count,
    role,
):
    find_roles(parents, child, count, role)
    lane = lax.broadcasted_iota(jnp.int32, (SEG, WIDE), 1)
    first = lane < DH
    low = (lane % DH) < (DH // 2)

    def sort(i, _):
        here, source = segment(i), segment(role[i])
        qr[here, :] = parts[source, 0:WIDE] * jnp.asarray(DH**-0.5, BF16)
        key = parts[source, WIDE : 2 * WIDE]
        kr[here, :] = key
        kt[:, here] = key.T
        vr[here, :] = parts[source, 2 * WIDE : 3 * WIDE]
        return 0

    lax.fori_loop(0, SEGS, sort, 0)
    dk[...] = jnp.zeros_like(dk)
    dv[...] = jnp.zeros_like(dv)
    key_at = lax.broadcasted_iota(jnp.int32, (SEG, 2 * SEG), 0)
    query_at = lax.broadcasted_iota(jnp.int32, (SEG, 2 * SEG), 1)
    causal = key_at <= jnp.where(query_at >= SEG, query_at - SEG, query_at)

    def rope_back(values, depth):
        at = segment(depth)
        return values * cosine[at, :] - swap_halves(values, low) * sine[at, :]

    def query(index, depth, count_big, big, extra):
        here = segment(role[index])
        queries = heads_apart(qr[segment(index), :], first)
        up = upstream[here, :]
        ups = heads_apart(up, first)
        turned = logsum[here, :].T
        log = jnp.concatenate([turned[0:1, :], turned[DH : DH + 1, :]], axis=1)
        product = (up.astype(F32) * attended[here, :].astype(F32)).T
        inner = jnp.concatenate(
            [
                jnp.sum(product[:DH], axis=0, keepdims=True),
                jnp.sum(product[DH:], axis=0, keepdims=True),
            ],
            axis=1,
        )
        dqt[...] = jnp.zeros_like(dqt)

        def add(keys, mask=None):
            weights = jnp.exp(nt(kr[keys, :], queries) - log)
            if mask is not None:
                weights = jnp.where(mask, weights, 0.0)
            back = (weights * (nt(vr[keys, :], ups) - inner)).astype(BF16)
            dv[keys, :] += nn(weights.astype(BF16), ups)
            dk[keys, :] += nn(back, queries)
            dqt[...] += nn(kt[:, keys], back)

        add(segment(index), causal)
        for other in extra:
            add(segment(other))

        def use(c, _):
            add(pl.ds(pl.multiple_of(c * big, big), big))
            return 0

        lax.fori_loop(0, count_big, use, 0)
        both = jnp.concatenate([dqt[:DH, :SEG], dqt[DH:, SEG:]], axis=0) * (DH**-0.5)
        out[here, 0:WIDE] = rope_back(both.T, depth).astype(BF16)

    def leaf(i, _):
        query(TRUNK + BRANCH + i, TRUNK + 1, TRUNK * SEG // KEYS, KEYS, [TRUNK + i // LEAVES])
        return 0

    def branch(i, _):
        query(TRUNK + i, TRUNK, TRUNK * SEG // KEYS, KEYS, [])
        return 0

    def trunk(i, _):
        query(i, i, i, SEG, [])
        return 0

    lax.fori_loop(0, BRANCH * LEAVES, leaf, 0)
    lax.fori_loop(0, BRANCH, branch, 0)
    lax.fori_loop(0, TRUNK, trunk, 0)

    def finish(i, _):
        here = segment(role[i])
        depth = jnp.where(i < TRUNK + BRANCH, jnp.minimum(i, TRUNK), TRUNK + 1)
        out[here, WIDE : 2 * WIDE] = rope_back(dk[segment(i), :], depth).astype(BF16)
        out[here, 2 * WIDE : 3 * WIDE] = dv[segment(i), :].astype(BF16)
        return 0

    lax.fori_loop(0, SEGS, finish, 0)


def attention_backward(parents, parts, upstream, attended, logsum, cosine, sine):
    tokens = SEGS * SEG
    vmem = pl.BlockSpec(memory_space=pltpu.VMEM)
    return pl.pallas_call(
        attention_back_kernel,
        out_shape=jax.ShapeDtypeStruct((tokens, 3 * WIDE), BF16),
        in_specs=[pl.BlockSpec(memory_space=pltpu.SMEM)] + [vmem] * 6,
        out_specs=vmem,
        scratch_shapes=[pltpu.VMEM((tokens, WIDE), BF16)] * 3
        + [pltpu.VMEM((WIDE, tokens), BF16)]
        + [pltpu.VMEM((tokens, WIDE), F32)] * 2
        + [
            pltpu.VMEM((WIDE, 2 * SEG), F32),
            pltpu.SMEM((SEGS * BRANCH,), jnp.int32),
            pltpu.SMEM((SEGS,), jnp.int32),
            pltpu.SMEM((SEGS,), jnp.int32),
        ],
        compiler_params=pltpu.CompilerParams(vmem_limit_bytes=VMEM_BYTES),
        cost_estimate=pl.CostEstimate(
            flops=152 * 2 * 10 * SEG * SEG * 128,
            bytes_accessed=tokens * WIDE * 24,
            transcendentals=152 * 2 * SEG * SEG,
        ),
        name="attention_backward",
    )(parents, parts.reshape(tokens, 3 * WIDE), upstream, attended, logsum, cosine, sine)


def angle_tables(positions):
    lane = jnp.arange(WIDE)
    freq = THETA ** (-(lane % (DH // 2)).astype(F32) * 2.0 / DH)
    angle = positions.astype(F32)[:, None] * freq[None, :]
    sign = jnp.where((lane % DH) < DH // 2, -1.0, 1.0)
    return jnp.cos(angle), jnp.sin(angle) * sign[None, :]


MESH = pl.DeviceIdType.MESH


def neighbours():
    x, core = lax.axis_index("x"), lax.axis_index("core")
    others = []
    for step in (1, 2, 3):
        to_x = lax.rem(x + step // 2, 2)
        to_core = lax.rem(core + step % 2, 2)
        others.append((2 * to_x + to_core, {"x": to_x, "core": to_core}))
    return 2 * x + core, others


def greet(tensor_peer, others):
    barrier = pltpu.get_barrier_semaphore()
    for target in [tensor_peer] + [where for _, where in others]:
        pl.semaphore_signal(barrier, inc=1, device_id=target, device_id_type=MESH)
    pl.semaphore_wait(barrier, 1 + len(others))


def enter_kernel(
    mine,
    gain,
    query_w,
    key_w,
    value_w,
    cosine,
    sine,
    parts,
    low_out,
    theirs,
    ready,
    swap_send,
    swap_recv,
    part_send,
    part_recv,
):
    me, others = neighbours()
    tensor_peer = {"tensor": 1 - lax.axis_index("tensor")}
    greet(tensor_peer, others)
    steps = mine.shape[0] // SEG

    def exchange(i):
        return pltpu.make_async_remote_copy(
            src_ref=mine.at[segment(i)],
            dst_ref=theirs.at[segment(i)],
            send_sem=swap_send.at[i],
            recv_sem=swap_recv.at[i],
            device_id=tensor_peer,
            device_id_type=MESH,
        )

    def scatter(i, at):
        place, where = others[at]
        return pltpu.make_async_remote_copy(
            src_ref=ready.at[place, segment(i)],
            dst_ref=parts.at[me, segment(i)],
            send_sem=part_send.at[i, at],
            recv_sem=part_recv.at[i, at],
            device_id=where,
            device_id_type=MESH,
        )

    for i in range(steps):
        exchange(i).start()
    low = (lax.broadcasted_iota(jnp.int32, (SEG, WIDE), 1) % DH) < (DH // 2)

    def step(i, _):
        here = segment(i)
        exchange(i).wait_recv()
        total = mine[here, :].astype(F32) + theirs[here, :].astype(F32)
        scale = lax.rsqrt(jnp.mean(total * total, axis=-1, keepdims=True) + EPSILON)
        rounded = (total * scale * gain[...]).astype(BF16)
        low_out[here, :] = rounded
        for at, weight in enumerate((query_w, key_w, value_w)):
            raw = nn(rounded, weight[...])
            for peer in range(ready.shape[0]):
                part = raw[:, peer * WIDE : (peer + 1) * WIDE]
                if at < 2:
                    part = part * cosine[here, :] + swap_halves(part, low) * sine[here, :]
                ready[peer, here, at * WIDE : (at + 1) * WIDE] = part.astype(BF16)
        for at in range(len(others)):
            scatter(i, at).start()
        parts[me, here, :] = ready[me, here, :]
        return 0

    lax.fori_loop(0, steps, step, 0)

    def finish(i, _):
        exchange(i).wait_send()
        for at in range(len(others)):
            scatter(i, at).wait()
        return 0

    lax.fori_loop(0, steps, finish, 0)


def enter(mine, gain, query_w, key_w, value_w, cosine, sine):
    rows, width = mine.shape
    inner = query_w.shape[1]
    peers = inner // WIDE
    steps = rows // SEG
    vmem = pl.BlockSpec(memory_space=pltpu.VMEM)
    return pl.pallas_call(
        enter_kernel,
        out_shape=(
            jax.ShapeDtypeStruct((peers, rows, 3 * WIDE), BF16),
            jax.ShapeDtypeStruct((rows, width), BF16),
            jax.ShapeDtypeStruct((rows, width), BF16),
        ),
        in_specs=[vmem] * 7,
        out_specs=(vmem,) * 3,
        scratch_shapes=[
            pltpu.VMEM((peers, rows, 3 * WIDE), BF16),
            pltpu.SemaphoreType.DMA((steps,)),
            pltpu.SemaphoreType.DMA((steps,)),
            pltpu.SemaphoreType.DMA((steps, 3)),
            pltpu.SemaphoreType.DMA((steps, 3)),
        ],
        compiler_params=pltpu.CompilerParams(
            vmem_limit_bytes=VMEM_BYTES, collective_id=0, has_side_effects=True
        ),
        cost_estimate=pl.CostEstimate(
            flops=2 * rows * width * 3 * inner,
            bytes_accessed=200 << 20,
            transcendentals=rows,
        ),
        name="enter",
    )(mine, gain, query_w, key_w, value_w, cosine, sine)


def middle_kernel(
    meta,
    adapted,
    heads,
    cotangent,
    second_gain,
    third_gain,
    fourth_gain,
    wo_own,
    wg_own,
    wu_own,
    wd_own,
    pair_all,
    stack_all,
    layer_out,
    middle_out,
    attended_out,
    attention_out,
    third_out,
    mixed_out,
    hidden_out,
    pair_out,
    heads_back,
    gains_out,
    wo,
    wg,
    wu,
    wd,
    gate_s,
    up_s,
    sums,
    sem,
):
    step = pl.program_id(0)
    tensor = meta[0]
    copies = []

    def copy(src, weight, row, lane):
        rows, lanes = src.shape
        dst = weight.at[pl.ds(row, rows), pl.ds(lane, lanes)]
        copies.append(pltpu.make_async_copy(src, dst, sem.at[len(copies)]))

    quarters = stack_all.shape[0] // 2
    first_other = (1 - tensor) * quarters
    inner, split = wo_own.shape[0], wg_own.shape[1]
    width = wg_own.shape[0]
    for weight, own, start in ((wo, wo_own, 0), (wd, wd_own, inner // quarters)):
        rows = own.shape[0]
        copy(own, weight, 0, 0)
        for i in range(quarters):
            piece = stack_all.at[first_other + i, pl.ds(start, rows // quarters)]
            copy(piece, weight, rows + i * (rows // quarters), 0)
    others = pl.ds(pl.multiple_of((1 - tensor) * width, width), width)
    for weight, own, lane in ((wg, wg_own, 0), (wu, wu_own, split)):
        copy(own, weight, 0, 0)
        copy(pair_all.at[others, pl.ds(lane, split)], weight, 0, split)

    @pl.when(step == 0)
    def _():
        for copy in copies:
            copy.start()
        gains_out[...] = jnp.zeros_like(gains_out)
        for copy in copies[: 1 + quarters]:
            copy.wait()

    groups = heads.shape[0] // 2
    for side in range(2):
        for group in range(groups):
            at = (side * groups + group) * WIDE
            source = group * 2 + (tensor if side == 0 else 1 - tensor)
            attended_out[:, at : at + WIDE] = heads[source]
    attention = nn(attended_out[...], wo[...])

    def scaling(values):
        return lax.rsqrt(jnp.mean(values * values, axis=-1, keepdims=True) + EPSILON)

    def inward(upstream, gain, normed, scale):
        scaled = upstream * gain
        return scale * (scaled - normed * jnp.mean(scaled * normed, axis=-1, keepdims=True))

    second_scale = scaling(attention)
    second_normed = attention * second_scale
    middle = adapted[...] + second_normed * second_gain[...]
    third_scale = scaling(middle)
    third_normed = middle * third_scale
    third_out[...] = (third_normed * third_gain[...]).astype(BF16)

    @pl.when(step == 0)
    def _():
        for copy in copies[1 + quarters :]:
            copy.wait()

    sums[...] = jnp.zeros_like(sums)

    def forward(c, _):
        cut = pl.ds(pl.multiple_of(c * HIDDEN, HIDDEN), HIDDEN)
        gate = nn(third_out[...], wg[:, cut])
        upward = nn(third_out[...], wu[:, cut])
        gate_s[c] = gate
        up_s[c] = upward
        hidden = (gate / (1.0 + jnp.exp(-gate)) * upward).astype(BF16)
        hidden_out[:, cut] = hidden
        sums[...] += nn(hidden, wd[cut, :])
        return 0

    lax.fori_loop(0, gate_s.shape[0], forward, 0)
    mixed = sums[...]
    fourth_scale = scaling(mixed)
    fourth_normed = mixed * fourth_scale
    layer_out[...] = (middle + fourth_normed * fourth_gain[...]).astype(BF16)
    upstream = cotangent[...].astype(F32)
    gains_out[2:3, :] += jnp.sum(upstream * fourth_normed, axis=0, keepdims=True)
    mixed_out[...] = inward(upstream, fourth_gain[...], fourth_normed, fourth_scale).astype(BF16)
    sums[...] = jnp.zeros_like(sums)
    side_units = wg_own.shape[1] // 128

    def backward(c, _):
        cut = pl.ds(pl.multiple_of(c * HIDDEN, HIDDEN), HIDDEN)
        back = nt(mixed_out[...], wd[cut, :]).astype(BF16).astype(F32)
        gate = gate_s[c]
        sigmoid = 1.0 / (1.0 + jnp.exp(-gate))
        silu = gate * sigmoid
        gate_back = (back * up_s[c] * (sigmoid + silu * (1.0 - sigmoid))).astype(BF16)
        up_back = (back * silu).astype(BF16)
        for piece in range(HIDDEN // 128):
            unit = c * (HIDDEN // 128) + piece
            unit = jnp.where(unit < side_units, unit, unit + side_units)
            lanes = slice(piece * 128, (piece + 1) * 128)
            pair_out[:, pl.ds(pl.multiple_of(unit * 128, 128), 128)] = gate_back[:, lanes]
            unit += side_units
            pair_out[:, pl.ds(pl.multiple_of(unit * 128, 128), 128)] = up_back[:, lanes]
        sums[...] += nt(gate_back, wg[:, cut]) + nt(up_back, wu[:, cut])
        return 0

    lax.fori_loop(0, gate_s.shape[0], backward, 0)
    third_back = sums[...]
    gains_out[1:2, :] += jnp.sum(third_back * third_normed, axis=0, keepdims=True)
    middle_back = upstream + inward(third_back, third_gain[...], third_normed, third_scale)
    middle_out[...] = middle_back
    gains_out[0:1, :] += jnp.sum(middle_back * second_normed, axis=0, keepdims=True)
    attention_out[...] = inward(
        middle_back, second_gain[...], second_normed, second_scale
    ).astype(BF16)
    heads_low = nt(attention_out[...], wo[...]).astype(BF16)
    for side in range(2):
        for group in range(groups):
            at = (side * groups + group) * WIDE
            target = group * 2 + (tensor if side == 0 else 1 - tensor)
            heads_back[target] = heads_low[:, at : at + WIDE]


def middle_section(meta, adapted, heads, cotangent, gains, weights):
    rows, width = adapted.shape
    sources = heads.shape[0]
    inner = sources * WIDE
    hidden = 2 * weights[1].shape[1]
    block = rows // 2
    steps = rows // block
    row = pl.BlockSpec((block, width), lambda i, meta: (i, 0))
    wide = pl.BlockSpec((block, hidden), lambda i, meta: (i, 0))
    head = pl.BlockSpec((sources, block, WIDE), lambda i, meta: (0, i, 0))
    gain = pl.BlockSpec((1, width), lambda i, meta: (0, 0))
    hbm = pl.BlockSpec(memory_space=pl.ANY)
    return pl.pallas_call(
        middle_kernel,
        grid_spec=pltpu.PrefetchScalarGridSpec(
            num_scalar_prefetch=1,
            grid=(steps,),
            in_specs=[
                row,
                head,
                pl.BlockSpec((block, width), lambda i, meta: (meta[0] * steps + i, 0)),
                gain,
                gain,
                gain,
            ]
            + [hbm] * 6,
            out_specs=(
                row,
                row,
                pl.BlockSpec((block, inner), lambda i, meta: (i, 0)),
                row,
                row,
                row,
                wide,
                pl.BlockSpec((block, 2 * hidden), lambda i, meta: (i, 0)),
                head,
                pl.BlockSpec((8, width), lambda i, meta: (0, 0)),
            ),
            scratch_shapes=[
                pltpu.VMEM((inner, width), BF16),
                pltpu.VMEM((width, hidden), BF16),
                pltpu.VMEM((width, hidden), BF16),
                pltpu.VMEM((hidden, width), BF16),
                pltpu.VMEM((hidden // HIDDEN, block, HIDDEN), F32),
                pltpu.VMEM((hidden // HIDDEN, block, HIDDEN), F32),
                pltpu.VMEM((block, width), F32),
                pltpu.SemaphoreType.DMA((14,)),
            ],
        ),
        out_shape=(
            jax.ShapeDtypeStruct((rows, width), BF16),
            jax.ShapeDtypeStruct((rows, width), F32),
            jax.ShapeDtypeStruct((rows, inner), BF16),
            jax.ShapeDtypeStruct((rows, width), BF16),
            jax.ShapeDtypeStruct((rows, width), BF16),
            jax.ShapeDtypeStruct((rows, width), BF16),
            jax.ShapeDtypeStruct((rows, hidden), BF16),
            jax.ShapeDtypeStruct((rows, 2 * hidden), BF16),
            jax.ShapeDtypeStruct((sources, rows, WIDE), BF16),
            jax.ShapeDtypeStruct((8, width), F32),
        ),
        compiler_params=pltpu.CompilerParams(vmem_limit_bytes=VMEM_BYTES),
        cost_estimate=pl.CostEstimate(
            flops=rows * width * (4 * inner + 12 * hidden),
            bytes_accessed=6 * width * hidden + 2 * width * inner + rows * (hidden * 6 + width * 20),
            transcendentals=rows * hidden * 2,
        ),
        name="middle_section",
    )(meta, adapted, heads, cotangent, *gains, *weights)


LEAVE = 128


def leave_kernel(
    sent,
    adapted,
    middle_back,
    gain,
    query_w,
    key_w,
    value_w,
    joined,
    adapted_low,
    gain_out,
    landed,
    away,
    away_landed,
    part_send,
    part_recv,
    away_send,
    away_recv,
    low_send,
    low_recv,
):
    me, others = neighbours()
    tensor = lax.axis_index("tensor")
    tensor_peer = {"tensor": 1 - tensor}
    greet(tensor_peer, others)
    half = adapted.shape[0]
    inner = query_w.shape[1]
    steps = half // LEAVE

    def block(start, i):
        return pl.ds(pl.multiple_of(start + i * LEAVE, LEAVE), LEAVE)

    def gather(side, i, at):
        here = block((tensor if side else 1 - tensor) * half, i)
        place, where = others[at]
        return pltpu.make_async_remote_copy(
            src_ref=sent.at[place, here],
            dst_ref=landed.at[me, here],
            send_sem=part_send.at[side, i, at],
            recv_sem=part_recv.at[side, i, at],
            device_id=where,
            device_id_type=MESH,
        )

    def hand_over(i):
        return pltpu.make_async_remote_copy(
            src_ref=away.at[block(0, i)],
            dst_ref=away_landed.at[block(0, i)],
            send_sem=away_send.at[i],
            recv_sem=away_recv.at[i],
            device_id=tensor_peer,
            device_id_type=MESH,
        )

    def share(i):
        here = block(tensor * half, i)
        return pltpu.make_async_remote_copy(
            src_ref=adapted_low.at[here],
            dst_ref=adapted_low.at[here],
            send_sem=low_send.at[i],
            recv_sem=low_recv.at[i],
            device_id=tensor_peer,
            device_id_type=MESH,
        )

    for side in range(2):

        def begin(i, _):
            for at in range(len(others)):
                gather(side, i, at).start()
            return 0

        lax.fori_loop(0, steps, begin, 0)
    landed[me] = sent[me]
    gain_out[...] = jnp.zeros_like(gain_out)

    def input_grad(side, i):
        for at in range(len(others)):
            gather(side, i, at).wait_recv()
        here = block((tensor if side else 1 - tensor) * half, i)
        for at in range(3):
            for group in range(landed.shape[0]):
                to = at * inner + group * WIDE
                joined[here, to : to + WIDE] = landed[group, here, at * WIDE : (at + 1) * WIDE]
        total = nt(joined[here, 0:inner], query_w[...])
        total += nt(joined[here, inner : 2 * inner], key_w[...])
        total += nt(joined[here, 2 * inner : 3 * inner], value_w[...])
        return total

    def away_step(i, _):
        away[block(0, i), :] = input_grad(0, i).astype(BF16)
        hand_over(i).start()
        return 0

    lax.fori_loop(0, steps, away_step, 0)

    def home_step(i, _):
        total = input_grad(1, i)
        hand_over(i).wait_recv()
        rows = block(0, i)
        upstream = total + away_landed[rows, :].astype(F32)
        values = adapted[rows, :]
        scale = lax.rsqrt(jnp.mean(values * values, axis=-1, keepdims=True) + EPSILON)
        normed = values * scale
        scaled = upstream * gain[...]
        inward = scale * (scaled - normed * jnp.mean(scaled * normed, axis=-1, keepdims=True))
        gain_out[0:1, :] += jnp.sum(upstream * normed, axis=0, keepdims=True)
        adapted_low[block(tensor * half, i), :] = (middle_back[rows, :] + inward).astype(BF16)
        share(i).start()
        return 0

    lax.fori_loop(0, steps, home_step, 0)

    def finish(i, _):
        for side in range(2):
            for at in range(len(others)):
                gather(side, i, at).wait_send()
        hand_over(i).wait_send()
        share(i).wait()
        return 0

    lax.fori_loop(0, steps, finish, 0)


def leave(sent, adapted, middle_back, gain, query_w, key_w, value_w):
    peers, rows, lanes = sent.shape
    half, width = adapted.shape
    inner = query_w.shape[1]
    steps = half // LEAVE
    vmem = pl.BlockSpec(memory_space=pltpu.VMEM)
    return pl.pallas_call(
        leave_kernel,
        out_shape=(
            jax.ShapeDtypeStruct((rows, 3 * inner), BF16),
            jax.ShapeDtypeStruct((rows, width), BF16),
            jax.ShapeDtypeStruct((8, width), F32),
        ),
        in_specs=[vmem] * 7,
        out_specs=(vmem,) * 3,
        scratch_shapes=[
            pltpu.VMEM((peers, rows, lanes), BF16),
            pltpu.VMEM((half, width), BF16),
            pltpu.VMEM((half, width), BF16),
            pltpu.SemaphoreType.DMA((2, steps, 3)),
            pltpu.SemaphoreType.DMA((2, steps, 3)),
        ]
        + [pltpu.SemaphoreType.DMA((steps,))] * 4,
        compiler_params=pltpu.CompilerParams(
            vmem_limit_bytes=VMEM_BYTES, collective_id=1, has_side_effects=True
        ),
        cost_estimate=pl.CostEstimate(
            flops=2 * rows * width * 3 * inner, bytes_accessed=200 << 20, transcendentals=rows
        ),
        name="leave",
    )(sent, adapted, middle_back, gain, query_w, key_w, value_w)


class Reduction:
    def __init__(self, shape, by_lane, halved):
        self.rows, self.lanes = shape
        self.by_lane = by_lane
        self.halved = halved

    def scratch(self, dp):
        rows, lanes = self.rows, self.lanes
        quarter = (rows // 4, lanes)
        chunk = (rows // 4, lanes // dp) if self.by_lane else (rows // 4 // dp, lanes)
        refs = [
            pltpu.VMEM(quarter, BF16),
            pltpu.VMEM(quarter, BF16),
            pltpu.VMEM((dp + 1,) + chunk, BF16),
            pltpu.VMEM(quarter, BF16),
            pltpu.VMEM((3,) + quarter, BF16),
            pltpu.VMEM(quarter, F32),
            pltpu.SemaphoreType.DMA((5,)),
            pltpu.SemaphoreType.DMA((5,)),
            pltpu.SemaphoreType.DMA((dp,)),
            pltpu.SemaphoreType.DMA((dp + 1,)),
            pltpu.SemaphoreType.DMA((2, dp)),
            pltpu.SemaphoreType.DMA((dp,)),
            pltpu.SemaphoreType.DMA((4,)),
        ]
        if not self.halved:
            refs += [pltpu.VMEM((rows // 2, lanes), BF16)] * 2
        return refs

    def bind(self, part, out, refs):
        self.part, self.out = part, out
        (
            self.x_land,
            self.quarter,
            self.z_land,
            self.whole,
            self.others,
            self.wide,
            self.send,
            self.recv,
            self.sum_send,
            self.sum_recv,
            self.all_send,
            self.all_recv,
            self.out_sem,
        ) = refs[:13]
        if self.halved:
            self.half = part
        else:
            self.half, self.core_land = refs[13:]
        self.x, self.core, self.z = (lax.axis_index(name) for name in ("x", "core", "dp"))
        self.dp = lax.axis_size("dp")
        self.to_core = {"core": 1 - self.core}
        self.to_x = {"x": 1 - self.x}
        self.sends = []

    def copy(self, src, dst, send, recv, where):
        return pltpu.make_async_remote_copy(
            src_ref=src,
            dst_ref=dst,
            send_sem=send,
            recv_sem=recv,
            device_id=where,
            device_id_type=MESH,
        )

    def part_of(self, ref, index, rows):
        return ref.at[pl.ds(pl.multiple_of(index * rows, rows), rows)]

    def chunk(self, ref, index):
        if self.by_lane:
            lanes = self.lanes // self.dp
            return ref.at[:, pl.ds(pl.multiple_of(index * lanes, lanes), lanes)]
        return self.part_of(ref, index, self.rows // 4 // self.dp)

    def core_sum(self):
        half = self.rows // 2
        return self.copy(
            self.part_of(self.part, 1 - self.core, half),
            self.core_land,
            self.send.at[0],
            self.recv.at[0],
            self.to_core,
        )

    def x_sum(self):
        quarter = self.rows // 4
        return self.copy(
            self.part_of(self.half, 1 - self.x, quarter),
            self.x_land,
            self.send.at[1],
            self.recv.at[1],
            self.to_x,
        )

    def z_sum(self, j, step):
        up = {"dp": self.z + step}
        index = j
        lands = index if step > 0 else jnp.where(self.z - 1 == index, self.dp, index)
        return self.copy(
            self.chunk(self.quarter, index),
            self.z_land.at[lands],
            self.sum_send.at[index],
            self.sum_recv.at[lands],
            up,
        )

    def z_all(self, j, step):
        return self.copy(
            self.chunk(self.whole, j),
            self.chunk(self.whole, j),
            self.all_send.at[0 if step > 0 else 1, j],
            self.all_recv.at[j],
            {"dp": self.z + step},
        )

    def spread(self, which):
        src = self.others.at[0] if which == 2 else self.whole
        return self.copy(
            src,
            self.others.at[which],
            self.send.at[2 + which],
            self.recv.at[2 + which],
            self.to_x if which == 0 else self.to_core,
        )

    def write(self, at, core, x, value):
        quarter = self.rows // 4
        row = pl.multiple_of((2 * core + x) * quarter, quarter)
        return pltpu.make_async_copy(
            self.wide, self.out.at[pl.ds(row, quarter)], self.out_sem.at[at]
        )

    def emit(self, at, core, x, ref):
        if at > 0:
            self.last_write.wait()
        self.wide[...] = ref[...].astype(F32)
        self.last_write = self.write(at, core, x, ref)
        self.last_write.start()

    def add(self, into, left, right):
        into[...] = (left[...].astype(F32) + right[...].astype(F32)).astype(BF16)

    def hop(self, h):
        last = self.dp - 1

        @pl.when(self.z == h)
        def _():
            for j in range(last, h, -1):
                if h > 0:
                    self.wait_sum(j)
                    self.add(self.chunk(self.quarter, j), self.chunk(self.quarter, j), self.z_land.at[j])
                self.z_sum(j, 1).start()

        @pl.when(self.z == last - h)
        def _():
            for j in range(0, last - h):
                if h > 0:
                    self.wait_sum(j)
                    self.add(self.chunk(self.quarter, j), self.chunk(self.quarter, j), self.z_land.at[j])
                self.z_sum(j, -1).start()

    def wait_sum(self, lands):
        self.copy(
            self.z_land.at[lands],
            self.z_land.at[lands],
            self.sum_send.at[0],
            self.sum_recv.at[lands],
            self.to_x,
        ).wait_recv()

    def all_hop(self, h):
        z, last = self.z, self.dp - 1
        low, high = jnp.maximum(z - h, 0), jnp.minimum(z + h, last)

        @pl.when(z >= h)
        def _():
            self.z_all(low, 1).wait_recv()

        @pl.when((z >= h) & (z < last))
        def _():
            self.z_all(low, 1).start()

        @pl.when(z <= last - h)
        def _():
            self.z_all(high, -1).wait_recv()

        @pl.when((z <= last - h) & (z > 0))
        def _():
            self.z_all(high, -1).start()

    def stages(self):
        def start():
            if self.halved:
                self.x_sum().start()
            else:
                self.core_sum().start()

        def fold_core():
            if not self.halved:
                self.core_sum().wait_recv()
                self.add(
                    self.half, self.part_of(self.part, self.core, self.rows // 2), self.core_land
                )
                self.x_sum().start()

        def fold_x():
            self.x_sum().wait_recv()
            self.add(
                self.quarter, self.part_of(self.half, self.x, self.rows // 4), self.x_land
            )
            self.hop(0)

        def settle():
            z, last = self.z, self.dp - 1
            mine = self.chunk(self.quarter, z)

            @pl.when(z > 0)
            def _():
                self.wait_sum(z)
                self.add(mine, mine, self.z_land.at[z])

            @pl.when(z < last)
            def _():
                self.wait_sum(self.dp)
                self.add(mine, mine, self.z_land.at[self.dp])

            self.chunk(self.whole, z)[...] = mine[...]

            @pl.when(z < last)
            def _():
                self.z_all(z, 1).start()

            @pl.when(z > 0)
            def _():
                self.z_all(z, -1).start()

        def share():
            self.all_hop(self.dp - 1)
            self.spread(0).start()
            self.spread(1).start()
            self.emit(0, self.core, self.x, self.whole)

        def pass_on():
            self.spread(0).wait_recv()
            self.spread(2).start()
            self.emit(1, self.core, 1 - self.x, self.others.at[0])

        def last():
            self.spread(1).wait_recv()
            self.emit(2, 1 - self.core, self.x, self.others.at[1])
            self.spread(2).wait_recv()
            self.emit(3, 1 - self.core, 1 - self.x, self.others.at[2])

        return (
            [start, fold_core, fold_x]
            + [functools.partial(self.hop, h) for h in range(1, self.dp - 1)]
            + [settle]
            + [functools.partial(self.all_hop, h) for h in range(1, self.dp - 1)]
            + [share, pass_on, last]
        )

    def drain(self):
        z, last = self.z, self.dp - 1
        if not self.halved:
            self.core_sum().wait_send()
        self.x_sum().wait_send()
        for j in range(self.dp):

            @pl.when(z < j)
            def _():
                self.z_sum(j, 1).wait_send()

            @pl.when(z > j)
            def _():
                self.z_sum(j, -1).wait_send()

            @pl.when((z >= j) & (z < last))
            def _():
                self.z_all(j, 1).wait_send()

            @pl.when((z <= j) & (z > 0))
            def _():
                self.z_all(j, -1).wait_send()

        for which in range(3):
            self.spread(which).wait_send()
        self.last_write.wait()


def reduce_kernel(items, *refs):
    count = len(items)
    parts, outs, rest = refs[:count], refs[count : 2 * count], refs[2 * count :]
    dp = lax.axis_size("dp")
    z = lax.axis_index("dp")
    for item, part, out in zip(items, parts, outs):
        size = len(item.scratch(dp))
        item.bind(part, out, rest[:size])
        rest = rest[size:]
    barrier = pltpu.get_barrier_semaphore()
    pl.semaphore_signal(barrier, inc=1, device_id=items[0].to_core, device_id_type=MESH)
    pl.semaphore_signal(barrier, inc=1, device_id=items[0].to_x, device_id_type=MESH)

    @pl.when(z > 0)
    def _():
        pl.semaphore_signal(barrier, inc=1, device_id={"dp": z - 1}, device_id_type=MESH)

    @pl.when(z < dp - 1)
    def _():
        pl.semaphore_signal(barrier, inc=1, device_id={"dp": z + 1}, device_id_type=MESH)

    pl.semaphore_wait(barrier, 2 + jnp.minimum(z, 1) + jnp.minimum(dp - 1 - z, 1))
    plans = [item.stages() for item in items]
    for time in range(len(plans[0]) + count - 1):
        for at, plan in enumerate(plans):
            if 0 <= time - at < len(plan):
                plan[time - at]()
    for item in items:
        item.drain()


def reduce_all(parts, kinds, name, number):
    dp = lax.axis_size("dp")
    items = []
    for part, (by_lane, halved) in zip(parts, kinds):
        rows, lanes = part.shape
        items.append(Reduction((2 * rows if halved else rows, lanes), by_lane, halved))
    scratch = []
    for item in items:
        scratch += item.scratch(dp)
    moved = sum(item.rows * item.lanes for item in items)
    return pl.pallas_call(
        functools.partial(reduce_kernel, items),
        out_shape=tuple(jax.ShapeDtypeStruct((item.rows, item.lanes), F32) for item in items),
        in_specs=[pl.BlockSpec(memory_space=pltpu.VMEM)] * len(items),
        out_specs=(pl.BlockSpec(memory_space=pl.ANY),) * len(items),
        scratch_shapes=scratch,
        compiler_params=pltpu.CompilerParams(
            vmem_limit_bytes=VMEM_BYTES, collective_id=number, has_side_effects=True
        ),
        cost_estimate=pl.CostEstimate(
            flops=moved * 4, bytes_accessed=moved * 30, transcendentals=0
        ),
        name=name,
    )(*parts)


def swap(value, axis):
    return lax.ppermute(value, axis, [(0, 1), (1, 0)])


def together(*values):
    return lax.optimization_barrier(values)


def cut(value, index, rows):
    return lax.dynamic_slice_in_dim(value, index * rows, rows, 0)


def add_low(left, right):
    return (left.astype(F32) + right.astype(F32)).astype(BF16)


def fold(value, index, axis):
    half = value.shape[0] // 2
    return add_low(cut(value, index, half), swap(cut(value, 1 - index, half), axis))


def unfold(value, index, axis):
    other = swap(value, axis)
    return jnp.concatenate(
        [jnp.where(index == 0, value, other), jnp.where(index == 0, other, value)], axis=0
    )


def sum_small(value):
    for axis in ("tensor", "core", "x"):
        value = value + swap(value, axis)
    for pairs in ([(0, 1), (1, 0), (2, 3), (3, 2)], [(0, 2), (2, 0), (1, 3), (3, 1)]):
        value = value + lax.ppermute(value, "dp", pairs)
    return value


def tn(left, right):
    return lax.dot_general(
        left, right, (((0,), (0,)), ((), ())), preferred_element_type=F32
    ).astype(BF16)


def on_device_paired(
    latent_embed,
    adapter,
    first_gain,
    query_weight,
    key_weight,
    value_weight,
    output_weight,
    second_gain,
    third_gain,
    gate_weight,
    up_weight,
    down_weight,
    fourth_gain,
    parents,
    positions,
    cotangent,
):
    rows = latent_embed.shape[0]
    width = adapter.shape[2]
    half_rows = rows // 2
    tensor = lax.axis_index("tensor")
    core = lax.axis_index("core")
    x = lax.axis_index("x")
    everyone = ("x", "core", "tensor")
    meta = jnp.stack([tensor, core]).astype(jnp.int32)
    one_row = lambda gain: gain.reshape(1, -1)

    cosine, sine = angle_tables(positions)
    mine = jnp.einsum(
        "rcd,cde->re", latent_embed, adapter, preferred_element_type=F32
    ).astype(BF16)
    parts, first_low, theirs = enter(
        mine, one_row(first_gain), query_weight, key_weight, value_weight, cosine, sine
    )
    adapted = cut(mine, tensor, half_rows).astype(F32) + cut(theirs, tensor, half_rows).astype(
        F32
    )
    quarter = 2 * x + core
    pair = jnp.concatenate(
        [cut(weight, quarter, width // 4) for weight in (gate_weight, up_weight)], axis=1
    )
    stack = jnp.concatenate(
        [cut(weight, quarter, weight.shape[0] // 4) for weight in (output_weight, down_weight)],
        axis=0,
    )
    pair, stack, parts = together(pair, stack, parts)
    pair_all = lax.all_gather(pair, ("tensor", "x", "core"), axis=0, tiled=True)
    stack_all = lax.all_gather(stack, ("tensor", "x", "core"), axis=0, tiled=False)

    attended, logsum = attention_forward(parents, parts)
    heads = lax.all_to_all(
        attended.reshape(8, half_rows, WIDE), everyone, 0, 0, tiled=False
    )
    (
        layer_half,
        middle_back,
        attended_all,
        attention_low,
        third_low,
        mixed_low,
        hidden,
        pair_low,
        heads_back,
        gain_parts,
    ) = middle_section(
        meta,
        adapted,
        heads,
        cotangent,
        (one_row(second_gain), one_row(third_gain), one_row(fourth_gain)),
        (output_weight, gate_weight, up_weight, down_weight, pair_all, stack_all),
    )
    upstream = lax.all_to_all(heads_back, everyone, 0, 0, tiled=False).reshape(-1, WIDE)
    layer_other = swap(layer_half, "tensor")
    layer_out = jnp.concatenate(
        [
            jnp.where(tensor == 0, layer_half, layer_other),
            jnp.where(tensor == 0, layer_other, layer_half),
        ],
        axis=0,
    ).astype(F32)

    split = gate_weight.shape[1]
    inner = output_weight.shape[0]
    sides = []
    for left, right, cut_at in (
        (third_low, pair_low, 2 * split),
        (hidden, mixed_low, split),
        (attended_all, attention_low, inner),
    ):
        for side in (slice(None, cut_at), slice(cut_at, None)):
            part = (
                tn(left, right[:, side]) if right is pair_low else tn(left[:, side], right)
            )
            sides.append(fold(part, core, "core"))
    upstream, *sides = together(upstream, *sides)
    away = [swap(side, "tensor") for side in sides[1::2]]

    table_cosine, table_sine = angle_tables(jnp.arange((TRUNK + 2) * SEG))
    sent = attention_backward(
        parents, parts, upstream, attended, logsum, table_cosine, table_sine
    )
    joined, adapted_low, first_gain_part = leave(
        sent.reshape(4, rows, 3 * WIDE),
        adapted,
        middle_back,
        one_row(first_gain),
        query_weight,
        key_weight,
        value_weight,
    )
    adapter_part = jnp.einsum(
        "rcd,re->cde", latent_embed, adapted_low, preferred_element_type=F32
    ).astype(BF16)
    kept = [add_low(own, theirs) for own, theirs in zip(sides[0::2], away)]
    pair_total, down_total, output_total, input_total, adapter_total = reduce_all(
        kept + [tn(first_low, joined), adapter_part.reshape(-1, width)],
        [(False, True), (True, True), (False, True), (False, False), (False, False)],
        "reduce_all",
        2,
    )
    latent_gradient = jnp.einsum("re,cde->rcd", adapted_low, adapter, preferred_element_type=F32)
    gains = sum_small(jnp.concatenate([gain_parts[:3], first_gain_part[:1]], axis=0))
    return (
        layer_out,
        latent_gradient,
        adapter_total.reshape(adapter.shape),
        gains[3],
        input_total[:, :inner],
        input_total[:, inner : 2 * inner],
        input_total[:, 2 * inner :],
        output_total,
        gains[0],
        gains[1],
        pair_total[:, :split],
        pair_total[:, split:],
        down_total,
        gains[2],
    )


def specs(rows):
    split = P(None, "tensor")
    in_specs = (
        P(rows, None, "tensor"),
        P(None, "tensor", None),
        P(),
        split,
        split,
        split,
        P("tensor", None),
        P(),
        P(),
        split,
        split,
        P("tensor", None),
        P(),
        P("dp", None),
        P(rows),
        P(rows, None),
    )
    out_specs = (
        P(rows, None),
        P(rows, None, "tensor"),
        P(None, "tensor", None),
        P(),
        split,
        split,
        split,
        P("tensor", None),
        P(),
        P(),
        split,
        split,
        P("tensor", None),
        P(),
    )
    return in_specs, out_specs


def solution(mesh):
    sizes = dict(mesh.shape)
    if sizes["seq"] == 4 and sizes["tensor"] == 2:
        fine = Mesh(
            mesh.devices.reshape(sizes["dp"], 2, 2, 2), ("dp", "x", "core", "tensor")
        )
        in_specs, out_specs = specs(("dp", "x", "core"))
        return jax.shard_map(
            on_device_paired, mesh=fine, in_specs=in_specs, out_specs=out_specs, check_vma=False
        )
    in_specs, out_specs = specs(("dp", "seq"))
    return jax.shard_map(
        on_device, mesh=mesh, in_specs=in_specs, out_specs=out_specs, check_vma=False
    )
```

```python
import functools

import jax
import jax.numpy as jnp
from jax import lax
from jax.experimental import pallas as pl
from jax.experimental.pallas import tpu as pltpu
from jax.sharding import Mesh
from jax.sharding import PartitionSpec as P

DH = 64
SEG = 256


EPSILON = 1e-06
THETA = 50000.0


def normalize(values, gain):
    scale = lax.rsqrt(jnp.mean(values * values, axis=-1, keepdims=True) + EPSILON)
    normed = values * scale
    return (normed * gain, normed, scale)


def normalize_back(upstream, gain, normed, scale):
    scaled = upstream * gain
    inward = scale * (scaled - normed * jnp.mean(scaled * normed, axis=-1, keepdims=True))
    return (inward, jnp.sum(upstream * normed, axis=0))


def angles(positions, width):
    half = width // 2
    freq = THETA ** (-jnp.arange(half, dtype=jnp.float32) * 2.0 / width)
    angle = positions.astype(jnp.float32)[:, None] * freq[None, :]
    return (jnp.cos(angle)[:, None, :], jnp.sin(angle)[:, None, :])


def rotate(values, cosine, sine, sign):
    half = values.shape[-1] // 2
    first = values[..., :half]
    second = values[..., half:]
    return jnp.concatenate(
        [first * cosine - sign * second * sine, second * cosine + sign * first * sine], axis=-1
    )


def ancestry(parent_row):
    labels = jnp.arange(parent_row.shape[0], dtype=jnp.int32)

    def extend(index, state):
        current, total = state
        total = total | (current[:, None] == labels[None, :])
        current = jnp.where(current >= 0, jnp.take(parent_row, jnp.maximum(current, 0)), -1)
        return (current, total)

    start = (parent_row, jnp.zeros((parent_row.shape[0], parent_row.shape[0]), jnp.bool_))
    current, total = lax.fori_loop(0, parent_row.shape[0], extend, start)
    return total


def path_mask(parent_row, query_ids, key_ids):
    table = ancestry(parent_row)
    query_seg = query_ids // SEG
    key_seg = key_ids // SEG
    far = jnp.take(jnp.take(table, query_seg, axis=0), key_seg, axis=1)
    near = (query_seg[:, None] == key_seg[None, :]) & (key_ids[None, :] <= query_ids[:, None])
    return far | near


def on_device(
    latent_embed,
    adapter,
    first_gain,
    query_weight,
    key_weight,
    value_weight,
    output_weight,
    second_gain,
    third_gain,
    gate_weight,
    up_weight,
    down_weight,
    fourth_gain,
    parents,
    positions,
    cotangent,
):
    rows = latent_embed.shape[0]
    local_heads = query_weight.shape[1] // DH
    scale = DH ** (-0.5)
    adapted = lax.psum(
        jnp.einsum("rcd,cde->re", latent_embed, adapter, preferred_element_type=jnp.float32),
        "tensor",
    )
    first_out, first_normed, first_scale = normalize(adapted, first_gain)
    first_low = first_out.astype(jnp.bfloat16)
    cosine, sine = angles(positions, DH)
    query_raw = jnp.dot(first_low, query_weight, preferred_element_type=jnp.float32).reshape(
        rows, local_heads, DH
    )
    queries = rotate(query_raw, cosine, sine, 1.0).astype(jnp.bfloat16)
    key_raw = jnp.dot(first_low, key_weight, preferred_element_type=jnp.float32).reshape(
        rows, local_heads, DH
    )
    keys_local = rotate(key_raw, cosine, sine, 1.0).astype(jnp.bfloat16)
    values_local = (
        jnp.dot(first_low, value_weight, preferred_element_type=jnp.float32)
        .astype(jnp.bfloat16)
        .reshape(rows, local_heads, DH)
    )
    keys_all, values_all = (
        lax.all_gather(keys_local, "seq", axis=0, tiled=True),
        lax.all_gather(values_local, "seq", axis=0, tiled=True),
    )
    tree_rows = keys_all.shape[0]
    query_ids = lax.axis_index("seq") * rows + jnp.arange(rows, dtype=jnp.int32)
    key_ids = jnp.arange(tree_rows, dtype=jnp.int32)
    allowed = path_mask(parents[0], query_ids, key_ids)[None]

    def score_block(keys):
        raw = jnp.einsum("qhd,khd->hqk", queries, keys, preferred_element_type=jnp.float32) * scale
        return jnp.where(allowed, raw, -1e30)

    scores = score_block(keys_all)
    top = jnp.max(scores, axis=-1, keepdims=True)
    weights = jnp.exp(scores - top)
    total = jnp.sum(weights, axis=-1, keepdims=True)
    probs = weights / total
    logsum = top + jnp.log(total)
    attended = jnp.einsum(
        "hqk,khd->qhd", probs.astype(jnp.bfloat16), values_all, preferred_element_type=jnp.float32
    )
    attended = attended.reshape(rows, local_heads * DH).astype(jnp.bfloat16)
    attention = lax.psum(
        jnp.dot(attended, output_weight, preferred_element_type=jnp.float32).astype(jnp.bfloat16),
        "tensor",
    ).astype(jnp.float32)
    second_out, second_normed, second_scale = normalize(attention, second_gain)
    middle = adapted + second_out
    third_out, third_normed, third_scale = normalize(middle, third_gain)
    third_low = third_out.astype(jnp.bfloat16)
    gate = jnp.dot(third_low, gate_weight, preferred_element_type=jnp.float32)
    upward = jnp.dot(third_low, up_weight, preferred_element_type=jnp.float32)
    hidden = (jax.nn.silu(gate) * upward).astype(jnp.bfloat16)
    mixed = lax.psum(
        jnp.dot(hidden, down_weight, preferred_element_type=jnp.float32).astype(jnp.bfloat16),
        "tensor",
    ).astype(jnp.float32)
    fourth_out, fourth_normed, fourth_scale = normalize(mixed, fourth_gain)
    layer_out = middle + fourth_out
    upstream = cotangent.astype(jnp.float32)
    mixed_back, fourth_gain_part = normalize_back(
        upstream, fourth_gain, fourth_normed, fourth_scale
    )
    mixed_low = mixed_back.astype(jnp.bfloat16)
    down_part = jnp.einsum("rf,rd->fd", hidden, mixed_low, preferred_element_type=jnp.float32)
    hidden_back = (
        jnp.einsum("rd,fd->rf", mixed_low, down_weight, preferred_element_type=jnp.float32)
        .astype(jnp.bfloat16)
        .astype(jnp.float32)
    )
    swiglu_value, product_back = jax.vjp(
        lambda left, right: jax.nn.silu(left) * right, gate, upward
    )
    gate_back, up_back = product_back(hidden_back)
    gate_low = gate_back.astype(jnp.bfloat16)
    up_low = up_back.astype(jnp.bfloat16)
    gate_part = jnp.einsum("rd,rf->df", third_low, gate_low, preferred_element_type=jnp.float32)
    up_part = jnp.einsum("rd,rf->df", third_low, up_low, preferred_element_type=jnp.float32)
    third_term = jnp.einsum(
        "rf,df->rd", gate_low, gate_weight, preferred_element_type=jnp.float32
    ) + jnp.einsum("rf,df->rd", up_low, up_weight, preferred_element_type=jnp.float32)
    third_back = lax.psum(third_term.astype(jnp.bfloat16), "tensor").astype(jnp.float32)
    middle_part, third_gain_part = normalize_back(third_back, third_gain, third_normed, third_scale)
    middle_back = upstream + middle_part
    attention_back, second_gain_part = normalize_back(
        middle_back, second_gain, second_normed, second_scale
    )
    attention_low = attention_back.astype(jnp.bfloat16)
    output_part = jnp.einsum(
        "re,rd->ed", attended, attention_low, preferred_element_type=jnp.float32
    )
    attended_back = (
        jnp.einsum("rd,ed->re", attention_low, output_weight, preferred_element_type=jnp.float32)
        .astype(jnp.bfloat16)
        .reshape(rows, local_heads, DH)
    )
    keys_back, values_back = (
        lax.all_gather(keys_local, "seq", axis=0, tiled=True),
        lax.all_gather(values_local, "seq", axis=0, tiled=True),
    )
    probs_back = jnp.exp(score_block(keys_back) - logsum)
    prob_grad = jnp.einsum(
        "qhd,khd->hqk", attended_back, values_back, preferred_element_type=jnp.float32
    )
    score_grad = (
        probs_back * (prob_grad - jnp.sum(prob_grad * probs_back, axis=-1, keepdims=True))
    ).astype(jnp.bfloat16)
    query_rot = (
        jnp.einsum("hqk,khd->qhd", score_grad, keys_back, preferred_element_type=jnp.float32)
        * scale
    )
    key_rot_all = (
        jnp.einsum("hqk,qhd->khd", score_grad, queries, preferred_element_type=jnp.float32) * scale
    )
    value_back_all = jnp.einsum(
        "hqk,qhd->khd",
        probs_back.astype(jnp.bfloat16),
        attended_back,
        preferred_element_type=jnp.float32,
    )
    key_rot, value_back = (
        lax.psum_scatter(
            key_rot_all.astype(jnp.bfloat16), "seq", scatter_dimension=0, tiled=True
        ).astype(jnp.float32),
        lax.psum_scatter(
            value_back_all.astype(jnp.bfloat16), "seq", scatter_dimension=0, tiled=True
        ).astype(jnp.float32),
    )
    query_low = (
        rotate(query_rot, cosine, sine, -1.0).astype(jnp.bfloat16).reshape(rows, local_heads * DH)
    )
    key_low = (
        rotate(key_rot, cosine, sine, -1.0).astype(jnp.bfloat16).reshape(rows, local_heads * DH)
    )
    value_low = value_back.astype(jnp.bfloat16).reshape(rows, local_heads * DH)
    query_part = jnp.einsum("rd,re->de", first_low, query_low, preferred_element_type=jnp.float32)
    key_part = jnp.einsum("rd,re->de", first_low, key_low, preferred_element_type=jnp.float32)
    value_part = jnp.einsum("rd,re->de", first_low, value_low, preferred_element_type=jnp.float32)
    first_term = jnp.einsum(
        "re,de->rd", query_low, query_weight, preferred_element_type=jnp.float32
    )
    first_term = first_term + jnp.einsum(
        "re,de->rd", key_low, key_weight, preferred_element_type=jnp.float32
    )
    first_term = first_term + jnp.einsum(
        "re,de->rd", value_low, value_weight, preferred_element_type=jnp.float32
    )
    first_back = lax.psum(first_term.astype(jnp.bfloat16), "tensor").astype(jnp.float32)
    adapted_part, first_gain_part = normalize_back(
        first_back, first_gain, first_normed, first_scale
    )
    adapted_low = (middle_back + adapted_part).astype(jnp.bfloat16)
    latent_gradient = jnp.einsum(
        "re,cde->rcd", adapted_low, adapter, preferred_element_type=jnp.float32
    )
    adapter_part = jnp.einsum(
        "rcd,re->cde", latent_embed, adapted_low, preferred_element_type=jnp.float32
    )
    summed = (
        lax.psum(gate_part.astype(jnp.bfloat16), ("dp", "seq")).astype(jnp.float32),
        lax.psum(up_part.astype(jnp.bfloat16), ("dp", "seq")).astype(jnp.float32),
        lax.psum(down_part.astype(jnp.bfloat16), ("dp", "seq")).astype(jnp.float32),
        lax.psum(third_gain_part.astype(jnp.bfloat16), ("dp", "seq")).astype(jnp.float32),
        lax.psum(fourth_gain_part.astype(jnp.bfloat16), ("dp", "seq")).astype(jnp.float32),
        lax.psum(query_part.astype(jnp.bfloat16), ("dp", "seq")).astype(jnp.float32),
        lax.psum(key_part.astype(jnp.bfloat16), ("dp", "seq")).astype(jnp.float32),
        lax.psum(value_part.astype(jnp.bfloat16), ("dp", "seq")).astype(jnp.float32),
        lax.psum(output_part.astype(jnp.bfloat16), ("dp", "seq")).astype(jnp.float32),
        lax.psum(first_gain_part.astype(jnp.bfloat16), ("dp", "seq")).astype(jnp.float32),
        lax.psum(second_gain_part.astype(jnp.bfloat16), ("dp", "seq")).astype(jnp.float32),
        lax.psum(adapter_part.astype(jnp.bfloat16), ("dp", "seq")).astype(jnp.float32),
    )
    gate_total, up_total, down_total, third_total, fourth_total = (
        summed[0],
        summed[1],
        summed[2],
        summed[3],
        summed[4],
    )
    query_total, key_total, value_total, output_total, first_total, second_total = (
        summed[5],
        summed[6],
        summed[7],
        summed[8],
        summed[9],
        summed[10],
    )
    adapter_total = summed[11]
    return (
        layer_out,
        latent_gradient,
        adapter_total,
        first_total,
        query_total,
        key_total,
        value_total,
        output_total,
        second_total,
        third_total,
        gate_total,
        up_total,
        down_total,
        fourth_total,
    )


TRUNK = 8
BRANCH = 4
LEAVES = 2
SEGS = TRUNK + BRANCH + BRANCH * LEAVES
WIDE = 2 * DH
NEG = -1e30
F32 = jnp.float32
BF16 = jnp.bfloat16
KEYS = 512
HIDDEN = 256
VMEM_BYTES = 60 << 20


def nt(left, right):
    return lax.dot_general(left, right, (((1,), (1,)), ((), ())), preferred_element_type=F32)


def nn(left, right):
    return lax.dot_general(left, right, (((1,), (0,)), ((), ())), preferred_element_type=F32)


def segment(index, size=SEG):
    return pl.ds(pl.multiple_of(index * SEG, SEG), size)


def find_roles(parents, child, count, role):
    for s in range(SEGS):
        count[s] = 0
    role[0] = 0
    for s in range(SEGS):
        parent = parents[0, s]

        @pl.when(parent < 0)
        def _():
            role[0] = s

        @pl.when(parent >= 0)
        def _():
            seen = count[parent]
            child[parent * BRANCH + seen] = s
            count[parent] = seen + 1

    for i in range(TRUNK - 1):
        role[i + 1] = child[role[i] * BRANCH]
    for b in range(BRANCH):
        role[TRUNK + b] = child[role[TRUNK - 1] * BRANCH + b]
    for b in range(BRANCH):
        for leaf in range(LEAVES):
            role[TRUNK + BRANCH + b * LEAVES + leaf] = child[role[TRUNK + b] * BRANCH + leaf]


def roles_kernel(parents, parts, role, place, out, child, count):
    find_roles(parents, child, count, role)
    for i in range(SEGS):
        place[role[i]] = i
    pick_segments(role, parts, out)


def pick_segments(order, source, out):
    for i in range(SEGS):
        out[segment(i), :] = source[segment(order[i]), :]


def sort_parts(parents, parts):
    smem = pl.BlockSpec(memory_space=pltpu.SMEM)
    vmem = pl.BlockSpec(memory_space=pltpu.VMEM)
    return pl.pallas_call(
        roles_kernel,
        out_shape=(jax.ShapeDtypeStruct((SEGS,), jnp.int32),) * 2
        + (jax.ShapeDtypeStruct(parts.shape, parts.dtype),),
        in_specs=[smem, vmem],
        out_specs=(smem, smem, vmem),
        scratch_shapes=[
            pltpu.SMEM((SEGS * BRANCH,), jnp.int32),
            pltpu.SMEM((SEGS,), jnp.int32),
        ],
        name="sort_parts",
    )(parents, parts)


def pick(order, source):
    smem = pl.BlockSpec(memory_space=pltpu.SMEM)
    vmem = pl.BlockSpec(memory_space=pltpu.VMEM)
    return pl.pallas_call(
        pick_segments,
        out_shape=jax.ShapeDtypeStruct(source.shape, source.dtype),
        in_specs=[smem, vmem],
        out_specs=vmem,
        name="pick",
    )(order, source)


def heads_apart(values, first):
    zero = jnp.zeros_like(values)
    return jnp.concatenate(
        [jnp.where(first, values, zero), jnp.where(first, zero, values)], axis=0
    )


MESH = pl.DeviceIdType.MESH


def at_step(index, plan):
    for step, calls in plan.items():

        @pl.when(index == step)
        def _(calls=calls):
            for call in calls:
                call()


class Fetch:
    def __init__(self, shape, pieces):
        self.rows, self.lanes = shape
        self.pieces = pieces

    def scratch(self):
        return [pltpu.SemaphoreType.DMA((4, self.pieces))] * 2

    def bind(self, own, out, refs):
        self.own, self.out = own, out
        self.send, self.recv = refs
        self.x, self.core = lax.axis_index("x"), lax.axis_index("core")
        self.to_core = {"core": 1 - self.core}
        self.to_x = {"x": 1 - self.x}
        self.to_tensor = {"tensor": 1 - lax.axis_index("tensor")}

    def copy(self, kind, piece):
        rows = self.rows // 4 // self.pieces
        x = 1 - self.x if kind == 3 else self.x
        row = (2 * x + self.core) * (self.rows // 4) + piece * rows
        here = pl.ds(pl.multiple_of(row, 16), rows)
        return pltpu.make_async_remote_copy(
            src_ref=(self.own if kind == 0 else self.out).at[here],
            dst_ref=self.out.at[here],
            send_sem=self.send.at[kind, piece],
            recv_sem=self.recv.at[kind, piece],
            device_id=(self.to_tensor, self.to_x, self.to_core, self.to_core)[kind],
            device_id_type=MESH,
        )

    def start(self):
        for piece in range(self.pieces):
            self.copy(0, piece).start()

    def second(self, piece):
        self.copy(0, piece).wait_recv()
        self.copy(1, piece).start()
        self.copy(2, piece).start()

    def third(self, piece):
        self.copy(1, piece).wait_recv()
        self.copy(3, piece).start()

    def drain(self):
        for piece in range(self.pieces):
            for kind in range(4):
                self.copy(kind, piece).wait_send()
            self.copy(2, piece).wait_recv()
            self.copy(3, piece).wait_recv()


def attention_kernel(fetches, *refs):
    parts = refs[0]
    count = len(fetches)
    own_weights, refs = refs[1 : 1 + count], refs[1 + count :]
    out, logsum, other_weights = refs[0], refs[1], refs[2 : 2 + count]
    qr, kr, v0, v1, kept, acc, top, total = refs[2 + count : 10 + count]
    sems = refs[10 + count :]
    for i, fetch in enumerate(fetches):
        fetch.bind(own_weights[i], other_weights[i], sems[2 * i : 2 * i + 2])
    output, gate, up, down = fetches
    barrier = pltpu.get_barrier_semaphore()
    for target in (gate.to_core, gate.to_x, gate.to_tensor):
        pl.semaphore_signal(barrier, inc=1, device_id=target, device_id_type=MESH)
    pl.semaphore_wait(barrier, 3)
    for fetch in fetches:
        fetch.start()
    call = functools.partial
    leaf_plan = {
        2: [call(output.second, 0)],
        4: [call(gate.second, 0), call(output.third, 0)],
        6: [call(gate.second, 1)],
        7: [call(gate.third, 0)],
    }
    branch_plan = {
        0: [call(up.second, 0)],
        1: [call(gate.third, 1)],
        2: [call(up.second, 1)],
        3: [call(up.third, 0)],
    }
    trunk_plan = {
        3: [call(down.second, 0), call(up.third, 1)],
        6: [call(down.second, 1)],
    }
    first = lax.broadcasted_iota(jnp.int32, (SEG, WIDE), 1) < DH

    def sort(i, _):
        here = source = segment(i)
        qr[here, :] = parts[source, 0:WIDE] * jnp.asarray(DH**-0.5, BF16)
        kr[here, :] = parts[source, WIDE : 2 * WIDE]
        value = parts[source, 2 * WIDE : 3 * WIDE]
        zero = jnp.zeros_like(value)
        v0[here, :] = jnp.where(first, value, zero)
        v1[here, :] = jnp.where(first, zero, value)
        return 0

    lax.fori_loop(0, SEGS, sort, 0)
    row = lax.broadcasted_iota(jnp.int32, (2 * SEG, SEG), 0)
    col = lax.broadcasted_iota(jnp.int32, (2 * SEG, SEG), 1)
    causal = col <= jnp.where(row >= SEG, row - SEG, row)

    def fold(values, op):
        result = values[:, 0:128]
        for at in range(128, values.shape[1], 128):
            result = op(result, values[:, at : at + 128])
        return result

    def query(index, count_big, big, extra):
        queries = heads_apart(qr[segment(index), :], first)
        own = jnp.where(causal, nt(queries, kr[segment(index), :]), NEG)
        top[...] = fold(own, jnp.maximum)
        others = []
        for other in extra:
            scores = nt(queries, kr[segment(other), :])
            top[...] = jnp.maximum(top[...], fold(scores, jnp.maximum))
            others.append(scores)

        def find(c, _):
            scores = nt(queries, kr[pl.ds(pl.multiple_of(c * big, big), big), :])
            kept[c, :, 0:big] = scores
            top[...] = jnp.maximum(top[...], fold(scores, jnp.maximum))
            return 0

        lax.fori_loop(0, count_big, find, 0)
        most = jnp.max(top[...], axis=1, keepdims=True)

        def add(scores, keys, fresh=False):
            weights = jnp.exp(scores - most)
            summed = fold(weights, jnp.add)
            low = weights.astype(BF16)
            product = nn(low[:SEG], v0[keys, :]) + nn(low[SEG:], v1[keys, :])
            total[...] = summed if fresh else total[...] + summed
            acc[...] = product if fresh else acc[...] + product

        add(own, segment(index), True)
        for other, scores in zip(extra, others):
            add(scores, segment(other))

        def use(c, _):
            add(kept[c, :, 0:big], pl.ds(pl.multiple_of(c * big, big), big))
            return 0

        lax.fori_loop(0, count_big, use, 0)
        whole = jnp.sum(total[...], axis=1, keepdims=True)
        inverse = 1.0 / whole
        log = most + jnp.log(whole)
        here = segment(index)
        out[here, :] = (acc[...] * jnp.where(first, inverse[:SEG], inverse[SEG:])).astype(BF16)
        logsum[here, :] = jnp.where(first, log[:SEG], log[SEG:])

    def trunk(i, _):
        at_step(i, trunk_plan)
        query(i, i, SEG, [])
        return 0

    def branch(i, _):
        at_step(i, branch_plan)
        query(TRUNK + i, TRUNK * SEG // KEYS, KEYS, [])
        return 0

    def leaf(i, _):
        at_step(i, leaf_plan)
        query(TRUNK + BRANCH + i, TRUNK * SEG // KEYS, KEYS, [TRUNK + i // LEAVES])
        return 0

    lax.fori_loop(0, BRANCH * LEAVES, leaf, 0)
    lax.fori_loop(0, BRANCH, branch, 0)
    lax.fori_loop(0, TRUNK, trunk, 0)
    down.third(0)

    down.third(1)
    for fetch in fetches:
        fetch.drain()


def attention_forward(parts, weights):
    fetches = [Fetch(weight.shape, 1 if i == 0 else 2) for i, weight in enumerate(weights)]
    sems = []
    for fetch in fetches:
        sems += fetch.scratch()
    hbm = pl.BlockSpec(memory_space=pl.ANY)
    tokens = SEGS * SEG
    vmem = pl.BlockSpec(memory_space=pltpu.VMEM)
    return pl.pallas_call(
        functools.partial(attention_kernel, fetches),
        out_shape=(
            jax.ShapeDtypeStruct((tokens, WIDE), BF16),
            jax.ShapeDtypeStruct((tokens, WIDE), F32),
        )
        + tuple(jax.ShapeDtypeStruct(weight.shape, BF16) for weight in weights),
        in_specs=[vmem] + [hbm] * len(weights),
        out_specs=(vmem, vmem) + (hbm,) * len(weights),
        scratch_shapes=[pltpu.VMEM((tokens, WIDE), BF16)] * 4
        + [
            pltpu.VMEM((TRUNK, 2 * SEG, KEYS), F32),
            pltpu.VMEM((SEG, WIDE), F32),
            pltpu.VMEM((2 * SEG, 128), F32),
            pltpu.VMEM((2 * SEG, 128), F32),
        ]
        + sems,
        compiler_params=pltpu.CompilerParams(
            vmem_limit_bytes=VMEM_BYTES, collective_id=4, has_side_effects=True
        ),
        cost_estimate=pl.CostEstimate(
            flops=152 * 2 * 4 * SEG * SEG * 128,
            bytes_accessed=tokens * WIDE * 12,
            transcendentals=152 * 2 * SEG * SEG,
        ),
        name="attention_forward",
    )(parts, *weights)


def add_rows(dst, dst_row, left, left_row, right, right_row, rows, step=32):
    def one(i, _):
        at = i * step
        total = left[pl.ds(pl.multiple_of(left_row + at, step), step), :].astype(F32)
        total += right[pl.ds(pl.multiple_of(right_row + at, step), step), :].astype(F32)
        dst[pl.ds(pl.multiple_of(dst_row + at, step), step), :] = total.astype(BF16)
        return 0

    lax.fori_loop(0, rows // step, one, 0)


class PairFold:
    def __init__(self, shape, x_first, pieces=1):
        self.rows, self.lanes = shape
        self.x_first = x_first
        self.pieces = pieces if x_first else 2

    def scratch(self):
        half, quarter = (self.rows // 2, self.lanes), (self.rows // 4, self.lanes)
        return (
            [pltpu.VMEM(half, BF16)] * 4
            + [pltpu.VMEM(quarter, BF16)] * (2 if self.x_first else 1)
            + [pltpu.VMEM(quarter if self.x_first else half, BF16)]
            + [pltpu.SemaphoreType.DMA((2,))] * 3
            + [pltpu.SemaphoreType.DMA((2, self.pieces))] * 2
            + [pltpu.SemaphoreType.DMA((self.pieces,))] * 2
        )

    def bind(self, parts, out, refs):
        self.parts, self.out = parts, out
        self.keep, self.land = refs[0:2], refs[2:4]
        count = 2 if self.x_first else 1
        self.x_land = refs[4 : 4 + count]
        (
            self.y_land,
            self.local,
            self.core_send,
            self.core_recv,
            self.x_send,
            self.x_recv,
            self.y_send,
            self.y_recv,
        ) = refs[4 + count :]
        self.x, self.core = lax.axis_index("x"), lax.axis_index("core")
        self.to_core = {"core": 1 - self.core}
        self.to_x = {"x": 1 - self.x}
        self.to_tensor = {"tensor": 1 - lax.axis_index("tensor")}
        self.half, self.quarter = self.rows // 2, self.rows // 4

    def rows_at(self, ref, row, rows):
        return ref.at[pl.ds(pl.multiple_of(row, 32), rows)]

    def remote(self, src, dst, send, recv, where):
        return pltpu.make_async_remote_copy(
            src_ref=src,
            dst_ref=dst,
            send_sem=send,
            recv_sem=recv,
            device_id=where,
            device_id_type=MESH,
        )

    def over_core(self, side):
        return self.remote(
            self.rows_at(self.parts[side], (1 - self.core) * self.half, self.half),
            self.land[side],
            self.core_send.at[side],
            self.core_recv.at[side],
            self.to_core,
        )

    def kept(self, side):
        return pltpu.make_async_copy(
            self.rows_at(self.parts[side], self.core * self.half, self.half),
            self.keep[side],
            self.local.at[side],
        )

    def over_x(self, side, piece):
        rows = self.quarter // self.pieces if self.x_first else self.quarter
        start = piece * rows if self.x_first else 0
        return self.remote(
            self.rows_at(self.keep[side], (1 - self.x) * self.quarter + start, rows),
            self.rows_at(self.x_land[side], start, rows),
            self.x_send.at[side, piece],
            self.x_recv.at[side, piece],
            self.to_x,
        )

    def over_tensor(self, piece):
        if self.x_first:
            rows = self.quarter // self.pieces
            source, target = self.x * self.quarter + piece * rows, piece * rows
        else:
            rows = self.quarter
            source = (1 - self.x if piece == 0 else self.x) * rows
            target = source
        return self.remote(
            self.rows_at(self.keep[1], source, rows),
            self.rows_at(self.y_land, target, rows),
            self.y_send.at[piece],
            self.y_recv.at[piece],
            self.to_tensor,
        )

    def start(self):
        for side in range(2):
            self.over_core(side).start()
            self.kept(side).start()

    def fold_core(self):
        for side in (1, 0):
            self.kept(side).wait()
            self.over_core(side).wait_recv()
            add_rows(self.keep[side], 0, self.keep[side], 0, self.land[side], 0, self.half)
        for piece in range(self.pieces):
            if self.x_first:
                self.over_x(1, piece).start()
                self.over_x(0, piece).start()
            else:
                self.over_tensor(piece).start()

    def second(self, piece):
        if self.x_first:
            rows = self.quarter // self.pieces
            at = self.x * self.quarter + piece * rows
            for side in (1, 0):
                self.over_x(side, piece).wait_recv()
                keep, land = self.keep[side], self.x_land[side]
                add_rows(keep, at, keep, at, land, piece * rows, rows)
                if side == 1:
                    self.over_tensor(piece).start()
        else:
            at = (1 - self.x if piece == 0 else self.x) * self.quarter
            self.over_tensor(piece).wait_recv()
            add_rows(self.keep[0], at, self.keep[0], at, self.y_land, at, self.quarter)
            if piece == 0:
                self.over_x(0, 0).start()

    def third(self, piece):
        if self.x_first:
            rows = self.quarter // self.pieces
            self.over_tensor(piece).wait_recv()
            at = self.x * self.quarter + piece * rows
            add_rows(self.out, piece * rows, self.keep[0], at, self.y_land, piece * rows, rows)
        elif piece == 0:
            self.over_x(0, 0).wait_recv()
            at = self.x * self.quarter
            add_rows(self.out, 0, self.keep[0], at, self.x_land[0], 0, self.quarter)

    def drain(self):
        for side in range(2):
            self.over_core(side).wait_send()
        for piece in range(self.pieces):
            if self.x_first:
                self.over_x(0, piece).wait_send()
                self.over_x(1, piece).wait_send()
            self.over_tensor(piece).wait_send()
        if not self.x_first:
            self.over_x(0, 0).wait_send()


def swap_halves(values, low):
    return jnp.where(
        low, pltpu.roll(values, WIDE - DH // 2, 1), pltpu.roll(values, DH // 2, 1)
    )


def attention_back_kernel(folds, *refs):
    parts, upstream, attended, logsum, cosine, sine = refs[:6]
    sides, refs = refs[6 : 6 + 2 * len(folds)], refs[6 + 2 * len(folds) :]
    out, sums, refs = refs[0], refs[1 : 1 + len(folds)], refs[1 + len(folds) :]
    qr, kr, vr, kt, dk, dv, dqt = refs[:7]
    refs = refs[7:]
    for i, fold in enumerate(folds):
        size = len(fold.scratch())
        fold.bind(sides[2 * i : 2 * i + 2], sums[i], refs[:size])
        refs = refs[size:]
    gate, down, up, output = folds
    barrier = pltpu.get_barrier_semaphore()
    for target in (gate.to_core, gate.to_x, gate.to_tensor):
        pl.semaphore_signal(barrier, inc=1, device_id=target, device_id_type=MESH)
    pl.semaphore_wait(barrier, 3)
    for fold in folds:
        fold.start()
    call = functools.partial
    leaf_plan = {
        2: [gate.fold_core, up.fold_core],
        3: [down.fold_core, output.fold_core],
    }
    branch_plan = {3: [call(gate.second, 0), call(up.second, 0), call(output.second, 0)]}
    trunk_plan = {5: [call(up.second, 1), call(output.second, 1)]}
    lane = lax.broadcasted_iota(jnp.int32, (SEG, WIDE), 1)
    first = lane < DH
    low = (lane % DH) < (DH // 2)

    def sort(i, _):
        here = source = segment(i)
        qr[here, :] = parts[source, 0:WIDE] * jnp.asarray(DH**-0.5, BF16)
        key = parts[source, WIDE : 2 * WIDE]
        kr[here, :] = key
        kt[:, here] = key.T
        vr[here, :] = parts[source, 2 * WIDE : 3 * WIDE]
        return 0

    lax.fori_loop(0, SEGS, sort, 0)
    dk[...] = jnp.zeros_like(dk)
    dv[...] = jnp.zeros_like(dv)
    key_at = lax.broadcasted_iota(jnp.int32, (SEG, 2 * SEG), 0)
    query_at = lax.broadcasted_iota(jnp.int32, (SEG, 2 * SEG), 1)
    causal = key_at <= jnp.where(query_at >= SEG, query_at - SEG, query_at)

    def rope_back(values, depth):
        at = segment(depth)
        return values * cosine[at, :] - swap_halves(values, low) * sine[at, :]

    def query(index, depth, count_big, big, extra):
        here = segment(index)
        queries = heads_apart(qr[segment(index), :], first)
        up = upstream[here, :]
        ups = heads_apart(up, first)
        turned = logsum[segment(index), :].T
        log = jnp.concatenate([turned[0:1, :], turned[DH : DH + 1, :]], axis=1)
        product = (up.astype(F32) * attended[here, :].astype(F32)).T
        inner = jnp.concatenate(
            [
                jnp.sum(product[:DH], axis=0, keepdims=True),
                jnp.sum(product[DH:], axis=0, keepdims=True),
            ],
            axis=1,
        )
        dqt[...] = jnp.zeros_like(dqt)

        def add(keys, mask=None):
            weights = jnp.exp(nt(kr[keys, :], queries) - log)
            if mask is not None:
                weights = jnp.where(mask, weights, 0.0)
            back = (weights * (nt(vr[keys, :], ups) - inner)).astype(BF16)
            dv[keys, :] += nn(weights.astype(BF16), ups)
            dk[keys, :] += nn(back, queries)
            dqt[...] += nn(kt[:, keys], back)

        add(segment(index), causal)
        for other in extra:
            add(segment(other))

        def use(c, _):
            add(pl.ds(pl.multiple_of(c * big, big), big))
            return 0

        lax.fori_loop(0, count_big, use, 0)
        both = jnp.concatenate([dqt[:DH, :SEG], dqt[DH:, SEG:]], axis=0) * (DH**-0.5)
        out[here, 0:WIDE] = rope_back(both.T, depth).astype(BF16)

    def leaf(i, _):
        at_step(i, leaf_plan)
        query(TRUNK + BRANCH + i, TRUNK + 1, TRUNK * SEG // KEYS, KEYS, [TRUNK + i // LEAVES])
        return 0

    def branch(i, _):
        at_step(i, branch_plan)
        query(TRUNK + i, TRUNK, TRUNK * SEG // KEYS, KEYS, [])
        return 0

    def trunk(i, _):
        at_step(i, trunk_plan)
        query(i, i, i, SEG, [])
        return 0

    lax.fori_loop(0, BRANCH * LEAVES, leaf, 0)
    lax.fori_loop(0, BRANCH, branch, 0)
    lax.fori_loop(0, TRUNK, trunk, 0)

    down.second(0)

    def settle(i, _):
        here = segment(i)
        depth = jnp.where(i < TRUNK + BRANCH, jnp.minimum(i, TRUNK), TRUNK + 1)
        out[here, WIDE : 2 * WIDE] = rope_back(dk[here, :], depth).astype(BF16)
        out[here, 2 * WIDE : 3 * WIDE] = dv[here, :].astype(BF16)
        return 0

    lax.fori_loop(0, SEGS, settle, 0)
    for fold in (gate, up, output, down):
        fold.third(0)
    for fold in folds:
        fold.drain()


def attention_backward(parts, upstream, attended, logsum, cosine, sine, sides):
    tokens = SEGS * SEG
    vmem = pl.BlockSpec(memory_space=pltpu.VMEM)
    folds = [PairFold(own.shape, i < 2) for i, own in enumerate(sides[::2])]
    scratch = []
    for fold in folds:
        scratch += fold.scratch()
    return pl.pallas_call(
        functools.partial(attention_back_kernel, folds),
        out_shape=(jax.ShapeDtypeStruct((tokens, 3 * WIDE), BF16),)
        + tuple(jax.ShapeDtypeStruct((fold.rows // 4, fold.lanes), BF16) for fold in folds),
        in_specs=[vmem] * 6 + [pl.BlockSpec(memory_space=pl.ANY)] * len(sides),
        out_specs=(vmem,) * (1 + len(folds)),
        scratch_shapes=[pltpu.VMEM((tokens, WIDE), BF16)] * 3
        + [pltpu.VMEM((WIDE, tokens), BF16)]
        + [pltpu.VMEM((tokens, WIDE), F32)] * 2
        + [pltpu.VMEM((WIDE, 2 * SEG), F32)]
        + scratch,
        compiler_params=pltpu.CompilerParams(
            vmem_limit_bytes=VMEM_BYTES, collective_id=3, has_side_effects=True
        ),
        cost_estimate=pl.CostEstimate(
            flops=152 * 2 * 10 * SEG * SEG * 128,
            bytes_accessed=tokens * WIDE * 24,
            transcendentals=152 * 2 * SEG * SEG,
        ),
        name="attention_backward",
    )(
        parts,
        upstream,
        attended,
        logsum,
        cosine,
        sine,
        *sides,
    )


def angle_tables(positions):
    lane = jnp.arange(WIDE)
    freq = THETA ** (-(lane % (DH // 2)).astype(F32) * 2.0 / DH)
    angle = positions.astype(F32)[:, None] * freq[None, :]
    sign = jnp.where((lane % DH) < DH // 2, -1.0, 1.0)
    return jnp.cos(angle), jnp.sin(angle) * sign[None, :]


def neighbours():
    x, core = lax.axis_index("x"), lax.axis_index("core")
    others = []
    for step in (1, 2, 3):
        to_x = lax.rem(x + step // 2, 2)
        to_core = lax.rem(core + step % 2, 2)
        others.append((2 * to_x + to_core, {"x": to_x, "core": to_core}))
    return 2 * x + core, others


def greet(tensor_peer, others):
    barrier = pltpu.get_barrier_semaphore()
    for target in [tensor_peer] + [where for _, where in others]:
        pl.semaphore_signal(barrier, inc=1, device_id=target, device_id_type=MESH)
    pl.semaphore_wait(barrier, 1 + len(others))


def enter_kernel(
    mine,
    gain,
    query_w,
    key_w,
    value_w,
    cosine,
    sine,
    parts,
    low_out,
    theirs,
    ready,
    swap_send,
    swap_recv,
    part_send,
    part_recv,
):
    me, others = neighbours()
    tensor_peer = {"tensor": 1 - lax.axis_index("tensor")}
    greet(tensor_peer, others)
    steps = mine.shape[0] // SEG

    def exchange(i):
        return pltpu.make_async_remote_copy(
            src_ref=mine.at[segment(i)],
            dst_ref=theirs.at[segment(i)],
            send_sem=swap_send.at[i],
            recv_sem=swap_recv.at[i],
            device_id=tensor_peer,
            device_id_type=MESH,
        )

    def scatter(i, at):
        place, where = others[at]
        return pltpu.make_async_remote_copy(
            src_ref=ready.at[place, segment(i)],
            dst_ref=parts.at[me, segment(i)],
            send_sem=part_send.at[i, at],
            recv_sem=part_recv.at[i, at],
            device_id=where,
            device_id_type=MESH,
        )

    for i in range(steps):
        exchange(i).start()
    low = (lax.broadcasted_iota(jnp.int32, (SEG, WIDE), 1) % DH) < (DH // 2)

    def step(i, _):
        here = segment(i)
        exchange(i).wait_recv()
        total = mine[here, :].astype(F32) + theirs[here, :].astype(F32)
        scale = lax.rsqrt(jnp.mean(total * total, axis=-1, keepdims=True) + EPSILON)
        rounded = (total * scale * gain[...]).astype(BF16)
        low_out[here, :] = rounded
        for at, weight in enumerate((query_w, key_w, value_w)):
            raw = nn(rounded, weight[...])
            for peer in range(ready.shape[0]):
                part = raw[:, peer * WIDE : (peer + 1) * WIDE]
                if at < 2:
                    part = part * cosine[here, :] + swap_halves(part, low) * sine[here, :]
                ready[peer, here, at * WIDE : (at + 1) * WIDE] = part.astype(BF16)
        for at in range(len(others)):
            scatter(i, at).start()
        parts[me, here, :] = ready[me, here, :]
        return 0

    lax.fori_loop(0, steps, step, 0)

    def finish(i, _):
        exchange(i).wait_send()
        for at in range(len(others)):
            scatter(i, at).wait()
        return 0

    lax.fori_loop(0, steps, finish, 0)


def enter(mine, gain, query_w, key_w, value_w, cosine, sine):
    rows, width = mine.shape
    inner = query_w.shape[1]
    peers = inner // WIDE
    steps = rows // SEG
    vmem = pl.BlockSpec(memory_space=pltpu.VMEM)
    return pl.pallas_call(
        enter_kernel,
        out_shape=(
            jax.ShapeDtypeStruct((peers, rows, 3 * WIDE), BF16),
            jax.ShapeDtypeStruct((rows, width), BF16),
            jax.ShapeDtypeStruct((rows, width), BF16),
        ),
        in_specs=[vmem] * 7,
        out_specs=(vmem,) * 3,
        scratch_shapes=[
            pltpu.VMEM((peers, rows, 3 * WIDE), BF16),
            pltpu.SemaphoreType.DMA((steps,)),
            pltpu.SemaphoreType.DMA((steps,)),
            pltpu.SemaphoreType.DMA((steps, 3)),
            pltpu.SemaphoreType.DMA((steps, 3)),
        ],
        compiler_params=pltpu.CompilerParams(
            vmem_limit_bytes=VMEM_BYTES, collective_id=0, has_side_effects=True
        ),
        cost_estimate=pl.CostEstimate(
            flops=2 * rows * width * 3 * inner,
            bytes_accessed=200 << 20,
            transcendentals=rows,
        ),
        name="enter",
    )(mine, gain, query_w, key_w, value_w, cosine, sine)


def middle_kernel(
    meta,
    adapted,
    heads,
    cotangent,
    second_gain,
    third_gain,
    fourth_gain,
    wo_own,
    wg_own,
    wu_own,
    wd_own,
    wo_other,
    wg_other,
    wu_other,
    wd_other,
    layer_out,
    middle_out,
    attended_out,
    attention_out,
    third_out,
    mixed_out,
    hidden_out,
    pair_out,
    heads_back,
    gains_out,
    wo,
    wg,
    wu,
    wd,
    gate_s,
    up_s,
    sums,
    sem,
):
    step = pl.program_id(0)
    tensor = meta[0]
    copies = []

    def copy(src, weight, row, lane):
        rows, lanes = src.shape
        dst = weight.at[pl.ds(row, rows), pl.ds(lane, lanes)]
        copies.append(pltpu.make_async_copy(src, dst, sem.at[len(copies)]))

    for weight, own, other, by_lane in (
        (wo, wo_own, wo_other, False),
        (wg, wg_own, wg_other, True),
        (wu, wu_own, wu_other, True),
        (wd, wd_own, wd_other, False),
    ):
        rows, lanes = own.shape
        copy(own, weight, 0, 0)
        copy(other, weight, 0 if by_lane else rows, lanes if by_lane else 0)

    @pl.when(step == 0)
    def _():
        for copy in copies:
            copy.start()
        gains_out[...] = jnp.zeros_like(gains_out)
        for copy in copies[:2]:
            copy.wait()

    groups = heads.shape[0] // 2
    for side in range(2):
        for group in range(groups):
            at = (side * groups + group) * WIDE
            source = group * 2 + (tensor if side == 0 else 1 - tensor)
            attended_out[:, at : at + WIDE] = heads[source]
    attention = nn(attended_out[...], wo[...])

    def scaling(values):
        return lax.rsqrt(jnp.mean(values * values, axis=-1, keepdims=True) + EPSILON)

    def inward(upstream, gain, normed, scale):
        scaled = upstream * gain
        return scale * (scaled - normed * jnp.mean(scaled * normed, axis=-1, keepdims=True))

    second_scale = scaling(attention)
    second_normed = attention * second_scale
    middle = adapted[...] + second_normed * second_gain[...]
    third_scale = scaling(middle)
    third_normed = middle * third_scale
    third_out[...] = (third_normed * third_gain[...]).astype(BF16)

    @pl.when(step == 0)
    def _():
        for copy in copies[2:]:
            copy.wait()

    sums[...] = jnp.zeros_like(sums)

    def forward(c, _):
        cut = pl.ds(pl.multiple_of(c * HIDDEN, HIDDEN), HIDDEN)
        gate = nn(third_out[...], wg[:, cut])
        upward = nn(third_out[...], wu[:, cut])
        gate_s[c] = gate
        up_s[c] = upward
        hidden = (gate / (1.0 + jnp.exp(-gate)) * upward).astype(BF16)
        hidden_out[:, cut] = hidden
        sums[...] += nn(hidden, wd[cut, :])
        return 0

    lax.fori_loop(0, gate_s.shape[0], forward, 0)
    mixed = sums[...]
    fourth_scale = scaling(mixed)
    fourth_normed = mixed * fourth_scale
    layer_out[...] = (middle + fourth_normed * fourth_gain[...]).astype(BF16)
    upstream = cotangent[...].astype(F32)
    gains_out[2:3, :] += jnp.sum(upstream * fourth_normed, axis=0, keepdims=True)
    mixed_out[...] = inward(upstream, fourth_gain[...], fourth_normed, fourth_scale).astype(BF16)
    sums[...] = jnp.zeros_like(sums)
    side_units = wg_own.shape[1] // 128

    def backward(c, _):
        cut = pl.ds(pl.multiple_of(c * HIDDEN, HIDDEN), HIDDEN)
        back = nt(mixed_out[...], wd[cut, :]).astype(BF16).astype(F32)
        gate = gate_s[c]
        sigmoid = 1.0 / (1.0 + jnp.exp(-gate))
        silu = gate * sigmoid
        gate_back = (back * up_s[c] * (sigmoid + silu * (1.0 - sigmoid))).astype(BF16)
        up_back = (back * silu).astype(BF16)
        for piece in range(HIDDEN // 128):
            unit = c * (HIDDEN // 128) + piece
            unit = jnp.where(unit < side_units, unit, unit + side_units)
            lanes = slice(piece * 128, (piece + 1) * 128)
            pair_out[:, pl.ds(pl.multiple_of(unit * 128, 128), 128)] = gate_back[:, lanes]
            unit += side_units
            pair_out[:, pl.ds(pl.multiple_of(unit * 128, 128), 128)] = up_back[:, lanes]
        sums[...] += nt(gate_back, wg[:, cut]) + nt(up_back, wu[:, cut])
        return 0

    lax.fori_loop(0, gate_s.shape[0], backward, 0)
    third_back = sums[...]
    gains_out[1:2, :] += jnp.sum(third_back * third_normed, axis=0, keepdims=True)
    middle_back = upstream + inward(third_back, third_gain[...], third_normed, third_scale)
    middle_out[...] = middle_back
    gains_out[0:1, :] += jnp.sum(middle_back * second_normed, axis=0, keepdims=True)
    attention_out[...] = inward(
        middle_back, second_gain[...], second_normed, second_scale
    ).astype(BF16)
    heads_low = nt(attention_out[...], wo[...]).astype(BF16)
    for side in range(2):
        for group in range(groups):
            at = (side * groups + group) * WIDE
            target = group * 2 + (tensor if side == 0 else 1 - tensor)
            heads_back[target] = heads_low[:, at : at + WIDE]


def middle_section(meta, adapted, heads, cotangent, gains, weights):
    rows, width = adapted.shape
    sources = heads.shape[0]
    inner = sources * WIDE
    hidden = 2 * weights[1].shape[1]
    block = rows // 2
    steps = rows // block
    row = pl.BlockSpec((block, width), lambda i, meta: (i, 0))
    wide = pl.BlockSpec((block, hidden), lambda i, meta: (i, 0))
    head = pl.BlockSpec((sources, block, WIDE), lambda i, meta: (0, i, 0))
    gain = pl.BlockSpec((1, width), lambda i, meta: (0, 0))
    hbm = pl.BlockSpec(memory_space=pl.ANY)
    return pl.pallas_call(
        middle_kernel,
        grid_spec=pltpu.PrefetchScalarGridSpec(
            num_scalar_prefetch=1,
            grid=(steps,),
            in_specs=[
                row,
                head,
                pl.BlockSpec((block, width), lambda i, meta: (meta[0] * steps + i, 0)),
                gain,
                gain,
                gain,
            ]
            + [hbm] * 8,
            out_specs=(
                row,
                row,
                pl.BlockSpec((block, inner), lambda i, meta: (i, 0)),
                row,
                row,
                row,
                wide,
                pl.BlockSpec((block, 2 * hidden), lambda i, meta: (i, 0)),
                head,
                pl.BlockSpec((8, width), lambda i, meta: (0, 0)),
            ),
            scratch_shapes=[
                pltpu.VMEM((inner, width), BF16),
                pltpu.VMEM((width, hidden), BF16),
                pltpu.VMEM((width, hidden), BF16),
                pltpu.VMEM((hidden, width), BF16),
                pltpu.VMEM((hidden // HIDDEN, block, HIDDEN), F32),
                pltpu.VMEM((hidden // HIDDEN, block, HIDDEN), F32),
                pltpu.VMEM((block, width), F32),
                pltpu.SemaphoreType.DMA((8,)),
            ],
        ),
        out_shape=(
            jax.ShapeDtypeStruct((rows, width), BF16),
            jax.ShapeDtypeStruct((rows, width), F32),
            jax.ShapeDtypeStruct((rows, inner), BF16),
            jax.ShapeDtypeStruct((rows, width), BF16),
            jax.ShapeDtypeStruct((rows, width), BF16),
            jax.ShapeDtypeStruct((rows, width), BF16),
            jax.ShapeDtypeStruct((rows, hidden), BF16),
            jax.ShapeDtypeStruct((rows, 2 * hidden), BF16),
            jax.ShapeDtypeStruct((sources, rows, WIDE), BF16),
            jax.ShapeDtypeStruct((8, width), F32),
        ),
        compiler_params=pltpu.CompilerParams(vmem_limit_bytes=VMEM_BYTES),
        cost_estimate=pl.CostEstimate(
            flops=rows * width * (4 * inner + 12 * hidden),
            bytes_accessed=6 * width * hidden + 2 * width * inner + rows * (hidden * 6 + width * 20),
            transcendentals=rows * hidden * 2,
        ),
        name="middle_section",
    )(meta, adapted, heads, cotangent, *gains, *weights)


class Reduction:
    def __init__(self, shape, by_lane=False, folded=False, cuts=None):
        self.rows, self.lanes = shape
        self.by_lane = by_lane
        self.folded = folded
        self.cuts = cuts or [self.lanes]

    def outputs(self):
        return [jax.ShapeDtypeStruct((self.rows, lanes), F32) for lanes in self.cuts]

    def scratch(self, dp):
        rows, lanes = self.rows, self.lanes
        quarter = (rows // 4, lanes)
        chunk = (rows // 4, lanes // dp) if self.by_lane else (rows // 4 // dp, lanes)
        refs = [
            pltpu.VMEM(quarter, BF16),
            pltpu.VMEM((dp + 1,) + chunk, BF16),
            pltpu.VMEM(quarter, BF16),
            pltpu.VMEM((3,) + quarter, BF16),
            [pltpu.VMEM((rows // 4, cut), F32) for cut in self.cuts],
            pltpu.SemaphoreType.DMA((5,)),
            pltpu.SemaphoreType.DMA((5,)),
            pltpu.SemaphoreType.DMA((dp,)),
            pltpu.SemaphoreType.DMA((dp + 1,)),
            pltpu.SemaphoreType.DMA((2, dp)),
            pltpu.SemaphoreType.DMA((dp,)),
            pltpu.SemaphoreType.DMA((len(self.cuts),)),
        ]
        refs = refs[:4] + refs[4] + refs[5:]
        if not self.folded:
            refs += [pltpu.VMEM((rows // 2, lanes), BF16)] * 2 + [pltpu.VMEM(quarter, BF16)]
        return refs

    def bind(self, part, outs, refs):
        self.part, self.outs = part, outs
        count = len(self.cuts)
        self.quarter, self.z_land, self.whole, self.others = refs[:4]
        self.wide = refs[4 : 4 + count]
        (
            self.send,
            self.recv,
            self.sum_send,
            self.sum_recv,
            self.all_send,
            self.all_recv,
            self.out_sem,
        ) = refs[4 + count : 11 + count]
        if not self.folded:
            self.half, self.core_land, self.x_land = refs[11 + count :]
        self.x, self.core, self.z = (lax.axis_index(name) for name in ("x", "core", "dp"))
        self.dp = lax.axis_size("dp")
        self.to_core = {"core": 1 - self.core}
        self.to_x = {"x": 1 - self.x}
        self.sends = []

    def copy(self, src, dst, send, recv, where):
        return pltpu.make_async_remote_copy(
            src_ref=src,
            dst_ref=dst,
            send_sem=send,
            recv_sem=recv,
            device_id=where,
            device_id_type=MESH,
        )

    def part_of(self, ref, index, rows):
        return ref.at[pl.ds(pl.multiple_of(index * rows, rows), rows)]

    def chunk(self, ref, index):
        if self.by_lane:
            lanes = self.lanes // self.dp
            return ref.at[:, pl.ds(pl.multiple_of(index * lanes, lanes), lanes)]
        return self.part_of(ref, index, self.rows // 4 // self.dp)

    def core_sum(self):
        half = self.rows // 2
        return self.copy(
            self.part_of(self.part, 1 - self.core, half),
            self.core_land,
            self.send.at[0],
            self.recv.at[0],
            self.to_core,
        )

    def x_sum(self):
        quarter = self.rows // 4
        return self.copy(
            self.part_of(self.half, 1 - self.x, quarter),
            self.x_land,
            self.send.at[1],
            self.recv.at[1],
            self.to_x,
        )

    def z_sum(self, j, step):
        up = {"dp": self.z + step}
        index = j
        lands = index if step > 0 else jnp.where(self.z - 1 == index, self.dp, index)
        return self.copy(
            self.chunk(self.quarter, index),
            self.z_land.at[lands],
            self.sum_send.at[index],
            self.sum_recv.at[lands],
            up,
        )

    def z_all(self, j, step):
        return self.copy(
            self.chunk(self.whole, j),
            self.chunk(self.whole, j),
            self.all_send.at[0 if step > 0 else 1, j],
            self.all_recv.at[j],
            {"dp": self.z + step},
        )

    def spread(self, which):
        src = self.others.at[0] if which == 2 else self.whole
        return self.copy(
            src,
            self.others.at[which],
            self.send.at[2 + which],
            self.recv.at[2 + which],
            self.to_x if which == 0 else self.to_core,
        )

    def writes(self, at):
        quarter = self.rows // 4
        core = self.core if at < 2 else 1 - self.core
        x = self.x if at % 2 == 0 else 1 - self.x
        row = pl.multiple_of((2 * core + x) * quarter, quarter)
        return [
            pltpu.make_async_copy(wide, out.at[pl.ds(row, quarter)], self.out_sem.at[i])
            for i, (wide, out) in enumerate(zip(self.wide, self.outs))
        ]

    def emit(self, at, ref):
        if at > 0:
            for copy in self.writes(at - 1):
                copy.wait()
        lane = 0
        for wide, lanes in zip(self.wide, self.cuts):
            wide[...] = ref[:, lane : lane + lanes].astype(F32)
            lane += lanes
        for copy in self.writes(at):
            copy.start()

    def add(self, into, left, right):
        into[...] = (left[...].astype(F32) + right[...].astype(F32)).astype(BF16)

    def hop(self, h):
        last = self.dp - 1

        @pl.when(self.z == h)
        def _():
            for j in range(last, h, -1):
                if h > 0:
                    self.wait_sum(j)
                    self.add(self.chunk(self.quarter, j), self.chunk(self.quarter, j), self.z_land.at[j])
                self.z_sum(j, 1).start()

        @pl.when(self.z == last - h)
        def _():
            for j in range(0, last - h):
                if h > 0:
                    self.wait_sum(j)
                    self.add(self.chunk(self.quarter, j), self.chunk(self.quarter, j), self.z_land.at[j])
                self.z_sum(j, -1).start()

    def wait_sum(self, lands):
        self.copy(
            self.z_land.at[lands],
            self.z_land.at[lands],
            self.sum_send.at[0],
            self.sum_recv.at[lands],
            self.to_x,
        ).wait_recv()

    def all_hop(self, h):
        z, last = self.z, self.dp - 1
        low, high = jnp.maximum(z - h, 0), jnp.minimum(z + h, last)

        @pl.when(z >= h)
        def _():
            self.z_all(low, 1).wait_recv()

        @pl.when((z >= h) & (z < last))
        def _():
            self.z_all(low, 1).start()

        @pl.when(z <= last - h)
        def _():
            self.z_all(high, -1).wait_recv()

        @pl.when((z <= last - h) & (z > 0))
        def _():
            self.z_all(high, -1).start()

    def stages(self):
        def start():
            self.core_sum().start()

        def fold_core():
            self.core_sum().wait_recv()
            self.add(
                self.half, self.part_of(self.part, self.core, self.rows // 2), self.core_land
            )
            self.x_sum().start()

        def begin():
            self.quarter[...] = self.part[...]
            self.hop(0)

        def fold_x():
            self.x_sum().wait_recv()
            self.add(
                self.quarter, self.part_of(self.half, self.x, self.rows // 4), self.x_land
            )
            self.hop(0)

        def settle():
            z, last = self.z, self.dp - 1
            mine = self.chunk(self.quarter, z)

            @pl.when(z > 0)
            def _():
                self.wait_sum(z)
                self.add(mine, mine, self.z_land.at[z])

            @pl.when(z < last)
            def _():
                self.wait_sum(self.dp)
                self.add(mine, mine, self.z_land.at[self.dp])

            self.chunk(self.whole, z)[...] = mine[...]

            @pl.when(z < last)
            def _():
                self.z_all(z, 1).start()

            @pl.when(z > 0)
            def _():
                self.z_all(z, -1).start()

        def share():
            self.all_hop(self.dp - 1)
            self.spread(0).start()
            self.spread(1).start()
            self.emit(0, self.whole)

        def pass_on():
            self.spread(0).wait_recv()
            self.spread(2).start()
            self.emit(1, self.others.at[0])

        def last():
            self.spread(1).wait_recv()
            self.emit(2, self.others.at[1])
            self.spread(2).wait_recv()
            self.emit(3, self.others.at[2])

        return (
            ([begin] if self.folded else [start, fold_core, fold_x])
            + [functools.partial(self.hop, h) for h in range(1, self.dp - 1)]
            + [settle]
            + [functools.partial(self.all_hop, h) for h in range(1, self.dp - 1)]
            + [share, pass_on, last]
        )

    def drain(self):
        z, last = self.z, self.dp - 1
        if not self.folded:
            self.core_sum().wait_send()
            self.x_sum().wait_send()
        for j in range(self.dp):

            @pl.when(z < j)
            def _():
                self.z_sum(j, 1).wait_send()

            @pl.when(z > j)
            def _():
                self.z_sum(j, -1).wait_send()

            @pl.when((z >= j) & (z < last))
            def _():
                self.z_all(j, 1).wait_send()

            @pl.when((z <= j) & (z > 0))
            def _():
                self.z_all(j, -1).wait_send()

        for which in range(3):
            self.spread(which).wait_send()
        for copy in self.writes(3):
            copy.wait()


def bind_all(items, parts, outs, scratch):
    dp = lax.axis_size("dp")
    for item, part in zip(items, parts):
        size = len(item.scratch(dp))
        item.bind(part, outs[: len(item.cuts)], scratch[:size])
        outs, scratch = outs[len(item.cuts) :], scratch[size:]


def waves(plans):
    length = max(len(plan) + i for i, plan in enumerate(plans))
    return [
        [plan[t - i] for i, plan in enumerate(plans) if 0 <= t - i < len(plan)]
        for t in range(length)
    ]


def greet_line(barrier):
    z, last = lax.axis_index("dp"), lax.axis_size("dp") - 1

    @pl.when(z > 0)
    def _():
        pl.semaphore_signal(barrier, inc=1, device_id={"dp": z - 1}, device_id_type=MESH)

    @pl.when(z < last)
    def _():
        pl.semaphore_signal(barrier, inc=1, device_id={"dp": z + 1}, device_id_type=MESH)

    return jnp.minimum(z, 1) + jnp.minimum(last - z, 1)


LEAVE = 128


def leave_kernel(items, *refs):
    sent, adapted, middle_back, gain, query_w, key_w, value_w = refs[:7]
    parts, refs = refs[7 : 7 + len(items)], refs[7 + len(items) :]
    joined, adapted_low, gain_out = refs[:3]
    count = sum(len(item.cuts) for item in items)
    outs, refs = refs[3 : 3 + count], refs[3 + count :]
    landed, away, away_landed = refs[:3]
    part_send, part_recv, away_send, away_recv, low_send, low_recv = refs[3:9]
    bind_all(items, parts, outs, refs[9:])
    plans = [item.stages() for item in items]
    stages = list(zip(*plans))
    away_plan = {0: stages[0]}
    home_plan = {1: stages[1], 4: stages[2]}
    me, others = neighbours()
    tensor = lax.axis_index("tensor")
    tensor_peer = {"tensor": 1 - tensor}
    barrier = pltpu.get_barrier_semaphore()
    for target in [tensor_peer] + [where for _, where in others]:
        pl.semaphore_signal(barrier, inc=1, device_id=target, device_id_type=MESH)
    pl.semaphore_wait(barrier, 1 + len(others) + greet_line(barrier))
    half = adapted.shape[0]
    inner = query_w.shape[1]
    steps = half // LEAVE

    def block(start, i):
        return pl.ds(pl.multiple_of(start + i * LEAVE, LEAVE), LEAVE)

    def gather(side, i, at):
        here = block((tensor if side else 1 - tensor) * half, i)
        place, where = others[at]
        return pltpu.make_async_remote_copy(
            src_ref=sent.at[place, here],
            dst_ref=landed.at[me, here],
            send_sem=part_send.at[side, i, at],
            recv_sem=part_recv.at[side, i, at],
            device_id=where,
            device_id_type=MESH,
        )

    def hand_over(i):
        return pltpu.make_async_remote_copy(
            src_ref=away.at[block(0, i)],
            dst_ref=away_landed.at[block(0, i)],
            send_sem=away_send.at[i],
            recv_sem=away_recv.at[i],
            device_id=tensor_peer,
            device_id_type=MESH,
        )

    def share(i):
        here = block(tensor * half, i)
        return pltpu.make_async_remote_copy(
            src_ref=adapted_low.at[here],
            dst_ref=adapted_low.at[here],
            send_sem=low_send.at[i],
            recv_sem=low_recv.at[i],
            device_id=tensor_peer,
            device_id_type=MESH,
        )

    for side in range(2):

        def begin(i, _):
            for at in range(len(others)):
                gather(side, i, at).start()
            return 0

        lax.fori_loop(0, steps, begin, 0)
    landed[me] = sent[me]
    gain_out[...] = jnp.zeros_like(gain_out)

    def input_grad(side, i):
        for at in range(len(others)):
            gather(side, i, at).wait_recv()
        here = block((tensor if side else 1 - tensor) * half, i)
        for at in range(3):
            for group in range(landed.shape[0]):
                to = at * inner + group * WIDE
                joined[here, to : to + WIDE] = landed[group, here, at * WIDE : (at + 1) * WIDE]
        total = nt(joined[here, 0:inner], query_w[...])
        total += nt(joined[here, inner : 2 * inner], key_w[...])
        total += nt(joined[here, 2 * inner : 3 * inner], value_w[...])
        return total

    def away_step(i, _):
        away[block(0, i), :] = input_grad(0, i).astype(BF16)
        hand_over(i).start()
        at_step(i, away_plan)
        return 0

    lax.fori_loop(0, steps, away_step, 0)

    def home_step(i, _):
        total = input_grad(1, i)
        hand_over(i).wait_recv()
        rows = block(0, i)
        upstream = total + away_landed[rows, :].astype(F32)
        values = adapted[rows, :]
        scale = lax.rsqrt(jnp.mean(values * values, axis=-1, keepdims=True) + EPSILON)
        normed = values * scale
        scaled = upstream * gain[...]
        inward = scale * (scaled - normed * jnp.mean(scaled * normed, axis=-1, keepdims=True))
        gain_out[0:1, :] += jnp.sum(upstream * normed, axis=0, keepdims=True)
        adapted_low[block(tensor * half, i), :] = (middle_back[rows, :] + inward).astype(BF16)
        share(i).start()
        at_step(i, home_plan)
        return 0

    lax.fori_loop(0, steps, home_step, 0)
    for wave in waves([plan[3:] for plan in plans]):
        for call in wave:
            call()
    for item in items:
        item.drain()

    def finish(i, _):
        for side in range(2):
            for at in range(len(others)):
                gather(side, i, at).wait_send()
        hand_over(i).wait_send()
        share(i).wait()
        return 0

    lax.fori_loop(0, steps, finish, 0)


def leave(sent, adapted, middle_back, gain, query_w, key_w, value_w, parts, kinds):
    items = [
        Reduction((4 * part.shape[0], part.shape[1]), by_lane, True, cuts)
        for part, (by_lane, cuts) in zip(parts, kinds)
    ]
    scratch, outs = [], []
    for item in items:
        scratch += item.scratch(lax.axis_size("dp"))
        outs += item.outputs()
    peers, rows, lanes = sent.shape
    half, width = adapted.shape
    inner = query_w.shape[1]
    steps = half // LEAVE
    vmem = pl.BlockSpec(memory_space=pltpu.VMEM)
    return pl.pallas_call(
        functools.partial(leave_kernel, items),
        out_shape=(
            jax.ShapeDtypeStruct((rows, 3 * inner), BF16),
            jax.ShapeDtypeStruct((rows, width), BF16),
            jax.ShapeDtypeStruct((8, width), F32),
        )
        + tuple(outs),
        in_specs=[vmem] * (7 + len(items)),
        out_specs=(vmem,) * 3 + (pl.BlockSpec(memory_space=pl.ANY),) * len(outs),
        scratch_shapes=[
            pltpu.VMEM((peers, rows, lanes), BF16),
            pltpu.VMEM((half, width), BF16),
            pltpu.VMEM((half, width), BF16),
            pltpu.SemaphoreType.DMA((2, steps, 3)),
            pltpu.SemaphoreType.DMA((2, steps, 3)),
        ]
        + [pltpu.SemaphoreType.DMA((steps,))] * 4
        + scratch,
        compiler_params=pltpu.CompilerParams(
            vmem_limit_bytes=VMEM_BYTES, collective_id=1, has_side_effects=True
        ),
        cost_estimate=pl.CostEstimate(
            flops=2 * rows * width * 3 * inner, bytes_accessed=200 << 20, transcendentals=rows
        ),
        name="leave",
    )(sent, adapted, middle_back, gain, query_w, key_w, value_w, *parts)


def reduce_kernel(items, *refs):
    count = len(items)
    outs = sum(len(item.cuts) for item in items)
    bind_all(items, refs[:count], refs[count : count + outs], refs[count + outs :])
    barrier = pltpu.get_barrier_semaphore()
    for target in (items[0].to_core, items[0].to_x):
        pl.semaphore_signal(barrier, inc=1, device_id=target, device_id_type=MESH)
    pl.semaphore_wait(barrier, 2 + greet_line(barrier))
    plans = [item.stages() for item in items]
    for plan in plans:
        plan[0]()
    for plan in plans:
        plan[1]()
    for wave in waves([plan[2:] for plan in plans]):
        for call in wave:
            call()
    for item in items:
        item.drain()


def reduce_all(parts, cuts):
    dp = lax.axis_size("dp")
    items = [Reduction(part.shape, cuts=cut) for part, cut in zip(parts, cuts)]
    scratch, outs = [], []
    for item in items:
        scratch += item.scratch(dp)
        outs += item.outputs()
    moved = sum(item.rows * item.lanes for item in items)
    return pl.pallas_call(
        functools.partial(reduce_kernel, items),
        out_shape=tuple(outs),
        in_specs=[pl.BlockSpec(memory_space=pltpu.VMEM)] * len(items),
        out_specs=(pl.BlockSpec(memory_space=pl.ANY),) * len(outs),
        scratch_shapes=scratch,
        compiler_params=pltpu.CompilerParams(
            vmem_limit_bytes=VMEM_BYTES, collective_id=2, has_side_effects=True
        ),
        cost_estimate=pl.CostEstimate(
            flops=moved * 4, bytes_accessed=moved * 30, transcendentals=0
        ),
        name="reduce_all",
    )(*parts)


def swap(value, axis):
    return lax.ppermute(value, axis, [(0, 1), (1, 0)])


def together(*values):
    return lax.optimization_barrier(values)


def cut(value, index, rows):
    return lax.dynamic_slice_in_dim(value, index * rows, rows, 0)


def add_low(left, right):
    return (left.astype(F32) + right.astype(F32)).astype(BF16)


def fold(value, index, axis):
    half = value.shape[0] // 2
    return add_low(cut(value, index, half), swap(cut(value, 1 - index, half), axis))


def unfold(value, index, axis):
    other = swap(value, axis)
    return jnp.concatenate(
        [jnp.where(index == 0, value, other), jnp.where(index == 0, other, value)], axis=0
    )


def sum_small(value):
    for axis in ("tensor", "core", "x"):
        value = value + swap(value, axis)
    for pairs in ([(0, 1), (1, 0), (2, 3), (3, 2)], [(0, 2), (2, 0), (1, 3), (3, 1)]):
        value = value + lax.ppermute(value, "dp", pairs)
    return value


def tn(left, right):
    return lax.dot_general(
        left, right, (((0,), (0,)), ((), ())), preferred_element_type=F32
    ).astype(BF16)


def on_device_paired(
    latent_embed,
    adapter,
    first_gain,
    query_weight,
    key_weight,
    value_weight,
    output_weight,
    second_gain,
    third_gain,
    gate_weight,
    up_weight,
    down_weight,
    fourth_gain,
    parents,
    positions,
    cotangent,
):
    rows = latent_embed.shape[0]
    width = adapter.shape[2]
    half_rows = rows // 2
    tensor = lax.axis_index("tensor")
    core = lax.axis_index("core")
    x = lax.axis_index("x")
    everyone = ("x", "core", "tensor")
    meta = jnp.stack([tensor, core]).astype(jnp.int32)
    one_row = lambda gain: gain.reshape(1, -1)

    cosine, sine = angle_tables(positions)
    mine = jnp.einsum(
        "rcd,cde->re", latent_embed, adapter, preferred_element_type=F32
    ).astype(BF16)
    parts, first_low, theirs = enter(
        mine, one_row(first_gain), query_weight, key_weight, value_weight, cosine, sine
    )
    adapted = cut(mine, tensor, half_rows).astype(F32) + cut(theirs, tensor, half_rows).astype(
        F32
    )
    role, place, parts = sort_parts(parents, parts.reshape(-1, 3 * WIDE))
    own_weights = (output_weight, gate_weight, up_weight, down_weight)
    attended, logsum, *other_weights = attention_forward(parts, own_weights)
    heads = lax.all_to_all(
        pick(place, attended).reshape(8, half_rows, WIDE), everyone, 0, 0, tiled=False
    )
    (
        layer_half,
        middle_back,
        attended_all,
        attention_low,
        third_low,
        mixed_low,
        hidden,
        pair_low,
        heads_back,
        gain_parts,
    ) = middle_section(
        meta,
        adapted,
        heads,
        cotangent,
        (one_row(second_gain), one_row(third_gain), one_row(fourth_gain)),
        own_weights + tuple(other_weights),
    )
    upstream = lax.all_to_all(heads_back, everyone, 0, 0, tiled=False).reshape(-1, WIDE)
    layer_other = swap(layer_half, "tensor")
    layer_out = jnp.concatenate(
        [
            jnp.where(tensor == 0, layer_half, layer_other),
            jnp.where(tensor == 0, layer_other, layer_half),
        ],
        axis=0,
    ).astype(F32)

    split = gate_weight.shape[1]
    inner = output_weight.shape[0]
    sides = []
    lanes = [pair_low[:, i * split : (i + 1) * split] for i in range(4)]
    sides += [tn(third_low, lanes[0]), tn(third_low, lanes[2])]
    sides += [tn(hidden[:, :split], mixed_low), tn(hidden[:, split:], mixed_low)]
    sides += [tn(third_low, lanes[1]), tn(third_low, lanes[3])]
    sides += [
        tn(attended_all[:, :inner], attention_low),
        tn(attended_all[:, inner:], attention_low),
    ]
    table_cosine, table_sine = angle_tables(jnp.arange((TRUNK + 2) * SEG))
    sent, *sums = attention_backward(
        parts, pick(role, upstream), attended, logsum, table_cosine, table_sine, sides
    )
    (
        joined,
        adapted_low,
        first_gain_part,
        gate_total,
        down_total,
        up_total,
        output_total,
    ) = leave(
        pick(place, sent).reshape(4, rows, 3 * WIDE),
        adapted,
        middle_back,
        one_row(first_gain),
        query_weight,
        key_weight,
        value_weight,
        sums,
        [(False, None), (True, None), (False, None), (False, None)],
    )
    adapter_part = jnp.einsum(
        "rcd,re->cde", latent_embed, adapted_low, preferred_element_type=F32
    ).astype(BF16)
    query_total, key_total, value_total, *adapter_total = reduce_all(
        [tn(first_low, joined[:, i * inner : (i + 1) * inner]) for i in range(3)]
        + [adapter_part[0], adapter_part[1]],
        [None] * 5,
    )
    adapter_total = jnp.stack(adapter_total)
    latent_gradient = jnp.einsum("re,cde->rcd", adapted_low, adapter, preferred_element_type=F32)
    gains = sum_small(jnp.concatenate([gain_parts[:3], first_gain_part[:1]], axis=0))
    return (
        layer_out,
        latent_gradient,
        adapter_total,
        gains[3],
        query_total,
        key_total,
        value_total,
        output_total,
        gains[0],
        gains[1],
        gate_total,
        up_total,
        down_total,
        gains[2],
    )


def specs(rows):
    split = P(None, "tensor")
    in_specs = (
        P(rows, None, "tensor"),
        P(None, "tensor", None),
        P(),
        split,
        split,
        split,
        P("tensor", None),
        P(),
        P(),
        split,
        split,
        P("tensor", None),
        P(),
        P("dp", None),
        P(rows),
        P(rows, None),
    )
    out_specs = (
        P(rows, None),
        P(rows, None, "tensor"),
        P(None, "tensor", None),
        P(),
        split,
        split,
        split,
        P("tensor", None),
        P(),
        P(),
        split,
        split,
        P("tensor", None),
        P(),
    )
    return in_specs, out_specs


def solution(mesh):
    sizes = dict(mesh.shape)
    if sizes["seq"] == 4 and sizes["tensor"] == 2:
        fine = Mesh(
            mesh.devices.reshape(sizes["dp"], 2, 2, 2), ("dp", "x", "core", "tensor")
        )
        in_specs, out_specs = specs(("dp", "x", "core"))
        return jax.shard_map(
            on_device_paired, mesh=fine, in_specs=in_specs, out_specs=out_specs, check_vma=False
        )
    in_specs, out_specs = specs(("dp", "seq"))
    return jax.shard_map(
        on_device, mesh=mesh, in_specs=in_specs, out_specs=out_specs, check_vma=False
    )
```

```python
import functools

import jax
import jax.numpy as jnp
from jax import lax
from jax.experimental import pallas as pl
from jax.experimental.pallas import tpu as pltpu
from jax.sharding import Mesh
from jax.sharding import PartitionSpec as P

DH = 64
SEG = 256


EPSILON = 1e-06
THETA = 50000.0


def normalize(values, gain):
    scale = lax.rsqrt(jnp.mean(values * values, axis=-1, keepdims=True) + EPSILON)
    normed = values * scale
    return (normed * gain, normed, scale)


def normalize_back(upstream, gain, normed, scale):
    scaled = upstream * gain
    inward = scale * (scaled - normed * jnp.mean(scaled * normed, axis=-1, keepdims=True))
    return (inward, jnp.sum(upstream * normed, axis=0))


def angles(positions, width):
    half = width // 2
    freq = THETA ** (-jnp.arange(half, dtype=jnp.float32) * 2.0 / width)
    angle = positions.astype(jnp.float32)[:, None] * freq[None, :]
    return (jnp.cos(angle)[:, None, :], jnp.sin(angle)[:, None, :])


def rotate(values, cosine, sine, sign):
    half = values.shape[-1] // 2
    first = values[..., :half]
    second = values[..., half:]
    return jnp.concatenate(
        [first * cosine - sign * second * sine, second * cosine + sign * first * sine], axis=-1
    )


def ancestry(parent_row):
    labels = jnp.arange(parent_row.shape[0], dtype=jnp.int32)

    def extend(index, state):
        current, total = state
        total = total | (current[:, None] == labels[None, :])
        current = jnp.where(current >= 0, jnp.take(parent_row, jnp.maximum(current, 0)), -1)
        return (current, total)

    start = (parent_row, jnp.zeros((parent_row.shape[0], parent_row.shape[0]), jnp.bool_))
    current, total = lax.fori_loop(0, parent_row.shape[0], extend, start)
    return total


def path_mask(parent_row, query_ids, key_ids):
    table = ancestry(parent_row)
    query_seg = query_ids // SEG
    key_seg = key_ids // SEG
    far = jnp.take(jnp.take(table, query_seg, axis=0), key_seg, axis=1)
    near = (query_seg[:, None] == key_seg[None, :]) & (key_ids[None, :] <= query_ids[:, None])
    return far | near


def on_device(
    latent_embed,
    adapter,
    first_gain,
    query_weight,
    key_weight,
    value_weight,
    output_weight,
    second_gain,
    third_gain,
    gate_weight,
    up_weight,
    down_weight,
    fourth_gain,
    parents,
    positions,
    cotangent,
):
    rows = latent_embed.shape[0]
    local_heads = query_weight.shape[1] // DH
    scale = DH ** (-0.5)
    adapted = lax.psum(
        jnp.einsum("rcd,cde->re", latent_embed, adapter, preferred_element_type=jnp.float32),
        "tensor",
    )
    first_out, first_normed, first_scale = normalize(adapted, first_gain)
    first_low = first_out.astype(jnp.bfloat16)
    cosine, sine = angles(positions, DH)
    query_raw = jnp.dot(first_low, query_weight, preferred_element_type=jnp.float32).reshape(
        rows, local_heads, DH
    )
    queries = rotate(query_raw, cosine, sine, 1.0).astype(jnp.bfloat16)
    key_raw = jnp.dot(first_low, key_weight, preferred_element_type=jnp.float32).reshape(
        rows, local_heads, DH
    )
    keys_local = rotate(key_raw, cosine, sine, 1.0).astype(jnp.bfloat16)
    values_local = (
        jnp.dot(first_low, value_weight, preferred_element_type=jnp.float32)
        .astype(jnp.bfloat16)
        .reshape(rows, local_heads, DH)
    )
    keys_all, values_all = (
        lax.all_gather(keys_local, "seq", axis=0, tiled=True),
        lax.all_gather(values_local, "seq", axis=0, tiled=True),
    )
    tree_rows = keys_all.shape[0]
    query_ids = lax.axis_index("seq") * rows + jnp.arange(rows, dtype=jnp.int32)
    key_ids = jnp.arange(tree_rows, dtype=jnp.int32)
    allowed = path_mask(parents[0], query_ids, key_ids)[None]

    def score_block(keys):
        raw = jnp.einsum("qhd,khd->hqk", queries, keys, preferred_element_type=jnp.float32) * scale
        return jnp.where(allowed, raw, -1e30)

    scores = score_block(keys_all)
    top = jnp.max(scores, axis=-1, keepdims=True)
    weights = jnp.exp(scores - top)
    total = jnp.sum(weights, axis=-1, keepdims=True)
    probs = weights / total
    logsum = top + jnp.log(total)
    attended = jnp.einsum(
        "hqk,khd->qhd", probs.astype(jnp.bfloat16), values_all, preferred_element_type=jnp.float32
    )
    attended = attended.reshape(rows, local_heads * DH).astype(jnp.bfloat16)
    attention = lax.psum(
        jnp.dot(attended, output_weight, preferred_element_type=jnp.float32).astype(jnp.bfloat16),
        "tensor",
    ).astype(jnp.float32)
    second_out, second_normed, second_scale = normalize(attention, second_gain)
    middle = adapted + second_out
    third_out, third_normed, third_scale = normalize(middle, third_gain)
    third_low = third_out.astype(jnp.bfloat16)
    gate = jnp.dot(third_low, gate_weight, preferred_element_type=jnp.float32)
    upward = jnp.dot(third_low, up_weight, preferred_element_type=jnp.float32)
    hidden = (jax.nn.silu(gate) * upward).astype(jnp.bfloat16)
    mixed = lax.psum(
        jnp.dot(hidden, down_weight, preferred_element_type=jnp.float32).astype(jnp.bfloat16),
        "tensor",
    ).astype(jnp.float32)
    fourth_out, fourth_normed, fourth_scale = normalize(mixed, fourth_gain)
    layer_out = middle + fourth_out
    upstream = cotangent.astype(jnp.float32)
    mixed_back, fourth_gain_part = normalize_back(
        upstream, fourth_gain, fourth_normed, fourth_scale
    )
    mixed_low = mixed_back.astype(jnp.bfloat16)
    down_part = jnp.einsum("rf,rd->fd", hidden, mixed_low, preferred_element_type=jnp.float32)
    hidden_back = (
        jnp.einsum("rd,fd->rf", mixed_low, down_weight, preferred_element_type=jnp.float32)
        .astype(jnp.bfloat16)
        .astype(jnp.float32)
    )
    swiglu_value, product_back = jax.vjp(
        lambda left, right: jax.nn.silu(left) * right, gate, upward
    )
    gate_back, up_back = product_back(hidden_back)
    gate_low = gate_back.astype(jnp.bfloat16)
    up_low = up_back.astype(jnp.bfloat16)
    gate_part = jnp.einsum("rd,rf->df", third_low, gate_low, preferred_element_type=jnp.float32)
    up_part = jnp.einsum("rd,rf->df", third_low, up_low, preferred_element_type=jnp.float32)
    third_term = jnp.einsum(
        "rf,df->rd", gate_low, gate_weight, preferred_element_type=jnp.float32
    ) + jnp.einsum("rf,df->rd", up_low, up_weight, preferred_element_type=jnp.float32)
    third_back = lax.psum(third_term.astype(jnp.bfloat16), "tensor").astype(jnp.float32)
    middle_part, third_gain_part = normalize_back(third_back, third_gain, third_normed, third_scale)
    middle_back = upstream + middle_part
    attention_back, second_gain_part = normalize_back(
        middle_back, second_gain, second_normed, second_scale
    )
    attention_low = attention_back.astype(jnp.bfloat16)
    output_part = jnp.einsum(
        "re,rd->ed", attended, attention_low, preferred_element_type=jnp.float32
    )
    attended_back = (
        jnp.einsum("rd,ed->re", attention_low, output_weight, preferred_element_type=jnp.float32)
        .astype(jnp.bfloat16)
        .reshape(rows, local_heads, DH)
    )
    keys_back, values_back = (
        lax.all_gather(keys_local, "seq", axis=0, tiled=True),
        lax.all_gather(values_local, "seq", axis=0, tiled=True),
    )
    probs_back = jnp.exp(score_block(keys_back) - logsum)
    prob_grad = jnp.einsum(
        "qhd,khd->hqk", attended_back, values_back, preferred_element_type=jnp.float32
    )
    score_grad = (
        probs_back * (prob_grad - jnp.sum(prob_grad * probs_back, axis=-1, keepdims=True))
    ).astype(jnp.bfloat16)
    query_rot = (
        jnp.einsum("hqk,khd->qhd", score_grad, keys_back, preferred_element_type=jnp.float32)
        * scale
    )
    key_rot_all = (
        jnp.einsum("hqk,qhd->khd", score_grad, queries, preferred_element_type=jnp.float32) * scale
    )
    value_back_all = jnp.einsum(
        "hqk,qhd->khd",
        probs_back.astype(jnp.bfloat16),
        attended_back,
        preferred_element_type=jnp.float32,
    )
    key_rot, value_back = (
        lax.psum_scatter(
            key_rot_all.astype(jnp.bfloat16), "seq", scatter_dimension=0, tiled=True
        ).astype(jnp.float32),
        lax.psum_scatter(
            value_back_all.astype(jnp.bfloat16), "seq", scatter_dimension=0, tiled=True
        ).astype(jnp.float32),
    )
    query_low = (
        rotate(query_rot, cosine, sine, -1.0).astype(jnp.bfloat16).reshape(rows, local_heads * DH)
    )
    key_low = (
        rotate(key_rot, cosine, sine, -1.0).astype(jnp.bfloat16).reshape(rows, local_heads * DH)
    )
    value_low = value_back.astype(jnp.bfloat16).reshape(rows, local_heads * DH)
    query_part = jnp.einsum("rd,re->de", first_low, query_low, preferred_element_type=jnp.float32)
    key_part = jnp.einsum("rd,re->de", first_low, key_low, preferred_element_type=jnp.float32)
    value_part = jnp.einsum("rd,re->de", first_low, value_low, preferred_element_type=jnp.float32)
    first_term = jnp.einsum(
        "re,de->rd", query_low, query_weight, preferred_element_type=jnp.float32
    )
    first_term = first_term + jnp.einsum(
        "re,de->rd", key_low, key_weight, preferred_element_type=jnp.float32
    )
    first_term = first_term + jnp.einsum(
        "re,de->rd", value_low, value_weight, preferred_element_type=jnp.float32
    )
    first_back = lax.psum(first_term.astype(jnp.bfloat16), "tensor").astype(jnp.float32)
    adapted_part, first_gain_part = normalize_back(
        first_back, first_gain, first_normed, first_scale
    )
    adapted_low = (middle_back + adapted_part).astype(jnp.bfloat16)
    latent_gradient = jnp.einsum(
        "re,cde->rcd", adapted_low, adapter, preferred_element_type=jnp.float32
    )
    adapter_part = jnp.einsum(
        "rcd,re->cde", latent_embed, adapted_low, preferred_element_type=jnp.float32
    )
    summed = (
        lax.psum(gate_part.astype(jnp.bfloat16), ("dp", "seq")).astype(jnp.float32),
        lax.psum(up_part.astype(jnp.bfloat16), ("dp", "seq")).astype(jnp.float32),
        lax.psum(down_part.astype(jnp.bfloat16), ("dp", "seq")).astype(jnp.float32),
        lax.psum(third_gain_part.astype(jnp.bfloat16), ("dp", "seq")).astype(jnp.float32),
        lax.psum(fourth_gain_part.astype(jnp.bfloat16), ("dp", "seq")).astype(jnp.float32),
        lax.psum(query_part.astype(jnp.bfloat16), ("dp", "seq")).astype(jnp.float32),
        lax.psum(key_part.astype(jnp.bfloat16), ("dp", "seq")).astype(jnp.float32),
        lax.psum(value_part.astype(jnp.bfloat16), ("dp", "seq")).astype(jnp.float32),
        lax.psum(output_part.astype(jnp.bfloat16), ("dp", "seq")).astype(jnp.float32),
        lax.psum(first_gain_part.astype(jnp.bfloat16), ("dp", "seq")).astype(jnp.float32),
        lax.psum(second_gain_part.astype(jnp.bfloat16), ("dp", "seq")).astype(jnp.float32),
        lax.psum(adapter_part.astype(jnp.bfloat16), ("dp", "seq")).astype(jnp.float32),
    )
    gate_total, up_total, down_total, third_total, fourth_total = (
        summed[0],
        summed[1],
        summed[2],
        summed[3],
        summed[4],
    )
    query_total, key_total, value_total, output_total, first_total, second_total = (
        summed[5],
        summed[6],
        summed[7],
        summed[8],
        summed[9],
        summed[10],
    )
    adapter_total = summed[11]
    return (
        layer_out,
        latent_gradient,
        adapter_total,
        first_total,
        query_total,
        key_total,
        value_total,
        output_total,
        second_total,
        third_total,
        gate_total,
        up_total,
        down_total,
        fourth_total,
    )


TRUNK = 8
BRANCH = 4
LEAVES = 2
SEGS = TRUNK + BRANCH + BRANCH * LEAVES
WIDE = 2 * DH
NEG = -1e30
F32 = jnp.float32
BF16 = jnp.bfloat16
KEYS = 512
HIDDEN = 256
VMEM_BYTES = 60 << 20


def nt(left, right):
    return lax.dot_general(left, right, (((1,), (1,)), ((), ())), preferred_element_type=F32)


def nn(left, right):
    return lax.dot_general(left, right, (((1,), (0,)), ((), ())), preferred_element_type=F32)


def segment(index, size=SEG):
    return pl.ds(pl.multiple_of(index * SEG, SEG), size)


def find_roles(parents, child, count, role):
    for s in range(SEGS):
        count[s] = 0
    role[0] = 0
    for s in range(SEGS):
        parent = parents[0, s]

        @pl.when(parent < 0)
        def _():
            role[0] = s

        @pl.when(parent >= 0)
        def _():
            seen = count[parent]
            child[parent * BRANCH + seen] = s
            count[parent] = seen + 1

    for i in range(TRUNK - 1):
        role[i + 1] = child[role[i] * BRANCH]
    for b in range(BRANCH):
        role[TRUNK + b] = child[role[TRUNK - 1] * BRANCH + b]
    for b in range(BRANCH):
        for leaf in range(LEAVES):
            role[TRUNK + BRANCH + b * LEAVES + leaf] = child[role[TRUNK + b] * BRANCH + leaf]


def roles_kernel(parents, parts, role, place, out, child, count):
    find_roles(parents, child, count, role)
    for i in range(SEGS):
        place[role[i]] = i
    pick_segments(role, parts, out)


def pick_segments(order, source, out):
    for i in range(SEGS):
        out[segment(i), :] = source[segment(order[i]), :]


def sort_parts(parents, parts):
    smem = pl.BlockSpec(memory_space=pltpu.SMEM)
    vmem = pl.BlockSpec(memory_space=pltpu.VMEM)
    return pl.pallas_call(
        roles_kernel,
        out_shape=(jax.ShapeDtypeStruct((SEGS,), jnp.int32),) * 2
        + (jax.ShapeDtypeStruct(parts.shape, parts.dtype),),
        in_specs=[smem, vmem],
        out_specs=(smem, smem, vmem),
        scratch_shapes=[
            pltpu.SMEM((SEGS * BRANCH,), jnp.int32),
            pltpu.SMEM((SEGS,), jnp.int32),
        ],
        name="sort_parts",
    )(parents, parts)


def pick(order, source):
    smem = pl.BlockSpec(memory_space=pltpu.SMEM)
    vmem = pl.BlockSpec(memory_space=pltpu.VMEM)
    return pl.pallas_call(
        pick_segments,
        out_shape=jax.ShapeDtypeStruct(source.shape, source.dtype),
        in_specs=[smem, vmem],
        out_specs=vmem,
        name="pick",
    )(order, source)


def heads_apart(values, first):
    zero = jnp.zeros_like(values)
    return jnp.concatenate(
        [jnp.where(first, values, zero), jnp.where(first, zero, values)], axis=0
    )


MESH = pl.DeviceIdType.MESH


def at_step(index, plan):
    for step, calls in plan.items():

        @pl.when(index == step)
        def _(calls=calls):
            for call in calls:
                call()


class Fetch:
    def __init__(self, shape, pieces):
        self.rows, self.lanes = shape
        self.pieces = pieces

    def scratch(self):
        return [pltpu.SemaphoreType.DMA((4, self.pieces))] * 2

    def bind(self, own, out, refs):
        self.own, self.out = own, out
        self.send, self.recv = refs
        self.x, self.core = lax.axis_index("x"), lax.axis_index("core")
        self.to_core = {"core": 1 - self.core}
        self.to_x = {"x": 1 - self.x}
        self.to_tensor = {"tensor": 1 - lax.axis_index("tensor")}

    def copy(self, kind, piece):
        rows = self.rows // 4 // self.pieces
        x = 1 - self.x if kind == 3 else self.x
        row = (2 * x + self.core) * (self.rows // 4) + piece * rows
        here = pl.ds(pl.multiple_of(row, 16), rows)
        return pltpu.make_async_remote_copy(
            src_ref=(self.own if kind == 0 else self.out).at[here],
            dst_ref=self.out.at[here],
            send_sem=self.send.at[kind, piece],
            recv_sem=self.recv.at[kind, piece],
            device_id=(self.to_tensor, self.to_x, self.to_core, self.to_core)[kind],
            device_id_type=MESH,
        )

    def start(self):
        for piece in range(self.pieces):
            self.copy(0, piece).start()

    def second(self, piece):
        self.copy(0, piece).wait_recv()
        self.copy(1, piece).start()
        self.copy(2, piece).start()

    def third(self, piece):
        self.copy(1, piece).wait_recv()
        self.copy(3, piece).start()

    def drain(self):
        for piece in range(self.pieces):
            for kind in range(4):
                self.copy(kind, piece).wait_send()
            self.copy(2, piece).wait_recv()
            self.copy(3, piece).wait_recv()


def attention_kernel(fetches, *refs):
    parts = refs[0]
    count = len(fetches)
    own_weights, refs = refs[1 : 1 + count], refs[1 + count :]
    out, logsum, other_weights = refs[0], refs[1], refs[2 : 2 + count]
    qr, kr, v0, v1, kept, acc, top, total = refs[2 + count : 10 + count]
    sems = refs[10 + count :]
    for i, fetch in enumerate(fetches):
        fetch.bind(own_weights[i], other_weights[i], sems[2 * i : 2 * i + 2])
    output, gate, up, down = fetches
    barrier = pltpu.get_barrier_semaphore()
    for target in (gate.to_core, gate.to_x, gate.to_tensor):
        pl.semaphore_signal(barrier, inc=1, device_id=target, device_id_type=MESH)
    pl.semaphore_wait(barrier, 3)
    for fetch in fetches:
        fetch.start()
    call = functools.partial
    leaf_plan = {
        2: [call(output.second, 0)],
        4: [call(gate.second, 0), call(output.third, 0)],
        6: [call(gate.second, 1)],
        7: [call(gate.third, 0)],
    }
    branch_plan = {
        0: [call(up.second, 0)],
        1: [call(gate.third, 1)],
        2: [call(up.second, 1)],
        3: [call(up.third, 0)],
    }
    trunk_plan = {
        3: [call(down.second, 0), call(up.third, 1)],
        6: [call(down.second, 1)],
    }
    first = lax.broadcasted_iota(jnp.int32, (SEG, WIDE), 1) < DH

    def sort(i, _):
        here = source = segment(i)
        qr[here, :] = parts[source, 0:WIDE] * jnp.asarray(DH**-0.5, BF16)
        kr[here, :] = parts[source, WIDE : 2 * WIDE]
        value = parts[source, 2 * WIDE : 3 * WIDE]
        zero = jnp.zeros_like(value)
        v0[here, :] = jnp.where(first, value, zero)
        v1[here, :] = jnp.where(first, zero, value)
        return 0

    lax.fori_loop(0, SEGS, sort, 0)
    row = lax.broadcasted_iota(jnp.int32, (2 * SEG, SEG), 0)
    col = lax.broadcasted_iota(jnp.int32, (2 * SEG, SEG), 1)
    causal = col <= jnp.where(row >= SEG, row - SEG, row)

    def fold(values, op):
        result = values[:, 0:128]
        for at in range(128, values.shape[1], 128):
            result = op(result, values[:, at : at + 128])
        return result

    def query(index, count_big, big, extra):
        queries = heads_apart(qr[segment(index), :], first)
        own = jnp.where(causal, nt(queries, kr[segment(index), :]), NEG)
        top[...] = fold(own, jnp.maximum)
        others = []
        for other in extra:
            scores = nt(queries, kr[segment(other), :])
            top[...] = jnp.maximum(top[...], fold(scores, jnp.maximum))
            others.append(scores)

        def find(c, _):
            scores = nt(queries, kr[pl.ds(pl.multiple_of(c * big, big), big), :])
            kept[c, :, 0:big] = scores
            top[...] = jnp.maximum(top[...], fold(scores, jnp.maximum))
            return 0

        lax.fori_loop(0, count_big, find, 0)
        most = jnp.max(top[...], axis=1, keepdims=True)

        def add(scores, keys, fresh=False):
            weights = jnp.exp(scores - most)
            summed = fold(weights, jnp.add)
            low = weights.astype(BF16)
            product = nn(low[:SEG], v0[keys, :]) + nn(low[SEG:], v1[keys, :])
            total[...] = summed if fresh else total[...] + summed
            acc[...] = product if fresh else acc[...] + product

        add(own, segment(index), True)
        for other, scores in zip(extra, others):
            add(scores, segment(other))

        def use(c, _):
            add(kept[c, :, 0:big], pl.ds(pl.multiple_of(c * big, big), big))
            return 0

        lax.fori_loop(0, count_big, use, 0)
        whole = jnp.sum(total[...], axis=1, keepdims=True)
        inverse = 1.0 / whole
        log = most + jnp.log(whole)
        here = segment(index)
        out[here, :] = (acc[...] * jnp.where(first, inverse[:SEG], inverse[SEG:])).astype(BF16)
        logsum[here, :] = jnp.where(first, log[:SEG], log[SEG:])

    def trunk(i, _):
        at_step(i, trunk_plan)
        query(i, i, SEG, [])
        return 0

    def branch(i, _):
        at_step(i, branch_plan)
        query(TRUNK + i, TRUNK * SEG // KEYS, KEYS, [])
        return 0

    def leaf(i, _):
        at_step(i, leaf_plan)
        query(TRUNK + BRANCH + i, TRUNK * SEG // KEYS, KEYS, [TRUNK + i // LEAVES])
        return 0

    lax.fori_loop(0, BRANCH * LEAVES, leaf, 0)
    lax.fori_loop(0, BRANCH, branch, 0)
    lax.fori_loop(0, TRUNK, trunk, 0)
    down.third(0)

    down.third(1)
    for fetch in fetches:
        fetch.drain()


def attention_forward(parts, weights):
    fetches = [Fetch(weight.shape, 1 if i == 0 else 2) for i, weight in enumerate(weights)]
    sems = []
    for fetch in fetches:
        sems += fetch.scratch()
    hbm = pl.BlockSpec(memory_space=pl.ANY)
    tokens = SEGS * SEG
    vmem = pl.BlockSpec(memory_space=pltpu.VMEM)
    return pl.pallas_call(
        functools.partial(attention_kernel, fetches),
        out_shape=(
            jax.ShapeDtypeStruct((tokens, WIDE), BF16),
            jax.ShapeDtypeStruct((tokens, WIDE), F32),
        )
        + tuple(jax.ShapeDtypeStruct(weight.shape, BF16) for weight in weights),
        in_specs=[vmem] + [hbm] * len(weights),
        out_specs=(vmem, vmem) + (hbm,) * len(weights),
        scratch_shapes=[pltpu.VMEM((tokens, WIDE), BF16)] * 4
        + [
            pltpu.VMEM((TRUNK, 2 * SEG, KEYS), F32),
            pltpu.VMEM((SEG, WIDE), F32),
            pltpu.VMEM((2 * SEG, 128), F32),
            pltpu.VMEM((2 * SEG, 128), F32),
        ]
        + sems,
        compiler_params=pltpu.CompilerParams(
            vmem_limit_bytes=VMEM_BYTES, collective_id=4, has_side_effects=True
        ),
        cost_estimate=pl.CostEstimate(
            flops=152 * 2 * 4 * SEG * SEG * 128,
            bytes_accessed=tokens * WIDE * 12,
            transcendentals=152 * 2 * SEG * SEG,
        ),
        name="attention_forward",
    )(parts, *weights)


def add_rows(dst, dst_row, left, left_row, right, right_row, rows, step=32):
    def one(i, _):
        at = i * step
        total = left[pl.ds(pl.multiple_of(left_row + at, step), step), :].astype(F32)
        total += right[pl.ds(pl.multiple_of(right_row + at, step), step), :].astype(F32)
        dst[pl.ds(pl.multiple_of(dst_row + at, step), step), :] = total.astype(BF16)
        return 0

    lax.fori_loop(0, rows // step, one, 0)


class PairFold:
    def __init__(self, shape, x_first, pieces=1):
        self.rows, self.lanes = shape
        self.x_first = x_first
        self.pieces = pieces if x_first else 2

    def scratch(self):
        half, quarter = (self.rows // 2, self.lanes), (self.rows // 4, self.lanes)
        return (
            [pltpu.VMEM(half, BF16)] * 4
            + [pltpu.VMEM(quarter, BF16)] * (2 if self.x_first else 1)
            + [pltpu.VMEM(quarter if self.x_first else half, BF16)]
            + [pltpu.SemaphoreType.DMA((2,))] * 3
            + [pltpu.SemaphoreType.DMA((2, self.pieces))] * 2
            + [pltpu.SemaphoreType.DMA((self.pieces,))] * 2
        )

    def bind(self, parts, out, refs):
        self.parts, self.out = parts, out
        self.keep, self.land = refs[0:2], refs[2:4]
        count = 2 if self.x_first else 1
        self.x_land = refs[4 : 4 + count]
        (
            self.y_land,
            self.local,
            self.core_send,
            self.core_recv,
            self.x_send,
            self.x_recv,
            self.y_send,
            self.y_recv,
        ) = refs[4 + count :]
        self.x, self.core = lax.axis_index("x"), lax.axis_index("core")
        self.to_core = {"core": 1 - self.core}
        self.to_x = {"x": 1 - self.x}
        self.to_tensor = {"tensor": 1 - lax.axis_index("tensor")}
        self.half, self.quarter = self.rows // 2, self.rows // 4

    def rows_at(self, ref, row, rows):
        return ref.at[pl.ds(pl.multiple_of(row, 32), rows)]

    def remote(self, src, dst, send, recv, where):
        return pltpu.make_async_remote_copy(
            src_ref=src,
            dst_ref=dst,
            send_sem=send,
            recv_sem=recv,
            device_id=where,
            device_id_type=MESH,
        )

    def over_core(self, side):
        return self.remote(
            self.rows_at(self.parts[side], (1 - self.core) * self.half, self.half),
            self.land[side],
            self.core_send.at[side],
            self.core_recv.at[side],
            self.to_core,
        )

    def kept(self, side):
        return pltpu.make_async_copy(
            self.rows_at(self.parts[side], self.core * self.half, self.half),
            self.keep[side],
            self.local.at[side],
        )

    def over_x(self, side, piece):
        rows = self.quarter // self.pieces if self.x_first else self.quarter
        start = piece * rows if self.x_first else 0
        return self.remote(
            self.rows_at(self.keep[side], (1 - self.x) * self.quarter + start, rows),
            self.rows_at(self.x_land[side], start, rows),
            self.x_send.at[side, piece],
            self.x_recv.at[side, piece],
            self.to_x,
        )

    def over_tensor(self, piece):
        if self.x_first:
            rows = self.quarter // self.pieces
            source, target = self.x * self.quarter + piece * rows, piece * rows
        else:
            rows = self.quarter
            source = (1 - self.x if piece == 0 else self.x) * rows
            target = source
        return self.remote(
            self.rows_at(self.keep[1], source, rows),
            self.rows_at(self.y_land, target, rows),
            self.y_send.at[piece],
            self.y_recv.at[piece],
            self.to_tensor,
        )

    def start(self):
        for side in range(2):
            self.over_core(side).start()
            self.kept(side).start()

    def fold_core(self):
        for side in (1, 0):
            self.kept(side).wait()
            self.over_core(side).wait_recv()
            add_rows(self.keep[side], 0, self.keep[side], 0, self.land[side], 0, self.half)
        for piece in range(self.pieces):
            if self.x_first:
                self.over_x(1, piece).start()
                self.over_x(0, piece).start()
            else:
                self.over_tensor(piece).start()

    def second(self, piece):
        if self.x_first:
            rows = self.quarter // self.pieces
            at = self.x * self.quarter + piece * rows
            for side in (1, 0):
                self.over_x(side, piece).wait_recv()
                keep, land = self.keep[side], self.x_land[side]
                add_rows(keep, at, keep, at, land, piece * rows, rows)
                if side == 1:
                    self.over_tensor(piece).start()
        else:
            at = (1 - self.x if piece == 0 else self.x) * self.quarter
            self.over_tensor(piece).wait_recv()
            add_rows(self.keep[0], at, self.keep[0], at, self.y_land, at, self.quarter)
            if piece == 0:
                self.over_x(0, 0).start()

    def third(self, piece):
        if self.x_first:
            rows = self.quarter // self.pieces
            self.over_tensor(piece).wait_recv()
            at = self.x * self.quarter + piece * rows
            add_rows(self.out, piece * rows, self.keep[0], at, self.y_land, piece * rows, rows)
        elif piece == 0:
            self.over_x(0, 0).wait_recv()
            at = self.x * self.quarter
            add_rows(self.out, 0, self.keep[0], at, self.x_land[0], 0, self.quarter)

    def drain(self):
        for side in range(2):
            self.over_core(side).wait_send()
        for piece in range(self.pieces):
            if self.x_first:
                self.over_x(0, piece).wait_send()
                self.over_x(1, piece).wait_send()
            self.over_tensor(piece).wait_send()
        if not self.x_first:
            self.over_x(0, 0).wait_send()


def swap_halves(values, low):
    return jnp.where(
        low, pltpu.roll(values, WIDE - DH // 2, 1), pltpu.roll(values, DH // 2, 1)
    )


def attention_back_kernel(folds, *refs):
    parts, upstream, attended, logsum, cosine, sine = refs[:6]
    pair_grad, down_grad, output_grad = refs[6:9]
    refs = refs[9:]
    split, hidden = folds[0].lanes, folds[1].rows
    inner = folds[3].rows
    sides = [pair_grad.at[:, pl.ds(0, split)], pair_grad.at[:, pl.ds(2 * split, split)]]
    sides += [down_grad.at[pl.ds(0, hidden)], down_grad.at[pl.ds(hidden, hidden)]]
    sides += [pair_grad.at[:, pl.ds(split, split)], pair_grad.at[:, pl.ds(3 * split, split)]]
    sides += [output_grad.at[pl.ds(0, inner)], output_grad.at[pl.ds(inner, inner)]]
    out, sums, refs = refs[0], refs[1 : 1 + len(folds)], refs[1 + len(folds) :]
    qr, kr, vr, kt, dk, dv, dqt = refs[:7]
    refs = refs[7:]
    for i, fold in enumerate(folds):
        size = len(fold.scratch())
        fold.bind(sides[2 * i : 2 * i + 2], sums[i], refs[:size])
        refs = refs[size:]
    gate, down, up, output = folds
    barrier = pltpu.get_barrier_semaphore()
    for target in (gate.to_core, gate.to_x, gate.to_tensor):
        pl.semaphore_signal(barrier, inc=1, device_id=target, device_id_type=MESH)
    pl.semaphore_wait(barrier, 3)
    for fold in folds:
        fold.start()
    call = functools.partial
    leaf_plan = {
        2: [gate.fold_core, up.fold_core],
        3: [down.fold_core, output.fold_core],
    }
    branch_plan = {3: [call(gate.second, 0), call(up.second, 0), call(output.second, 0)]}
    trunk_plan = {5: [call(up.second, 1), call(output.second, 1)]}
    lane = lax.broadcasted_iota(jnp.int32, (SEG, WIDE), 1)
    first = lane < DH
    low = (lane % DH) < (DH // 2)

    def sort(i, _):
        here = source = segment(i)
        qr[here, :] = parts[source, 0:WIDE] * jnp.asarray(DH**-0.5, BF16)
        key = parts[source, WIDE : 2 * WIDE]
        kr[here, :] = key
        kt[:, here] = key.T
        vr[here, :] = parts[source, 2 * WIDE : 3 * WIDE]
        return 0

    lax.fori_loop(0, SEGS, sort, 0)
    dk[...] = jnp.zeros_like(dk)
    dv[...] = jnp.zeros_like(dv)
    key_at = lax.broadcasted_iota(jnp.int32, (SEG, 2 * SEG), 0)
    query_at = lax.broadcasted_iota(jnp.int32, (SEG, 2 * SEG), 1)
    causal = key_at <= jnp.where(query_at >= SEG, query_at - SEG, query_at)

    def rope_back(values, depth):
        at = segment(depth)
        return values * cosine[at, :] - swap_halves(values, low) * sine[at, :]

    def query(index, depth, count_big, big, extra):
        here = segment(index)
        queries = heads_apart(qr[segment(index), :], first)
        up = upstream[here, :]
        ups = heads_apart(up, first)
        turned = logsum[segment(index), :].T
        log = jnp.concatenate([turned[0:1, :], turned[DH : DH + 1, :]], axis=1)
        product = (up.astype(F32) * attended[here, :].astype(F32)).T
        inner = jnp.concatenate(
            [
                jnp.sum(product[:DH], axis=0, keepdims=True),
                jnp.sum(product[DH:], axis=0, keepdims=True),
            ],
            axis=1,
        )
        dqt[...] = jnp.zeros_like(dqt)

        def add(keys, mask=None):
            weights = jnp.exp(nt(kr[keys, :], queries) - log)
            if mask is not None:
                weights = jnp.where(mask, weights, 0.0)
            back = (weights * (nt(vr[keys, :], ups) - inner)).astype(BF16)
            dv[keys, :] += nn(weights.astype(BF16), ups)
            dk[keys, :] += nn(back, queries)
            dqt[...] += nn(kt[:, keys], back)

        add(segment(index), causal)
        for other in extra:
            add(segment(other))

        def use(c, _):
            add(pl.ds(pl.multiple_of(c * big, big), big))
            return 0

        lax.fori_loop(0, count_big, use, 0)
        both = jnp.concatenate([dqt[:DH, :SEG], dqt[DH:, SEG:]], axis=0) * (DH**-0.5)
        out[here, 0:WIDE] = rope_back(both.T, depth).astype(BF16)

    def leaf(i, _):
        at_step(i, leaf_plan)
        query(TRUNK + BRANCH + i, TRUNK + 1, TRUNK * SEG // KEYS, KEYS, [TRUNK + i // LEAVES])
        return 0

    def branch(i, _):
        at_step(i, branch_plan)
        query(TRUNK + i, TRUNK, TRUNK * SEG // KEYS, KEYS, [])
        return 0

    def trunk(i, _):
        at_step(i, trunk_plan)
        query(i, i, i, SEG, [])
        return 0

    lax.fori_loop(0, BRANCH * LEAVES, leaf, 0)
    lax.fori_loop(0, BRANCH, branch, 0)
    lax.fori_loop(0, TRUNK, trunk, 0)

    down.second(0)

    def settle(i, _):
        here = segment(i)
        depth = jnp.where(i < TRUNK + BRANCH, jnp.minimum(i, TRUNK), TRUNK + 1)
        out[here, WIDE : 2 * WIDE] = rope_back(dk[here, :], depth).astype(BF16)
        out[here, 2 * WIDE : 3 * WIDE] = dv[here, :].astype(BF16)
        return 0

    lax.fori_loop(0, SEGS, settle, 0)
    for fold in (gate, up, output, down):
        fold.third(0)
    for fold in folds:
        fold.drain()


def attention_backward(parts, upstream, attended, logsum, cosine, sine, grads, shapes):
    tokens = SEGS * SEG
    vmem = pl.BlockSpec(memory_space=pltpu.VMEM)
    folds = [PairFold(shape, i < 2) for i, shape in enumerate(shapes)]
    scratch = []
    for fold in folds:
        scratch += fold.scratch()
    return pl.pallas_call(
        functools.partial(attention_back_kernel, folds),
        out_shape=(jax.ShapeDtypeStruct((tokens, 3 * WIDE), BF16),)
        + tuple(jax.ShapeDtypeStruct((fold.rows // 4, fold.lanes), BF16) for fold in folds),
        in_specs=[vmem] * 6 + [pl.BlockSpec(memory_space=pl.ANY)] * len(grads),
        out_specs=(vmem,) * (1 + len(folds)),
        scratch_shapes=[pltpu.VMEM((tokens, WIDE), BF16)] * 3
        + [pltpu.VMEM((WIDE, tokens), BF16)]
        + [pltpu.VMEM((tokens, WIDE), F32)] * 2
        + [pltpu.VMEM((WIDE, 2 * SEG), F32)]
        + scratch,
        compiler_params=pltpu.CompilerParams(
            vmem_limit_bytes=VMEM_BYTES, collective_id=3, has_side_effects=True
        ),
        cost_estimate=pl.CostEstimate(
            flops=152 * 2 * 10 * SEG * SEG * 128,
            bytes_accessed=tokens * WIDE * 24,
            transcendentals=152 * 2 * SEG * SEG,
        ),
        name="attention_backward",
    )(
        parts,
        upstream,
        attended,
        logsum,
        cosine,
        sine,
        *grads,
    )


def angle_tables(positions):
    lane = jnp.arange(WIDE)
    freq = THETA ** (-(lane % (DH // 2)).astype(F32) * 2.0 / DH)
    angle = positions.astype(F32)[:, None] * freq[None, :]
    sign = jnp.where((lane % DH) < DH // 2, -1.0, 1.0)
    return jnp.cos(angle), jnp.sin(angle) * sign[None, :]


def neighbours():
    x, core = lax.axis_index("x"), lax.axis_index("core")
    others = []
    for step in (1, 2, 3):
        to_x = lax.rem(x + step // 2, 2)
        to_core = lax.rem(core + step % 2, 2)
        others.append((2 * to_x + to_core, {"x": to_x, "core": to_core}))
    return 2 * x + core, others


def greet(tensor_peer, others):
    barrier = pltpu.get_barrier_semaphore()
    for target in [tensor_peer] + [where for _, where in others]:
        pl.semaphore_signal(barrier, inc=1, device_id=target, device_id_type=MESH)
    pl.semaphore_wait(barrier, 1 + len(others))


def enter_kernel(
    mine,
    gain,
    query_w,
    key_w,
    value_w,
    cosine,
    sine,
    parts,
    low_out,
    theirs,
    ready,
    swap_send,
    swap_recv,
    part_send,
    part_recv,
):
    me, others = neighbours()
    tensor_peer = {"tensor": 1 - lax.axis_index("tensor")}
    greet(tensor_peer, others)
    steps = mine.shape[0] // SEG

    def exchange(i):
        return pltpu.make_async_remote_copy(
            src_ref=mine.at[segment(i)],
            dst_ref=theirs.at[segment(i)],
            send_sem=swap_send.at[i],
            recv_sem=swap_recv.at[i],
            device_id=tensor_peer,
            device_id_type=MESH,
        )

    def scatter(i, at):
        place, where = others[at]
        return pltpu.make_async_remote_copy(
            src_ref=ready.at[place, segment(i)],
            dst_ref=parts.at[me, segment(i)],
            send_sem=part_send.at[i, at],
            recv_sem=part_recv.at[i, at],
            device_id=where,
            device_id_type=MESH,
        )

    for i in range(steps):
        exchange(i).start()
    low = (lax.broadcasted_iota(jnp.int32, (SEG, WIDE), 1) % DH) < (DH // 2)

    def step(i, _):
        here = segment(i)
        exchange(i).wait_recv()
        total = mine[here, :].astype(F32) + theirs[here, :].astype(F32)
        scale = lax.rsqrt(jnp.mean(total * total, axis=-1, keepdims=True) + EPSILON)
        rounded = (total * scale * gain[...]).astype(BF16)
        low_out[here, :] = rounded
        for at, weight in enumerate((query_w, key_w, value_w)):
            raw = nn(rounded, weight[...])
            for peer in range(ready.shape[0]):
                part = raw[:, peer * WIDE : (peer + 1) * WIDE]
                if at < 2:
                    part = part * cosine[here, :] + swap_halves(part, low) * sine[here, :]
                ready[peer, here, at * WIDE : (at + 1) * WIDE] = part.astype(BF16)
        for at in range(len(others)):
            scatter(i, at).start()
        parts[me, here, :] = ready[me, here, :]
        return 0

    lax.fori_loop(0, steps, step, 0)

    def finish(i, _):
        exchange(i).wait_send()
        for at in range(len(others)):
            scatter(i, at).wait()
        return 0

    lax.fori_loop(0, steps, finish, 0)


def enter(mine, gain, query_w, key_w, value_w, cosine, sine):
    rows, width = mine.shape
    inner = query_w.shape[1]
    peers = inner // WIDE
    steps = rows // SEG
    vmem = pl.BlockSpec(memory_space=pltpu.VMEM)
    return pl.pallas_call(
        enter_kernel,
        out_shape=(
            jax.ShapeDtypeStruct((peers, rows, 3 * WIDE), BF16),
            jax.ShapeDtypeStruct((rows, width), BF16),
            jax.ShapeDtypeStruct((rows, width), BF16),
        ),
        in_specs=[vmem] * 7,
        out_specs=(vmem,) * 3,
        scratch_shapes=[
            pltpu.VMEM((peers, rows, 3 * WIDE), BF16),
            pltpu.SemaphoreType.DMA((steps,)),
            pltpu.SemaphoreType.DMA((steps,)),
            pltpu.SemaphoreType.DMA((steps, 3)),
            pltpu.SemaphoreType.DMA((steps, 3)),
        ],
        compiler_params=pltpu.CompilerParams(
            vmem_limit_bytes=VMEM_BYTES, collective_id=0, has_side_effects=True
        ),
        cost_estimate=pl.CostEstimate(
            flops=2 * rows * width * 3 * inner,
            bytes_accessed=200 << 20,
            transcendentals=rows,
        ),
        name="enter",
    )(mine, gain, query_w, key_w, value_w, cosine, sine)


def middle_kernel(
    meta,
    adapted,
    heads,
    cotangent,
    second_gain,
    third_gain,
    fourth_gain,
    wo_own,
    wg_own,
    wu_own,
    wd_own,
    wo_other,
    wg_other,
    wu_other,
    wd_other,
    layer_out,
    middle_out,
    attended_out,
    attention_out,
    third_out,
    mixed_out,
    hidden_out,
    pair_out,
    heads_back,
    gains_out,
    wo,
    wg,
    wu,
    wd,
    gate_s,
    up_s,
    sums,
    sem,
):
    step = pl.program_id(0)
    tensor = meta[0]
    copies = []

    def copy(src, weight, row, lane):
        rows, lanes = src.shape
        dst = weight.at[pl.ds(row, rows), pl.ds(lane, lanes)]
        copies.append(pltpu.make_async_copy(src, dst, sem.at[len(copies)]))

    for weight, own, other, by_lane in (
        (wo, wo_own, wo_other, False),
        (wg, wg_own, wg_other, True),
        (wu, wu_own, wu_other, True),
        (wd, wd_own, wd_other, False),
    ):
        rows, lanes = own.shape
        copy(own, weight, 0, 0)
        copy(other, weight, 0 if by_lane else rows, lanes if by_lane else 0)

    @pl.when(step == 0)
    def _():
        for copy in copies:
            copy.start()
        gains_out[...] = jnp.zeros_like(gains_out)
        for copy in copies[:2]:
            copy.wait()

    groups = heads.shape[0] // 2
    for side in range(2):
        for group in range(groups):
            at = (side * groups + group) * WIDE
            source = group * 2 + (tensor if side == 0 else 1 - tensor)
            attended_out[:, at : at + WIDE] = heads[source]
    attention = nn(attended_out[...], wo[...])

    def scaling(values):
        return lax.rsqrt(jnp.mean(values * values, axis=-1, keepdims=True) + EPSILON)

    def inward(upstream, gain, normed, scale):
        scaled = upstream * gain
        return scale * (scaled - normed * jnp.mean(scaled * normed, axis=-1, keepdims=True))

    second_scale = scaling(attention)
    second_normed = attention * second_scale
    middle = adapted[...] + second_normed * second_gain[...]
    third_scale = scaling(middle)
    third_normed = middle * third_scale
    third_out[...] = (third_normed * third_gain[...]).astype(BF16)

    @pl.when(step == 0)
    def _():
        for copy in copies[2:]:
            copy.wait()

    sums[...] = jnp.zeros_like(sums)

    def forward(c, _):
        cut = pl.ds(pl.multiple_of(c * HIDDEN, HIDDEN), HIDDEN)
        gate = nn(third_out[...], wg[:, cut])
        upward = nn(third_out[...], wu[:, cut])
        gate_s[c] = gate
        up_s[c] = upward
        hidden = (gate / (1.0 + jnp.exp(-gate)) * upward).astype(BF16)
        hidden_out[:, cut] = hidden
        sums[...] += nn(hidden, wd[cut, :])
        return 0

    lax.fori_loop(0, gate_s.shape[0], forward, 0)
    mixed = sums[...]
    fourth_scale = scaling(mixed)
    fourth_normed = mixed * fourth_scale
    layer_out[...] = (middle + fourth_normed * fourth_gain[...]).astype(BF16)
    upstream = cotangent[...].astype(F32)
    gains_out[2:3, :] += jnp.sum(upstream * fourth_normed, axis=0, keepdims=True)
    mixed_out[...] = inward(upstream, fourth_gain[...], fourth_normed, fourth_scale).astype(BF16)
    sums[...] = jnp.zeros_like(sums)
    side_units = wg_own.shape[1] // 128

    def backward(c, _):
        cut = pl.ds(pl.multiple_of(c * HIDDEN, HIDDEN), HIDDEN)
        back = nt(mixed_out[...], wd[cut, :]).astype(BF16).astype(F32)
        gate = gate_s[c]
        sigmoid = 1.0 / (1.0 + jnp.exp(-gate))
        silu = gate * sigmoid
        gate_back = (back * up_s[c] * (sigmoid + silu * (1.0 - sigmoid))).astype(BF16)
        up_back = (back * silu).astype(BF16)
        for piece in range(HIDDEN // 128):
            unit = c * (HIDDEN // 128) + piece
            unit = jnp.where(unit < side_units, unit, unit + side_units)
            lanes = slice(piece * 128, (piece + 1) * 128)
            pair_out[:, pl.ds(pl.multiple_of(unit * 128, 128), 128)] = gate_back[:, lanes]
            unit += side_units
            pair_out[:, pl.ds(pl.multiple_of(unit * 128, 128), 128)] = up_back[:, lanes]
        sums[...] += nt(gate_back, wg[:, cut]) + nt(up_back, wu[:, cut])
        return 0

    lax.fori_loop(0, gate_s.shape[0], backward, 0)
    third_back = sums[...]
    gains_out[1:2, :] += jnp.sum(third_back * third_normed, axis=0, keepdims=True)
    middle_back = upstream + inward(third_back, third_gain[...], third_normed, third_scale)
    middle_out[...] = middle_back
    gains_out[0:1, :] += jnp.sum(middle_back * second_normed, axis=0, keepdims=True)
    attention_out[...] = inward(
        middle_back, second_gain[...], second_normed, second_scale
    ).astype(BF16)
    heads_low = nt(attention_out[...], wo[...]).astype(BF16)
    for side in range(2):
        for group in range(groups):
            at = (side * groups + group) * WIDE
            target = group * 2 + (tensor if side == 0 else 1 - tensor)
            heads_back[target] = heads_low[:, at : at + WIDE]


def middle_section(meta, adapted, heads, cotangent, gains, weights):
    rows, width = adapted.shape
    sources = heads.shape[0]
    inner = sources * WIDE
    hidden = 2 * weights[1].shape[1]
    block = rows // 2
    steps = rows // block
    row = pl.BlockSpec((block, width), lambda i, meta: (i, 0))
    wide = pl.BlockSpec((block, hidden), lambda i, meta: (i, 0))
    head = pl.BlockSpec((sources, block, WIDE), lambda i, meta: (0, i, 0))
    gain = pl.BlockSpec((1, width), lambda i, meta: (0, 0))
    hbm = pl.BlockSpec(memory_space=pl.ANY)
    return pl.pallas_call(
        middle_kernel,
        grid_spec=pltpu.PrefetchScalarGridSpec(
            num_scalar_prefetch=1,
            grid=(steps,),
            in_specs=[
                row,
                head,
                pl.BlockSpec((block, width), lambda i, meta: (meta[0] * steps + i, 0)),
                gain,
                gain,
                gain,
            ]
            + [hbm] * 8,
            out_specs=(
                row,
                row,
                pl.BlockSpec((block, inner), lambda i, meta: (i, 0)),
                row,
                row,
                row,
                wide,
                pl.BlockSpec((block, 2 * hidden), lambda i, meta: (i, 0)),
                head,
                pl.BlockSpec((8, width), lambda i, meta: (0, 0)),
            ),
            scratch_shapes=[
                pltpu.VMEM((inner, width), BF16),
                pltpu.VMEM((width, hidden), BF16),
                pltpu.VMEM((width, hidden), BF16),
                pltpu.VMEM((hidden, width), BF16),
                pltpu.VMEM((hidden // HIDDEN, block, HIDDEN), F32),
                pltpu.VMEM((hidden // HIDDEN, block, HIDDEN), F32),
                pltpu.VMEM((block, width), F32),
                pltpu.SemaphoreType.DMA((8,)),
            ],
        ),
        out_shape=(
            jax.ShapeDtypeStruct((rows, width), BF16),
            jax.ShapeDtypeStruct((rows, width), F32),
            jax.ShapeDtypeStruct((rows, inner), BF16),
            jax.ShapeDtypeStruct((rows, width), BF16),
            jax.ShapeDtypeStruct((rows, width), BF16),
            jax.ShapeDtypeStruct((rows, width), BF16),
            jax.ShapeDtypeStruct((rows, hidden), BF16),
            jax.ShapeDtypeStruct((rows, 2 * hidden), BF16),
            jax.ShapeDtypeStruct((sources, rows, WIDE), BF16),
            jax.ShapeDtypeStruct((8, width), F32),
        ),
        compiler_params=pltpu.CompilerParams(vmem_limit_bytes=VMEM_BYTES),
        cost_estimate=pl.CostEstimate(
            flops=rows * width * (4 * inner + 12 * hidden),
            bytes_accessed=6 * width * hidden + 2 * width * inner + rows * (hidden * 6 + width * 20),
            transcendentals=rows * hidden * 2,
        ),
        name="middle_section",
    )(meta, adapted, heads, cotangent, *gains, *weights)


class Reduction:
    def __init__(self, shape, by_lane=False, kind="all", cuts=None):
        self.rows, self.lanes = shape
        self.by_lane = by_lane
        self.kind = kind
        self.cuts = cuts or [self.lanes]

    def chunk_shape(self, dp):
        rows, lanes = self.rows // 4, self.lanes
        return (rows, lanes // dp) if self.by_lane else (rows // dp, lanes)

    def outputs(self, dp):
        if self.kind == "sum":
            return [jax.ShapeDtypeStruct(self.chunk_shape(dp), BF16)]
        return [jax.ShapeDtypeStruct((self.rows, lanes), F32) for lanes in self.cuts]

    def scratch(self, dp):
        rows, lanes = self.rows, self.lanes
        half, quarter = pltpu.VMEM((rows // 2, lanes), BF16), pltpu.VMEM((rows // 4, lanes), BF16)
        dma = pltpu.SemaphoreType.DMA
        refs = {}
        if self.kind == "all":
            refs.update(half=half, core_land=half, x_land=quarter)
            refs.update(fold_send=dma((2,)), fold_recv=dma((2,)))
        if self.kind != "gather":
            refs.update(
                quarter=quarter,
                z_land=pltpu.VMEM((dp + 1,) + self.chunk_shape(dp), BF16),
                sum_send=dma((dp,)),
                sum_recv=dma((dp + 1,)),
            )
        if self.kind != "sum":
            refs.update(
                whole=quarter,
                others=pltpu.VMEM((3, rows // 4, lanes), BF16),
                send=dma((3,)),
                recv=dma((3,)),
                all_send=dma((2, dp)),
                all_recv=dma((dp,)),
                out_sem=dma((len(self.cuts),)),
            )
            for i, cut in enumerate(self.cuts):
                refs[f"wide{i}"] = pltpu.VMEM((rows // 4, cut), F32)
        self.names = list(refs)
        return list(refs.values())

    def bind(self, part, outs, refs):
        self.part, self.outs = part, outs
        for name, ref in zip(self.names, refs):
            setattr(self, name, ref)
        self.wide = [getattr(self, f"wide{i}", None) for i in range(len(self.cuts))]
        self.x, self.core, self.z = (lax.axis_index(name) for name in ("x", "core", "dp"))
        self.dp = lax.axis_size("dp")
        self.to_core = {"core": 1 - self.core}
        self.to_x = {"x": 1 - self.x}
        self.sends = []

    def copy(self, src, dst, send, recv, where):
        return pltpu.make_async_remote_copy(
            src_ref=src,
            dst_ref=dst,
            send_sem=send,
            recv_sem=recv,
            device_id=where,
            device_id_type=MESH,
        )

    def part_of(self, ref, index, rows):
        return ref.at[pl.ds(pl.multiple_of(index * rows, rows), rows)]

    def chunk(self, ref, index):
        if self.by_lane:
            lanes = self.lanes // self.dp
            return ref.at[:, pl.ds(pl.multiple_of(index * lanes, lanes), lanes)]
        return self.part_of(ref, index, self.rows // 4 // self.dp)

    def core_sum(self):
        half = self.rows // 2
        return self.copy(
            self.part_of(self.part, 1 - self.core, half),
            self.core_land,
            self.fold_send.at[0],
            self.fold_recv.at[0],
            self.to_core,
        )

    def x_sum(self):
        quarter = self.rows // 4
        return self.copy(
            self.part_of(self.half, 1 - self.x, quarter),
            self.x_land,
            self.fold_send.at[1],
            self.fold_recv.at[1],
            self.to_x,
        )

    def z_sum(self, j, step):
        up = {"dp": self.z + step}
        index = j
        lands = index if step > 0 else jnp.where(self.z - 1 == index, self.dp, index)
        return self.copy(
            self.chunk(self.quarter, index),
            self.z_land.at[lands],
            self.sum_send.at[index],
            self.sum_recv.at[lands],
            up,
        )

    def z_all(self, j, step):
        return self.copy(
            self.chunk(self.whole, j),
            self.chunk(self.whole, j),
            self.all_send.at[0 if step > 0 else 1, j],
            self.all_recv.at[j],
            {"dp": self.z + step},
        )

    def spread(self, which):
        src = self.others.at[0] if which == 2 else self.whole
        return self.copy(
            src,
            self.others.at[which],
            self.send.at[which],
            self.recv.at[which],
            self.to_x if which == 0 else self.to_core,
        )

    def writes(self, at):
        quarter = self.rows // 4
        core = self.core if at < 2 else 1 - self.core
        x = self.x if at % 2 == 0 else 1 - self.x
        row = pl.multiple_of((2 * core + x) * quarter, quarter)
        return [
            pltpu.make_async_copy(wide, out.at[pl.ds(row, quarter)], self.out_sem.at[i])
            for i, (wide, out) in enumerate(zip(self.wide, self.outs))
        ]

    def emit(self, at, ref):
        if at > 0:
            for copy in self.writes(at - 1):
                copy.wait()
        lane = 0
        for wide, lanes in zip(self.wide, self.cuts):
            wide[...] = ref[:, lane : lane + lanes].astype(F32)
            lane += lanes
        for copy in self.writes(at):
            copy.start()

    def add(self, into, left, right):
        into[...] = (left[...].astype(F32) + right[...].astype(F32)).astype(BF16)

    def hop(self, h):
        last = self.dp - 1

        @pl.when(self.z == h)
        def _():
            for j in range(last, h, -1):
                if h > 0:
                    self.wait_sum(j)
                    self.add(self.chunk(self.quarter, j), self.chunk(self.quarter, j), self.z_land.at[j])
                self.z_sum(j, 1).start()

        @pl.when(self.z == last - h)
        def _():
            for j in range(0, last - h):
                if h > 0:
                    self.wait_sum(j)
                    self.add(self.chunk(self.quarter, j), self.chunk(self.quarter, j), self.z_land.at[j])
                self.z_sum(j, -1).start()

    def wait_sum(self, lands):
        self.copy(
            self.z_land.at[lands],
            self.z_land.at[lands],
            self.sum_send.at[0],
            self.sum_recv.at[lands],
            self.to_x,
        ).wait_recv()

    def all_hop(self, h):
        z, last = self.z, self.dp - 1
        low, high = jnp.maximum(z - h, 0), jnp.minimum(z + h, last)

        @pl.when(z >= h)
        def _():
            self.z_all(low, 1).wait_recv()

        @pl.when((z >= h) & (z < last))
        def _():
            self.z_all(low, 1).start()

        @pl.when(z <= last - h)
        def _():
            self.z_all(high, -1).wait_recv()

        @pl.when((z <= last - h) & (z > 0))
        def _():
            self.z_all(high, -1).start()

    def stages(self):
        def start():
            self.core_sum().start()

        def fold_core():
            self.core_sum().wait_recv()
            self.add(
                self.half, self.part_of(self.part, self.core, self.rows // 2), self.core_land
            )
            self.x_sum().start()

        def begin():
            self.quarter[...] = self.part[...]
            self.hop(0)

        def fold_x():
            self.x_sum().wait_recv()
            self.add(
                self.quarter, self.part_of(self.half, self.x, self.rows // 4), self.x_land
            )
            self.hop(0)

        def settle():
            z, last = self.z, self.dp - 1
            mine = self.chunk(self.quarter, z)

            @pl.when(z > 0)
            def _():
                self.wait_sum(z)
                self.add(mine, mine, self.z_land.at[z])

            @pl.when(z < last)
            def _():
                self.wait_sum(self.dp)
                self.add(mine, mine, self.z_land.at[self.dp])

            if self.kind == "sum":
                self.outs[0][...] = mine[...]
            else:
                self.chunk(self.whole, z)[...] = mine[...]
                gather()

        def place():
            self.chunk(self.whole, self.z)[...] = self.part[...]
            gather()

        def gather():
            z, last = self.z, self.dp - 1

            @pl.when(z < last)
            def _():
                self.z_all(z, 1).start()

            @pl.when(z > 0)
            def _():
                self.z_all(z, -1).start()

        def share():
            self.all_hop(self.dp - 1)
            self.spread(0).start()
            self.spread(1).start()
            self.emit(0, self.whole)

        def pass_on():
            self.spread(0).wait_recv()
            self.spread(2).start()
            self.emit(1, self.others.at[0])

        def last():
            self.spread(1).wait_recv()
            self.emit(2, self.others.at[1])
            self.spread(2).wait_recv()
            self.emit(3, self.others.at[2])

        sums = [functools.partial(self.hop, h) for h in range(1, self.dp - 1)] + [settle]
        gathers = [functools.partial(self.all_hop, h) for h in range(1, self.dp - 1)]
        gathers += [share, pass_on, last]
        return {
            "all": [start, fold_core, fold_x] + sums + gathers,
            "sum": [begin] + sums,
            "gather": [place] + gathers,
        }[self.kind]

    def drain(self):
        z, last = self.z, self.dp - 1
        if self.kind == "all":
            self.core_sum().wait_send()
            self.x_sum().wait_send()
        if self.kind != "gather":
            for j in range(self.dp):

                @pl.when(z < j)
                def _():
                    self.z_sum(j, 1).wait_send()

                @pl.when(z > j)
                def _():
                    self.z_sum(j, -1).wait_send()

        if self.kind == "sum":
            return
        for j in range(self.dp):

            @pl.when((z >= j) & (z < last))
            def _():
                self.z_all(j, 1).wait_send()

            @pl.when((z <= j) & (z > 0))
            def _():
                self.z_all(j, -1).wait_send()

        for which in range(3):
            self.spread(which).wait_send()
        for copy in self.writes(3):
            copy.wait()


def bind_all(items, parts, outs, scratch):
    dp = lax.axis_size("dp")
    for item, part in zip(items, parts):
        size = len(item.scratch(dp))
        item.bind(part, outs[: len(item.cuts)], scratch[:size])
        outs, scratch = outs[len(item.cuts) :], scratch[size:]


def waves(plans):
    length = max(len(plan) + i for i, plan in enumerate(plans))
    return [
        [plan[t - i] for i, plan in enumerate(plans) if 0 <= t - i < len(plan)]
        for t in range(length)
    ]


def greet_line(barrier):
    z, last = lax.axis_index("dp"), lax.axis_size("dp") - 1

    @pl.when(z > 0)
    def _():
        pl.semaphore_signal(barrier, inc=1, device_id={"dp": z - 1}, device_id_type=MESH)

    @pl.when(z < last)
    def _():
        pl.semaphore_signal(barrier, inc=1, device_id={"dp": z + 1}, device_id_type=MESH)

    return jnp.minimum(z, 1) + jnp.minimum(last - z, 1)


LEAVE = 128


def leave_kernel(items, *refs):
    sent, adapted, middle_back, gain, query_w, key_w, value_w = refs[:7]
    parts, refs = refs[7 : 7 + len(items)], refs[7 + len(items) :]
    joined, adapted_low, gain_out = refs[:3]
    count = sum(len(item.cuts) for item in items)
    outs, refs = refs[3 : 3 + count], refs[3 + count :]
    landed, away, away_landed = refs[:3]
    part_send, part_recv, away_send, away_recv, low_send, low_recv = refs[3:9]
    bind_all(items, parts, outs, refs[9:])
    plans = [item.stages() for item in items]
    stages = list(zip(*plans))
    away_plan = {0: stages[0]}
    home_plan = {1: stages[1], 4: stages[2]}
    me, others = neighbours()
    tensor = lax.axis_index("tensor")
    tensor_peer = {"tensor": 1 - tensor}
    barrier = pltpu.get_barrier_semaphore()
    for target in [tensor_peer] + [where for _, where in others]:
        pl.semaphore_signal(barrier, inc=1, device_id=target, device_id_type=MESH)
    pl.semaphore_wait(barrier, 1 + len(others) + greet_line(barrier))
    half = adapted.shape[0]
    inner = query_w.shape[1]
    steps = half // LEAVE

    def block(start, i):
        return pl.ds(pl.multiple_of(start + i * LEAVE, LEAVE), LEAVE)

    def gather(side, i, at):
        here = block((tensor if side else 1 - tensor) * half, i)
        place, where = others[at]
        return pltpu.make_async_remote_copy(
            src_ref=sent.at[place, here],
            dst_ref=landed.at[me, here],
            send_sem=part_send.at[side, i, at],
            recv_sem=part_recv.at[side, i, at],
            device_id=where,
            device_id_type=MESH,
        )

    def hand_over(i):
        return pltpu.make_async_remote_copy(
            src_ref=away.at[block(0, i)],
            dst_ref=away_landed.at[block(0, i)],
            send_sem=away_send.at[i],
            recv_sem=away_recv.at[i],
            device_id=tensor_peer,
            device_id_type=MESH,
        )

    def share(i):
        here = block(tensor * half, i)
        return pltpu.make_async_remote_copy(
            src_ref=adapted_low.at[here],
            dst_ref=adapted_low.at[here],
            send_sem=low_send.at[i],
            recv_sem=low_recv.at[i],
            device_id=tensor_peer,
            device_id_type=MESH,
        )

    for side in range(2):

        def begin(i, _):
            for at in range(len(others)):
                gather(side, i, at).start()
            return 0

        lax.fori_loop(0, steps, begin, 0)
    landed[me] = sent[me]
    gain_out[...] = jnp.zeros_like(gain_out)

    def input_grad(side, i):
        for at in range(len(others)):
            gather(side, i, at).wait_recv()
        here = block((tensor if side else 1 - tensor) * half, i)
        for at in range(3):
            for group in range(landed.shape[0]):
                to = at * inner + group * WIDE
                joined[here, to : to + WIDE] = landed[group, here, at * WIDE : (at + 1) * WIDE]
        total = nt(joined[here, 0:inner], query_w[...])
        total += nt(joined[here, inner : 2 * inner], key_w[...])
        total += nt(joined[here, 2 * inner : 3 * inner], value_w[...])
        return total

    def away_step(i, _):
        away[block(0, i), :] = input_grad(0, i).astype(BF16)
        hand_over(i).start()
        at_step(i, away_plan)
        return 0

    lax.fori_loop(0, steps, away_step, 0)

    def home_step(i, _):
        total = input_grad(1, i)
        hand_over(i).wait_recv()
        rows = block(0, i)
        upstream = total + away_landed[rows, :].astype(F32)
        values = adapted[rows, :]
        scale = lax.rsqrt(jnp.mean(values * values, axis=-1, keepdims=True) + EPSILON)
        normed = values * scale
        scaled = upstream * gain[...]
        inward = scale * (scaled - normed * jnp.mean(scaled * normed, axis=-1, keepdims=True))
        gain_out[0:1, :] += jnp.sum(upstream * normed, axis=0, keepdims=True)
        adapted_low[block(tensor * half, i), :] = (middle_back[rows, :] + inward).astype(BF16)
        share(i).start()
        at_step(i, home_plan)
        return 0

    lax.fori_loop(0, steps, home_step, 0)
    for call in stages[3]:
        call()
    for item in items:
        item.drain()

    def finish(i, _):
        for side in range(2):
            for at in range(len(others)):
                gather(side, i, at).wait_send()
        hand_over(i).wait_send()
        share(i).wait()
        return 0

    lax.fori_loop(0, steps, finish, 0)


def leave(sent, adapted, middle_back, gain, query_w, key_w, value_w, parts, by_lanes):
    items = [
        Reduction((4 * part.shape[0], part.shape[1]), by_lane, "sum")
        for part, by_lane in zip(parts, by_lanes)
    ]
    dp = lax.axis_size("dp")
    scratch, outs = [], []
    for item in items:
        scratch += item.scratch(dp)
        outs += item.outputs(dp)
    peers, rows, lanes = sent.shape
    half, width = adapted.shape
    inner = query_w.shape[1]
    steps = half // LEAVE
    vmem = pl.BlockSpec(memory_space=pltpu.VMEM)
    return pl.pallas_call(
        functools.partial(leave_kernel, items),
        out_shape=(
            jax.ShapeDtypeStruct((rows, 3 * inner), BF16),
            jax.ShapeDtypeStruct((rows, width), BF16),
            jax.ShapeDtypeStruct((8, width), F32),
        )
        + tuple(outs),
        in_specs=[vmem] * (7 + len(items)),
        out_specs=(vmem,) * (3 + len(outs)),
        scratch_shapes=[
            pltpu.VMEM((peers, rows, lanes), BF16),
            pltpu.VMEM((half, width), BF16),
            pltpu.VMEM((half, width), BF16),
            pltpu.SemaphoreType.DMA((2, steps, 3)),
            pltpu.SemaphoreType.DMA((2, steps, 3)),
        ]
        + [pltpu.SemaphoreType.DMA((steps,))] * 4
        + scratch,
        compiler_params=pltpu.CompilerParams(
            vmem_limit_bytes=VMEM_BYTES, collective_id=1, has_side_effects=True
        ),
        cost_estimate=pl.CostEstimate(
            flops=2 * rows * width * 3 * inner, bytes_accessed=200 << 20, transcendentals=rows
        ),
        name="leave",
    )(sent, adapted, middle_back, gain, query_w, key_w, value_w, *parts)


def reduce_kernel(items, *refs):
    count = len(items)
    outs = sum(len(item.cuts) for item in items)
    bind_all(items, refs[:count], refs[count : count + outs], refs[count + outs :])
    barrier = pltpu.get_barrier_semaphore()
    for target in (items[0].to_core, items[0].to_x):
        pl.semaphore_signal(barrier, inc=1, device_id=target, device_id_type=MESH)
    pl.semaphore_wait(barrier, 2 + greet_line(barrier))
    plans = [item.stages() for item in items if item.kind == "all"]
    gathers = [item.stages() for item in items if item.kind == "gather"]
    for plan in plans:
        plan[0]()
    for plan in gathers:
        plan[0]()
    for plan in plans:
        plan[1]()
    for wave in waves([plan[2:] for plan in plans] + [plan[1:] for plan in gathers]):
        for call in wave:
            call()
    for item in items:
        item.drain()


def reduce_all(parts, chunks, shapes, by_lanes):
    dp = lax.axis_size("dp")
    items = [Reduction(part.shape) for part in parts]
    items += [Reduction(shape, by_lane, "gather") for shape, by_lane in zip(shapes, by_lanes)]
    scratch, outs = [], []
    for item in items:
        scratch += item.scratch(dp)
        outs += item.outputs(dp)
    moved = sum(item.rows * item.lanes for item in items)
    return pl.pallas_call(
        functools.partial(reduce_kernel, items),
        out_shape=tuple(outs),
        in_specs=[pl.BlockSpec(memory_space=pltpu.VMEM)] * len(items),
        out_specs=(pl.BlockSpec(memory_space=pl.ANY),) * len(outs),
        scratch_shapes=scratch,
        compiler_params=pltpu.CompilerParams(
            vmem_limit_bytes=VMEM_BYTES, collective_id=2, has_side_effects=True
        ),
        cost_estimate=pl.CostEstimate(
            flops=moved * 4, bytes_accessed=moved * 30, transcendentals=0
        ),
        name="reduce_all",
    )(*parts, *chunks)


def latent_kernel(low, weight, out):
    rows, inputs, lanes = low.shape[0], weight.shape[0], weight.shape[1]
    blocks = lanes // 128
    for at in range(inputs):
        values = nt(low[...], weight[at])
        for block in range(blocks):
            out[pl.ds(block * inputs + at, rows, stride=blocks * inputs), :] = values[
                :, block * 128 : (block + 1) * 128
            ]


def latent_grad(low, adapter):
    tokens, width = low.shape
    inputs, lanes, _ = adapter.shape
    blocks = lanes // 128
    step = SEG
    flat = pl.pallas_call(
        latent_kernel,
        grid=(tokens // step,),
        out_shape=jax.ShapeDtypeStruct((tokens * blocks * inputs, 128), F32),
        in_specs=[
            pl.BlockSpec((step, width), lambda i: (i, 0)),
            pl.BlockSpec(adapter.shape, lambda i: (0, 0, 0)),
        ],
        out_specs=pl.BlockSpec((step * blocks * inputs, 128), lambda i: (i, 0)),
        compiler_params=pltpu.CompilerParams(vmem_limit_bytes=VMEM_BYTES),
        cost_estimate=pl.CostEstimate(
            flops=2 * tokens * width * lanes * inputs,
            bytes_accessed=tokens * (2 * width + 4 * lanes * inputs) + 2 * width * lanes * inputs,
            transcendentals=0,
        ),
        name="latent_grad",
    )(low, adapter)
    flat = flat.reshape(tokens, blocks, inputs, 128)
    return flat.transpose(0, 2, 1, 3).reshape(tokens, inputs, lanes)


def swap(value, axis):
    return lax.ppermute(value, axis, [(0, 1), (1, 0)])


def together(*values):
    return lax.optimization_barrier(values)


def cut(value, index, rows):
    return lax.dynamic_slice_in_dim(value, index * rows, rows, 0)


def add_low(left, right):
    return (left.astype(F32) + right.astype(F32)).astype(BF16)


def fold(value, index, axis):
    half = value.shape[0] // 2
    return add_low(cut(value, index, half), swap(cut(value, 1 - index, half), axis))


def unfold(value, index, axis):
    other = swap(value, axis)
    return jnp.concatenate(
        [jnp.where(index == 0, value, other), jnp.where(index == 0, other, value)], axis=0
    )


def sum_small(value):
    for axis in ("tensor", "core", "x"):
        value = value + swap(value, axis)
    for pairs in ([(0, 1), (1, 0), (2, 3), (3, 2)], [(0, 2), (2, 0), (1, 3), (3, 1)]):
        value = value + lax.ppermute(value, "dp", pairs)
    return value


def tn(left, right):
    return lax.dot_general(
        left, right, (((0,), (0,)), ((), ())), preferred_element_type=F32
    ).astype(BF16)


def on_device_paired(
    latent_embed,
    adapter,
    first_gain,
    query_weight,
    key_weight,
    value_weight,
    output_weight,
    second_gain,
    third_gain,
    gate_weight,
    up_weight,
    down_weight,
    fourth_gain,
    parents,
    positions,
    cotangent,
):
    rows = latent_embed.shape[0]
    width = adapter.shape[2]
    half_rows = rows // 2
    tensor = lax.axis_index("tensor")
    core = lax.axis_index("core")
    x = lax.axis_index("x")
    everyone = ("x", "core", "tensor")
    meta = jnp.stack([tensor, core]).astype(jnp.int32)
    one_row = lambda gain: gain.reshape(1, -1)

    cosine, sine = angle_tables(positions)
    mine = jnp.einsum(
        "rcd,cde->re", latent_embed, adapter, preferred_element_type=F32
    ).astype(BF16)
    parts, first_low, theirs = enter(
        mine, one_row(first_gain), query_weight, key_weight, value_weight, cosine, sine
    )
    adapted = cut(mine, tensor, half_rows).astype(F32) + cut(theirs, tensor, half_rows).astype(
        F32
    )
    role, place, parts = sort_parts(parents, parts.reshape(-1, 3 * WIDE))
    own_weights = (output_weight, gate_weight, up_weight, down_weight)
    attended, logsum, *other_weights = attention_forward(parts, own_weights)
    heads = lax.all_to_all(
        pick(place, attended).reshape(8, half_rows, WIDE), everyone, 0, 0, tiled=False
    )
    (
        layer_half,
        middle_back,
        attended_all,
        attention_low,
        third_low,
        mixed_low,
        hidden,
        pair_low,
        heads_back,
        gain_parts,
    ) = middle_section(
        meta,
        adapted,
        heads,
        cotangent,
        (one_row(second_gain), one_row(third_gain), one_row(fourth_gain)),
        own_weights + tuple(other_weights),
    )
    upstream = lax.all_to_all(heads_back, everyone, 0, 0, tiled=False).reshape(-1, WIDE)
    layer_other = swap(layer_half, "tensor")
    layer_out = jnp.concatenate(
        [
            jnp.where(tensor == 0, layer_half, layer_other),
            jnp.where(tensor == 0, layer_other, layer_half),
        ],
        axis=0,
    ).astype(F32)

    inner = output_weight.shape[0]
    grads = (
        tn(third_low, pair_low),
        tn(hidden, mixed_low),
        tn(attended_all, attention_low),
    )
    shapes = [gate_weight.shape, down_weight.shape, up_weight.shape, output_weight.shape]

    table_cosine, table_sine = angle_tables(jnp.arange((TRUNK + 2) * SEG))
    by_lanes = [False, True, False, False]
    sent, *sums = attention_backward(
        parts, pick(role, upstream), attended, logsum, table_cosine, table_sine, grads, shapes
    )
    (
        joined,
        adapted_low,
        first_gain_part,
        *chunks,
    ) = leave(
        pick(place, sent).reshape(4, rows, 3 * WIDE),
        adapted,
        middle_back,
        one_row(first_gain),
        query_weight,
        key_weight,
        value_weight,
        sums,
        by_lanes,
    )
    adapter_part = jnp.einsum(
        "rcd,re->cde", latent_embed, adapted_low, preferred_element_type=F32
    ).astype(BF16)
    (
        query_total,
        key_total,
        value_total,
        adapter_first,
        adapter_second,
        gate_total,
        down_total,
        up_total,
        output_total,
    ) = reduce_all(
        [tn(first_low, joined[:, i * inner : (i + 1) * inner]) for i in range(3)]
        + [adapter_part[0], adapter_part[1]],
        chunks,
        shapes,
        by_lanes,
    )
    latent_gradient = latent_grad(adapted_low, adapter)
    gains = sum_small(jnp.concatenate([gain_parts[:3], first_gain_part[:1]], axis=0))
    return (
        layer_out,
        latent_gradient,
        jnp.stack([adapter_first, adapter_second]),
        gains[3],
        query_total,
        key_total,
        value_total,
        output_total,
        gains[0],
        gains[1],
        gate_total,
        up_total,
        down_total,
        gains[2],
    )


def specs(rows):
    split = P(None, "tensor")
    in_specs = (
        P(rows, None, "tensor"),
        P(None, "tensor", None),
        P(),
        split,
        split,
        split,
        P("tensor", None),
        P(),
        P(),
        split,
        split,
        P("tensor", None),
        P(),
        P("dp", None),
        P(rows),
        P(rows, None),
    )
    out_specs = (
        P(rows, None),
        P(rows, None, "tensor"),
        P(None, "tensor", None),
        P(),
        split,
        split,
        split,
        P("tensor", None),
        P(),
        P(),
        split,
        split,
        P("tensor", None),
        P(),
    )
    return in_specs, out_specs


def solution(mesh):
    sizes = dict(mesh.shape)
    if sizes["seq"] == 4 and sizes["tensor"] == 2:
        fine = Mesh(
            mesh.devices.reshape(sizes["dp"], 2, 2, 2), ("dp", "x", "core", "tensor")
        )
        in_specs, out_specs = specs(("dp", "x", "core"))
        return jax.shard_map(
            on_device_paired, mesh=fine, in_specs=in_specs, out_specs=out_specs, check_vma=False
        )
    in_specs, out_specs = specs(("dp", "seq"))
    return jax.shard_map(
        on_device, mesh=mesh, in_specs=in_specs, out_specs=out_specs, check_vma=False
    )
```

```python
import functools

import jax
import jax.numpy as jnp
from jax import lax
from jax.experimental import pallas as pl
from jax.experimental.pallas import tpu as pltpu
from jax.sharding import Mesh
from jax.sharding import PartitionSpec as P

DH = 64
SEG = 256


EPSILON = 1e-06
THETA = 50000.0


def normalize(values, gain):
    scale = lax.rsqrt(jnp.mean(values * values, axis=-1, keepdims=True) + EPSILON)
    normed = values * scale
    return (normed * gain, normed, scale)


def normalize_back(upstream, gain, normed, scale):
    scaled = upstream * gain
    inward = scale * (scaled - normed * jnp.mean(scaled * normed, axis=-1, keepdims=True))
    return (inward, jnp.sum(upstream * normed, axis=0))


def angles(positions, width):
    half = width // 2
    freq = THETA ** (-jnp.arange(half, dtype=jnp.float32) * 2.0 / width)
    angle = positions.astype(jnp.float32)[:, None] * freq[None, :]
    return (jnp.cos(angle)[:, None, :], jnp.sin(angle)[:, None, :])


def rotate(values, cosine, sine, sign):
    half = values.shape[-1] // 2
    first = values[..., :half]
    second = values[..., half:]
    return jnp.concatenate(
        [first * cosine - sign * second * sine, second * cosine + sign * first * sine], axis=-1
    )


def ancestry(parent_row):
    labels = jnp.arange(parent_row.shape[0], dtype=jnp.int32)

    def extend(index, state):
        current, total = state
        total = total | (current[:, None] == labels[None, :])
        current = jnp.where(current >= 0, jnp.take(parent_row, jnp.maximum(current, 0)), -1)
        return (current, total)

    start = (parent_row, jnp.zeros((parent_row.shape[0], parent_row.shape[0]), jnp.bool_))
    current, total = lax.fori_loop(0, parent_row.shape[0], extend, start)
    return total


def path_mask(parent_row, query_ids, key_ids):
    table = ancestry(parent_row)
    query_seg = query_ids // SEG
    key_seg = key_ids // SEG
    far = jnp.take(jnp.take(table, query_seg, axis=0), key_seg, axis=1)
    near = (query_seg[:, None] == key_seg[None, :]) & (key_ids[None, :] <= query_ids[:, None])
    return far | near


def on_device(
    latent_embed,
    adapter,
    first_gain,
    query_weight,
    key_weight,
    value_weight,
    output_weight,
    second_gain,
    third_gain,
    gate_weight,
    up_weight,
    down_weight,
    fourth_gain,
    parents,
    positions,
    cotangent,
):
    rows = latent_embed.shape[0]
    local_heads = query_weight.shape[1] // DH
    scale = DH ** (-0.5)
    adapted = lax.psum(
        jnp.einsum("rcd,cde->re", latent_embed, adapter, preferred_element_type=jnp.float32),
        "tensor",
    )
    first_out, first_normed, first_scale = normalize(adapted, first_gain)
    first_low = first_out.astype(jnp.bfloat16)
    cosine, sine = angles(positions, DH)
    query_raw = jnp.dot(first_low, query_weight, preferred_element_type=jnp.float32).reshape(
        rows, local_heads, DH
    )
    queries = rotate(query_raw, cosine, sine, 1.0).astype(jnp.bfloat16)
    key_raw = jnp.dot(first_low, key_weight, preferred_element_type=jnp.float32).reshape(
        rows, local_heads, DH
    )
    keys_local = rotate(key_raw, cosine, sine, 1.0).astype(jnp.bfloat16)
    values_local = (
        jnp.dot(first_low, value_weight, preferred_element_type=jnp.float32)
        .astype(jnp.bfloat16)
        .reshape(rows, local_heads, DH)
    )
    keys_all, values_all = (
        lax.all_gather(keys_local, "seq", axis=0, tiled=True),
        lax.all_gather(values_local, "seq", axis=0, tiled=True),
    )
    tree_rows = keys_all.shape[0]
    query_ids = lax.axis_index("seq") * rows + jnp.arange(rows, dtype=jnp.int32)
    key_ids = jnp.arange(tree_rows, dtype=jnp.int32)
    allowed = path_mask(parents[0], query_ids, key_ids)[None]

    def score_block(keys):
        raw = jnp.einsum("qhd,khd->hqk", queries, keys, preferred_element_type=jnp.float32) * scale
        return jnp.where(allowed, raw, -1e30)

    scores = score_block(keys_all)
    top = jnp.max(scores, axis=-1, keepdims=True)
    weights = jnp.exp(scores - top)
    total = jnp.sum(weights, axis=-1, keepdims=True)
    probs = weights / total
    logsum = top + jnp.log(total)
    attended = jnp.einsum(
        "hqk,khd->qhd", probs.astype(jnp.bfloat16), values_all, preferred_element_type=jnp.float32
    )
    attended = attended.reshape(rows, local_heads * DH).astype(jnp.bfloat16)
    attention = lax.psum(
        jnp.dot(attended, output_weight, preferred_element_type=jnp.float32).astype(jnp.bfloat16),
        "tensor",
    ).astype(jnp.float32)
    second_out, second_normed, second_scale = normalize(attention, second_gain)
    middle = adapted + second_out
    third_out, third_normed, third_scale = normalize(middle, third_gain)
    third_low = third_out.astype(jnp.bfloat16)
    gate = jnp.dot(third_low, gate_weight, preferred_element_type=jnp.float32)
    upward = jnp.dot(third_low, up_weight, preferred_element_type=jnp.float32)
    hidden = (jax.nn.silu(gate) * upward).astype(jnp.bfloat16)
    mixed = lax.psum(
        jnp.dot(hidden, down_weight, preferred_element_type=jnp.float32).astype(jnp.bfloat16),
        "tensor",
    ).astype(jnp.float32)
    fourth_out, fourth_normed, fourth_scale = normalize(mixed, fourth_gain)
    layer_out = middle + fourth_out
    upstream = cotangent.astype(jnp.float32)
    mixed_back, fourth_gain_part = normalize_back(
        upstream, fourth_gain, fourth_normed, fourth_scale
    )
    mixed_low = mixed_back.astype(jnp.bfloat16)
    down_part = jnp.einsum("rf,rd->fd", hidden, mixed_low, preferred_element_type=jnp.float32)
    hidden_back = (
        jnp.einsum("rd,fd->rf", mixed_low, down_weight, preferred_element_type=jnp.float32)
        .astype(jnp.bfloat16)
        .astype(jnp.float32)
    )
    swiglu_value, product_back = jax.vjp(
        lambda left, right: jax.nn.silu(left) * right, gate, upward
    )
    gate_back, up_back = product_back(hidden_back)
    gate_low = gate_back.astype(jnp.bfloat16)
    up_low = up_back.astype(jnp.bfloat16)
    gate_part = jnp.einsum("rd,rf->df", third_low, gate_low, preferred_element_type=jnp.float32)
    up_part = jnp.einsum("rd,rf->df", third_low, up_low, preferred_element_type=jnp.float32)
    third_term = jnp.einsum(
        "rf,df->rd", gate_low, gate_weight, preferred_element_type=jnp.float32
    ) + jnp.einsum("rf,df->rd", up_low, up_weight, preferred_element_type=jnp.float32)
    third_back = lax.psum(third_term.astype(jnp.bfloat16), "tensor").astype(jnp.float32)
    middle_part, third_gain_part = normalize_back(third_back, third_gain, third_normed, third_scale)
    middle_back = upstream + middle_part
    attention_back, second_gain_part = normalize_back(
        middle_back, second_gain, second_normed, second_scale
    )
    attention_low = attention_back.astype(jnp.bfloat16)
    output_part = jnp.einsum(
        "re,rd->ed", attended, attention_low, preferred_element_type=jnp.float32
    )
    attended_back = (
        jnp.einsum("rd,ed->re", attention_low, output_weight, preferred_element_type=jnp.float32)
        .astype(jnp.bfloat16)
        .reshape(rows, local_heads, DH)
    )
    keys_back, values_back = (
        lax.all_gather(keys_local, "seq", axis=0, tiled=True),
        lax.all_gather(values_local, "seq", axis=0, tiled=True),
    )
    probs_back = jnp.exp(score_block(keys_back) - logsum)
    prob_grad = jnp.einsum(
        "qhd,khd->hqk", attended_back, values_back, preferred_element_type=jnp.float32
    )
    score_grad = (
        probs_back * (prob_grad - jnp.sum(prob_grad * probs_back, axis=-1, keepdims=True))
    ).astype(jnp.bfloat16)
    query_rot = (
        jnp.einsum("hqk,khd->qhd", score_grad, keys_back, preferred_element_type=jnp.float32)
        * scale
    )
    key_rot_all = (
        jnp.einsum("hqk,qhd->khd", score_grad, queries, preferred_element_type=jnp.float32) * scale
    )
    value_back_all = jnp.einsum(
        "hqk,qhd->khd",
        probs_back.astype(jnp.bfloat16),
        attended_back,
        preferred_element_type=jnp.float32,
    )
    key_rot, value_back = (
        lax.psum_scatter(
            key_rot_all.astype(jnp.bfloat16), "seq", scatter_dimension=0, tiled=True
        ).astype(jnp.float32),
        lax.psum_scatter(
            value_back_all.astype(jnp.bfloat16), "seq", scatter_dimension=0, tiled=True
        ).astype(jnp.float32),
    )
    query_low = (
        rotate(query_rot, cosine, sine, -1.0).astype(jnp.bfloat16).reshape(rows, local_heads * DH)
    )
    key_low = (
        rotate(key_rot, cosine, sine, -1.0).astype(jnp.bfloat16).reshape(rows, local_heads * DH)
    )
    value_low = value_back.astype(jnp.bfloat16).reshape(rows, local_heads * DH)
    query_part = jnp.einsum("rd,re->de", first_low, query_low, preferred_element_type=jnp.float32)
    key_part = jnp.einsum("rd,re->de", first_low, key_low, preferred_element_type=jnp.float32)
    value_part = jnp.einsum("rd,re->de", first_low, value_low, preferred_element_type=jnp.float32)
    first_term = jnp.einsum(
        "re,de->rd", query_low, query_weight, preferred_element_type=jnp.float32
    )
    first_term = first_term + jnp.einsum(
        "re,de->rd", key_low, key_weight, preferred_element_type=jnp.float32
    )
    first_term = first_term + jnp.einsum(
        "re,de->rd", value_low, value_weight, preferred_element_type=jnp.float32
    )
    first_back = lax.psum(first_term.astype(jnp.bfloat16), "tensor").astype(jnp.float32)
    adapted_part, first_gain_part = normalize_back(
        first_back, first_gain, first_normed, first_scale
    )
    adapted_low = (middle_back + adapted_part).astype(jnp.bfloat16)
    latent_gradient = jnp.einsum(
        "re,cde->rcd", adapted_low, adapter, preferred_element_type=jnp.float32
    )
    adapter_part = jnp.einsum(
        "rcd,re->cde", latent_embed, adapted_low, preferred_element_type=jnp.float32
    )
    summed = (
        lax.psum(gate_part.astype(jnp.bfloat16), ("dp", "seq")).astype(jnp.float32),
        lax.psum(up_part.astype(jnp.bfloat16), ("dp", "seq")).astype(jnp.float32),
        lax.psum(down_part.astype(jnp.bfloat16), ("dp", "seq")).astype(jnp.float32),
        lax.psum(third_gain_part.astype(jnp.bfloat16), ("dp", "seq")).astype(jnp.float32),
        lax.psum(fourth_gain_part.astype(jnp.bfloat16), ("dp", "seq")).astype(jnp.float32),
        lax.psum(query_part.astype(jnp.bfloat16), ("dp", "seq")).astype(jnp.float32),
        lax.psum(key_part.astype(jnp.bfloat16), ("dp", "seq")).astype(jnp.float32),
        lax.psum(value_part.astype(jnp.bfloat16), ("dp", "seq")).astype(jnp.float32),
        lax.psum(output_part.astype(jnp.bfloat16), ("dp", "seq")).astype(jnp.float32),
        lax.psum(first_gain_part.astype(jnp.bfloat16), ("dp", "seq")).astype(jnp.float32),
        lax.psum(second_gain_part.astype(jnp.bfloat16), ("dp", "seq")).astype(jnp.float32),
        lax.psum(adapter_part.astype(jnp.bfloat16), ("dp", "seq")).astype(jnp.float32),
    )
    gate_total, up_total, down_total, third_total, fourth_total = (
        summed[0],
        summed[1],
        summed[2],
        summed[3],
        summed[4],
    )
    query_total, key_total, value_total, output_total, first_total, second_total = (
        summed[5],
        summed[6],
        summed[7],
        summed[8],
        summed[9],
        summed[10],
    )
    adapter_total = summed[11]
    return (
        layer_out,
        latent_gradient,
        adapter_total,
        first_total,
        query_total,
        key_total,
        value_total,
        output_total,
        second_total,
        third_total,
        gate_total,
        up_total,
        down_total,
        fourth_total,
    )


TRUNK = 8
BRANCH = 4
LEAVES = 2
SEGS = TRUNK + BRANCH + BRANCH * LEAVES
WIDE = 2 * DH
NEG = -1e30
F32 = jnp.float32
BF16 = jnp.bfloat16
KEYS = 512
HIDDEN = 256
VMEM_BYTES = 60 << 20


def nt(left, right):
    return lax.dot_general(left, right, (((1,), (1,)), ((), ())), preferred_element_type=F32)


def nn(left, right):
    return lax.dot_general(left, right, (((1,), (0,)), ((), ())), preferred_element_type=F32)


def segment(index, size=SEG):
    return pl.ds(pl.multiple_of(index * SEG, SEG), size)


def find_roles(parents, child, count, role):
    for s in range(SEGS):
        count[s] = 0
    role[0] = 0
    for s in range(SEGS):
        parent = parents[0, s]

        @pl.when(parent < 0)
        def _():
            role[0] = s

        @pl.when(parent >= 0)
        def _():
            seen = count[parent]
            child[parent * BRANCH + seen] = s
            count[parent] = seen + 1

    for i in range(TRUNK - 1):
        role[i + 1] = child[role[i] * BRANCH]
    for b in range(BRANCH):
        role[TRUNK + b] = child[role[TRUNK - 1] * BRANCH + b]
    for b in range(BRANCH):
        for leaf in range(LEAVES):
            role[TRUNK + BRANCH + b * LEAVES + leaf] = child[role[TRUNK + b] * BRANCH + leaf]


def roles_kernel(parents, parts, role, place, out, child, count):
    find_roles(parents, child, count, role)
    for i in range(SEGS):
        place[role[i]] = i
    pick_segments(role, parts, out)


def pick_segments(order, source, out):
    for i in range(SEGS):
        out[segment(i), :] = source[segment(order[i]), :]


def sort_parts(parents, parts):
    smem = pl.BlockSpec(memory_space=pltpu.SMEM)
    vmem = pl.BlockSpec(memory_space=pltpu.VMEM)
    return pl.pallas_call(
        roles_kernel,
        out_shape=(jax.ShapeDtypeStruct((SEGS,), jnp.int32),) * 2
        + (jax.ShapeDtypeStruct(parts.shape, parts.dtype),),
        in_specs=[smem, vmem],
        out_specs=(smem, smem, vmem),
        scratch_shapes=[
            pltpu.SMEM((SEGS * BRANCH,), jnp.int32),
            pltpu.SMEM((SEGS,), jnp.int32),
        ],
        name="sort_parts",
    )(parents, parts)


def pick(order, source):
    smem = pl.BlockSpec(memory_space=pltpu.SMEM)
    vmem = pl.BlockSpec(memory_space=pltpu.VMEM)
    return pl.pallas_call(
        pick_segments,
        out_shape=jax.ShapeDtypeStruct(source.shape, source.dtype),
        in_specs=[smem, vmem],
        out_specs=vmem,
        name="pick",
    )(order, source)


def heads_apart(values, first):
    zero = jnp.zeros_like(values)
    return jnp.concatenate(
        [jnp.where(first, values, zero), jnp.where(first, zero, values)], axis=0
    )


MESH = pl.DeviceIdType.MESH


def at_step(index, plan):
    for step, calls in plan.items():

        @pl.when(index == step)
        def _(calls=calls):
            for call in calls:
                call()


class Fetch:
    def __init__(self, shape, pieces):
        self.rows, self.lanes = shape
        self.pieces = pieces

    def scratch(self):
        return [pltpu.SemaphoreType.DMA((4, self.pieces))] * 2

    def bind(self, own, out, refs):
        self.own, self.out = own, out
        self.send, self.recv = refs
        self.x, self.core = lax.axis_index("x"), lax.axis_index("core")
        self.to_core = {"core": 1 - self.core}
        self.to_x = {"x": 1 - self.x}
        self.to_tensor = {"tensor": 1 - lax.axis_index("tensor")}

    def copy(self, kind, piece):
        rows = self.rows // 4 // self.pieces
        x = 1 - self.x if kind == 3 else self.x
        row = (2 * x + self.core) * (self.rows // 4) + piece * rows
        here = pl.ds(pl.multiple_of(row, 16), rows)
        return pltpu.make_async_remote_copy(
            src_ref=(self.own if kind == 0 else self.out).at[here],
            dst_ref=self.out.at[here],
            send_sem=self.send.at[kind, piece],
            recv_sem=self.recv.at[kind, piece],
            device_id=(self.to_tensor, self.to_x, self.to_core, self.to_core)[kind],
            device_id_type=MESH,
        )

    def start(self):
        for piece in range(self.pieces):
            self.copy(0, piece).start()

    def second(self, piece):
        self.copy(0, piece).wait_recv()
        self.copy(1, piece).start()
        self.copy(2, piece).start()

    def third(self, piece):
        self.copy(1, piece).wait_recv()
        self.copy(3, piece).start()

    def drain(self):
        for piece in range(self.pieces):
            for kind in range(4):
                self.copy(kind, piece).wait_send()
            self.copy(2, piece).wait_recv()
            self.copy(3, piece).wait_recv()


def attention_kernel(fetches, *refs):
    parts = refs[0]
    count = len(fetches)
    own_weights, refs = refs[1 : 1 + count], refs[1 + count :]
    out, logsum, other_weights = refs[0], refs[1], refs[2 : 2 + count]
    qr, kr, v0, v1, kept, acc, top, total = refs[2 + count : 10 + count]
    sems = refs[10 + count :]
    for i, fetch in enumerate(fetches):
        fetch.bind(own_weights[i], other_weights[i], sems[2 * i : 2 * i + 2])
    output, gate, up, down = fetches
    barrier = pltpu.get_barrier_semaphore()
    for target in (gate.to_core, gate.to_x, gate.to_tensor):
        pl.semaphore_signal(barrier, inc=1, device_id=target, device_id_type=MESH)
    pl.semaphore_wait(barrier, 3)
    for fetch in fetches:
        fetch.start()
    call = functools.partial
    leaf_plan = {
        2: [call(output.second, 0)],
        4: [call(gate.second, 0), call(output.third, 0)],
        6: [call(gate.second, 1)],
        7: [call(gate.third, 0)],
    }
    branch_plan = {
        0: [call(up.second, 0)],
        1: [call(gate.third, 1)],
        2: [call(up.second, 1)],
        3: [call(up.third, 0)],
    }
    trunk_plan = {
        3: [call(down.second, 0), call(up.third, 1)],
        6: [call(down.second, 1)],
    }
    first = lax.broadcasted_iota(jnp.int32, (SEG, WIDE), 1) < DH

    def sort(i, _):
        here = source = segment(i)
        qr[here, :] = parts[source, 0:WIDE] * jnp.asarray(DH**-0.5, BF16)
        kr[here, :] = parts[source, WIDE : 2 * WIDE]
        value = parts[source, 2 * WIDE : 3 * WIDE]
        zero = jnp.zeros_like(value)
        v0[here, :] = jnp.where(first, value, zero)
        v1[here, :] = jnp.where(first, zero, value)
        return 0

    lax.fori_loop(0, SEGS, sort, 0)
    row = lax.broadcasted_iota(jnp.int32, (2 * SEG, SEG), 0)
    col = lax.broadcasted_iota(jnp.int32, (2 * SEG, SEG), 1)
    causal = col <= jnp.where(row >= SEG, row - SEG, row)

    def fold(values, op):
        result = values[:, 0:128]
        for at in range(128, values.shape[1], 128):
            result = op(result, values[:, at : at + 128])
        return result

    def query(index, count_big, big, extra):
        queries = heads_apart(qr[segment(index), :], first)
        own = jnp.where(causal, nt(queries, kr[segment(index), :]), NEG)
        top[...] = fold(own, jnp.maximum)
        others = []
        for other in extra:
            scores = nt(queries, kr[segment(other), :])
            top[...] = jnp.maximum(top[...], fold(scores, jnp.maximum))
            others.append(scores)

        def find(c, _):
            scores = nt(queries, kr[pl.ds(pl.multiple_of(c * big, big), big), :])
            kept[c, :, 0:big] = scores
            top[...] = jnp.maximum(top[...], fold(scores, jnp.maximum))
            return 0

        lax.fori_loop(0, count_big, find, 0)
        most = jnp.max(top[...], axis=1, keepdims=True)

        def add(scores, keys, fresh=False):
            weights = jnp.exp(scores - most)
            summed = fold(weights, jnp.add)
            low = weights.astype(BF16)
            product = nn(low[:SEG], v0[keys, :]) + nn(low[SEG:], v1[keys, :])
            total[...] = summed if fresh else total[...] + summed
            acc[...] = product if fresh else acc[...] + product

        add(own, segment(index), True)
        for other, scores in zip(extra, others):
            add(scores, segment(other))

        def use(c, _):
            add(kept[c, :, 0:big], pl.ds(pl.multiple_of(c * big, big), big))
            return 0

        lax.fori_loop(0, count_big, use, 0)
        whole = jnp.sum(total[...], axis=1, keepdims=True)
        inverse = 1.0 / whole
        log = most + jnp.log(whole)
        here = segment(index)
        out[here, :] = (acc[...] * jnp.where(first, inverse[:SEG], inverse[SEG:])).astype(BF16)
        logsum[here, :] = jnp.where(first, log[:SEG], log[SEG:])

    def trunk(i, _):
        at_step(i, trunk_plan)
        query(i, i, SEG, [])
        return 0

    def branch(i, _):
        at_step(i, branch_plan)
        query(TRUNK + i, TRUNK * SEG // KEYS, KEYS, [])
        return 0

    def leaf(i, _):
        at_step(i, leaf_plan)
        query(TRUNK + BRANCH + i, TRUNK * SEG // KEYS, KEYS, [TRUNK + i // LEAVES])
        return 0

    lax.fori_loop(0, BRANCH * LEAVES, leaf, 0)
    lax.fori_loop(0, BRANCH, branch, 0)
    lax.fori_loop(0, TRUNK, trunk, 0)
    down.third(0)

    down.third(1)
    for fetch in fetches:
        fetch.drain()


def attention_forward(parts, weights):
    fetches = [Fetch(weight.shape, 1 if i == 0 else 2) for i, weight in enumerate(weights)]
    sems = []
    for fetch in fetches:
        sems += fetch.scratch()
    hbm = pl.BlockSpec(memory_space=pl.ANY)
    tokens = SEGS * SEG
    vmem = pl.BlockSpec(memory_space=pltpu.VMEM)
    return pl.pallas_call(
        functools.partial(attention_kernel, fetches),
        out_shape=(
            jax.ShapeDtypeStruct((tokens, WIDE), BF16),
            jax.ShapeDtypeStruct((tokens, WIDE), F32),
        )
        + tuple(jax.ShapeDtypeStruct(weight.shape, BF16) for weight in weights),
        in_specs=[vmem] + [hbm] * len(weights),
        out_specs=(vmem, vmem) + (hbm,) * len(weights),
        scratch_shapes=[pltpu.VMEM((tokens, WIDE), BF16)] * 4
        + [
            pltpu.VMEM((TRUNK, 2 * SEG, KEYS), F32),
            pltpu.VMEM((SEG, WIDE), F32),
            pltpu.VMEM((2 * SEG, 128), F32),
            pltpu.VMEM((2 * SEG, 128), F32),
        ]
        + sems,
        compiler_params=pltpu.CompilerParams(
            vmem_limit_bytes=VMEM_BYTES, collective_id=4, has_side_effects=True
        ),
        cost_estimate=pl.CostEstimate(
            flops=152 * 2 * 4 * SEG * SEG * 128,
            bytes_accessed=tokens * WIDE * 12,
            transcendentals=152 * 2 * SEG * SEG,
        ),
        name="attention_forward",
    )(parts, *weights)


def add_rows(dst, dst_row, left, left_row, right, right_row, rows, step=32):
    def one(i, _):
        at = i * step
        total = left[pl.ds(pl.multiple_of(left_row + at, step), step), :].astype(F32)
        total += right[pl.ds(pl.multiple_of(right_row + at, step), step), :].astype(F32)
        dst[pl.ds(pl.multiple_of(dst_row + at, step), step), :] = total.astype(BF16)
        return 0

    lax.fori_loop(0, rows // step, one, 0)


class PairFold:
    def __init__(self, shape, x_first, pieces=1):
        self.rows, self.lanes = shape
        self.x_first = x_first
        self.pieces = pieces if x_first else 2

    def scratch(self):
        half, quarter = (self.rows // 2, self.lanes), (self.rows // 4, self.lanes)
        return (
            [pltpu.VMEM(half, BF16)] * 4
            + [pltpu.VMEM(quarter, BF16)] * (2 if self.x_first else 1)
            + [pltpu.VMEM(quarter if self.x_first else half, BF16)]
            + [pltpu.SemaphoreType.DMA((2,))] * 3
            + [pltpu.SemaphoreType.DMA((2, self.pieces))] * 2
            + [pltpu.SemaphoreType.DMA((self.pieces,))] * 2
        )

    def bind(self, parts, out, refs):
        self.parts, self.out = parts, out
        self.keep, self.land = refs[0:2], refs[2:4]
        count = 2 if self.x_first else 1
        self.x_land = refs[4 : 4 + count]
        (
            self.y_land,
            self.local,
            self.core_send,
            self.core_recv,
            self.x_send,
            self.x_recv,
            self.y_send,
            self.y_recv,
        ) = refs[4 + count :]
        self.x, self.core = lax.axis_index("x"), lax.axis_index("core")
        self.to_core = {"core": 1 - self.core}
        self.to_x = {"x": 1 - self.x}
        self.to_tensor = {"tensor": 1 - lax.axis_index("tensor")}
        self.half, self.quarter = self.rows // 2, self.rows // 4

    def rows_at(self, ref, row, rows):
        return ref.at[pl.ds(pl.multiple_of(row, 32), rows)]

    def remote(self, src, dst, send, recv, where):
        return pltpu.make_async_remote_copy(
            src_ref=src,
            dst_ref=dst,
            send_sem=send,
            recv_sem=recv,
            device_id=where,
            device_id_type=MESH,
        )

    def over_core(self, side):
        return self.remote(
            self.rows_at(self.parts[side], (1 - self.core) * self.half, self.half),
            self.land[side],
            self.core_send.at[side],
            self.core_recv.at[side],
            self.to_core,
        )

    def kept(self, side):
        return pltpu.make_async_copy(
            self.rows_at(self.parts[side], self.core * self.half, self.half),
            self.keep[side],
            self.local.at[side],
        )

    def over_x(self, side, piece):
        rows = self.quarter // self.pieces if self.x_first else self.quarter
        start = piece * rows if self.x_first else 0
        return self.remote(
            self.rows_at(self.keep[side], (1 - self.x) * self.quarter + start, rows),
            self.rows_at(self.x_land[side], start, rows),
            self.x_send.at[side, piece],
            self.x_recv.at[side, piece],
            self.to_x,
        )

    def over_tensor(self, piece):
        if self.x_first:
            rows = self.quarter // self.pieces
            source, target = self.x * self.quarter + piece * rows, piece * rows
        else:
            rows = self.quarter
            source = (1 - self.x if piece == 0 else self.x) * rows
            target = source
        return self.remote(
            self.rows_at(self.keep[1], source, rows),
            self.rows_at(self.y_land, target, rows),
            self.y_send.at[piece],
            self.y_recv.at[piece],
            self.to_tensor,
        )

    def start(self):
        for side in range(2):
            self.over_core(side).start()
            self.kept(side).start()

    def fold_core(self):
        for side in (1, 0):
            self.kept(side).wait()
            self.over_core(side).wait_recv()
            add_rows(self.keep[side], 0, self.keep[side], 0, self.land[side], 0, self.half)
        for piece in range(self.pieces):
            if self.x_first:
                self.over_x(1, piece).start()
                self.over_x(0, piece).start()
            else:
                self.over_tensor(piece).start()

    def second(self, piece):
        if self.x_first:
            rows = self.quarter // self.pieces
            at = self.x * self.quarter + piece * rows
            for side in (1, 0):
                self.over_x(side, piece).wait_recv()
                keep, land = self.keep[side], self.x_land[side]
                add_rows(keep, at, keep, at, land, piece * rows, rows)
                if side == 1:
                    self.over_tensor(piece).start()
        else:
            at = (1 - self.x if piece == 0 else self.x) * self.quarter
            self.over_tensor(piece).wait_recv()
            add_rows(self.keep[0], at, self.keep[0], at, self.y_land, at, self.quarter)
            if piece == 0:
                self.over_x(0, 0).start()

    def third(self, piece):
        if self.x_first:
            rows = self.quarter // self.pieces
            self.over_tensor(piece).wait_recv()
            at = self.x * self.quarter + piece * rows
            add_rows(self.out, piece * rows, self.keep[0], at, self.y_land, piece * rows, rows)
        elif piece == 0:
            self.over_x(0, 0).wait_recv()
            at = self.x * self.quarter
            add_rows(self.out, 0, self.keep[0], at, self.x_land[0], 0, self.quarter)

    def drain(self):
        for side in range(2):
            self.over_core(side).wait_send()
        for piece in range(self.pieces):
            if self.x_first:
                self.over_x(0, piece).wait_send()
                self.over_x(1, piece).wait_send()
            self.over_tensor(piece).wait_send()
        if not self.x_first:
            self.over_x(0, 0).wait_send()


def swap_halves(values, low):
    return jnp.where(
        low, pltpu.roll(values, WIDE - DH // 2, 1), pltpu.roll(values, DH // 2, 1)
    )


def attention_back_kernel(folds, *refs):
    parts, upstream, attended, logsum, cosine, sine = refs[:6]
    pair_grad, down_grad, output_grad = refs[6:9]
    refs = refs[9:]
    split, hidden = folds[0].lanes, folds[1].rows
    inner = folds[3].rows
    sides = [pair_grad.at[:, pl.ds(0, split)], pair_grad.at[:, pl.ds(2 * split, split)]]
    sides += [down_grad.at[pl.ds(0, hidden)], down_grad.at[pl.ds(hidden, hidden)]]
    sides += [pair_grad.at[:, pl.ds(split, split)], pair_grad.at[:, pl.ds(3 * split, split)]]
    sides += [output_grad.at[pl.ds(0, inner)], output_grad.at[pl.ds(inner, inner)]]
    out, sums, refs = refs[0], refs[1 : 1 + len(folds)], refs[1 + len(folds) :]
    qr, kr, vr, kt, dk, dv, dqt = refs[:7]
    refs = refs[7:]
    for i, fold in enumerate(folds):
        size = len(fold.scratch())
        fold.bind(sides[2 * i : 2 * i + 2], sums[i], refs[:size])
        refs = refs[size:]
    gate, down, up, output = folds
    barrier = pltpu.get_barrier_semaphore()
    for target in (gate.to_core, gate.to_x, gate.to_tensor):
        pl.semaphore_signal(barrier, inc=1, device_id=target, device_id_type=MESH)
    pl.semaphore_wait(barrier, 3)
    for fold in folds:
        fold.start()
    call = functools.partial
    leaf_plan = {
        2: [gate.fold_core, up.fold_core],
        3: [down.fold_core, output.fold_core],
    }
    branch_plan = {3: [call(gate.second, 0), call(up.second, 0), call(output.second, 0)]}
    trunk_plan = {5: [call(up.second, 1), call(output.second, 1)]}
    lane = lax.broadcasted_iota(jnp.int32, (SEG, WIDE), 1)
    first = lane < DH
    low = (lane % DH) < (DH // 2)

    def sort(i, _):
        here = source = segment(i)
        qr[here, :] = parts[source, 0:WIDE] * jnp.asarray(DH**-0.5, BF16)
        key = parts[source, WIDE : 2 * WIDE]
        kr[here, :] = key
        kt[:, here] = key.T
        vr[here, :] = parts[source, 2 * WIDE : 3 * WIDE]
        return 0

    lax.fori_loop(0, SEGS, sort, 0)
    dk[...] = jnp.zeros_like(dk)
    dv[...] = jnp.zeros_like(dv)
    key_at = lax.broadcasted_iota(jnp.int32, (SEG, 2 * SEG), 0)
    query_at = lax.broadcasted_iota(jnp.int32, (SEG, 2 * SEG), 1)
    causal = key_at <= jnp.where(query_at >= SEG, query_at - SEG, query_at)

    def rope_back(values, depth):
        at = segment(depth)
        return values * cosine[at, :] - swap_halves(values, low) * sine[at, :]

    def query(index, depth, count_big, big, extra):
        here = segment(index)
        queries = heads_apart(qr[segment(index), :], first)
        up = upstream[here, :]
        ups = heads_apart(up, first)
        turned = logsum[segment(index), :].T
        log = jnp.concatenate([turned[0:1, :], turned[DH : DH + 1, :]], axis=1)
        product = (up.astype(F32) * attended[here, :].astype(F32)).T
        inner = jnp.concatenate(
            [
                jnp.sum(product[:DH], axis=0, keepdims=True),
                jnp.sum(product[DH:], axis=0, keepdims=True),
            ],
            axis=1,
        )
        dqt[...] = jnp.zeros_like(dqt)

        def add(keys, mask=None):
            weights = jnp.exp(nt(kr[keys, :], queries) - log)
            if mask is not None:
                weights = jnp.where(mask, weights, 0.0)
            back = (weights * (nt(vr[keys, :], ups) - inner)).astype(BF16)
            dv[keys, :] += nn(weights.astype(BF16), ups)
            dk[keys, :] += nn(back, queries)
            dqt[...] += nn(kt[:, keys], back)

        add(segment(index), causal)
        for other in extra:
            add(segment(other))

        def use(c, _):
            add(pl.ds(pl.multiple_of(c * big, big), big))
            return 0

        lax.fori_loop(0, count_big, use, 0)
        both = jnp.concatenate([dqt[:DH, :SEG], dqt[DH:, SEG:]], axis=0) * (DH**-0.5)
        out[here, 0:WIDE] = rope_back(both.T, depth).astype(BF16)

    def leaf(i, _):
        at_step(i, leaf_plan)
        query(TRUNK + BRANCH + i, TRUNK + 1, TRUNK * SEG // KEYS, KEYS, [TRUNK + i // LEAVES])
        return 0

    def branch(i, _):
        at_step(i, branch_plan)
        query(TRUNK + i, TRUNK, TRUNK * SEG // KEYS, KEYS, [])
        return 0

    def trunk(i, _):
        at_step(i, trunk_plan)
        query(i, i, i, SEG, [])
        return 0

    lax.fori_loop(0, BRANCH * LEAVES, leaf, 0)
    lax.fori_loop(0, BRANCH, branch, 0)
    lax.fori_loop(0, TRUNK, trunk, 0)

    down.second(0)

    def settle(i, _):
        here = segment(i)
        depth = jnp.where(i < TRUNK + BRANCH, jnp.minimum(i, TRUNK), TRUNK + 1)
        out[here, WIDE : 2 * WIDE] = rope_back(dk[here, :], depth).astype(BF16)
        out[here, 2 * WIDE : 3 * WIDE] = dv[here, :].astype(BF16)
        return 0

    lax.fori_loop(0, SEGS, settle, 0)
    for fold in (gate, up, output, down):
        fold.third(0)
    for fold in folds:
        fold.drain()


def attention_backward(parts, upstream, attended, logsum, cosine, sine, grads, shapes):
    tokens = SEGS * SEG
    vmem = pl.BlockSpec(memory_space=pltpu.VMEM)
    folds = [PairFold(shape, i < 2) for i, shape in enumerate(shapes)]
    scratch = []
    for fold in folds:
        scratch += fold.scratch()
    return pl.pallas_call(
        functools.partial(attention_back_kernel, folds),
        out_shape=(jax.ShapeDtypeStruct((tokens, 3 * WIDE), BF16),)
        + tuple(jax.ShapeDtypeStruct((fold.rows // 4, fold.lanes), BF16) for fold in folds),
        in_specs=[vmem] * 6 + [pl.BlockSpec(memory_space=pl.ANY)] * len(grads),
        out_specs=(vmem,) * (1 + len(folds)),
        scratch_shapes=[pltpu.VMEM((tokens, WIDE), BF16)] * 3
        + [pltpu.VMEM((WIDE, tokens), BF16)]
        + [pltpu.VMEM((tokens, WIDE), F32)] * 2
        + [pltpu.VMEM((WIDE, 2 * SEG), F32)]
        + scratch,
        compiler_params=pltpu.CompilerParams(
            vmem_limit_bytes=VMEM_BYTES, collective_id=3, has_side_effects=True
        ),
        cost_estimate=pl.CostEstimate(
            flops=152 * 2 * 10 * SEG * SEG * 128,
            bytes_accessed=tokens * WIDE * 24,
            transcendentals=152 * 2 * SEG * SEG,
        ),
        name="attention_backward",
    )(
        parts,
        upstream,
        attended,
        logsum,
        cosine,
        sine,
        *grads,
    )


def angle_tables(positions):
    lane = jnp.arange(WIDE)
    freq = THETA ** (-(lane % (DH // 2)).astype(F32) * 2.0 / DH)
    angle = positions.astype(F32)[:, None] * freq[None, :]
    sign = jnp.where((lane % DH) < DH // 2, -1.0, 1.0)
    return jnp.cos(angle), jnp.sin(angle) * sign[None, :]


def neighbours():
    x, core = lax.axis_index("x"), lax.axis_index("core")
    others = []
    for step in (1, 2, 3):
        to_x = lax.rem(x + step // 2, 2)
        to_core = lax.rem(core + step % 2, 2)
        others.append((2 * to_x + to_core, {"x": to_x, "core": to_core}))
    return 2 * x + core, others


def greet(tensor_peer, others):
    barrier = pltpu.get_barrier_semaphore()
    for target in [tensor_peer] + [where for _, where in others]:
        pl.semaphore_signal(barrier, inc=1, device_id=target, device_id_type=MESH)
    pl.semaphore_wait(barrier, 1 + len(others))


def enter_kernel(
    mine,
    gain,
    query_w,
    key_w,
    value_w,
    cosine,
    sine,
    parts,
    low_out,
    theirs,
    ready,
    swap_send,
    swap_recv,
    part_send,
    part_recv,
):
    me, others = neighbours()
    tensor_peer = {"tensor": 1 - lax.axis_index("tensor")}
    greet(tensor_peer, others)
    steps = mine.shape[0] // SEG

    def exchange(i):
        return pltpu.make_async_remote_copy(
            src_ref=mine.at[segment(i)],
            dst_ref=theirs.at[segment(i)],
            send_sem=swap_send.at[i],
            recv_sem=swap_recv.at[i],
            device_id=tensor_peer,
            device_id_type=MESH,
        )

    def scatter(i, at):
        place, where = others[at]
        return pltpu.make_async_remote_copy(
            src_ref=ready.at[place, segment(i)],
            dst_ref=parts.at[me, segment(i)],
            send_sem=part_send.at[i, at],
            recv_sem=part_recv.at[i, at],
            device_id=where,
            device_id_type=MESH,
        )

    for i in range(steps):
        exchange(i).start()
    low = (lax.broadcasted_iota(jnp.int32, (SEG, WIDE), 1) % DH) < (DH // 2)

    def step(i, _):
        here = segment(i)
        exchange(i).wait_recv()
        total = mine[here, :].astype(F32) + theirs[here, :].astype(F32)
        scale = lax.rsqrt(jnp.mean(total * total, axis=-1, keepdims=True) + EPSILON)
        rounded = (total * scale * gain[...]).astype(BF16)
        low_out[here, :] = rounded
        for at, weight in enumerate((query_w, key_w, value_w)):
            raw = nn(rounded, weight[...])
            for peer in range(ready.shape[0]):
                part = raw[:, peer * WIDE : (peer + 1) * WIDE]
                if at < 2:
                    part = part * cosine[here, :] + swap_halves(part, low) * sine[here, :]
                ready[peer, here, at * WIDE : (at + 1) * WIDE] = part.astype(BF16)
        for at in range(len(others)):
            scatter(i, at).start()
        parts[me, here, :] = ready[me, here, :]
        return 0

    lax.fori_loop(0, steps, step, 0)

    def finish(i, _):
        exchange(i).wait_send()
        for at in range(len(others)):
            scatter(i, at).wait()
        return 0

    lax.fori_loop(0, steps, finish, 0)


def enter(mine, gain, query_w, key_w, value_w, cosine, sine):
    rows, width = mine.shape
    inner = query_w.shape[1]
    peers = inner // WIDE
    steps = rows // SEG
    vmem = pl.BlockSpec(memory_space=pltpu.VMEM)
    return pl.pallas_call(
        enter_kernel,
        out_shape=(
            jax.ShapeDtypeStruct((peers, rows, 3 * WIDE), BF16),
            jax.ShapeDtypeStruct((rows, width), BF16),
            jax.ShapeDtypeStruct((rows, width), BF16),
        ),
        in_specs=[vmem] * 7,
        out_specs=(vmem,) * 3,
        scratch_shapes=[
            pltpu.VMEM((peers, rows, 3 * WIDE), BF16),
            pltpu.SemaphoreType.DMA((steps,)),
            pltpu.SemaphoreType.DMA((steps,)),
            pltpu.SemaphoreType.DMA((steps, 3)),
            pltpu.SemaphoreType.DMA((steps, 3)),
        ],
        compiler_params=pltpu.CompilerParams(
            vmem_limit_bytes=VMEM_BYTES, collective_id=0, has_side_effects=True
        ),
        cost_estimate=pl.CostEstimate(
            flops=2 * rows * width * 3 * inner,
            bytes_accessed=200 << 20,
            transcendentals=rows,
        ),
        name="enter",
    )(mine, gain, query_w, key_w, value_w, cosine, sine)


def middle_kernel(
    meta,
    adapted,
    heads,
    cotangent,
    second_gain,
    third_gain,
    fourth_gain,
    wo_own,
    wg_own,
    wu_own,
    wd_own,
    wo_other,
    wg_other,
    wu_other,
    wd_other,
    layer_out,
    middle_out,
    attended_out,
    attention_out,
    third_out,
    mixed_out,
    hidden_out,
    pair_out,
    heads_back,
    gains_out,
    wo,
    wg,
    wu,
    wd,
    gate_s,
    up_s,
    sums,
    sem,
):
    step = pl.program_id(0)
    tensor = meta[0]
    copies = []

    def copy(src, weight, row, lane):
        rows, lanes = src.shape
        dst = weight.at[pl.ds(row, rows), pl.ds(lane, lanes)]
        copies.append(pltpu.make_async_copy(src, dst, sem.at[len(copies)]))

    for weight, own, other, by_lane in (
        (wo, wo_own, wo_other, False),
        (wg, wg_own, wg_other, True),
        (wu, wu_own, wu_other, True),
        (wd, wd_own, wd_other, False),
    ):
        rows, lanes = own.shape
        copy(own, weight, 0, 0)
        copy(other, weight, 0 if by_lane else rows, lanes if by_lane else 0)

    @pl.when(step == 0)
    def _():
        for copy in copies:
            copy.start()
        gains_out[...] = jnp.zeros_like(gains_out)
        for copy in copies[:2]:
            copy.wait()

    groups = heads.shape[0] // 2
    for side in range(2):
        for group in range(groups):
            at = (side * groups + group) * WIDE
            source = group * 2 + (tensor if side == 0 else 1 - tensor)
            attended_out[:, at : at + WIDE] = heads[source]
    attention = nn(attended_out[...], wo[...])

    def scaling(values):
        return lax.rsqrt(jnp.mean(values * values, axis=-1, keepdims=True) + EPSILON)

    def inward(upstream, gain, normed, scale):
        scaled = upstream * gain
        return scale * (scaled - normed * jnp.mean(scaled * normed, axis=-1, keepdims=True))

    second_scale = scaling(attention)
    second_normed = attention * second_scale
    middle = adapted[...] + second_normed * second_gain[...]
    third_scale = scaling(middle)
    third_normed = middle * third_scale
    third_out[...] = (third_normed * third_gain[...]).astype(BF16)

    @pl.when(step == 0)
    def _():
        for copy in copies[2:]:
            copy.wait()

    sums[...] = jnp.zeros_like(sums)

    def forward(c, _):
        cut = pl.ds(pl.multiple_of(c * HIDDEN, HIDDEN), HIDDEN)
        gate = nn(third_out[...], wg[:, cut])
        upward = nn(third_out[...], wu[:, cut])
        gate_s[c] = gate
        up_s[c] = upward
        hidden = (gate / (1.0 + jnp.exp(-gate)) * upward).astype(BF16)
        hidden_out[:, cut] = hidden
        sums[...] += nn(hidden, wd[cut, :])
        return 0

    lax.fori_loop(0, gate_s.shape[0], forward, 0)
    mixed = sums[...]
    fourth_scale = scaling(mixed)
    fourth_normed = mixed * fourth_scale
    layer_out[...] = (middle + fourth_normed * fourth_gain[...]).astype(BF16)
    upstream = cotangent[...].astype(F32)
    gains_out[2:3, :] += jnp.sum(upstream * fourth_normed, axis=0, keepdims=True)
    mixed_out[...] = inward(upstream, fourth_gain[...], fourth_normed, fourth_scale).astype(BF16)
    sums[...] = jnp.zeros_like(sums)
    side_units = wg_own.shape[1] // 128

    def backward(c, _):
        cut = pl.ds(pl.multiple_of(c * HIDDEN, HIDDEN), HIDDEN)
        back = nt(mixed_out[...], wd[cut, :]).astype(BF16).astype(F32)
        gate = gate_s[c]
        sigmoid = 1.0 / (1.0 + jnp.exp(-gate))
        silu = gate * sigmoid
        gate_back = (back * up_s[c] * (sigmoid + silu * (1.0 - sigmoid))).astype(BF16)
        up_back = (back * silu).astype(BF16)
        for piece in range(HIDDEN // 128):
            unit = c * (HIDDEN // 128) + piece
            unit = jnp.where(unit < side_units, unit, unit + side_units)
            lanes = slice(piece * 128, (piece + 1) * 128)
            pair_out[:, pl.ds(pl.multiple_of(unit * 128, 128), 128)] = gate_back[:, lanes]
            unit += side_units
            pair_out[:, pl.ds(pl.multiple_of(unit * 128, 128), 128)] = up_back[:, lanes]
        sums[...] += nt(gate_back, wg[:, cut]) + nt(up_back, wu[:, cut])
        return 0

    lax.fori_loop(0, gate_s.shape[0], backward, 0)
    third_back = sums[...]
    gains_out[1:2, :] += jnp.sum(third_back * third_normed, axis=0, keepdims=True)
    middle_back = upstream + inward(third_back, third_gain[...], third_normed, third_scale)
    middle_out[...] = middle_back
    gains_out[0:1, :] += jnp.sum(middle_back * second_normed, axis=0, keepdims=True)
    attention_out[...] = inward(
        middle_back, second_gain[...], second_normed, second_scale
    ).astype(BF16)
    heads_low = nt(attention_out[...], wo[...]).astype(BF16)
    for side in range(2):
        for group in range(groups):
            at = (side * groups + group) * WIDE
            target = group * 2 + (tensor if side == 0 else 1 - tensor)
            heads_back[target] = heads_low[:, at : at + WIDE]


def middle_section(meta, adapted, heads, cotangent, gains, weights):
    rows, width = adapted.shape
    sources = heads.shape[0]
    inner = sources * WIDE
    hidden = 2 * weights[1].shape[1]
    block = rows // 2
    steps = rows // block
    row = pl.BlockSpec((block, width), lambda i, meta: (i, 0))
    wide = pl.BlockSpec((block, hidden), lambda i, meta: (i, 0))
    head = pl.BlockSpec((sources, block, WIDE), lambda i, meta: (0, i, 0))
    gain = pl.BlockSpec((1, width), lambda i, meta: (0, 0))
    hbm = pl.BlockSpec(memory_space=pl.ANY)
    return pl.pallas_call(
        middle_kernel,
        grid_spec=pltpu.PrefetchScalarGridSpec(
            num_scalar_prefetch=1,
            grid=(steps,),
            in_specs=[
                row,
                head,
                pl.BlockSpec((block, width), lambda i, meta: (meta[0] * steps + i, 0)),
                gain,
                gain,
                gain,
            ]
            + [hbm] * 8,
            out_specs=(
                row,
                row,
                pl.BlockSpec((block, inner), lambda i, meta: (i, 0)),
                row,
                row,
                row,
                wide,
                pl.BlockSpec((block, 2 * hidden), lambda i, meta: (i, 0)),
                head,
                pl.BlockSpec((8, width), lambda i, meta: (0, 0)),
            ),
            scratch_shapes=[
                pltpu.VMEM((inner, width), BF16),
                pltpu.VMEM((width, hidden), BF16),
                pltpu.VMEM((width, hidden), BF16),
                pltpu.VMEM((hidden, width), BF16),
                pltpu.VMEM((hidden // HIDDEN, block, HIDDEN), F32),
                pltpu.VMEM((hidden // HIDDEN, block, HIDDEN), F32),
                pltpu.VMEM((block, width), F32),
                pltpu.SemaphoreType.DMA((8,)),
            ],
        ),
        out_shape=(
            jax.ShapeDtypeStruct((rows, width), BF16),
            jax.ShapeDtypeStruct((rows, width), F32),
            jax.ShapeDtypeStruct((rows, inner), BF16),
            jax.ShapeDtypeStruct((rows, width), BF16),
            jax.ShapeDtypeStruct((rows, width), BF16),
            jax.ShapeDtypeStruct((rows, width), BF16),
            jax.ShapeDtypeStruct((rows, hidden), BF16),
            jax.ShapeDtypeStruct((rows, 2 * hidden), BF16),
            jax.ShapeDtypeStruct((sources, rows, WIDE), BF16),
            jax.ShapeDtypeStruct((8, width), F32),
        ),
        compiler_params=pltpu.CompilerParams(vmem_limit_bytes=VMEM_BYTES),
        cost_estimate=pl.CostEstimate(
            flops=rows * width * (4 * inner + 12 * hidden),
            bytes_accessed=6 * width * hidden + 2 * width * inner + rows * (hidden * 6 + width * 20),
            transcendentals=rows * hidden * 2,
        ),
        name="middle_section",
    )(meta, adapted, heads, cotangent, *gains, *weights)


class Reduction:
    def __init__(self, shape, by_lane=False, kind="all", cuts=None, base=0):
        self.base = base
        self.rows, self.lanes = shape
        self.by_lane = by_lane
        self.kind = kind
        self.cuts = cuts or [self.lanes]

    def chunk_shape(self, dp):
        rows, lanes = self.rows // 4, self.lanes
        return (rows, lanes // dp) if self.by_lane else (rows // dp, lanes)

    def outputs(self, dp):
        if self.kind == "sum":
            return [jax.ShapeDtypeStruct(self.chunk_shape(dp), BF16)]
        if self.base > 0:
            return []
        return [jax.ShapeDtypeStruct((self.rows, lanes), F32) for lanes in self.cuts]

    def scratch(self, dp):
        rows, lanes = self.rows, self.lanes
        half, quarter = pltpu.VMEM((rows // 2, lanes), BF16), pltpu.VMEM((rows // 4, lanes), BF16)
        dma = pltpu.SemaphoreType.DMA
        refs = {}
        if self.kind == "all":
            refs.update(half=half, core_land=half, x_land=quarter)
            refs.update(fold_send=dma((2,)), fold_recv=dma((2,)))
        if self.kind != "gather":
            refs.update(
                quarter=quarter,
                z_land=pltpu.VMEM((dp + 1,) + self.chunk_shape(dp), BF16),
                sum_send=dma((dp,)),
                sum_recv=dma((dp + 1,)),
            )
        if self.kind != "sum":
            refs.update(
                whole=quarter,
                others=pltpu.VMEM((3, rows // 4, lanes), BF16),
                send=dma((3,)),
                recv=dma((3,)),
                all_send=dma((2, dp)),
                all_recv=dma((dp,)),
                out_sem=dma((len(self.cuts),)),
            )
            for i, cut in enumerate(self.cuts):
                refs[f"wide{i}"] = pltpu.VMEM((rows // 4, cut), F32)
        self.names = list(refs)
        return list(refs.values())

    def bind(self, part, outs, refs):
        self.part, self.outs = part, outs
        for name, ref in zip(self.names, refs):
            setattr(self, name, ref)
        self.wide = [getattr(self, f"wide{i}", None) for i in range(len(self.cuts))]
        self.x, self.core, self.z = (lax.axis_index(name) for name in ("x", "core", "dp"))
        self.dp = lax.axis_size("dp")
        self.to_core = {"core": 1 - self.core}
        self.to_x = {"x": 1 - self.x}
        self.sends = []

    def copy(self, src, dst, send, recv, where):
        return pltpu.make_async_remote_copy(
            src_ref=src,
            dst_ref=dst,
            send_sem=send,
            recv_sem=recv,
            device_id=where,
            device_id_type=MESH,
        )

    def part_of(self, ref, index, rows):
        return ref.at[pl.ds(pl.multiple_of(index * rows, rows), rows)]

    def chunk(self, ref, index):
        if self.by_lane:
            lanes = self.lanes // self.dp
            return ref.at[:, pl.ds(pl.multiple_of(index * lanes, lanes), lanes)]
        return self.part_of(ref, index, self.rows // 4 // self.dp)

    def core_sum(self):
        half = self.rows // 2
        return self.copy(
            self.part_of(self.part, 1 - self.core, half),
            self.core_land,
            self.fold_send.at[0],
            self.fold_recv.at[0],
            self.to_core,
        )

    def x_sum(self):
        quarter = self.rows // 4
        return self.copy(
            self.part_of(self.half, 1 - self.x, quarter),
            self.x_land,
            self.fold_send.at[1],
            self.fold_recv.at[1],
            self.to_x,
        )

    def z_sum(self, j, step):
        up = {"dp": self.z + step}
        index = j
        lands = index if step > 0 else jnp.where(self.z - 1 == index, self.dp, index)
        return self.copy(
            self.chunk(self.quarter, index),
            self.z_land.at[lands],
            self.sum_send.at[index],
            self.sum_recv.at[lands],
            up,
        )

    def z_all(self, j, step):
        return self.copy(
            self.chunk(self.whole, j),
            self.chunk(self.whole, j),
            self.all_send.at[0 if step > 0 else 1, j],
            self.all_recv.at[j],
            {"dp": self.z + step},
        )

    def spread(self, which):
        src = self.others.at[0] if which == 2 else self.whole
        return self.copy(
            src,
            self.others.at[which],
            self.send.at[which],
            self.recv.at[which],
            self.to_x if which == 0 else self.to_core,
        )

    def writes(self, at):
        quarter = self.rows // 4
        core = self.core if at < 2 else 1 - self.core
        x = self.x if at % 2 == 0 else 1 - self.x
        row = pl.multiple_of(self.base + (2 * core + x) * quarter, quarter)
        return [
            pltpu.make_async_copy(wide, out.at[pl.ds(row, quarter)], self.out_sem.at[i])
            for i, (wide, out) in enumerate(zip(self.wide, self.outs))
        ]

    def emit(self, at, ref):
        if at > 0:
            for copy in self.writes(at - 1):
                copy.wait()
        lane = 0
        for wide, lanes in zip(self.wide, self.cuts):
            wide[...] = ref[:, lane : lane + lanes].astype(F32)
            lane += lanes
        for copy in self.writes(at):
            copy.start()

    def add(self, into, left, right):
        into[...] = (left[...].astype(F32) + right[...].astype(F32)).astype(BF16)

    def hop(self, h):
        last = self.dp - 1

        @pl.when(self.z == h)
        def _():
            for j in range(last, h, -1):
                if h > 0:
                    self.wait_sum(j)
                    self.add(self.chunk(self.quarter, j), self.chunk(self.quarter, j), self.z_land.at[j])
                self.z_sum(j, 1).start()

        @pl.when(self.z == last - h)
        def _():
            for j in range(0, last - h):
                if h > 0:
                    self.wait_sum(j)
                    self.add(self.chunk(self.quarter, j), self.chunk(self.quarter, j), self.z_land.at[j])
                self.z_sum(j, -1).start()

    def wait_sum(self, lands):
        self.copy(
            self.z_land.at[lands],
            self.z_land.at[lands],
            self.sum_send.at[0],
            self.sum_recv.at[lands],
            self.to_x,
        ).wait_recv()

    def all_hop(self, h):
        z, last = self.z, self.dp - 1
        low, high = jnp.maximum(z - h, 0), jnp.minimum(z + h, last)

        @pl.when(z >= h)
        def _():
            self.z_all(low, 1).wait_recv()

        @pl.when((z >= h) & (z < last))
        def _():
            self.z_all(low, 1).start()

        @pl.when(z <= last - h)
        def _():
            self.z_all(high, -1).wait_recv()

        @pl.when((z <= last - h) & (z > 0))
        def _():
            self.z_all(high, -1).start()

    def stages(self):
        def start():
            self.core_sum().start()

        def fold_core():
            self.core_sum().wait_recv()
            self.add(
                self.half, self.part_of(self.part, self.core, self.rows // 2), self.core_land
            )
            self.x_sum().start()

        def begin():
            self.quarter[...] = self.part[...]
            self.hop(0)

        def fold_x():
            self.x_sum().wait_recv()
            self.add(
                self.quarter, self.part_of(self.half, self.x, self.rows // 4), self.x_land
            )
            self.hop(0)

        def settle():
            z, last = self.z, self.dp - 1
            mine = self.chunk(self.quarter, z)

            @pl.when(z > 0)
            def _():
                self.wait_sum(z)
                self.add(mine, mine, self.z_land.at[z])

            @pl.when(z < last)
            def _():
                self.wait_sum(self.dp)
                self.add(mine, mine, self.z_land.at[self.dp])

            if self.kind == "sum":
                self.outs[0][...] = mine[...]
            else:
                self.chunk(self.whole, z)[...] = mine[...]
                gather()

        def place():
            self.chunk(self.whole, self.z)[...] = self.part[...]
            gather()

        def gather():
            z, last = self.z, self.dp - 1

            @pl.when(z < last)
            def _():
                self.z_all(z, 1).start()

            @pl.when(z > 0)
            def _():
                self.z_all(z, -1).start()

        def share():
            self.all_hop(self.dp - 1)
            self.spread(0).start()
            self.spread(1).start()
            self.emit(0, self.whole)

        def pass_on():
            self.spread(0).wait_recv()
            self.spread(2).start()
            self.emit(1, self.others.at[0])

        def last():
            self.spread(1).wait_recv()
            self.emit(2, self.others.at[1])
            self.spread(2).wait_recv()
            self.emit(3, self.others.at[2])

        sums = [functools.partial(self.hop, h) for h in range(1, self.dp - 1)] + [settle]
        gathers = [functools.partial(self.all_hop, h) for h in range(1, self.dp - 1)]
        gathers += [share, pass_on, last]
        return {
            "all": [start, fold_core, fold_x] + sums + gathers,
            "sum": [begin] + sums,
            "gather": [place] + gathers,
        }[self.kind]

    def drain(self):
        z, last = self.z, self.dp - 1
        if self.kind == "all":
            self.core_sum().wait_send()
            self.x_sum().wait_send()
        if self.kind != "gather":
            for j in range(self.dp):

                @pl.when(z < j)
                def _():
                    self.z_sum(j, 1).wait_send()

                @pl.when(z > j)
                def _():
                    self.z_sum(j, -1).wait_send()

        if self.kind == "sum":
            return
        for j in range(self.dp):

            @pl.when((z >= j) & (z < last))
            def _():
                self.z_all(j, 1).wait_send()

            @pl.when((z <= j) & (z > 0))
            def _():
                self.z_all(j, -1).wait_send()

        for which in range(3):
            self.spread(which).wait_send()
        for copy in self.writes(3):
            copy.wait()


def bind_all(items, parts, outs, scratch):
    dp = lax.axis_size("dp")
    for item, part in zip(items, parts):
        size = len(item.scratch(dp))
        if item.base == 0:
            own, outs = outs[: len(item.cuts)], outs[len(item.cuts) :]
        item.bind(part, own, scratch[:size])
        scratch = scratch[size:]


def waves(plans, offsets):
    length = max(len(plan) + i for i, plan in zip(offsets, plans))
    return [
        [plan[t - i] for i, plan in zip(offsets, plans) if 0 <= t - i < len(plan)]
        for t in range(length)
    ]


def greet_line(barrier):
    z, last = lax.axis_index("dp"), lax.axis_size("dp") - 1

    @pl.when(z > 0)
    def _():
        pl.semaphore_signal(barrier, inc=1, device_id={"dp": z - 1}, device_id_type=MESH)

    @pl.when(z < last)
    def _():
        pl.semaphore_signal(barrier, inc=1, device_id={"dp": z + 1}, device_id_type=MESH)

    return jnp.minimum(z, 1) + jnp.minimum(last - z, 1)


LEAVE = 128


def leave_kernel(items, *refs):
    sent, adapted, middle_back, first_low, gain, query_w, key_w, value_w = refs[:8]
    parts, refs = refs[8 : 8 + len(items)], refs[8 + len(items) :]
    grads, adapted_low, gain_out = refs[:3], refs[3], refs[4]
    count = sum(len(item.cuts) for item in items)
    outs, refs = refs[5 : 5 + count], refs[5 + count :]
    landed, away, away_landed, joined, grad_sum = refs[:5]
    part_send, part_recv, away_send, away_recv, low_send, low_recv = refs[5:11]
    bind_all(items, parts, outs, refs[11:])
    plans = [item.stages() for item in items]
    stages = list(zip(*plans))
    away_plan = {0: stages[0]}
    home_plan = {1: stages[1], 4: stages[2]}
    me, others = neighbours()
    tensor = lax.axis_index("tensor")
    tensor_peer = {"tensor": 1 - tensor}
    barrier = pltpu.get_barrier_semaphore()
    for target in [tensor_peer] + [where for _, where in others]:
        pl.semaphore_signal(barrier, inc=1, device_id=target, device_id_type=MESH)
    pl.semaphore_wait(barrier, 1 + len(others) + greet_line(barrier))
    half = adapted.shape[0]
    inner = query_w.shape[1]
    steps = half // LEAVE

    def block(start, i):
        return pl.ds(pl.multiple_of(start + i * LEAVE, LEAVE), LEAVE)

    def gather(side, i, at):
        here = block((tensor if side else 1 - tensor) * half, i)
        place, where = others[at]
        return pltpu.make_async_remote_copy(
            src_ref=sent.at[place, here],
            dst_ref=landed.at[me, here],
            send_sem=part_send.at[side, i, at],
            recv_sem=part_recv.at[side, i, at],
            device_id=where,
            device_id_type=MESH,
        )

    def hand_over(i):
        return pltpu.make_async_remote_copy(
            src_ref=away.at[block(0, i)],
            dst_ref=away_landed.at[block(0, i)],
            send_sem=away_send.at[i],
            recv_sem=away_recv.at[i],
            device_id=tensor_peer,
            device_id_type=MESH,
        )

    def share(i):
        here = block(tensor * half, i)
        return pltpu.make_async_remote_copy(
            src_ref=adapted_low.at[here],
            dst_ref=adapted_low.at[here],
            send_sem=low_send.at[i],
            recv_sem=low_recv.at[i],
            device_id=tensor_peer,
            device_id_type=MESH,
        )

    for side in range(2):

        def begin(i, _):
            for at in range(len(others)):
                gather(side, i, at).start()
            return 0

        lax.fori_loop(0, steps, begin, 0)
    landed[me] = sent[me]
    gain_out[...] = jnp.zeros_like(gain_out)
    grad_sum[...] = jnp.zeros_like(grad_sum)

    def input_grad(side, i):
        for at in range(len(others)):
            gather(side, i, at).wait_recv()
        here = block((tensor if side else 1 - tensor) * half, i)
        for at in range(3):
            for group in range(landed.shape[0]):
                to = at * inner + group * WIDE
                joined[:, to : to + WIDE] = landed[group, here, at * WIDE : (at + 1) * WIDE]
        total = nt(joined[:, 0:inner], query_w[...])
        total += nt(joined[:, inner : 2 * inner], key_w[...])
        total += nt(joined[:, 2 * inner : 3 * inner], value_w[...])
        return total

    def weight_grad(side, i):
        here = block((tensor if side else 1 - tensor) * half, i)
        low = first_low[here, :].T
        for at in range(3):
            lanes = slice(at * inner, (at + 1) * inner)
            grad_sum[:, lanes] += nn(low, joined[:, lanes])

    def away_step(i, _):
        away[block(0, i), :] = input_grad(0, i).astype(BF16)
        hand_over(i).start()
        weight_grad(0, i)
        at_step(i, away_plan)
        return 0

    lax.fori_loop(0, steps, away_step, 0)

    def home_step(i, _):
        total = input_grad(1, i)
        hand_over(i).wait_recv()
        rows = block(0, i)
        upstream = total + away_landed[rows, :].astype(F32)
        values = adapted[rows, :]
        scale = lax.rsqrt(jnp.mean(values * values, axis=-1, keepdims=True) + EPSILON)
        normed = values * scale
        scaled = upstream * gain[...]
        inward = scale * (scaled - normed * jnp.mean(scaled * normed, axis=-1, keepdims=True))
        gain_out[0:1, :] += jnp.sum(upstream * normed, axis=0, keepdims=True)
        adapted_low[block(tensor * half, i), :] = (middle_back[rows, :] + inward).astype(BF16)
        share(i).start()
        weight_grad(1, i)
        at_step(i, home_plan)
        return 0

    lax.fori_loop(0, steps, home_step, 0)
    for at in range(3):
        grads[at][...] = grad_sum[:, at * inner : (at + 1) * inner].astype(BF16)
    for call in stages[3]:
        call()
    for item in items:
        item.drain()

    def finish(i, _):
        for side in range(2):
            for at in range(len(others)):
                gather(side, i, at).wait_send()
        hand_over(i).wait_send()
        share(i).wait()
        return 0

    lax.fori_loop(0, steps, finish, 0)


def leave(
    sent, adapted, middle_back, first_low, gain, query_w, key_w, value_w, parts, by_lanes
):
    items = [
        Reduction((4 * part.shape[0], part.shape[1]), by_lane, "sum")
        for part, by_lane in zip(parts, by_lanes)
    ]
    dp = lax.axis_size("dp")
    scratch, outs = [], []
    for item in items:
        scratch += item.scratch(dp)
        outs += item.outputs(dp)
    peers, rows, lanes = sent.shape
    half, width = adapted.shape
    inner = query_w.shape[1]
    steps = half // LEAVE
    vmem = pl.BlockSpec(memory_space=pltpu.VMEM)
    return pl.pallas_call(
        functools.partial(leave_kernel, items),
        out_shape=(jax.ShapeDtypeStruct((width, inner), BF16),) * 3
        + (
            jax.ShapeDtypeStruct((rows, width), BF16),
            jax.ShapeDtypeStruct((8, width), F32),
        )
        + tuple(outs),
        in_specs=[vmem] * (8 + len(items)),
        out_specs=(vmem,) * (5 + len(outs)),
        scratch_shapes=[
            pltpu.VMEM((peers, rows, lanes), BF16),
            pltpu.VMEM((half, width), BF16),
            pltpu.VMEM((half, width), BF16),
            pltpu.VMEM((LEAVE, 3 * inner), BF16),
            pltpu.VMEM((width, 3 * inner), F32),
            pltpu.SemaphoreType.DMA((2, steps, 3)),
            pltpu.SemaphoreType.DMA((2, steps, 3)),
        ]
        + [pltpu.SemaphoreType.DMA((steps,))] * 4
        + scratch,
        compiler_params=pltpu.CompilerParams(
            vmem_limit_bytes=VMEM_BYTES, collective_id=1, has_side_effects=True
        ),
        cost_estimate=pl.CostEstimate(
            flops=4 * rows * width * 3 * inner, bytes_accessed=200 << 20, transcendentals=rows
        ),
        name="leave",
    )(sent, adapted, middle_back, first_low, gain, query_w, key_w, value_w, *parts)


class SmallSum:
    def __init__(self, shape):
        self.shape = shape

    def scratch(self, dp):
        return [
            pltpu.VMEM((3,) + self.shape, F32),
            pltpu.VMEM((3,) + self.shape, F32),
            pltpu.VMEM((dp,) + self.shape, F32),
            pltpu.SemaphoreType.DMA((3,)),
            pltpu.SemaphoreType.DMA((3,)),
            pltpu.SemaphoreType.DMA((2, dp)),
            pltpu.SemaphoreType.DMA((dp,)),
        ]

    def bind(self, part, out, refs):
        self.part, self.out = part, out
        (
            self.mine,
            self.theirs,
            self.line,
            self.send,
            self.recv,
            self.line_send,
            self.line_recv,
        ) = refs
        self.z, self.dp = lax.axis_index("dp"), lax.axis_size("dp")
        self.targets = [{name: 1 - lax.axis_index(name)} for name in ("tensor", "core", "x")]

    def pair(self, at):
        return pltpu.make_async_remote_copy(
            src_ref=self.mine.at[at],
            dst_ref=self.theirs.at[at],
            send_sem=self.send.at[at],
            recv_sem=self.recv.at[at],
            device_id=self.targets[at],
            device_id_type=MESH,
        )

    def pass_along(self, j, step):
        return pltpu.make_async_remote_copy(
            src_ref=self.line.at[j],
            dst_ref=self.line.at[j],
            send_sem=self.line_send.at[0 if step > 0 else 1, j],
            recv_sem=self.line_recv.at[j],
            device_id={"dp": self.z + step},
            device_id_type=MESH,
        )

    def stages(self):
        def begin():
            self.mine[0] = self.part[...]
            self.pair(0).start()

        def fold(at):
            self.pair(at - 1).wait_recv()
            total = self.mine[at - 1] + self.theirs[at - 1]
            if at < 3:
                self.mine[at] = total
                self.pair(at).start()
            else:
                self.line[self.z] = total
                self.send_on(self.z, self.z)

        def hop(h):
            z, last = self.z, self.dp - 1
            low, high = jnp.maximum(z - h, 0), jnp.minimum(z + h, last)

            @pl.when(z >= h)
            def _():
                self.pass_along(low, 1).wait_recv()

            @pl.when((z >= h) & (z < last))
            def _():
                self.pass_along(low, 1).start()

            @pl.when(z <= last - h)
            def _():
                self.pass_along(high, -1).wait_recv()

            @pl.when((z <= last - h) & (z > 0))
            def _():
                self.pass_along(high, -1).start()

        def last():
            total = self.line[0]
            for j in range(1, self.dp):
                total = total + self.line[j]
            self.out[...] = total

        call = functools.partial
        return (
            [begin]
            + [call(fold, at) for at in (1, 2, 3)]
            + [call(hop, h) for h in range(1, self.dp)]
            + [last]
        )

    def send_on(self, up, down):
        @pl.when(self.z < self.dp - 1)
        def _():
            self.pass_along(up, 1).start()

        @pl.when(self.z > 0)
        def _():
            self.pass_along(down, -1).start()

    def drain(self):
        z, last = self.z, self.dp - 1
        for at in range(3):
            self.pair(at).wait_send()
        for j in range(self.dp):

            @pl.when((z >= j) & (z < last))
            def _():
                self.pass_along(j, 1).wait_send()

            @pl.when((z <= j) & (z > 0))
            def _():
                self.pass_along(j, -1).wait_send()


def reduce_kernel(items, small, *refs):
    count = len(items)
    outs = sum(len(item.cuts) for item in items if item.base == 0)
    parts, refs = refs[: count + 1], refs[count + 1 :]
    small_refs = len(small.scratch(lax.axis_size("dp")))
    small.bind(parts[count], refs[outs], refs[outs + 1 : outs + 1 + small_refs])
    bind_all(items, parts[:count], refs[:outs], refs[outs + 1 + small_refs :])
    barrier = pltpu.get_barrier_semaphore()
    for target in small.targets:
        pl.semaphore_signal(barrier, inc=1, device_id=target, device_id_type=MESH)
    pl.semaphore_wait(barrier, 3 + greet_line(barrier))
    plans = [item.stages() for item in items if item.kind == "all"]
    gathers = [item.stages() for item in items if item.kind == "gather"]
    for plan in plans:
        plan[0]()
    for plan in gathers:
        plan[0]()
    for plan in plans:
        plan[1]()
    offsets = list(range(len(plans))) + [2 + i for i in range(len(gathers))]
    rest = [plan[2:] for plan in plans] + [plan[1:] for plan in gathers] + [small.stages()]
    for wave in waves(rest, offsets + [1]):
        for call in wave:
            call()
    for item in items + [small]:
        item.drain()


def reduce_all(parts, chunks, shapes, by_lanes, gains):
    dp = lax.axis_size("dp")
    items = [Reduction(part.shape) for part in parts[:-1]]
    items.append(Reduction(parts[-1].shape, base=parts[-2].shape[0]))
    items += [Reduction(shape, by_lane, "gather") for shape, by_lane in zip(shapes, by_lanes)]
    small = SmallSum(gains.shape)
    scratch, outs = small.scratch(dp), []
    for item in items:
        scratch += item.scratch(dp)
        outs += item.outputs(dp)
    both = len(parts) - 2
    outs[both] = jax.ShapeDtypeStruct((2 * parts[-1].shape[0], parts[-1].shape[1]), F32)
    moved = sum(item.rows * item.lanes for item in items)
    return pl.pallas_call(
        functools.partial(reduce_kernel, items, small),
        out_shape=tuple(outs) + (jax.ShapeDtypeStruct(gains.shape, F32),),
        in_specs=[pl.BlockSpec(memory_space=pltpu.VMEM)] * (len(items) + 1),
        out_specs=(pl.BlockSpec(memory_space=pl.ANY),) * len(outs)
        + (pl.BlockSpec(memory_space=pltpu.VMEM),),
        scratch_shapes=scratch,
        compiler_params=pltpu.CompilerParams(
            vmem_limit_bytes=VMEM_BYTES, collective_id=2, has_side_effects=True
        ),
        cost_estimate=pl.CostEstimate(
            flops=moved * 4, bytes_accessed=moved * 30, transcendentals=0
        ),
        name="reduce_all",
    )(*parts, *chunks, gains)


def latent_kernel(low, weight, out):
    rows, inputs, lanes = low.shape[0], weight.shape[0], weight.shape[1]
    blocks = lanes // 128
    for at in range(inputs):
        values = nt(low[...], weight[at])
        for block in range(blocks):
            out[pl.ds(block * inputs + at, rows, stride=blocks * inputs), :] = values[
                :, block * 128 : (block + 1) * 128
            ]


def latent_grad(low, adapter):
    tokens, width = low.shape
    inputs, lanes, _ = adapter.shape
    blocks = lanes // 128
    step = SEG
    flat = pl.pallas_call(
        latent_kernel,
        grid=(tokens // step,),
        out_shape=jax.ShapeDtypeStruct((tokens * blocks * inputs, 128), F32),
        in_specs=[
            pl.BlockSpec((step, width), lambda i: (i, 0)),
            pl.BlockSpec(adapter.shape, lambda i: (0, 0, 0)),
        ],
        out_specs=pl.BlockSpec((step * blocks * inputs, 128), lambda i: (i, 0)),
        compiler_params=pltpu.CompilerParams(vmem_limit_bytes=VMEM_BYTES),
        cost_estimate=pl.CostEstimate(
            flops=2 * tokens * width * lanes * inputs,
            bytes_accessed=tokens * (2 * width + 4 * lanes * inputs) + 2 * width * lanes * inputs,
            transcendentals=0,
        ),
        name="latent_grad",
    )(low, adapter)
    flat = flat.reshape(tokens, blocks, inputs, 128)
    return flat.transpose(0, 2, 1, 3).reshape(tokens, inputs, lanes)


def swap(value, axis):
    return lax.ppermute(value, axis, [(0, 1), (1, 0)])


def together(*values):
    return lax.optimization_barrier(values)


def cut(value, index, rows):
    return lax.dynamic_slice_in_dim(value, index * rows, rows, 0)


def add_low(left, right):
    return (left.astype(F32) + right.astype(F32)).astype(BF16)


def fold(value, index, axis):
    half = value.shape[0] // 2
    return add_low(cut(value, index, half), swap(cut(value, 1 - index, half), axis))


def unfold(value, index, axis):
    other = swap(value, axis)
    return jnp.concatenate(
        [jnp.where(index == 0, value, other), jnp.where(index == 0, other, value)], axis=0
    )


def tn(left, right):
    return lax.dot_general(
        left, right, (((0,), (0,)), ((), ())), preferred_element_type=F32
    ).astype(BF16)


def on_device_paired(
    latent_embed,
    adapter,
    first_gain,
    query_weight,
    key_weight,
    value_weight,
    output_weight,
    second_gain,
    third_gain,
    gate_weight,
    up_weight,
    down_weight,
    fourth_gain,
    parents,
    positions,
    cotangent,
):
    rows = latent_embed.shape[0]
    width = adapter.shape[2]
    half_rows = rows // 2
    tensor = lax.axis_index("tensor")
    core = lax.axis_index("core")
    x = lax.axis_index("x")
    everyone = ("x", "core", "tensor")
    meta = jnp.stack([tensor, core]).astype(jnp.int32)
    one_row = lambda gain: gain.reshape(1, -1)

    cosine, sine = angle_tables(positions)
    mine = jnp.einsum(
        "rcd,cde->re", latent_embed, adapter, preferred_element_type=F32
    ).astype(BF16)
    parts, first_low, theirs = enter(
        mine, one_row(first_gain), query_weight, key_weight, value_weight, cosine, sine
    )
    adapted = cut(mine, tensor, half_rows).astype(F32) + cut(theirs, tensor, half_rows).astype(
        F32
    )
    role, place, parts = sort_parts(parents, parts.reshape(-1, 3 * WIDE))
    own_weights = (output_weight, gate_weight, up_weight, down_weight)
    attended, logsum, *other_weights = attention_forward(parts, own_weights)
    heads = lax.all_to_all(
        pick(place, attended).reshape(8, half_rows, WIDE), everyone, 0, 0, tiled=False
    )
    (
        layer_half,
        middle_back,
        attended_all,
        attention_low,
        third_low,
        mixed_low,
        hidden,
        pair_low,
        heads_back,
        gain_parts,
    ) = middle_section(
        meta,
        adapted,
        heads,
        cotangent,
        (one_row(second_gain), one_row(third_gain), one_row(fourth_gain)),
        own_weights + tuple(other_weights),
    )
    upstream = lax.all_to_all(heads_back, everyone, 0, 0, tiled=False).reshape(-1, WIDE)
    layer_other = swap(layer_half, "tensor")
    layer_out = jnp.concatenate(
        [
            jnp.where(tensor == 0, layer_half, layer_other),
            jnp.where(tensor == 0, layer_other, layer_half),
        ],
        axis=0,
    ).astype(F32)

    inner = output_weight.shape[0]
    grads = (
        tn(third_low, pair_low),
        tn(hidden, mixed_low),
        tn(attended_all, attention_low),
    )
    shapes = [gate_weight.shape, down_weight.shape, up_weight.shape, output_weight.shape]

    table_cosine, table_sine = angle_tables(jnp.arange((TRUNK + 2) * SEG))
    by_lanes = [False, True, False, False]
    sent, *sums = attention_backward(
        parts, pick(role, upstream), attended, logsum, table_cosine, table_sine, grads, shapes
    )
    (
        query_part,
        key_part,
        value_part,
        adapted_low,
        first_gain_part,
        *chunks,
    ) = leave(
        pick(place, sent).reshape(4, rows, 3 * WIDE),
        adapted,
        middle_back,
        first_low,
        one_row(first_gain),
        query_weight,
        key_weight,
        value_weight,
        sums,
        by_lanes,
    )
    adapter_part = jnp.einsum(
        "rcd,re->cde", latent_embed, adapted_low, preferred_element_type=F32
    ).astype(BF16)
    (
        query_total,
        key_total,
        value_total,
        adapter_total,
        gate_total,
        down_total,
        up_total,
        output_total,
        gains,
    ) = reduce_all(
        [query_part, key_part, value_part, adapter_part[0], adapter_part[1]],
        chunks,
        shapes,
        by_lanes,
        jnp.concatenate([gain_parts[:3], first_gain_part[:5]], axis=0),
    )
    latent_gradient = latent_grad(adapted_low, adapter)
    return (
        layer_out,
        latent_gradient,
        adapter_total.reshape(adapter.shape),
        gains[3],
        query_total,
        key_total,
        value_total,
        output_total,
        gains[0],
        gains[1],
        gate_total,
        up_total,
        down_total,
        gains[2],
    )


def specs(rows):
    split = P(None, "tensor")
    in_specs = (
        P(rows, None, "tensor"),
        P(None, "tensor", None),
        P(),
        split,
        split,
        split,
        P("tensor", None),
        P(),
        P(),
        split,
        split,
        P("tensor", None),
        P(),
        P("dp", None),
        P(rows),
        P(rows, None),
    )
    out_specs = (
        P(rows, None),
        P(rows, None, "tensor"),
        P(None, "tensor", None),
        P(),
        split,
        split,
        split,
        P("tensor", None),
        P(),
        P(),
        split,
        split,
        P("tensor", None),
        P(),
    )
    return in_specs, out_specs


def solution(mesh):
    sizes = dict(mesh.shape)
    if sizes["seq"] == 4 and sizes["tensor"] == 2:
        fine = Mesh(
            mesh.devices.reshape(sizes["dp"], 2, 2, 2), ("dp", "x", "core", "tensor")
        )
        in_specs, out_specs = specs(("dp", "x", "core"))
        return jax.shard_map(
            on_device_paired, mesh=fine, in_specs=in_specs, out_specs=out_specs, check_vma=False
        )
    in_specs, out_specs = specs(("dp", "seq"))
    return jax.shard_map(
        on_device, mesh=mesh, in_specs=in_specs, out_specs=out_specs, check_vma=False
    )
```

```python
import functools

import jax
import jax.numpy as jnp
from jax import lax
from jax.experimental import pallas as pl
from jax.experimental.pallas import tpu as pltpu
from jax.sharding import Mesh
from jax.sharding import PartitionSpec as P

DH = 64
SEG = 256


EPSILON = 1e-06
THETA = 50000.0


def normalize(values, gain):
    scale = lax.rsqrt(jnp.mean(values * values, axis=-1, keepdims=True) + EPSILON)
    normed = values * scale
    return (normed * gain, normed, scale)


def normalize_back(upstream, gain, normed, scale):
    scaled = upstream * gain
    inward = scale * (scaled - normed * jnp.mean(scaled * normed, axis=-1, keepdims=True))
    return (inward, jnp.sum(upstream * normed, axis=0))


def angles(positions, width):
    half = width // 2
    freq = THETA ** (-jnp.arange(half, dtype=jnp.float32) * 2.0 / width)
    angle = positions.astype(jnp.float32)[:, None] * freq[None, :]
    return (jnp.cos(angle)[:, None, :], jnp.sin(angle)[:, None, :])


def rotate(values, cosine, sine, sign):
    half = values.shape[-1] // 2
    first = values[..., :half]
    second = values[..., half:]
    return jnp.concatenate(
        [first * cosine - sign * second * sine, second * cosine + sign * first * sine], axis=-1
    )


def ancestry(parent_row):
    labels = jnp.arange(parent_row.shape[0], dtype=jnp.int32)

    def extend(index, state):
        current, total = state
        total = total | (current[:, None] == labels[None, :])
        current = jnp.where(current >= 0, jnp.take(parent_row, jnp.maximum(current, 0)), -1)
        return (current, total)

    start = (parent_row, jnp.zeros((parent_row.shape[0], parent_row.shape[0]), jnp.bool_))
    current, total = lax.fori_loop(0, parent_row.shape[0], extend, start)
    return total


def path_mask(parent_row, query_ids, key_ids):
    table = ancestry(parent_row)
    query_seg = query_ids // SEG
    key_seg = key_ids // SEG
    far = jnp.take(jnp.take(table, query_seg, axis=0), key_seg, axis=1)
    near = (query_seg[:, None] == key_seg[None, :]) & (key_ids[None, :] <= query_ids[:, None])
    return far | near


def on_device(
    latent_embed,
    adapter,
    first_gain,
    query_weight,
    key_weight,
    value_weight,
    output_weight,
    second_gain,
    third_gain,
    gate_weight,
    up_weight,
    down_weight,
    fourth_gain,
    parents,
    positions,
    cotangent,
):
    rows = latent_embed.shape[0]
    local_heads = query_weight.shape[1] // DH
    scale = DH ** (-0.5)
    adapted = lax.psum(
        jnp.einsum("rcd,cde->re", latent_embed, adapter, preferred_element_type=jnp.float32),
        "tensor",
    )
    first_out, first_normed, first_scale = normalize(adapted, first_gain)
    first_low = first_out.astype(jnp.bfloat16)
    cosine, sine = angles(positions, DH)
    query_raw = jnp.dot(first_low, query_weight, preferred_element_type=jnp.float32).reshape(
        rows, local_heads, DH
    )
    queries = rotate(query_raw, cosine, sine, 1.0).astype(jnp.bfloat16)
    key_raw = jnp.dot(first_low, key_weight, preferred_element_type=jnp.float32).reshape(
        rows, local_heads, DH
    )
    keys_local = rotate(key_raw, cosine, sine, 1.0).astype(jnp.bfloat16)
    values_local = (
        jnp.dot(first_low, value_weight, preferred_element_type=jnp.float32)
        .astype(jnp.bfloat16)
        .reshape(rows, local_heads, DH)
    )
    keys_all, values_all = (
        lax.all_gather(keys_local, "seq", axis=0, tiled=True),
        lax.all_gather(values_local, "seq", axis=0, tiled=True),
    )
    tree_rows = keys_all.shape[0]
    query_ids = lax.axis_index("seq") * rows + jnp.arange(rows, dtype=jnp.int32)
    key_ids = jnp.arange(tree_rows, dtype=jnp.int32)
    allowed = path_mask(parents[0], query_ids, key_ids)[None]

    def score_block(keys):
        raw = jnp.einsum("qhd,khd->hqk", queries, keys, preferred_element_type=jnp.float32) * scale
        return jnp.where(allowed, raw, -1e30)

    scores = score_block(keys_all)
    top = jnp.max(scores, axis=-1, keepdims=True)
    weights = jnp.exp(scores - top)
    total = jnp.sum(weights, axis=-1, keepdims=True)
    probs = weights / total
    logsum = top + jnp.log(total)
    attended = jnp.einsum(
        "hqk,khd->qhd", probs.astype(jnp.bfloat16), values_all, preferred_element_type=jnp.float32
    )
    attended = attended.reshape(rows, local_heads * DH).astype(jnp.bfloat16)
    attention = lax.psum(
        jnp.dot(attended, output_weight, preferred_element_type=jnp.float32).astype(jnp.bfloat16),
        "tensor",
    ).astype(jnp.float32)
    second_out, second_normed, second_scale = normalize(attention, second_gain)
    middle = adapted + second_out
    third_out, third_normed, third_scale = normalize(middle, third_gain)
    third_low = third_out.astype(jnp.bfloat16)
    gate = jnp.dot(third_low, gate_weight, preferred_element_type=jnp.float32)
    upward = jnp.dot(third_low, up_weight, preferred_element_type=jnp.float32)
    hidden = (jax.nn.silu(gate) * upward).astype(jnp.bfloat16)
    mixed = lax.psum(
        jnp.dot(hidden, down_weight, preferred_element_type=jnp.float32).astype(jnp.bfloat16),
        "tensor",
    ).astype(jnp.float32)
    fourth_out, fourth_normed, fourth_scale = normalize(mixed, fourth_gain)
    layer_out = middle + fourth_out
    upstream = cotangent.astype(jnp.float32)
    mixed_back, fourth_gain_part = normalize_back(
        upstream, fourth_gain, fourth_normed, fourth_scale
    )
    mixed_low = mixed_back.astype(jnp.bfloat16)
    down_part = jnp.einsum("rf,rd->fd", hidden, mixed_low, preferred_element_type=jnp.float32)
    hidden_back = (
        jnp.einsum("rd,fd->rf", mixed_low, down_weight, preferred_element_type=jnp.float32)
        .astype(jnp.bfloat16)
        .astype(jnp.float32)
    )
    swiglu_value, product_back = jax.vjp(
        lambda left, right: jax.nn.silu(left) * right, gate, upward
    )
    gate_back, up_back = product_back(hidden_back)
    gate_low = gate_back.astype(jnp.bfloat16)
    up_low = up_back.astype(jnp.bfloat16)
    gate_part = jnp.einsum("rd,rf->df", third_low, gate_low, preferred_element_type=jnp.float32)
    up_part = jnp.einsum("rd,rf->df", third_low, up_low, preferred_element_type=jnp.float32)
    third_term = jnp.einsum(
        "rf,df->rd", gate_low, gate_weight, preferred_element_type=jnp.float32
    ) + jnp.einsum("rf,df->rd", up_low, up_weight, preferred_element_type=jnp.float32)
    third_back = lax.psum(third_term.astype(jnp.bfloat16), "tensor").astype(jnp.float32)
    middle_part, third_gain_part = normalize_back(third_back, third_gain, third_normed, third_scale)
    middle_back = upstream + middle_part
    attention_back, second_gain_part = normalize_back(
        middle_back, second_gain, second_normed, second_scale
    )
    attention_low = attention_back.astype(jnp.bfloat16)
    output_part = jnp.einsum(
        "re,rd->ed", attended, attention_low, preferred_element_type=jnp.float32
    )
    attended_back = (
        jnp.einsum("rd,ed->re", attention_low, output_weight, preferred_element_type=jnp.float32)
        .astype(jnp.bfloat16)
        .reshape(rows, local_heads, DH)
    )
    keys_back, values_back = (
        lax.all_gather(keys_local, "seq", axis=0, tiled=True),
        lax.all_gather(values_local, "seq", axis=0, tiled=True),
    )
    probs_back = jnp.exp(score_block(keys_back) - logsum)
    prob_grad = jnp.einsum(
        "qhd,khd->hqk", attended_back, values_back, preferred_element_type=jnp.float32
    )
    score_grad = (
        probs_back * (prob_grad - jnp.sum(prob_grad * probs_back, axis=-1, keepdims=True))
    ).astype(jnp.bfloat16)
    query_rot = (
        jnp.einsum("hqk,khd->qhd", score_grad, keys_back, preferred_element_type=jnp.float32)
        * scale
    )
    key_rot_all = (
        jnp.einsum("hqk,qhd->khd", score_grad, queries, preferred_element_type=jnp.float32) * scale
    )
    value_back_all = jnp.einsum(
        "hqk,qhd->khd",
        probs_back.astype(jnp.bfloat16),
        attended_back,
        preferred_element_type=jnp.float32,
    )
    key_rot, value_back = (
        lax.psum_scatter(
            key_rot_all.astype(jnp.bfloat16), "seq", scatter_dimension=0, tiled=True
        ).astype(jnp.float32),
        lax.psum_scatter(
            value_back_all.astype(jnp.bfloat16), "seq", scatter_dimension=0, tiled=True
        ).astype(jnp.float32),
    )
    query_low = (
        rotate(query_rot, cosine, sine, -1.0).astype(jnp.bfloat16).reshape(rows, local_heads * DH)
    )
    key_low = (
        rotate(key_rot, cosine, sine, -1.0).astype(jnp.bfloat16).reshape(rows, local_heads * DH)
    )
    value_low = value_back.astype(jnp.bfloat16).reshape(rows, local_heads * DH)
    query_part = jnp.einsum("rd,re->de", first_low, query_low, preferred_element_type=jnp.float32)
    key_part = jnp.einsum("rd,re->de", first_low, key_low, preferred_element_type=jnp.float32)
    value_part = jnp.einsum("rd,re->de", first_low, value_low, preferred_element_type=jnp.float32)
    first_term = jnp.einsum(
        "re,de->rd", query_low, query_weight, preferred_element_type=jnp.float32
    )
    first_term = first_term + jnp.einsum(
        "re,de->rd", key_low, key_weight, preferred_element_type=jnp.float32
    )
    first_term = first_term + jnp.einsum(
        "re,de->rd", value_low, value_weight, preferred_element_type=jnp.float32
    )
    first_back = lax.psum(first_term.astype(jnp.bfloat16), "tensor").astype(jnp.float32)
    adapted_part, first_gain_part = normalize_back(
        first_back, first_gain, first_normed, first_scale
    )
    adapted_low = (middle_back + adapted_part).astype(jnp.bfloat16)
    latent_gradient = jnp.einsum(
        "re,cde->rcd", adapted_low, adapter, preferred_element_type=jnp.float32
    )
    adapter_part = jnp.einsum(
        "rcd,re->cde", latent_embed, adapted_low, preferred_element_type=jnp.float32
    )
    summed = (
        lax.psum(gate_part.astype(jnp.bfloat16), ("dp", "seq")).astype(jnp.float32),
        lax.psum(up_part.astype(jnp.bfloat16), ("dp", "seq")).astype(jnp.float32),
        lax.psum(down_part.astype(jnp.bfloat16), ("dp", "seq")).astype(jnp.float32),
        lax.psum(third_gain_part.astype(jnp.bfloat16), ("dp", "seq")).astype(jnp.float32),
        lax.psum(fourth_gain_part.astype(jnp.bfloat16), ("dp", "seq")).astype(jnp.float32),
        lax.psum(query_part.astype(jnp.bfloat16), ("dp", "seq")).astype(jnp.float32),
        lax.psum(key_part.astype(jnp.bfloat16), ("dp", "seq")).astype(jnp.float32),
        lax.psum(value_part.astype(jnp.bfloat16), ("dp", "seq")).astype(jnp.float32),
        lax.psum(output_part.astype(jnp.bfloat16), ("dp", "seq")).astype(jnp.float32),
        lax.psum(first_gain_part.astype(jnp.bfloat16), ("dp", "seq")).astype(jnp.float32),
        lax.psum(second_gain_part.astype(jnp.bfloat16), ("dp", "seq")).astype(jnp.float32),
        lax.psum(adapter_part.astype(jnp.bfloat16), ("dp", "seq")).astype(jnp.float32),
    )
    gate_total, up_total, down_total, third_total, fourth_total = (
        summed[0],
        summed[1],
        summed[2],
        summed[3],
        summed[4],
    )
    query_total, key_total, value_total, output_total, first_total, second_total = (
        summed[5],
        summed[6],
        summed[7],
        summed[8],
        summed[9],
        summed[10],
    )
    adapter_total = summed[11]
    return (
        layer_out,
        latent_gradient,
        adapter_total,
        first_total,
        query_total,
        key_total,
        value_total,
        output_total,
        second_total,
        third_total,
        gate_total,
        up_total,
        down_total,
        fourth_total,
    )


TRUNK = 8
BRANCH = 4
LEAVES = 2
SEGS = TRUNK + BRANCH + BRANCH * LEAVES
WIDE = 2 * DH
NEG = -1e30
F32 = jnp.float32
BF16 = jnp.bfloat16
KEYS = 512
HIDDEN = 256
VMEM_BYTES = 60 << 20


def nt(left, right):
    return lax.dot_general(left, right, (((1,), (1,)), ((), ())), preferred_element_type=F32)


def nn(left, right):
    return lax.dot_general(left, right, (((1,), (0,)), ((), ())), preferred_element_type=F32)


def segment(index, size=SEG):
    return pl.ds(pl.multiple_of(index * SEG, SEG), size)


def find_roles(parents, child, count, role):
    for s in range(SEGS):
        count[s] = 0
    role[0] = 0
    for s in range(SEGS):
        parent = parents[0, s]

        @pl.when(parent < 0)
        def _():
            role[0] = s

        @pl.when(parent >= 0)
        def _():
            seen = count[parent]
            child[parent * BRANCH + seen] = s
            count[parent] = seen + 1

    for i in range(TRUNK - 1):
        role[i + 1] = child[role[i] * BRANCH]
    for b in range(BRANCH):
        role[TRUNK + b] = child[role[TRUNK - 1] * BRANCH + b]
    for b in range(BRANCH):
        for leaf in range(LEAVES):
            role[TRUNK + BRANCH + b * LEAVES + leaf] = child[role[TRUNK + b] * BRANCH + leaf]


def roles_kernel(parents, parts, role, place, out, child, count):
    find_roles(parents, child, count, role)
    for i in range(SEGS):
        place[role[i]] = i
    pick_segments(role, parts, out)


def pick_segments(order, source, out):
    for i in range(SEGS):
        out[segment(i), :] = source[segment(order[i]), :]


def sort_parts(parents, parts):
    smem = pl.BlockSpec(memory_space=pltpu.SMEM)
    vmem = pl.BlockSpec(memory_space=pltpu.VMEM)
    return pl.pallas_call(
        roles_kernel,
        out_shape=(jax.ShapeDtypeStruct((SEGS,), jnp.int32),) * 2
        + (jax.ShapeDtypeStruct(parts.shape, parts.dtype),),
        in_specs=[smem, vmem],
        out_specs=(smem, smem, vmem),
        scratch_shapes=[
            pltpu.SMEM((SEGS * BRANCH,), jnp.int32),
            pltpu.SMEM((SEGS,), jnp.int32),
        ],
        name="sort_parts",
    )(parents, parts)


def pick(order, source):
    smem = pl.BlockSpec(memory_space=pltpu.SMEM)
    vmem = pl.BlockSpec(memory_space=pltpu.VMEM)
    return pl.pallas_call(
        pick_segments,
        out_shape=jax.ShapeDtypeStruct(source.shape, source.dtype),
        in_specs=[smem, vmem],
        out_specs=vmem,
        name="pick",
    )(order, source)


def heads_apart(values, first):
    zero = jnp.zeros_like(values)
    return jnp.concatenate(
        [jnp.where(first, values, zero), jnp.where(first, zero, values)], axis=0
    )


MESH = pl.DeviceIdType.MESH


def at_step(index, plan):
    for step, calls in plan.items():

        @pl.when(index == step)
        def _(calls=calls):
            for call in calls:
                call()


class Fetch:
    def __init__(self, shape, pieces):
        self.rows, self.lanes = shape
        self.pieces = pieces

    def scratch(self):
        return [pltpu.SemaphoreType.DMA((4, self.pieces))] * 2

    def bind(self, own, out, refs):
        self.own, self.out = own, out
        self.send, self.recv = refs
        self.x, self.core = lax.axis_index("x"), lax.axis_index("core")
        self.to_core = {"core": 1 - self.core}
        self.to_x = {"x": 1 - self.x}
        self.to_tensor = {"tensor": 1 - lax.axis_index("tensor")}

    def copy(self, kind, piece):
        rows = self.rows // 4 // self.pieces
        x = 1 - self.x if kind == 3 else self.x
        row = (2 * x + self.core) * (self.rows // 4) + piece * rows
        here = pl.ds(pl.multiple_of(row, 16), rows)
        return pltpu.make_async_remote_copy(
            src_ref=(self.own if kind == 0 else self.out).at[here],
            dst_ref=self.out.at[here],
            send_sem=self.send.at[kind, piece],
            recv_sem=self.recv.at[kind, piece],
            device_id=(self.to_tensor, self.to_x, self.to_core, self.to_core)[kind],
            device_id_type=MESH,
        )

    def start(self):
        for piece in range(self.pieces):
            self.copy(0, piece).start()

    def second(self, piece):
        self.copy(0, piece).wait_recv()
        self.copy(1, piece).start()
        self.copy(2, piece).start()

    def third(self, piece):
        self.copy(1, piece).wait_recv()
        self.copy(3, piece).start()

    def drain(self):
        for piece in range(self.pieces):
            for kind in range(4):
                self.copy(kind, piece).wait_send()
            self.copy(2, piece).wait_recv()
            self.copy(3, piece).wait_recv()


def attention_kernel(fetches, *refs):
    parts = refs[0]
    count = len(fetches)
    own_weights, refs = refs[1 : 1 + count], refs[1 + count :]
    out, logsum, other_weights = refs[0], refs[1], refs[2 : 2 + count]
    qr, kr, v0, v1, kept, acc, top, total = refs[2 + count : 10 + count]
    sems = refs[10 + count :]
    for i, fetch in enumerate(fetches):
        fetch.bind(own_weights[i], other_weights[i], sems[2 * i : 2 * i + 2])
    output, gate, up, down = fetches
    barrier = pltpu.get_barrier_semaphore()
    for target in (gate.to_core, gate.to_x, gate.to_tensor):
        pl.semaphore_signal(barrier, inc=1, device_id=target, device_id_type=MESH)
    pl.semaphore_wait(barrier, 3)
    for fetch in fetches:
        fetch.start()
    call = functools.partial
    leaf_plan = {
        2: [call(output.second, 0)],
        4: [call(gate.second, 0), call(output.third, 0)],
        6: [call(gate.second, 1)],
        7: [call(gate.third, 0)],
    }
    branch_plan = {
        0: [call(up.second, 0)],
        1: [call(gate.third, 1)],
        2: [call(up.second, 1)],
        3: [call(up.third, 0)],
    }
    trunk_plan = {
        3: [call(down.second, 0), call(up.third, 1)],
        6: [call(down.second, 1)],
    }
    first = lax.broadcasted_iota(jnp.int32, (SEG, WIDE), 1) < DH

    def sort(i, _):
        here = source = segment(i)
        qr[here, :] = parts[source, 0:WIDE] * jnp.asarray(DH**-0.5, BF16)
        kr[here, :] = parts[source, WIDE : 2 * WIDE]
        value = parts[source, 2 * WIDE : 3 * WIDE]
        zero = jnp.zeros_like(value)
        v0[here, :] = jnp.where(first, value, zero)
        v1[here, :] = jnp.where(first, zero, value)
        return 0

    lax.fori_loop(0, SEGS, sort, 0)
    row = lax.broadcasted_iota(jnp.int32, (2 * SEG, SEG), 0)
    col = lax.broadcasted_iota(jnp.int32, (2 * SEG, SEG), 1)
    causal = col <= jnp.where(row >= SEG, row - SEG, row)

    def fold(values, op):
        result = values[:, 0:128]
        for at in range(128, values.shape[1], 128):
            result = op(result, values[:, at : at + 128])
        return result

    def query(index, count_big, big, extra):
        queries = heads_apart(qr[segment(index), :], first)
        own = jnp.where(causal, nt(queries, kr[segment(index), :]), NEG)
        top[...] = fold(own, jnp.maximum)
        others = []
        for other in extra:
            scores = nt(queries, kr[segment(other), :])
            top[...] = jnp.maximum(top[...], fold(scores, jnp.maximum))
            others.append(scores)

        def find(c, _):
            scores = nt(queries, kr[pl.ds(pl.multiple_of(c * big, big), big), :])
            kept[c, :, 0:big] = scores
            top[...] = jnp.maximum(top[...], fold(scores, jnp.maximum))
            return 0

        lax.fori_loop(0, count_big, find, 0)
        most = jnp.max(top[...], axis=1, keepdims=True)

        def add(scores, keys, fresh=False):
            weights = jnp.exp(scores - most)
            summed = fold(weights, jnp.add)
            low = weights.astype(BF16)
            product = nn(low[:SEG], v0[keys, :]) + nn(low[SEG:], v1[keys, :])
            total[...] = summed if fresh else total[...] + summed
            acc[...] = product if fresh else acc[...] + product

        add(own, segment(index), True)
        for other, scores in zip(extra, others):
            add(scores, segment(other))

        def use(c, _):
            add(kept[c, :, 0:big], pl.ds(pl.multiple_of(c * big, big), big))
            return 0

        lax.fori_loop(0, count_big, use, 0)
        whole = jnp.sum(total[...], axis=1, keepdims=True)
        inverse = 1.0 / whole
        log = most + jnp.log(whole)
        here = segment(index)
        out[here, :] = (acc[...] * jnp.where(first, inverse[:SEG], inverse[SEG:])).astype(BF16)
        logsum[here, :] = jnp.where(first, log[:SEG], log[SEG:])

    def trunk(i, _):
        at_step(i, trunk_plan)
        query(i, i, SEG, [])
        return 0

    def branch(i, _):
        at_step(i, branch_plan)
        query(TRUNK + i, TRUNK * SEG // KEYS, KEYS, [])
        return 0

    def leaf(i, _):
        at_step(i, leaf_plan)
        query(TRUNK + BRANCH + i, TRUNK * SEG // KEYS, KEYS, [TRUNK + i // LEAVES])
        return 0

    lax.fori_loop(0, BRANCH * LEAVES, leaf, 0)
    lax.fori_loop(0, BRANCH, branch, 0)
    lax.fori_loop(0, TRUNK, trunk, 0)
    down.third(0)

    down.third(1)
    for fetch in fetches:
        fetch.drain()


def attention_forward(parts, weights):
    fetches = [Fetch(weight.shape, 1 if i == 0 else 2) for i, weight in enumerate(weights)]
    sems = []
    for fetch in fetches:
        sems += fetch.scratch()
    hbm = pl.BlockSpec(memory_space=pl.ANY)
    tokens = SEGS * SEG
    vmem = pl.BlockSpec(memory_space=pltpu.VMEM)
    return pl.pallas_call(
        functools.partial(attention_kernel, fetches),
        out_shape=(
            jax.ShapeDtypeStruct((tokens, WIDE), BF16),
            jax.ShapeDtypeStruct((tokens, WIDE), F32),
        )
        + tuple(jax.ShapeDtypeStruct(weight.shape, BF16) for weight in weights),
        in_specs=[vmem] + [hbm] * len(weights),
        out_specs=(vmem, vmem) + (hbm,) * len(weights),
        scratch_shapes=[pltpu.VMEM((tokens, WIDE), BF16)] * 4
        + [
            pltpu.VMEM((TRUNK, 2 * SEG, KEYS), F32),
            pltpu.VMEM((SEG, WIDE), F32),
            pltpu.VMEM((2 * SEG, 128), F32),
            pltpu.VMEM((2 * SEG, 128), F32),
        ]
        + sems,
        compiler_params=pltpu.CompilerParams(
            vmem_limit_bytes=VMEM_BYTES, collective_id=4, has_side_effects=True
        ),
        cost_estimate=pl.CostEstimate(
            flops=152 * 2 * 4 * SEG * SEG * 128,
            bytes_accessed=tokens * WIDE * 12,
            transcendentals=152 * 2 * SEG * SEG,
        ),
        name="attention_forward",
    )(parts, *weights)


def add_rows(dst, dst_row, left, left_row, right, right_row, rows, step=32):
    def one(i, _):
        at = i * step
        total = left[pl.ds(pl.multiple_of(left_row + at, step), step), :].astype(F32)
        total += right[pl.ds(pl.multiple_of(right_row + at, step), step), :].astype(F32)
        dst[pl.ds(pl.multiple_of(dst_row + at, step), step), :] = total.astype(BF16)
        return 0

    lax.fori_loop(0, rows // step, one, 0)


class PairFold:
    def __init__(self, shape, x_first, pieces=1):
        self.rows, self.lanes = shape
        self.x_first = x_first
        self.pieces = pieces if x_first else 2

    def scratch(self):
        half, quarter = (self.rows // 2, self.lanes), (self.rows // 4, self.lanes)
        return (
            [pltpu.VMEM(half, BF16)] * 4
            + [pltpu.VMEM(quarter, BF16)] * (2 if self.x_first else 1)
            + [pltpu.VMEM(quarter if self.x_first else half, BF16)]
            + [pltpu.SemaphoreType.DMA((2,))] * 3
            + [pltpu.SemaphoreType.DMA((2, self.pieces))] * 2
            + [pltpu.SemaphoreType.DMA((self.pieces,))] * 2
        )

    def bind(self, parts, out, refs):
        self.parts, self.out = parts, out
        self.keep, self.land = refs[0:2], refs[2:4]
        count = 2 if self.x_first else 1
        self.x_land = refs[4 : 4 + count]
        (
            self.y_land,
            self.local,
            self.core_send,
            self.core_recv,
            self.x_send,
            self.x_recv,
            self.y_send,
            self.y_recv,
        ) = refs[4 + count :]
        self.x, self.core = lax.axis_index("x"), lax.axis_index("core")
        self.to_core = {"core": 1 - self.core}
        self.to_x = {"x": 1 - self.x}
        self.to_tensor = {"tensor": 1 - lax.axis_index("tensor")}
        self.half, self.quarter = self.rows // 2, self.rows // 4

    def rows_at(self, ref, row, rows):
        return ref.at[pl.ds(pl.multiple_of(row, 32), rows)]

    def remote(self, src, dst, send, recv, where):
        return pltpu.make_async_remote_copy(
            src_ref=src,
            dst_ref=dst,
            send_sem=send,
            recv_sem=recv,
            device_id=where,
            device_id_type=MESH,
        )

    def over_core(self, side):
        return self.remote(
            self.rows_at(self.parts[side], (1 - self.core) * self.half, self.half),
            self.land[side],
            self.core_send.at[side],
            self.core_recv.at[side],
            self.to_core,
        )

    def kept(self, side):
        return pltpu.make_async_copy(
            self.rows_at(self.parts[side], self.core * self.half, self.half),
            self.keep[side],
            self.local.at[side],
        )

    def over_x(self, side, piece):
        rows = self.quarter // self.pieces if self.x_first else self.quarter
        start = piece * rows if self.x_first else 0
        return self.remote(
            self.rows_at(self.keep[side], (1 - self.x) * self.quarter + start, rows),
            self.rows_at(self.x_land[side], start, rows),
            self.x_send.at[side, piece],
            self.x_recv.at[side, piece],
            self.to_x,
        )

    def over_tensor(self, piece):
        if self.x_first:
            rows = self.quarter // self.pieces
            source, target = self.x * self.quarter + piece * rows, piece * rows
        else:
            rows = self.quarter
            source = (1 - self.x if piece == 0 else self.x) * rows
            target = source
        return self.remote(
            self.rows_at(self.keep[1], source, rows),
            self.rows_at(self.y_land, target, rows),
            self.y_send.at[piece],
            self.y_recv.at[piece],
            self.to_tensor,
        )

    def start(self):
        for side in range(2):
            self.over_core(side).start()
            self.kept(side).start()

    def fold_core(self):
        for side in (1, 0):
            self.kept(side).wait()
            self.over_core(side).wait_recv()
            add_rows(self.keep[side], 0, self.keep[side], 0, self.land[side], 0, self.half)
        for piece in range(self.pieces):
            if self.x_first:
                self.over_x(1, piece).start()
                self.over_x(0, piece).start()
            else:
                self.over_tensor(piece).start()

    def second(self, piece):
        if self.x_first:
            rows = self.quarter // self.pieces
            at = self.x * self.quarter + piece * rows
            for side in (1, 0):
                self.over_x(side, piece).wait_recv()
                keep, land = self.keep[side], self.x_land[side]
                add_rows(keep, at, keep, at, land, piece * rows, rows)
                if side == 1:
                    self.over_tensor(piece).start()
        else:
            at = (1 - self.x if piece == 0 else self.x) * self.quarter
            self.over_tensor(piece).wait_recv()
            add_rows(self.keep[0], at, self.keep[0], at, self.y_land, at, self.quarter)
            if piece == 0:
                self.over_x(0, 0).start()

    def third(self, piece):
        if self.x_first:
            rows = self.quarter // self.pieces
            self.over_tensor(piece).wait_recv()
            at = self.x * self.quarter + piece * rows
            add_rows(self.out, piece * rows, self.keep[0], at, self.y_land, piece * rows, rows)
        elif piece == 0:
            self.over_x(0, 0).wait_recv()
            at = self.x * self.quarter
            add_rows(self.out, 0, self.keep[0], at, self.x_land[0], 0, self.quarter)

    def drain(self):
        for side in range(2):
            self.over_core(side).wait_send()
        for piece in range(self.pieces):
            if self.x_first:
                self.over_x(0, piece).wait_send()
                self.over_x(1, piece).wait_send()
            self.over_tensor(piece).wait_send()
        if not self.x_first:
            self.over_x(0, 0).wait_send()


def swap_halves(values, low):
    return jnp.where(
        low, pltpu.roll(values, WIDE - DH // 2, 1), pltpu.roll(values, DH // 2, 1)
    )


def attention_back_kernel(folds, *refs):
    parts, upstream, attended, logsum, cosine, sine = refs[:6]
    pair_grad, down_grad, output_grad = refs[6:9]
    refs = refs[9:]
    split, hidden = folds[0].lanes, folds[2].rows
    inner = folds[3].rows
    sides = [pair_grad.at[:, pl.ds(0, split)], pair_grad.at[:, pl.ds(2 * split, split)]]
    sides += [pair_grad.at[:, pl.ds(split, split)], pair_grad.at[:, pl.ds(3 * split, split)]]
    sides += [down_grad.at[pl.ds(0, hidden)], down_grad.at[pl.ds(hidden, hidden)]]
    sides += [output_grad.at[pl.ds(0, inner)], output_grad.at[pl.ds(inner, inner)]]
    out, sums, refs = refs[0], refs[1 : 1 + len(folds)], refs[1 + len(folds) :]
    qr, kr, vr, kt, dk, dv, dqt = refs[:7]
    refs = refs[7:]
    for i, fold in enumerate(folds):
        size = len(fold.scratch())
        fold.bind(sides[2 * i : 2 * i + 2], sums[i], refs[:size])
        refs = refs[size:]
    gate, up, down, output = folds
    barrier = pltpu.get_barrier_semaphore()
    for target in (gate.to_core, gate.to_x, gate.to_tensor):
        pl.semaphore_signal(barrier, inc=1, device_id=target, device_id_type=MESH)
    pl.semaphore_wait(barrier, 3)
    for fold in folds:
        fold.start()
    call = functools.partial
    leaf_plan = {
        1: [gate.fold_core],
        2: [down.fold_core],
        3: [up.fold_core, output.fold_core],
        7: [call(down.second, 0)],
    }
    branch_plan = {
        2: [call(gate.second, 0), call(down.second, 1)],
        3: [call(output.second, 0)],
    }
    trunk_plan = {5: [call(output.second, 1), call(up.second, 0)]}
    lane = lax.broadcasted_iota(jnp.int32, (SEG, WIDE), 1)
    first = lane < DH
    low = (lane % DH) < (DH // 2)

    def sort(i, _):
        here = source = segment(i)
        qr[here, :] = parts[source, 0:WIDE] * jnp.asarray(DH**-0.5, BF16)
        key = parts[source, WIDE : 2 * WIDE]
        kr[here, :] = key
        kt[:, here] = key.T
        vr[here, :] = parts[source, 2 * WIDE : 3 * WIDE]
        return 0

    lax.fori_loop(0, SEGS, sort, 0)
    dk[...] = jnp.zeros_like(dk)
    dv[...] = jnp.zeros_like(dv)
    key_at = lax.broadcasted_iota(jnp.int32, (SEG, 2 * SEG), 0)
    query_at = lax.broadcasted_iota(jnp.int32, (SEG, 2 * SEG), 1)
    causal = key_at <= jnp.where(query_at >= SEG, query_at - SEG, query_at)

    def rope_back(values, depth):
        at = segment(depth)
        return values * cosine[at, :] - swap_halves(values, low) * sine[at, :]

    def query(index, depth, count_big, big, extra):
        here = segment(index)
        queries = heads_apart(qr[segment(index), :], first)
        up = upstream[here, :]
        ups = heads_apart(up, first)
        turned = logsum[segment(index), :].T
        log = jnp.concatenate([turned[0:1, :], turned[DH : DH + 1, :]], axis=1)
        product = (up.astype(F32) * attended[here, :].astype(F32)).T
        inner = jnp.concatenate(
            [
                jnp.sum(product[:DH], axis=0, keepdims=True),
                jnp.sum(product[DH:], axis=0, keepdims=True),
            ],
            axis=1,
        )
        dqt[...] = jnp.zeros_like(dqt)

        def add(keys, mask=None):
            weights = jnp.exp(nt(kr[keys, :], queries) - log)
            if mask is not None:
                weights = jnp.where(mask, weights, 0.0)
            back = (weights * (nt(vr[keys, :], ups) - inner)).astype(BF16)
            dv[keys, :] += nn(weights.astype(BF16), ups)
            dk[keys, :] += nn(back, queries)
            dqt[...] += nn(kt[:, keys], back)

        add(segment(index), causal)
        for other in extra:
            add(segment(other))

        def use(c, _):
            add(pl.ds(pl.multiple_of(c * big, big), big))
            return 0

        lax.fori_loop(0, count_big, use, 0)
        both = jnp.concatenate([dqt[:DH, :SEG], dqt[DH:, SEG:]], axis=0) * (DH**-0.5)
        out[here, 0:WIDE] = rope_back(both.T, depth).astype(BF16)

    def leaf(i, _):
        at_step(i, leaf_plan)
        query(TRUNK + BRANCH + i, TRUNK + 1, TRUNK * SEG // KEYS, KEYS, [TRUNK + i // LEAVES])
        return 0

    def branch(i, _):
        at_step(i, branch_plan)
        query(TRUNK + i, TRUNK, TRUNK * SEG // KEYS, KEYS, [])
        return 0

    def trunk(i, _):
        at_step(i, trunk_plan)
        query(i, i, i, SEG, [])
        return 0

    lax.fori_loop(0, BRANCH * LEAVES, leaf, 0)
    lax.fori_loop(0, BRANCH, branch, 0)
    lax.fori_loop(0, TRUNK, trunk, 0)

    up.second(1)

    def settle(i, _):
        here = segment(i)
        depth = jnp.where(i < TRUNK + BRANCH, jnp.minimum(i, TRUNK), TRUNK + 1)
        out[here, WIDE : 2 * WIDE] = rope_back(dk[here, :], depth).astype(BF16)
        out[here, 2 * WIDE : 3 * WIDE] = dv[here, :].astype(BF16)
        return 0

    lax.fori_loop(0, SEGS, settle, 0)
    for fold in (gate, output, down):
        fold.third(0)
    for piece in range(up.pieces):
        up.third(piece)
    for fold in folds:
        fold.drain()


def attention_backward(parts, upstream, attended, logsum, cosine, sine, grads, shapes):
    tokens = SEGS * SEG
    vmem = pl.BlockSpec(memory_space=pltpu.VMEM)
    folds = [PairFold(shape, i < 2, 1 + i % 2) for i, shape in enumerate(shapes)]
    scratch = []
    for fold in folds:
        scratch += fold.scratch()
    return pl.pallas_call(
        functools.partial(attention_back_kernel, folds),
        out_shape=(jax.ShapeDtypeStruct((tokens, 3 * WIDE), BF16),)
        + tuple(jax.ShapeDtypeStruct((fold.rows // 4, fold.lanes), BF16) for fold in folds),
        in_specs=[vmem] * 6 + [pl.BlockSpec(memory_space=pl.ANY)] * len(grads),
        out_specs=(vmem,) * (1 + len(folds)),
        scratch_shapes=[pltpu.VMEM((tokens, WIDE), BF16)] * 3
        + [pltpu.VMEM((WIDE, tokens), BF16)]
        + [pltpu.VMEM((tokens, WIDE), F32)] * 2
        + [pltpu.VMEM((WIDE, 2 * SEG), F32)]
        + scratch,
        compiler_params=pltpu.CompilerParams(
            vmem_limit_bytes=VMEM_BYTES, collective_id=3, has_side_effects=True
        ),
        cost_estimate=pl.CostEstimate(
            flops=152 * 2 * 10 * SEG * SEG * 128,
            bytes_accessed=tokens * WIDE * 24,
            transcendentals=152 * 2 * SEG * SEG,
        ),
        name="attention_backward",
    )(
        parts,
        upstream,
        attended,
        logsum,
        cosine,
        sine,
        *grads,
    )


def angle_tables(positions):
    lane = jnp.arange(WIDE)
    freq = THETA ** (-(lane % (DH // 2)).astype(F32) * 2.0 / DH)
    angle = positions.astype(F32)[:, None] * freq[None, :]
    sign = jnp.where((lane % DH) < DH // 2, -1.0, 1.0)
    return jnp.cos(angle), jnp.sin(angle) * sign[None, :]


def neighbours():
    x, core = lax.axis_index("x"), lax.axis_index("core")
    others = []
    for step in (1, 2, 3):
        to_x = lax.rem(x + step // 2, 2)
        to_core = lax.rem(core + step % 2, 2)
        others.append((2 * to_x + to_core, {"x": to_x, "core": to_core}))
    return 2 * x + core, others


def greet(tensor_peer, others):
    barrier = pltpu.get_barrier_semaphore()
    for target in [tensor_peer] + [where for _, where in others]:
        pl.semaphore_signal(barrier, inc=1, device_id=target, device_id_type=MESH)
    pl.semaphore_wait(barrier, 1 + len(others))


def enter_kernel(
    mine,
    gain,
    query_w,
    key_w,
    value_w,
    cosine,
    sine,
    parts,
    low_out,
    theirs,
    ready,
    swap_send,
    swap_recv,
    part_send,
    part_recv,
):
    me, others = neighbours()
    tensor_peer = {"tensor": 1 - lax.axis_index("tensor")}
    greet(tensor_peer, others)
    steps = mine.shape[0] // SEG

    def exchange(i):
        return pltpu.make_async_remote_copy(
            src_ref=mine.at[segment(i)],
            dst_ref=theirs.at[segment(i)],
            send_sem=swap_send.at[i],
            recv_sem=swap_recv.at[i],
            device_id=tensor_peer,
            device_id_type=MESH,
        )

    def scatter(i, at):
        place, where = others[at]
        return pltpu.make_async_remote_copy(
            src_ref=ready.at[place, segment(i)],
            dst_ref=parts.at[me, segment(i)],
            send_sem=part_send.at[i, at],
            recv_sem=part_recv.at[i, at],
            device_id=where,
            device_id_type=MESH,
        )

    for i in range(steps):
        exchange(i).start()
    low = (lax.broadcasted_iota(jnp.int32, (SEG, WIDE), 1) % DH) < (DH // 2)

    def step(i, _):
        here = segment(i)
        exchange(i).wait_recv()
        total = mine[here, :].astype(F32) + theirs[here, :].astype(F32)
        scale = lax.rsqrt(jnp.mean(total * total, axis=-1, keepdims=True) + EPSILON)
        rounded = (total * scale * gain[...]).astype(BF16)
        low_out[here, :] = rounded
        for at, weight in enumerate((query_w, key_w, value_w)):
            raw = nn(rounded, weight[...])
            for peer in range(ready.shape[0]):
                part = raw[:, peer * WIDE : (peer + 1) * WIDE]
                if at < 2:
                    part = part * cosine[here, :] + swap_halves(part, low) * sine[here, :]
                ready[peer, here, at * WIDE : (at + 1) * WIDE] = part.astype(BF16)
        for at in range(len(others)):
            scatter(i, at).start()
        parts[me, here, :] = ready[me, here, :]
        return 0

    lax.fori_loop(0, steps, step, 0)

    def finish(i, _):
        exchange(i).wait_send()
        for at in range(len(others)):
            scatter(i, at).wait()
        return 0

    lax.fori_loop(0, steps, finish, 0)


def enter(mine, gain, query_w, key_w, value_w, cosine, sine):
    rows, width = mine.shape
    inner = query_w.shape[1]
    peers = inner // WIDE
    steps = rows // SEG
    vmem = pl.BlockSpec(memory_space=pltpu.VMEM)
    return pl.pallas_call(
        enter_kernel,
        out_shape=(
            jax.ShapeDtypeStruct((peers, rows, 3 * WIDE), BF16),
            jax.ShapeDtypeStruct((rows, width), BF16),
            jax.ShapeDtypeStruct((rows, width), BF16),
        ),
        in_specs=[vmem] * 7,
        out_specs=(vmem,) * 3,
        scratch_shapes=[
            pltpu.VMEM((peers, rows, 3 * WIDE), BF16),
            pltpu.SemaphoreType.DMA((steps,)),
            pltpu.SemaphoreType.DMA((steps,)),
            pltpu.SemaphoreType.DMA((steps, 3)),
            pltpu.SemaphoreType.DMA((steps, 3)),
        ],
        compiler_params=pltpu.CompilerParams(
            vmem_limit_bytes=VMEM_BYTES, collective_id=0, has_side_effects=True
        ),
        cost_estimate=pl.CostEstimate(
            flops=2 * rows * width * 3 * inner,
            bytes_accessed=200 << 20,
            transcendentals=rows,
        ),
        name="enter",
    )(mine, gain, query_w, key_w, value_w, cosine, sine)


def middle_kernel(
    meta,
    adapted,
    heads,
    cotangent,
    second_gain,
    third_gain,
    fourth_gain,
    wo_own,
    wg_own,
    wu_own,
    wd_own,
    wo_other,
    wg_other,
    wu_other,
    wd_other,
    layer_out,
    middle_out,
    attended_out,
    attention_out,
    third_out,
    mixed_out,
    hidden_out,
    pair_out,
    heads_back,
    gains_out,
    wo,
    wg,
    wu,
    wd,
    gate_s,
    up_s,
    sums,
    sem,
):
    step = pl.program_id(0)
    tensor = meta[0]
    copies = []

    def copy(src, weight, row, lane):
        rows, lanes = src.shape
        dst = weight.at[pl.ds(row, rows), pl.ds(lane, lanes)]
        copies.append(pltpu.make_async_copy(src, dst, sem.at[len(copies)]))

    for weight, own, other, by_lane in (
        (wo, wo_own, wo_other, False),
        (wg, wg_own, wg_other, True),
        (wu, wu_own, wu_other, True),
        (wd, wd_own, wd_other, False),
    ):
        rows, lanes = own.shape
        copy(own, weight, 0, 0)
        copy(other, weight, 0 if by_lane else rows, lanes if by_lane else 0)

    @pl.when(step == 0)
    def _():
        for copy in copies:
            copy.start()
        gains_out[...] = jnp.zeros_like(gains_out)
        for copy in copies[:2]:
            copy.wait()

    groups = heads.shape[0] // 2
    for side in range(2):
        for group in range(groups):
            at = (side * groups + group) * WIDE
            source = group * 2 + (tensor if side == 0 else 1 - tensor)
            attended_out[:, at : at + WIDE] = heads[source]
    attention = nn(attended_out[...], wo[...])

    def scaling(values):
        return lax.rsqrt(jnp.mean(values * values, axis=-1, keepdims=True) + EPSILON)

    def inward(upstream, gain, normed, scale):
        scaled = upstream * gain
        return scale * (scaled - normed * jnp.mean(scaled * normed, axis=-1, keepdims=True))

    second_scale = scaling(attention)
    second_normed = attention * second_scale
    middle = adapted[...] + second_normed * second_gain[...]
    third_scale = scaling(middle)
    third_normed = middle * third_scale
    third_out[...] = (third_normed * third_gain[...]).astype(BF16)

    @pl.when(step == 0)
    def _():
        for copy in copies[2:]:
            copy.wait()

    sums[...] = jnp.zeros_like(sums)

    def forward(c, _):
        cut = pl.ds(pl.multiple_of(c * HIDDEN, HIDDEN), HIDDEN)
        gate = nn(third_out[...], wg[:, cut])
        upward = nn(third_out[...], wu[:, cut])
        gate_s[c] = gate
        up_s[c] = upward
        hidden = (gate / (1.0 + jnp.exp(-gate)) * upward).astype(BF16)
        hidden_out[:, cut] = hidden
        sums[...] += nn(hidden, wd[cut, :])
        return 0

    lax.fori_loop(0, gate_s.shape[0], forward, 0)
    mixed = sums[...]
    fourth_scale = scaling(mixed)
    fourth_normed = mixed * fourth_scale
    layer_out[...] = (middle + fourth_normed * fourth_gain[...]).astype(BF16)
    upstream = cotangent[...].astype(F32)
    gains_out[2:3, :] += jnp.sum(upstream * fourth_normed, axis=0, keepdims=True)
    mixed_out[...] = inward(upstream, fourth_gain[...], fourth_normed, fourth_scale).astype(BF16)
    sums[...] = jnp.zeros_like(sums)
    side_units = wg_own.shape[1] // 128

    def backward(c, _):
        cut = pl.ds(pl.multiple_of(c * HIDDEN, HIDDEN), HIDDEN)
        back = nt(mixed_out[...], wd[cut, :]).astype(BF16).astype(F32)
        gate = gate_s[c]
        sigmoid = 1.0 / (1.0 + jnp.exp(-gate))
        silu = gate * sigmoid
        gate_back = (back * up_s[c] * (sigmoid + silu * (1.0 - sigmoid))).astype(BF16)
        up_back = (back * silu).astype(BF16)
        for piece in range(HIDDEN // 128):
            unit = c * (HIDDEN // 128) + piece
            unit = jnp.where(unit < side_units, unit, unit + side_units)
            lanes = slice(piece * 128, (piece + 1) * 128)
            pair_out[:, pl.ds(pl.multiple_of(unit * 128, 128), 128)] = gate_back[:, lanes]
            unit += side_units
            pair_out[:, pl.ds(pl.multiple_of(unit * 128, 128), 128)] = up_back[:, lanes]
        sums[...] += nt(gate_back, wg[:, cut]) + nt(up_back, wu[:, cut])
        return 0

    lax.fori_loop(0, gate_s.shape[0], backward, 0)
    third_back = sums[...]
    gains_out[1:2, :] += jnp.sum(third_back * third_normed, axis=0, keepdims=True)
    middle_back = upstream + inward(third_back, third_gain[...], third_normed, third_scale)
    middle_out[...] = middle_back
    gains_out[0:1, :] += jnp.sum(middle_back * second_normed, axis=0, keepdims=True)
    attention_out[...] = inward(
        middle_back, second_gain[...], second_normed, second_scale
    ).astype(BF16)
    heads_low = nt(attention_out[...], wo[...]).astype(BF16)
    for side in range(2):
        for group in range(groups):
            at = (side * groups + group) * WIDE
            target = group * 2 + (tensor if side == 0 else 1 - tensor)
            heads_back[target] = heads_low[:, at : at + WIDE]


def middle_section(meta, adapted, heads, cotangent, gains, weights):
    rows, width = adapted.shape
    sources = heads.shape[0]
    inner = sources * WIDE
    hidden = 2 * weights[1].shape[1]
    block = rows // 2
    steps = rows // block
    row = pl.BlockSpec((block, width), lambda i, meta: (i, 0))
    wide = pl.BlockSpec((block, hidden), lambda i, meta: (i, 0))
    head = pl.BlockSpec((sources, block, WIDE), lambda i, meta: (0, i, 0))
    gain = pl.BlockSpec((1, width), lambda i, meta: (0, 0))
    hbm = pl.BlockSpec(memory_space=pl.ANY)
    return pl.pallas_call(
        middle_kernel,
        grid_spec=pltpu.PrefetchScalarGridSpec(
            num_scalar_prefetch=1,
            grid=(steps,),
            in_specs=[
                row,
                head,
                pl.BlockSpec((block, width), lambda i, meta: (meta[0] * steps + i, 0)),
                gain,
                gain,
                gain,
            ]
            + [hbm] * 8,
            out_specs=(
                row,
                row,
                pl.BlockSpec((block, inner), lambda i, meta: (i, 0)),
                row,
                row,
                row,
                wide,
                pl.BlockSpec((block, 2 * hidden), lambda i, meta: (i, 0)),
                head,
                pl.BlockSpec((8, width), lambda i, meta: (0, 0)),
            ),
            scratch_shapes=[
                pltpu.VMEM((inner, width), BF16),
                pltpu.VMEM((width, hidden), BF16),
                pltpu.VMEM((width, hidden), BF16),
                pltpu.VMEM((hidden, width), BF16),
                pltpu.VMEM((hidden // HIDDEN, block, HIDDEN), F32),
                pltpu.VMEM((hidden // HIDDEN, block, HIDDEN), F32),
                pltpu.VMEM((block, width), F32),
                pltpu.SemaphoreType.DMA((8,)),
            ],
        ),
        out_shape=(
            jax.ShapeDtypeStruct((rows, width), BF16),
            jax.ShapeDtypeStruct((rows, width), F32),
            jax.ShapeDtypeStruct((rows, inner), BF16),
            jax.ShapeDtypeStruct((rows, width), BF16),
            jax.ShapeDtypeStruct((rows, width), BF16),
            jax.ShapeDtypeStruct((rows, width), BF16),
            jax.ShapeDtypeStruct((rows, hidden), BF16),
            jax.ShapeDtypeStruct((rows, 2 * hidden), BF16),
            jax.ShapeDtypeStruct((sources, rows, WIDE), BF16),
            jax.ShapeDtypeStruct((8, width), F32),
        ),
        compiler_params=pltpu.CompilerParams(vmem_limit_bytes=VMEM_BYTES),
        cost_estimate=pl.CostEstimate(
            flops=rows * width * (4 * inner + 12 * hidden),
            bytes_accessed=6 * width * hidden + 2 * width * inner + rows * (hidden * 6 + width * 20),
            transcendentals=rows * hidden * 2,
        ),
        name="middle_section",
    )(meta, adapted, heads, cotangent, *gains, *weights)


class Reduction:
    def __init__(self, shape, by_lane=False, kind="all", cuts=None, base=0, x_early=False):
        self.x_early = x_early
        self.base = base
        self.rows, self.lanes = shape
        self.by_lane = by_lane
        self.kind = kind
        self.cuts = cuts or [self.lanes]

    def chunk_shape(self, dp):
        rows, lanes = self.rows // 4, self.lanes
        return (rows, lanes // dp) if self.by_lane else (rows // dp, lanes)

    def outputs(self, dp):
        if self.kind == "sum":
            return [jax.ShapeDtypeStruct(self.chunk_shape(dp), BF16)]
        if self.base > 0:
            return []
        return [jax.ShapeDtypeStruct((self.rows, lanes), F32) for lanes in self.cuts]

    def scratch(self, dp):
        rows, lanes = self.rows, self.lanes
        half, quarter = pltpu.VMEM((rows // 2, lanes), BF16), pltpu.VMEM((rows // 4, lanes), BF16)
        dma = pltpu.SemaphoreType.DMA
        refs = {}
        if self.kind == "all":
            refs.update(half=half, core_land=half, x_land=quarter)
            refs.update(fold_send=dma((2,)), fold_recv=dma((2,)))
        if self.kind != "gather":
            refs.update(
                quarter=quarter,
                z_land=pltpu.VMEM((dp + 1,) + self.chunk_shape(dp), BF16),
                sum_send=dma((dp,)),
                sum_recv=dma((dp + 1,)),
            )
        if self.kind != "sum":
            refs.update(
                whole=quarter,
                others=pltpu.VMEM((3, rows // 4, lanes), BF16),
                send=dma((3,)),
                recv=dma((3,)),
                all_send=dma((2, 2 * dp if self.x_early else dp)),
                all_recv=dma((2 * dp if self.x_early else dp,)),
                out_sem=dma((len(self.cuts),)),
            )
            for i, cut in enumerate(self.cuts):
                refs[f"wide{i}"] = pltpu.VMEM((rows // 4, cut), F32)
        self.names = list(refs)
        return list(refs.values())

    def bind(self, part, outs, refs):
        self.part, self.outs = part, outs
        for name, ref in zip(self.names, refs):
            setattr(self, name, ref)
        self.wide = [getattr(self, f"wide{i}", None) for i in range(len(self.cuts))]
        self.x, self.core, self.z = (lax.axis_index(name) for name in ("x", "core", "dp"))
        self.dp = lax.axis_size("dp")
        self.to_core = {"core": 1 - self.core}
        self.to_x = {"x": 1 - self.x}
        self.sends = []

    def copy(self, src, dst, send, recv, where):
        return pltpu.make_async_remote_copy(
            src_ref=src,
            dst_ref=dst,
            send_sem=send,
            recv_sem=recv,
            device_id=where,
            device_id_type=MESH,
        )

    def part_of(self, ref, index, rows):
        return ref.at[pl.ds(pl.multiple_of(index * rows, rows), rows)]

    def chunk(self, ref, index):
        if self.by_lane:
            lanes = self.lanes // self.dp
            return ref.at[:, pl.ds(pl.multiple_of(index * lanes, lanes), lanes)]
        return self.part_of(ref, index, self.rows // 4 // self.dp)

    def core_sum(self):
        half = self.rows // 2
        return self.copy(
            self.part_of(self.part, 1 - self.core, half),
            self.core_land,
            self.fold_send.at[0],
            self.fold_recv.at[0],
            self.to_core,
        )

    def x_sum(self):
        quarter = self.rows // 4
        return self.copy(
            self.part_of(self.half, 1 - self.x, quarter),
            self.x_land,
            self.fold_send.at[1],
            self.fold_recv.at[1],
            self.to_x,
        )

    def z_sum(self, j, step):
        up = {"dp": self.z + step}
        index = j
        lands = index if step > 0 else jnp.where(self.z - 1 == index, self.dp, index)
        return self.copy(
            self.chunk(self.quarter, index),
            self.z_land.at[lands],
            self.sum_send.at[index],
            self.sum_recv.at[lands],
            up,
        )

    def z_all(self, j, step, which=0):
        ref = self.others.at[0] if which else self.whole
        place = j + self.dp * which
        return self.copy(
            self.chunk(ref, j),
            self.chunk(ref, j),
            self.all_send.at[0 if step > 0 else 1, place],
            self.all_recv.at[place],
            {"dp": self.z + step},
        )

    def x_chunk(self):
        return self.copy(
            self.chunk(self.whole, self.z),
            self.chunk(self.others.at[0], self.z),
            self.send.at[0],
            self.recv.at[0],
            self.to_x,
        )

    def spread(self, which):
        src = self.others.at[0] if which == 2 else self.whole
        return self.copy(
            src,
            self.others.at[which],
            self.send.at[which],
            self.recv.at[which],
            self.to_x if which == 0 else self.to_core,
        )

    def writes(self, at):
        quarter = self.rows // 4
        core = self.core if at < 2 else 1 - self.core
        x = self.x if at % 2 == 0 else 1 - self.x
        row = pl.multiple_of(self.base + (2 * core + x) * quarter, quarter)
        return [
            pltpu.make_async_copy(wide, out.at[pl.ds(row, quarter)], self.out_sem.at[i])
            for i, (wide, out) in enumerate(zip(self.wide, self.outs))
        ]

    def emit(self, at, ref):
        if at > 0:
            for copy in self.writes(at - 1):
                copy.wait()
        lane = 0
        for wide, lanes in zip(self.wide, self.cuts):
            wide[...] = ref[:, lane : lane + lanes].astype(F32)
            lane += lanes
        for copy in self.writes(at):
            copy.start()

    def add(self, into, left, right):
        into[...] = (left[...].astype(F32) + right[...].astype(F32)).astype(BF16)

    def hop(self, h):
        last = self.dp - 1

        @pl.when(self.z == h)
        def _():
            for j in range(last, h, -1):
                if h > 0:
                    self.wait_sum(j)
                    self.add(self.chunk(self.quarter, j), self.chunk(self.quarter, j), self.z_land.at[j])
                self.z_sum(j, 1).start()

        @pl.when(self.z == last - h)
        def _():
            for j in range(0, last - h):
                if h > 0:
                    self.wait_sum(j)
                    self.add(self.chunk(self.quarter, j), self.chunk(self.quarter, j), self.z_land.at[j])
                self.z_sum(j, -1).start()

    def wait_sum(self, lands):
        self.copy(
            self.z_land.at[lands],
            self.z_land.at[lands],
            self.sum_send.at[0],
            self.sum_recv.at[lands],
            self.to_x,
        ).wait_recv()

    def all_hop(self, h, which=0):
        z, last = self.z, self.dp - 1
        low, high = jnp.maximum(z - h, 0), jnp.minimum(z + h, last)

        @pl.when(z >= h)
        def _():
            self.z_all(low, 1, which).wait_recv()

        @pl.when((z >= h) & (z < last))
        def _():
            self.z_all(low, 1, which).start()

        @pl.when(z <= last - h)
        def _():
            self.z_all(high, -1, which).wait_recv()

        @pl.when((z <= last - h) & (z > 0))
        def _():
            self.z_all(high, -1, which).start()

    def stages(self):
        def start():
            self.core_sum().start()

        def fold_core():
            self.core_sum().wait_recv()
            self.add(
                self.half, self.part_of(self.part, self.core, self.rows // 2), self.core_land
            )
            self.x_sum().start()

        def begin():
            self.quarter[...] = self.part[...]
            self.hop(0)

        def fold_x():
            self.x_sum().wait_recv()
            self.add(
                self.quarter, self.part_of(self.half, self.x, self.rows // 4), self.x_land
            )
            self.hop(0)

        def settle():
            z, last = self.z, self.dp - 1
            mine = self.chunk(self.quarter, z)

            @pl.when(z > 0)
            def _():
                self.wait_sum(z)
                self.add(mine, mine, self.z_land.at[z])

            @pl.when(z < last)
            def _():
                self.wait_sum(self.dp)
                self.add(mine, mine, self.z_land.at[self.dp])

            if self.kind == "sum":
                self.outs[0][...] = mine[...]
            else:
                self.chunk(self.whole, z)[...] = mine[...]
                gather()

        def place():
            self.chunk(self.whole, self.z)[...] = self.part[...]
            if self.x_early:
                self.x_chunk().start()
            gather()

        def gather(which=0):
            z, last = self.z, self.dp - 1

            @pl.when(z < last)
            def _():
                self.z_all(z, 1, which).start()

            @pl.when(z > 0)
            def _():
                self.z_all(z, -1, which).start()

        def gather_other():
            self.x_chunk().wait_recv()
            gather(1)

        def share_both():
            self.all_hop(self.dp - 1)
            self.spread(1).start()
            self.emit(0, self.whole)

        def pass_both():
            self.all_hop(self.dp - 1, 1)
            self.spread(2).start()
            self.emit(1, self.others.at[0])

        def share():
            self.all_hop(self.dp - 1)
            self.spread(0).start()
            self.spread(1).start()
            self.emit(0, self.whole)

        def pass_on():
            self.spread(0).wait_recv()
            self.spread(2).start()
            self.emit(1, self.others.at[0])

        def last():
            self.spread(1).wait_recv()
            self.emit(2, self.others.at[1])
            self.spread(2).wait_recv()
            self.emit(3, self.others.at[2])

        sums = [functools.partial(self.hop, h) for h in range(1, self.dp - 1)] + [settle]
        gathers = [functools.partial(self.all_hop, h) for h in range(1, self.dp - 1)]
        gathers += [share, pass_on, last]
        if self.x_early:
            hops = [
                [functools.partial(self.all_hop, h, which) for which in range(2)]
                for h in range(1, self.dp - 1)
            ]
            both = [call for pair in hops for call in pair]
            return [place, gather_other] + both + [share_both, pass_both, last]
        return {
            "all": [start, fold_core, fold_x] + sums + gathers,
            "sum": [begin] + sums,
            "gather": [place] + gathers,
        }[self.kind]

    def drain(self):
        z, last = self.z, self.dp - 1
        if self.kind == "all":
            self.core_sum().wait_send()
            self.x_sum().wait_send()
        if self.kind != "gather":
            for j in range(self.dp):

                @pl.when(z < j)
                def _():
                    self.z_sum(j, 1).wait_send()

                @pl.when(z > j)
                def _():
                    self.z_sum(j, -1).wait_send()

        if self.kind == "sum":
            return
        for j in range(self.dp):

            for which in range(2 if self.x_early else 1):

                @pl.when((z >= j) & (z < last))
                def _():
                    self.z_all(j, 1, which).wait_send()

                @pl.when((z <= j) & (z > 0))
                def _():
                    self.z_all(j, -1, which).wait_send()

        if self.x_early:
            self.x_chunk().wait_send()
        for which in range(1 if self.x_early else 0, 3):
            self.spread(which).wait_send()
        for copy in self.writes(3):
            copy.wait()


def bind_all(items, parts, outs, scratch):
    dp = lax.axis_size("dp")
    for item, part in zip(items, parts):
        size = len(item.scratch(dp))
        if item.base == 0:
            own, outs = outs[: len(item.cuts)], outs[len(item.cuts) :]
        item.bind(part, own, scratch[:size])
        scratch = scratch[size:]


def waves(plans, offsets):
    length = max(len(plan) + i for i, plan in zip(offsets, plans))
    return [
        [plan[t - i] for i, plan in zip(offsets, plans) if 0 <= t - i < len(plan)]
        for t in range(length)
    ]


def greet_line(barrier):
    z, last = lax.axis_index("dp"), lax.axis_size("dp") - 1

    @pl.when(z > 0)
    def _():
        pl.semaphore_signal(barrier, inc=1, device_id={"dp": z - 1}, device_id_type=MESH)

    @pl.when(z < last)
    def _():
        pl.semaphore_signal(barrier, inc=1, device_id={"dp": z + 1}, device_id_type=MESH)

    return jnp.minimum(z, 1) + jnp.minimum(last - z, 1)


LEAVE = 128


def leave_kernel(items, *refs):
    sent, adapted, middle_back, first_low, gain, query_w, key_w, value_w = refs[:8]
    parts, refs = refs[8 : 8 + len(items)], refs[8 + len(items) :]
    grads, adapted_low, gain_out = refs[:3], refs[3], refs[4]
    count = sum(len(item.cuts) for item in items)
    outs, refs = refs[5 : 5 + count], refs[5 + count :]
    landed, away, away_landed, joined, grad_sum = refs[:5]
    part_send, part_recv, away_send, away_recv, low_send, low_recv = refs[5:11]
    bind_all(items, parts, outs, refs[11:])
    plans = [item.stages() for item in items]
    stages = list(zip(*plans))
    away_plan = {0: stages[0]}
    home_plan = {1: stages[1], 4: stages[2]}
    me, others = neighbours()
    tensor = lax.axis_index("tensor")
    tensor_peer = {"tensor": 1 - tensor}
    barrier = pltpu.get_barrier_semaphore()
    for target in [tensor_peer] + [where for _, where in others]:
        pl.semaphore_signal(barrier, inc=1, device_id=target, device_id_type=MESH)
    pl.semaphore_wait(barrier, 1 + len(others) + greet_line(barrier))
    half = adapted.shape[0]
    inner = query_w.shape[1]
    steps = half // LEAVE

    def block(start, i):
        return pl.ds(pl.multiple_of(start + i * LEAVE, LEAVE), LEAVE)

    def gather(side, i, at):
        here = block((tensor if side else 1 - tensor) * half, i)
        place, where = others[at]
        return pltpu.make_async_remote_copy(
            src_ref=sent.at[place, here],
            dst_ref=landed.at[me, here],
            send_sem=part_send.at[side, i, at],
            recv_sem=part_recv.at[side, i, at],
            device_id=where,
            device_id_type=MESH,
        )

    def hand_over(i):
        return pltpu.make_async_remote_copy(
            src_ref=away.at[block(0, i)],
            dst_ref=away_landed.at[block(0, i)],
            send_sem=away_send.at[i],
            recv_sem=away_recv.at[i],
            device_id=tensor_peer,
            device_id_type=MESH,
        )

    def share(i):
        here = block(tensor * half, i)
        return pltpu.make_async_remote_copy(
            src_ref=adapted_low.at[here],
            dst_ref=adapted_low.at[here],
            send_sem=low_send.at[i],
            recv_sem=low_recv.at[i],
            device_id=tensor_peer,
            device_id_type=MESH,
        )

    for side in range(2):

        def begin(i, _):
            for at in range(len(others)):
                gather(side, i, at).start()
            return 0

        lax.fori_loop(0, steps, begin, 0)
    landed[me] = sent[me]
    gain_out[...] = jnp.zeros_like(gain_out)
    grad_sum[...] = jnp.zeros_like(grad_sum)

    def input_grad(side, i):
        for at in range(len(others)):
            gather(side, i, at).wait_recv()
        here = block((tensor if side else 1 - tensor) * half, i)
        for at in range(3):
            for group in range(landed.shape[0]):
                to = at * inner + group * WIDE
                joined[:, to : to + WIDE] = landed[group, here, at * WIDE : (at + 1) * WIDE]
        total = nt(joined[:, 0:inner], query_w[...])
        total += nt(joined[:, inner : 2 * inner], key_w[...])
        total += nt(joined[:, 2 * inner : 3 * inner], value_w[...])
        return total

    def weight_grad(side, i):
        here = block((tensor if side else 1 - tensor) * half, i)
        low = first_low[here, :].T
        for at in range(3):
            lanes = slice(at * inner, (at + 1) * inner)
            grad_sum[:, lanes] += nn(low, joined[:, lanes])

    def away_step(i, _):
        away[block(0, i), :] = input_grad(0, i).astype(BF16)
        hand_over(i).start()
        weight_grad(0, i)
        at_step(i, away_plan)
        return 0

    lax.fori_loop(0, steps, away_step, 0)

    def home_step(i, _):
        total = input_grad(1, i)
        hand_over(i).wait_recv()
        rows = block(0, i)
        upstream = total + away_landed[rows, :].astype(F32)
        values = adapted[rows, :]
        scale = lax.rsqrt(jnp.mean(values * values, axis=-1, keepdims=True) + EPSILON)
        normed = values * scale
        scaled = upstream * gain[...]
        inward = scale * (scaled - normed * jnp.mean(scaled * normed, axis=-1, keepdims=True))
        gain_out[0:1, :] += jnp.sum(upstream * normed, axis=0, keepdims=True)
        adapted_low[block(tensor * half, i), :] = (middle_back[rows, :] + inward).astype(BF16)
        share(i).start()
        weight_grad(1, i)
        at_step(i, home_plan)
        return 0

    lax.fori_loop(0, steps, home_step, 0)
    for at in range(3):
        grads[at][...] = grad_sum[:, at * inner : (at + 1) * inner].astype(BF16)
    for call in stages[3]:
        call()
    for item in items:
        item.drain()

    def finish(i, _):
        for side in range(2):
            for at in range(len(others)):
                gather(side, i, at).wait_send()
        hand_over(i).wait_send()
        share(i).wait()
        return 0

    lax.fori_loop(0, steps, finish, 0)


def leave(
    sent, adapted, middle_back, first_low, gain, query_w, key_w, value_w, parts, by_lanes
):
    items = [
        Reduction((4 * part.shape[0], part.shape[1]), by_lane, "sum")
        for part, by_lane in zip(parts, by_lanes)
    ]
    dp = lax.axis_size("dp")
    scratch, outs = [], []
    for item in items:
        scratch += item.scratch(dp)
        outs += item.outputs(dp)
    peers, rows, lanes = sent.shape
    half, width = adapted.shape
    inner = query_w.shape[1]
    steps = half // LEAVE
    vmem = pl.BlockSpec(memory_space=pltpu.VMEM)
    return pl.pallas_call(
        functools.partial(leave_kernel, items),
        out_shape=(jax.ShapeDtypeStruct((width, inner), BF16),) * 3
        + (
            jax.ShapeDtypeStruct((rows, width), BF16),
            jax.ShapeDtypeStruct((8, width), F32),
        )
        + tuple(outs),
        in_specs=[vmem] * (8 + len(items)),
        out_specs=(vmem,) * (5 + len(outs)),
        scratch_shapes=[
            pltpu.VMEM((peers, rows, lanes), BF16),
            pltpu.VMEM((half, width), BF16),
            pltpu.VMEM((half, width), BF16),
            pltpu.VMEM((LEAVE, 3 * inner), BF16),
            pltpu.VMEM((width, 3 * inner), F32),
            pltpu.SemaphoreType.DMA((2, steps, 3)),
            pltpu.SemaphoreType.DMA((2, steps, 3)),
        ]
        + [pltpu.SemaphoreType.DMA((steps,))] * 4
        + scratch,
        compiler_params=pltpu.CompilerParams(
            vmem_limit_bytes=VMEM_BYTES, collective_id=1, has_side_effects=True
        ),
        cost_estimate=pl.CostEstimate(
            flops=4 * rows * width * 3 * inner, bytes_accessed=200 << 20, transcendentals=rows
        ),
        name="leave",
    )(sent, adapted, middle_back, first_low, gain, query_w, key_w, value_w, *parts)


class SmallSum:
    def __init__(self, shape):
        self.shape = shape

    def scratch(self, dp):
        return [
            pltpu.VMEM((3,) + self.shape, F32),
            pltpu.VMEM((3,) + self.shape, F32),
            pltpu.VMEM((dp,) + self.shape, F32),
            pltpu.SemaphoreType.DMA((3,)),
            pltpu.SemaphoreType.DMA((3,)),
            pltpu.SemaphoreType.DMA((2, dp)),
            pltpu.SemaphoreType.DMA((dp,)),
        ]

    def bind(self, part, out, refs):
        self.part, self.out = part, out
        (
            self.mine,
            self.theirs,
            self.line,
            self.send,
            self.recv,
            self.line_send,
            self.line_recv,
        ) = refs
        self.z, self.dp = lax.axis_index("dp"), lax.axis_size("dp")
        self.targets = [{name: 1 - lax.axis_index(name)} for name in ("tensor", "core", "x")]

    def pair(self, at):
        return pltpu.make_async_remote_copy(
            src_ref=self.mine.at[at],
            dst_ref=self.theirs.at[at],
            send_sem=self.send.at[at],
            recv_sem=self.recv.at[at],
            device_id=self.targets[at],
            device_id_type=MESH,
        )

    def pass_along(self, j, step):
        return pltpu.make_async_remote_copy(
            src_ref=self.line.at[j],
            dst_ref=self.line.at[j],
            send_sem=self.line_send.at[0 if step > 0 else 1, j],
            recv_sem=self.line_recv.at[j],
            device_id={"dp": self.z + step},
            device_id_type=MESH,
        )

    def stages(self):
        def begin():
            self.mine[0] = self.part[...]
            self.pair(0).start()

        def fold(at):
            self.pair(at - 1).wait_recv()
            total = self.mine[at - 1] + self.theirs[at - 1]
            if at < 3:
                self.mine[at] = total
                self.pair(at).start()
            else:
                self.line[self.z] = total
                self.send_on(self.z, self.z)

        def hop(h):
            z, last = self.z, self.dp - 1
            low, high = jnp.maximum(z - h, 0), jnp.minimum(z + h, last)

            @pl.when(z >= h)
            def _():
                self.pass_along(low, 1).wait_recv()

            @pl.when((z >= h) & (z < last))
            def _():
                self.pass_along(low, 1).start()

            @pl.when(z <= last - h)
            def _():
                self.pass_along(high, -1).wait_recv()

            @pl.when((z <= last - h) & (z > 0))
            def _():
                self.pass_along(high, -1).start()

        def last():
            total = self.line[0]
            for j in range(1, self.dp):
                total = total + self.line[j]
            self.out[...] = total

        call = functools.partial
        return (
            [begin]
            + [call(fold, at) for at in (1, 2, 3)]
            + [call(hop, h) for h in range(1, self.dp)]
            + [last]
        )

    def send_on(self, up, down):
        @pl.when(self.z < self.dp - 1)
        def _():
            self.pass_along(up, 1).start()

        @pl.when(self.z > 0)
        def _():
            self.pass_along(down, -1).start()

    def drain(self):
        z, last = self.z, self.dp - 1
        for at in range(3):
            self.pair(at).wait_send()
        for j in range(self.dp):

            @pl.when((z >= j) & (z < last))
            def _():
                self.pass_along(j, 1).wait_send()

            @pl.when((z <= j) & (z > 0))
            def _():
                self.pass_along(j, -1).wait_send()


def reduce_kernel(items, small, *refs):
    count = len(items)
    outs = sum(len(item.cuts) for item in items if item.base == 0)
    parts, refs = refs[: count + 1], refs[count + 1 :]
    small_refs = len(small.scratch(lax.axis_size("dp")))
    small.bind(parts[count], refs[outs], refs[outs + 1 : outs + 1 + small_refs])
    bind_all(items, parts[:count], refs[:outs], refs[outs + 1 + small_refs :])
    barrier = pltpu.get_barrier_semaphore()
    for target in small.targets:
        pl.semaphore_signal(barrier, inc=1, device_id=target, device_id_type=MESH)
    pl.semaphore_wait(barrier, 3 + greet_line(barrier))
    plans = [item.stages() for item in items if item.kind == "all"]
    gathers = [item.stages() for item in items if item.kind == "gather"]
    for plan in plans:
        plan[0]()
    for plan in gathers:
        plan[0]()
    for plan in plans:
        plan[1]()
    offsets = list(range(len(plans))) + [2 + i for i in range(len(gathers))]
    rest = [plan[2:] for plan in plans] + [plan[1:] for plan in gathers] + [small.stages()]
    for wave in waves(rest, offsets + [1]):
        for call in wave:
            call()
    for item in items + [small]:
        item.drain()


def reduce_all(parts, chunks, shapes, by_lanes, gains):
    dp = lax.axis_size("dp")
    items = [Reduction(part.shape) for part in parts[:-1]]
    items.append(Reduction(parts[-1].shape, base=parts[-2].shape[0]))
    items += [
        Reduction(shape, by_lane, "gather", x_early=i == 0)
        for i, (shape, by_lane) in enumerate(zip(shapes, by_lanes))
    ]
    small = SmallSum(gains.shape)
    scratch, outs = small.scratch(dp), []
    for item in items:
        scratch += item.scratch(dp)
        outs += item.outputs(dp)
    both = len(parts) - 2
    outs[both] = jax.ShapeDtypeStruct((2 * parts[-1].shape[0], parts[-1].shape[1]), F32)
    moved = sum(item.rows * item.lanes for item in items)
    return pl.pallas_call(
        functools.partial(reduce_kernel, items, small),
        out_shape=tuple(outs) + (jax.ShapeDtypeStruct(gains.shape, F32),),
        in_specs=[pl.BlockSpec(memory_space=pltpu.VMEM)] * (len(items) + 1),
        out_specs=(pl.BlockSpec(memory_space=pl.ANY),) * len(outs)
        + (pl.BlockSpec(memory_space=pltpu.VMEM),),
        scratch_shapes=scratch,
        compiler_params=pltpu.CompilerParams(
            vmem_limit_bytes=VMEM_BYTES, collective_id=2, has_side_effects=True
        ),
        cost_estimate=pl.CostEstimate(
            flops=moved * 4, bytes_accessed=moved * 30, transcendentals=0
        ),
        name="reduce_all",
    )(*parts, *chunks, gains)


def latent_kernel(low, weight, out):
    rows, inputs, lanes = low.shape[0], weight.shape[0], weight.shape[1]
    blocks = lanes // 128
    for at in range(inputs):
        values = nt(low[...], weight[at])
        for block in range(blocks):
            out[pl.ds(block * inputs + at, rows, stride=blocks * inputs), :] = values[
                :, block * 128 : (block + 1) * 128
            ]


def latent_grad(low, adapter):
    tokens, width = low.shape
    inputs, lanes, _ = adapter.shape
    blocks = lanes // 128
    step = SEG
    flat = pl.pallas_call(
        latent_kernel,
        grid=(tokens // step,),
        out_shape=jax.ShapeDtypeStruct((tokens * blocks * inputs, 128), F32),
        in_specs=[
            pl.BlockSpec((step, width), lambda i: (i, 0)),
            pl.BlockSpec(adapter.shape, lambda i: (0, 0, 0)),
        ],
        out_specs=pl.BlockSpec((step * blocks * inputs, 128), lambda i: (i, 0)),
        compiler_params=pltpu.CompilerParams(vmem_limit_bytes=VMEM_BYTES),
        cost_estimate=pl.CostEstimate(
            flops=2 * tokens * width * lanes * inputs,
            bytes_accessed=tokens * (2 * width + 4 * lanes * inputs) + 2 * width * lanes * inputs,
            transcendentals=0,
        ),
        name="latent_grad",
    )(low, adapter)
    flat = flat.reshape(tokens, blocks, inputs, 128)
    return flat.transpose(0, 2, 1, 3).reshape(tokens, inputs, lanes)


def swap(value, axis):
    return lax.ppermute(value, axis, [(0, 1), (1, 0)])


def together(*values):
    return lax.optimization_barrier(values)


def cut(value, index, rows):
    return lax.dynamic_slice_in_dim(value, index * rows, rows, 0)


def add_low(left, right):
    return (left.astype(F32) + right.astype(F32)).astype(BF16)


def fold(value, index, axis):
    half = value.shape[0] // 2
    return add_low(cut(value, index, half), swap(cut(value, 1 - index, half), axis))


def unfold(value, index, axis):
    other = swap(value, axis)
    return jnp.concatenate(
        [jnp.where(index == 0, value, other), jnp.where(index == 0, other, value)], axis=0
    )


def tn(left, right):
    return lax.dot_general(
        left, right, (((0,), (0,)), ((), ())), preferred_element_type=F32
    ).astype(BF16)


def on_device_paired(
    latent_embed,
    adapter,
    first_gain,
    query_weight,
    key_weight,
    value_weight,
    output_weight,
    second_gain,
    third_gain,
    gate_weight,
    up_weight,
    down_weight,
    fourth_gain,
    parents,
    positions,
    cotangent,
):
    rows = latent_embed.shape[0]
    width = adapter.shape[2]
    half_rows = rows // 2
    tensor = lax.axis_index("tensor")
    core = lax.axis_index("core")
    x = lax.axis_index("x")
    everyone = ("x", "core", "tensor")
    meta = jnp.stack([tensor, core]).astype(jnp.int32)
    one_row = lambda gain: gain.reshape(1, -1)

    cosine, sine = angle_tables(positions)
    mine = jnp.einsum(
        "rcd,cde->re", latent_embed, adapter, preferred_element_type=F32
    ).astype(BF16)
    parts, first_low, theirs = enter(
        mine, one_row(first_gain), query_weight, key_weight, value_weight, cosine, sine
    )
    adapted = cut(mine, tensor, half_rows).astype(F32) + cut(theirs, tensor, half_rows).astype(
        F32
    )
    role, place, parts = sort_parts(parents, parts.reshape(-1, 3 * WIDE))
    own_weights = (output_weight, gate_weight, up_weight, down_weight)
    attended, logsum, *other_weights = attention_forward(parts, own_weights)
    heads = lax.all_to_all(
        pick(place, attended).reshape(8, half_rows, WIDE), everyone, 0, 0, tiled=False
    )
    (
        layer_half,
        middle_back,
        attended_all,
        attention_low,
        third_low,
        mixed_low,
        hidden,
        pair_low,
        heads_back,
        gain_parts,
    ) = middle_section(
        meta,
        adapted,
        heads,
        cotangent,
        (one_row(second_gain), one_row(third_gain), one_row(fourth_gain)),
        own_weights + tuple(other_weights),
    )
    upstream = lax.all_to_all(heads_back, everyone, 0, 0, tiled=False).reshape(-1, WIDE)
    layer_other = swap(layer_half, "tensor")
    layer_out = jnp.concatenate(
        [
            jnp.where(tensor == 0, layer_half, layer_other),
            jnp.where(tensor == 0, layer_other, layer_half),
        ],
        axis=0,
    ).astype(F32)

    inner = output_weight.shape[0]
    grads = (
        tn(third_low, pair_low),
        tn(hidden, mixed_low),
        tn(attended_all, attention_low),
    )
    shapes = [gate_weight.shape, up_weight.shape, down_weight.shape, output_weight.shape]

    table_cosine, table_sine = angle_tables(jnp.arange((TRUNK + 2) * SEG))
    by_lanes = [False, False, True, False]
    sent, *sums = attention_backward(
        parts, pick(role, upstream), attended, logsum, table_cosine, table_sine, grads, shapes
    )
    (
        query_part,
        key_part,
        value_part,
        adapted_low,
        first_gain_part,
        *chunks,
    ) = leave(
        pick(place, sent).reshape(4, rows, 3 * WIDE),
        adapted,
        middle_back,
        first_low,
        one_row(first_gain),
        query_weight,
        key_weight,
        value_weight,
        sums,
        by_lanes,
    )
    adapter_part = jnp.einsum(
        "rcd,re->cde", latent_embed, adapted_low, preferred_element_type=F32
    ).astype(BF16)
    (
        query_total,
        key_total,
        value_total,
        adapter_total,
        gate_total,
        up_total,
        down_total,
        output_total,
        gains,
    ) = reduce_all(
        [query_part, key_part, value_part, adapter_part[0], adapter_part[1]],
        chunks,
        shapes,
        by_lanes,
        jnp.concatenate([gain_parts[:3], first_gain_part[:5]], axis=0),
    )
    latent_gradient = latent_grad(adapted_low, adapter)
    return (
        layer_out,
        latent_gradient,
        adapter_total.reshape(adapter.shape),
        gains[3],
        query_total,
        key_total,
        value_total,
        output_total,
        gains[0],
        gains[1],
        gate_total,
        up_total,
        down_total,
        gains[2],
    )


def specs(rows):
    split = P(None, "tensor")
    in_specs = (
        P(rows, None, "tensor"),
        P(None, "tensor", None),
        P(),
        split,
        split,
        split,
        P("tensor", None),
        P(),
        P(),
        split,
        split,
        P("tensor", None),
        P(),
        P("dp", None),
        P(rows),
        P(rows, None),
    )
    out_specs = (
        P(rows, None),
        P(rows, None, "tensor"),
        P(None, "tensor", None),
        P(),
        split,
        split,
        split,
        P("tensor", None),
        P(),
        P(),
        split,
        split,
        P("tensor", None),
        P(),
    )
    return in_specs, out_specs


def solution(mesh):
    sizes = dict(mesh.shape)
    if sizes["seq"] == 4 and sizes["tensor"] == 2:
        fine = Mesh(
            mesh.devices.reshape(sizes["dp"], 2, 2, 2), ("dp", "x", "core", "tensor")
        )
        in_specs, out_specs = specs(("dp", "x", "core"))
        return jax.shard_map(
            on_device_paired, mesh=fine, in_specs=in_specs, out_specs=out_specs, check_vma=False
        )
    in_specs, out_specs = specs(("dp", "seq"))
    return jax.shard_map(
        on_device, mesh=mesh, in_specs=in_specs, out_specs=out_specs, check_vma=False
    )
```
